32 devices in a mesh: fsdp: 4 (over y, core), context: 4 (over z), tensor: 2 (over x).
Axes of the slice: x: 2, y: 2, z: 4, core: 2. Of those that a mesh axis runs over, the one named last changes fastest.
Arguments:
- tokens: bfloat16 [4, 1024, 1536], P('fsdp', 'context'), may hold values from -6 to 6
- positions: int32 [4, 1024], P('fsdp', 'context'), may hold values from 0 to 1023, as said below
- expert_ids: int32 [4, 1024, 8], P('fsdp', 'context'), may hold values from 0 to 23, all different within a row; in each aligned block of 256 rows (0 to 255, 256 to 511, ..., all dimensions but the last counted through in order) at most 128 rows name the same one
- norm1_gain: bfloat16 [1536], P('fsdp'), may hold values from 0.5 to 1.5
- w_query: bfloat16 [1536, 1536], P('fsdp', 'tensor'), may hold values from -1 to 1
- key_projection_weight: bfloat16 [1536, 512], P('fsdp', 'tensor'), may hold values from -1 to 1
- value_projection_weight: bfloat16 [1536, 512], P('fsdp', 'tensor'), may hold values from -0.15625 to 0.15625
- w_out: bfloat16 [1536, 1536], P('tensor', 'fsdp'), may hold values from -0.875 to 0.875
- norm2_gain: bfloat16 [1536], P('fsdp'), may hold values from 0.5 to 1.5
- w_router: bfloat16 [1536, 24], P('fsdp'), may hold values from -0.15625 to 0.15625
- w_gate: bfloat16 [24, 1536, 512], P('fsdp', None, 'tensor'), may hold values from -0.15625 to 0.15625
- w_up: bfloat16 [24, 1536, 512], P('fsdp', None, 'tensor'), may hold values from -0.15625 to 0.15625
- w_down: bfloat16 [24, 512, 1536], P('fsdp', 'tensor'), may hold values from -0.5 to 0.5
- grad_output: bfloat16 [4, 1024, 1536], P('fsdp', 'context'), may hold values from -6 to 6
Outputs:
- output: bfloat16 [4, 1024, 1536], P('fsdp', 'context')
- grad_tokens: bfloat16 [4, 1024, 1536], P('fsdp', 'context')
- grad_norm1_gain: float32 [1536], P('fsdp')
- grad_w_query: float32 [1536, 1536], P('fsdp', 'tensor')
- grad_w_key: float32 [1536, 512], P('fsdp', 'tensor')
- grad_w_value: float32 [1536, 512], P('fsdp', 'tensor')
- grad_w_out: float32 [1536, 1536], P('tensor', 'fsdp')
- grad_norm2_gain: float32 [1536], P('fsdp')
- grad_w_router: float32 [1536, 24], P('fsdp')
- grad_w_gate: float32 [24, 1536, 512], P('fsdp', None, 'tensor')
- grad_w_up: float32 [24, 1536, 512], P('fsdp', None, 'tensor')
- grad_w_down: float32 [24, 512, 1536], P('fsdp', 'tensor')
The draws below stay inside these ranges and needn't reach their ends.
Inputs may be any that keep to these rules, and one draw needn't show every extreme that they name: `expert_ids`: within each aligned block of 256 tokens of a sequence no expert is named by more than 128 tokens, a bound that some block reaches; a token names 8 different experts. `positions`: each sequence begins at position 0; every later position is 0 or one more than the position before it; the first sequence never restarts.
All inputs are finite; a program needn't handle non-finite values.
Results may differ from the reference program's by a relative error of at most 0.022.
Values may be sent and summed in bfloat16 or wider, within the bound.
A program may use at most 384 MiB of HBM per device.

```python
import math
import jax
import jax.numpy as jnp
import numpy as np
from jax import lax

MODEL_WIDTH = 1536
QUERY_HEADS = 24
KEY_VALUE_HEADS = 8
HEAD_DIMENSION = 64
EXPERTS = 24
FFE = 512
TOPK = 8
BLK = 256
CAP = 128
SEQ_LEN = 1024
SEQS = 4


def draw_positions(key, part):
    index = jnp.broadcast_to(jnp.arange(SEQ_LEN, dtype=jnp.int32)[None, :], (SEQS, SEQ_LEN))
    which = jnp.broadcast_to(jnp.arange(SEQS, dtype=jnp.int32)[:, None], (SEQS, SEQ_LEN))
    marks = jax.random.randint(key, (SEQS, SEQ_LEN), 0, max(SEQ_LEN // 4, 2))
    begins = jnp.where((marks == 0) & (which > 0) | (index == 0), index, 0).astype(jnp.int32)
    return (index - lax.cummax(begins, axis=1)).astype(jnp.int32)


def key_projected(key):
    value_matrix = jax.random.normal(jax.random.fold_in(key, 7101), (MODEL_WIDTH, KEY_VALUE_HEADS * HEAD_DIMENSION), jnp.float32) * (1.0 / MODEL_WIDTH ** 0.5)
    return jnp.clip(value_matrix, -1.0, 1.0)


def draw_key_projection_weight(key, part):
    return key_projected(key).astype(jnp.bfloat16)


def draw_w_query(key, part):
    local_part = jax.random.normal(jax.random.fold_in(key, 7102), (MODEL_WIDTH, QUERY_HEADS * HEAD_DIMENSION), jnp.float32) * (1.0 / MODEL_WIDTH ** 0.5)
    local_part = jnp.clip(local_part, -1.0, 1.0)
    return local_part.astype(jnp.bfloat16)


def draw_tokens(key, part):
    value_matrix = jnp.clip(jax.random.normal(jax.random.fold_in(key, 7201), (SEQS, SEQ_LEN, MODEL_WIDTH), jnp.float32), -6.0, 6.0)
    return value_matrix.astype(jnp.bfloat16)


def steps_of(stream_key, extent, cuts, least, high):
    def one(axis_at, shards_of):
        steps = jax.random.uniform(jax.random.fold_in(jax.random.fold_in(stream_key, 6), axis_at), (shards_of,), jnp.float32, least / len(cuts), high / len(cuts))
        return jnp.repeat(jnp.exp(steps), extent[axis_at] // shards_of).reshape((-1,) + (1,) * (len(extent) - axis_at - 1))

    level = one(*cuts[0])
    for cut in cuts[1:]:
        level = level * one(*cut)
    return level


def shared_out(key, own, number, rows, number_of, top, reach, skew):
    ranking = jax.random.permutation(key, number_of)
    heavy_load, common = portions_of(number_of, rows * top, reach, skew, True), portions_of(number_of, rows * top, reach, skew, False)
    places = jnp.arange(number_of)

    def named(sizes, offset_by):
        used = int((sizes > 0).sum())
        fixed = max(1, used // 4)
        passed = fixed + (places - fixed + offset_by * (used - fixed)) % max(1, number_of - fixed)
        return jnp.zeros((number_of,), jnp.int32).at[ranking[jnp.where(places < fixed, places, passed)]].set(jnp.asarray(sizes, jnp.int32))

    sizes = jnp.where(number % 4 == 0, named(heavy_load, number // 4), named(common, number - number // 4 - 1))
    mixed = jax.random.permutation(jax.random.fold_in(own, 3), number_of)
    giver, taker = mixed[0:number_of // 2 * 2:2], mixed[1:number_of // 2 * 2:2]
    slack = jnp.minimum(sizes[giver] - 1, reach - sizes[taker]) // 2
    slack = jnp.where((giver == ranking[0]) | (taker == ranking[0]) | (sizes[taker] == 0), 0, jnp.maximum(slack, 0))
    passed = jax.random.randint(jax.random.fold_in(own, 4), (number_of // 2,), 0, 1 << 20) % (slack + 1)
    sizes = sizes.at[giver].add(-passed).at[taker].add(passed)
    members = jnp.searchsorted(jnp.cumsum(sizes), jnp.arange(rows * top), side="right").astype(jnp.int32)
    table = members.reshape(top, rows).T
    table = table[jax.random.permutation(jax.random.fold_in(own, 1), rows)]
    offset_by = jax.random.randint(jax.random.fold_in(own, 2), (rows, 1), 0, top)
    return jnp.take_along_axis(table, (jnp.arange(top)[None, :] + offset_by) % top, axis=1)


def portions_of(number_of, total, limit, slope, full):
    loads = [(1 << 20) // math.isqrt(grade ** slope) + 1 for grade in range(1, number_of + 1)]
    largest = limit if full else min(limit, max(-(-total // number_of), total * loads[0] // sum(loads)))
    least = 1 if total - largest >= number_of - 1 else 0
    counts, spare = [largest] + [least] * (number_of - 1), total - largest - least * (number_of - 1)
    while spare > 0:
        movable = [i for i in range(1, number_of) if counts[i] < largest] or [i for i in range(1, number_of) if counts[i] < limit]
        whole, left = sum([loads[i] for i in movable]), spare
        for i in movable:
            more = min(limit - counts[i], max(1, left * loads[i] // whole), spare)
            counts[i] = counts[i] + more
            spare = spare - more
    return np.array(counts)


def normal_values(key, dims, spread, limit, split=(), kind=jnp.bfloat16):
    drawn = jax.random.normal(key, dims, jnp.float32) * spread
    if len(split) > 0:
        drawn = steps_of(key, dims, split, -0.22, 0.18) * drawn
    return jnp.clip(drawn, min=-limit, max=limit).astype(kind)


def setup_inputs(seed: int = 0) -> dict:
    seeds = jax.random.split(jax.random.key(seed), 15)
    tokens = draw_tokens(jax.random.fold_in(seeds[14], 71), 0)
    positions = draw_positions(jax.random.fold_in(seeds[14], 71), 0)
    expert_ids_keys = jax.random.split(jax.random.fold_in(seeds[2], 1), SEQS * SEQ_LEN // BLK)
    expert_ids_turns = jax.random.permutation(jax.random.fold_in(seeds[2], 3), SEQS * SEQ_LEN // BLK)
    expert_ids = jax.vmap(lambda own, number: shared_out(jax.random.fold_in(seeds[2], 2), own, number, BLK, EXPERTS, TOPK, CAP, 2))(expert_ids_keys, expert_ids_turns).reshape((SEQS, SEQ_LEN, TOPK))
    norm1_gain = jnp.clip(1.0 + 0.1 * jax.random.normal(seeds[3], (MODEL_WIDTH,), jnp.float32), 0.5, 1.5).astype(jnp.bfloat16)
    w_query = draw_w_query(jax.random.fold_in(seeds[14], 71), 0)
    key_projection_weight = draw_key_projection_weight(jax.random.fold_in(seeds[14], 71), 0)
    value_projection_weight = normal_values(seeds[6], (MODEL_WIDTH, KEY_VALUE_HEADS * HEAD_DIMENSION), MODEL_WIDTH ** -0.5, 0.15625, ((0, 4), (1, 2)))
    w_out = normal_values(seeds[7], (QUERY_HEADS * HEAD_DIMENSION, MODEL_WIDTH), (QUERY_HEADS * HEAD_DIMENSION // 32) ** -0.5, 0.875, ((0, 2), (1, 4)))
    norm2_gain = jnp.clip(1.0 + 0.1 * jax.random.normal(seeds[8], (MODEL_WIDTH,), jnp.float32), 0.5, 1.5).astype(jnp.bfloat16)
    w_router = normal_values(seeds[9], (MODEL_WIDTH, EXPERTS), MODEL_WIDTH ** -0.5, 0.15625, ((0, 4),))
    w_gate = normal_values(seeds[10], (EXPERTS, MODEL_WIDTH, FFE), MODEL_WIDTH ** -0.5, 0.15625, ((0, 4), (2, 2)))
    w_up = normal_values(seeds[11], (EXPERTS, MODEL_WIDTH, FFE), MODEL_WIDTH ** -0.5, 0.15625, ((0, 4), (2, 2)))
    w_down = normal_values(seeds[12], (EXPERTS, FFE, MODEL_WIDTH), (FFE // 4) ** -0.5, 0.5, ((0, 4), (1, 2)))
    grad_output = normal_values(seeds[13], (SEQS, SEQ_LEN, MODEL_WIDTH), 1.0, 6.0, ((0, 4), (1, 4)))
    return dict(tokens=tokens, positions=positions, expert_ids=expert_ids, norm1_gain=norm1_gain, w_query=w_query, key_projection_weight=key_projection_weight, value_projection_weight=value_projection_weight, w_out=w_out, norm2_gain=norm2_gain, w_router=w_router, w_gate=w_gate, w_up=w_up, w_down=w_down, grad_output=grad_output)


norm_eps = 1e-06
masked_score = -1e+30

def rounded_values(value_matrix):
    return lax.optimization_barrier(value_matrix.astype(jnp.bfloat16)).astype(jnp.float32)

def rms_scale(rows):
    return lax.rsqrt(lax.optimization_barrier(jnp.mean(rows * rows, axis=-1, keepdims=True)) + norm_eps)

def norm_backward(rows, scale, gain, grad_out):
    weighted = grad_out * gain
    cubed = scale * scale * scale
    grad_in = scale * weighted - rows * cubed * lax.optimization_barrier(jnp.mean(weighted * rows, axis=-1, keepdims=True))
    return (grad_in, lax.optimization_barrier(jnp.sum(grad_out * rows * scale, axis=0)))

def rope_tables(place_ids, head_size):
    half = head_size // 2
    freq = jnp.exp(-math.log(10000.0) * 2.0 * jnp.arange(half, dtype=jnp.float32) / head_size)
    angle = place_ids.astype(jnp.float32)[:, None] * freq[None, :]
    return (jnp.cos(angle), jnp.sin(angle))

def apply_rotation(value_matrix, cosine_table, sine_table, sign):
    half = value_matrix.shape[-1] // 2
    first = value_matrix[..., :half]
    second = value_matrix[..., half:]
    cos_b = cosine_table[:, None, :]
    sin_b = sine_table[:, None, :] * sign
    return jnp.concatenate([first * cos_b - second * sin_b, second * cos_b + first * sin_b], axis=-1)

def slot_table(routes, experts, capacity):
    flat = routes.reshape(-1).astype(jnp.int32)
    onehot = (flat[:, None] == jnp.arange(experts, dtype=jnp.int32)[None, :]).astype(jnp.int32)
    before = (jnp.cumsum(onehot, axis=0).astype(jnp.int32) - onehot).astype(jnp.int32)
    slots = lax.optimization_barrier(jnp.sum(before * onehot, axis=1)).astype(jnp.int32)
    place = (flat * capacity + slots).astype(jnp.int32)
    owners = (jnp.arange(flat.shape[0], dtype=jnp.int32) // routes.shape[1] + 1).astype(jnp.int32)
    owner = jnp.zeros((experts * capacity,), jnp.int32).at[place].set(owners)
    filled = owner > 0
    source = jnp.maximum(owner - 1, 0).astype(jnp.int32)
    return (place, source, filled)

def expert_block(normed_blk, route_blk, gradient_block, w_router, w_gate, w_up, w_down):
    experts = w_router.shape[1]
    rows_n = normed_blk.shape[0]
    logits = jnp.dot(normed_blk, w_router, preferred_element_type=jnp.float32)
    chooser = (route_blk[:, :, None] == jnp.arange(experts, dtype=jnp.int32)[None, None, :]).astype(logits.dtype)
    chosen = lax.optimization_barrier(jnp.sum(chooser * logits[:, None, :], axis=-1))
    gates = jax.nn.softmax(chosen, axis=-1)
    place, source, filled = slot_table(route_blk, experts, CAP)
    dispatched = jnp.where(filled[:, None], normed_blk[source], jnp.zeros((), normed_blk.dtype)).reshape(experts, CAP, -1)
    disp_f = dispatched.astype(jnp.float32)
    gate_f = w_gate.astype(jnp.float32)
    up_f = w_up.astype(jnp.float32)
    down_f = w_down.astype(jnp.float32)
    gate_pre = jnp.einsum('ecd,edf->ecf', disp_f, gate_f)
    up_pre = jnp.einsum('ecd,edf->ecf', disp_f, up_f)
    sigma = jax.nn.sigmoid(gate_pre)
    activated = gate_pre * sigma
    inner_f = rounded_values(activated * up_pre)
    expert_out = jnp.einsum('ecf,efd->ecd', inner_f, down_f).reshape(experts * CAP, -1)
    picked = expert_out[place].reshape(rows_n, TOPK, -1)
    moe = lax.optimization_barrier(jnp.sum(gates[:, :, None] * picked, axis=1))
    slot_gate = jnp.zeros((experts * CAP,), gates.dtype).at[place].set(gates.reshape(-1))
    grad_expert = rounded_values(jnp.where(filled[:, None], gradient_block[source] * slot_gate[:, None], 0.0)).reshape(experts, CAP, -1)
    grad_gates = lax.optimization_barrier(jnp.sum(picked * gradient_block[:, None, :], axis=-1))
    grad_inner = jnp.einsum('ecd,efd->ecf', grad_expert, down_f)
    grad_down = jnp.einsum('ecf,ecd->efd', inner_f, grad_expert)
    grad_g = rounded_values(grad_inner * up_pre * sigma * (1.0 + gate_pre * (1.0 - sigma)))
    grad_u = rounded_values(grad_inner * activated)
    grad_disp = jnp.einsum('ecf,edf->ecd', grad_g, gate_f) + jnp.einsum('ecf,edf->ecd', grad_u, up_f)
    grad_gate_w = jnp.einsum('ecd,ecf->edf', disp_f, grad_g)
    grad_up_w = jnp.einsum('ecd,ecf->edf', disp_f, grad_u)
    grad_normed_e = lax.optimization_barrier(jnp.sum(grad_disp.reshape(experts * CAP, -1)[place].reshape(rows_n, TOPK, -1), axis=1))
    grad_chosen = gates * (grad_gates - lax.optimization_barrier(jnp.sum(gates * grad_gates, axis=-1, keepdims=True)))
    grad_logits = lax.optimization_barrier(jnp.sum(grad_chosen[:, :, None] * chooser, axis=1)).astype(jnp.bfloat16)
    grad_normed = grad_normed_e + jnp.dot(grad_logits, w_router.T, preferred_element_type=jnp.float32)
    grad_router = jnp.dot(normed_blk.T, grad_logits, preferred_element_type=jnp.float32)
    return (moe, grad_normed, (grad_router, grad_gate_w, grad_up_w, grad_down))

def attention_forward(query_fourdim, key_row_list, value_row_list):
    sequence_length = key_row_list.shape[0]
    width = math.gcd(sequence_length, 512)
    key_single = key_row_list.astype(jnp.float32)
    value_single = value_row_list.astype(jnp.float32)
    key_pos = jnp.arange(sequence_length, dtype=jnp.int32)
    softmax_scale = 1.0 / math.sqrt(HEAD_DIMENSION)

    def one_block(first):
        query_block_tile = lax.dynamic_slice_in_dim(query_fourdim, first, width, 0).astype(jnp.float32)
        score_matrix = jnp.einsum('ijzq,pjq->jzip', query_block_tile, key_single) * softmax_scale
        allowed = key_pos[None, :] <= (first + jnp.arange(width, dtype=jnp.int32))[:, None]
        score_matrix = jnp.where(allowed, score_matrix, masked_score)
        top = lax.optimization_barrier(jnp.max(score_matrix, axis=-1))
        exponent_values = jnp.where(allowed, jnp.exp(score_matrix - top[..., None]), 0.0)
        total = lax.optimization_barrier(jnp.sum(exponent_values, axis=-1))
        running_total = jnp.einsum('hevu,uhw->vhew', rounded_values(exponent_values), value_single)
        attended = running_total / jnp.transpose(total, (2, 0, 1))[..., None]
        return (attended, top + jnp.log(total))
    firsts = (jnp.arange(sequence_length // width, dtype=jnp.int32) * width).astype(jnp.int32)
    attended, logsumexp_total = lax.map(one_block, firsts)
    attended = attended.reshape((sequence_length,) + query_fourdim.shape[1:])
    logsumexp_total = jnp.transpose(logsumexp_total, (1, 2, 0, 3)).reshape(query_fourdim.shape[1], query_fourdim.shape[2], sequence_length)
    return (attended, logsumexp_total)

def attention_reverse_pass(query_fourdim, key_row_list, value_row_list, attended_four, logsumexp_total, gradient_fourdim):
    sequence_length = key_row_list.shape[0]
    width = math.gcd(sequence_length, 512)
    key_single = key_row_list.astype(jnp.float32)
    value_single = value_row_list.astype(jnp.float32)
    key_pos = jnp.arange(sequence_length, dtype=jnp.int32)
    softmax_scale = 1.0 / math.sqrt(HEAD_DIMENSION)
    delta = lax.optimization_barrier(jnp.sum(gradient_fourdim.astype(jnp.float32) * attended_four.astype(jnp.float32), axis=-1))

    def one_block(carry, first):
        key_rows_gradient, value_rows_gradient = carry
        query_block_tile = lax.dynamic_slice_in_dim(query_fourdim, first, width, 0).astype(jnp.float32)
        gradient_block = lax.dynamic_slice_in_dim(gradient_fourdim, first, width, 0).astype(jnp.float32)
        lse_blk = lax.dynamic_slice_in_dim(logsumexp_total, first, width, 2)
        delta_blk = jnp.transpose(lax.dynamic_slice_in_dim(delta, first, width, 0), (1, 2, 0))
        score_matrix = jnp.einsum('ijzq,pjq->jzip', query_block_tile, key_single) * softmax_scale
        allowed = key_pos[None, :] <= (first + jnp.arange(width, dtype=jnp.int32))[:, None]
        probabilities = jnp.where(allowed, jnp.exp(score_matrix - lse_blk[..., None]), 0.0)
        value_rows_gradient = value_rows_gradient + jnp.einsum('ihne,nihf->eif', rounded_values(probabilities), gradient_block)
        probability_gradient = jnp.einsum('ijzq,pjq->jzip', gradient_block, value_single)
        score_gradient = rounded_values(probabilities * (probability_gradient - delta_blk[..., None]))
        query_gradient = jnp.einsum('hevu,uhw->vhew', score_gradient, key_single) * softmax_scale
        key_rows_gradient = key_rows_gradient + jnp.einsum('ihne,nihf->eif', score_gradient, query_block_tile) * softmax_scale
        return ((key_rows_gradient, value_rows_gradient), query_gradient)
    firsts = (jnp.arange(sequence_length // width, dtype=jnp.int32) * width).astype(jnp.int32)
    start_carry = (jnp.zeros(key_single.shape, jnp.float32), jnp.zeros(value_single.shape, jnp.float32))
    (key_rows_gradient, value_rows_gradient), query_gradient = lax.scan(one_block, start_carry, firsts)
    return (query_gradient.reshape(query_fourdim.shape), key_rows_gradient, value_rows_gradient)

def reference(tokens, positions, expert_ids, norm1_gain, w_query, key_projection_weight, value_projection_weight, w_out, norm2_gain, w_router, w_gate, w_up, w_down, grad_output):
    gain_one = norm1_gain.astype(jnp.float32)
    gain_two = norm2_gain.astype(jnp.float32)
    group_repeat = QUERY_HEADS // KEY_VALUE_HEADS

    def sequence_pass(carry, inputs):
        rows_b, place_ids, routes, grad_b = inputs
        rows = rows_b.astype(jnp.float32)
        sequence_length = rows.shape[0]
        scale_one = rms_scale(rows)
        first_normalized = (rows * scale_one * gain_one).astype(jnp.bfloat16)
        cosine_table, sine_table = rope_tables(place_ids, HEAD_DIMENSION)
        query_rows = apply_rotation(jnp.dot(first_normalized, w_query, preferred_element_type=jnp.float32).reshape(sequence_length, QUERY_HEADS, HEAD_DIMENSION), cosine_table, sine_table, 1.0).astype(jnp.bfloat16)
        key_row_list = apply_rotation(jnp.dot(first_normalized, key_projection_weight, preferred_element_type=jnp.float32).reshape(sequence_length, KEY_VALUE_HEADS, HEAD_DIMENSION), cosine_table, sine_table, 1.0).astype(jnp.bfloat16)
        value_row_list = jnp.dot(first_normalized, value_projection_weight, preferred_element_type=jnp.float32).astype(jnp.bfloat16).reshape(sequence_length, KEY_VALUE_HEADS, HEAD_DIMENSION)
        query_fourdim = query_rows.reshape(sequence_length, KEY_VALUE_HEADS, group_repeat, HEAD_DIMENSION)
        attended, logsumexp_total = attention_forward(query_fourdim, key_row_list, value_row_list)
        attended_batch = attended.astype(jnp.bfloat16).reshape(sequence_length, QUERY_HEADS * HEAD_DIMENSION)
        hidden = rows + jnp.dot(attended_batch, w_out, preferred_element_type=jnp.float32)
        scale_two = rms_scale(hidden)
        normed_two = (hidden * scale_two * gain_two).astype(jnp.bfloat16)
        grad_rows_out = grad_b.astype(jnp.float32)
        count = sequence_length // BLK

        def block_pass(acc, item):
            normed_blk, route_blk, gradient_block = item
            moe_blk, grad_normed, terms = expert_block(normed_blk, route_blk, gradient_block, w_router, w_gate, w_up, w_down)
            return (tuple((left + right for left, right in zip(acc, terms))), (moe_blk, grad_normed))
        expert_acc, (moe, grad_normed_two) = lax.scan(block_pass, carry[6:], (normed_two.reshape(count, BLK, -1), routes.reshape(count, BLK, -1), grad_rows_out.reshape(count, BLK, -1)))
        output = (hidden + moe.reshape(sequence_length, -1)).astype(jnp.bfloat16)
        grad_hidden_n, grad_gain_two = norm_backward(hidden, scale_two, gain_two, grad_normed_two.reshape(sequence_length, -1))
        grad_hidden = grad_rows_out + grad_hidden_n
        grad_hidden_b = grad_hidden.astype(jnp.bfloat16)
        attended_gradient = jnp.dot(grad_hidden_b, w_out.T, preferred_element_type=jnp.float32).astype(jnp.bfloat16)
        grad_out_w = jnp.dot(attended_batch.T, grad_hidden_b, preferred_element_type=jnp.float32)
        gradient_fourdim = attended_gradient.reshape(sequence_length, KEY_VALUE_HEADS, group_repeat, HEAD_DIMENSION)
        query_gradient, key_gradient, value_gradient = attention_reverse_pass(query_fourdim, key_row_list, value_row_list, attended_batch.reshape(sequence_length, KEY_VALUE_HEADS, group_repeat, HEAD_DIMENSION), logsumexp_total, gradient_fourdim)
        grad_queries = apply_rotation(query_gradient.reshape(sequence_length, QUERY_HEADS, HEAD_DIMENSION), cosine_table, sine_table, -1.0).astype(jnp.bfloat16).reshape(sequence_length, -1)
        key_rows_gradient = apply_rotation(key_gradient, cosine_table, sine_table, -1.0).astype(jnp.bfloat16).reshape(sequence_length, -1)
        value_rows_gradient = value_gradient.astype(jnp.bfloat16).reshape(sequence_length, -1)
        grad_normed_one = jnp.dot(grad_queries, w_query.T, preferred_element_type=jnp.float32)
        grad_normed_one = grad_normed_one + jnp.dot(key_rows_gradient, key_projection_weight.T, preferred_element_type=jnp.float32)
        grad_normed_one = grad_normed_one + jnp.dot(value_rows_gradient, value_projection_weight.T, preferred_element_type=jnp.float32)
        grad_rows_n, grad_gain_one = norm_backward(rows, scale_one, gain_one, grad_normed_one)
        grad_tokens = (grad_hidden + grad_rows_n).astype(jnp.bfloat16)
        terms = (grad_gain_one, jnp.dot(first_normalized.T, grad_queries, preferred_element_type=jnp.float32), jnp.dot(first_normalized.T, key_rows_gradient, preferred_element_type=jnp.float32), jnp.dot(first_normalized.T, value_rows_gradient, preferred_element_type=jnp.float32), grad_out_w, grad_gain_two)
        new_carry = tuple((left + right for left, right in zip(carry[:6], terms))) + tuple(expert_acc)
        return (new_carry, (output, grad_tokens))
    weights = (norm1_gain, w_query, key_projection_weight, value_projection_weight, w_out, norm2_gain, w_router, w_gate, w_up, w_down)
    zeros = tuple((jnp.zeros(item.shape, jnp.float32) for item in weights))
    grads, (output, grad_tokens) = lax.scan(sequence_pass, zeros, (tokens, positions, expert_ids, grad_output))
    return (output, grad_tokens, grads[0], grads[1], grads[2], grads[3], grads[4], grads[5], grads[6], grads[7], grads[8], grads[9])
```

```python
import math

import jax
import jax.numpy as jnp
from jax import lax
from jax.experimental import pallas as pl
from jax.experimental.pallas import tpu as pltpu
from jax.sharding import PartitionSpec as P

HEAD_DIMENSION = 64
TOPK = 8
CAP = 128


norm_eps = 1e-06
masked_score = -1e30


def rms_scale(rows):
    return lax.rsqrt(jnp.mean(rows * rows, axis=-1, keepdims=True) + norm_eps)


def norm_backward(rows, scale, gain, grad_out):
    weighted = grad_out * gain
    cubed = scale * scale * scale
    grad_in = scale * weighted - rows * cubed * jnp.mean(weighted * rows, axis=-1, keepdims=True)
    return (grad_in, jnp.sum(grad_out * rows * scale, axis=0))


def rope_tables(place_ids, head_size):
    half = head_size // 2
    freq = jnp.exp(-math.log(10000.0) * 2.0 * jnp.arange(half, dtype=jnp.float32) / head_size)
    angle = place_ids.astype(jnp.float32)[:, None] * freq[None, :]
    return (jnp.cos(angle), jnp.sin(angle))


def apply_rotation(value_matrix, cosine_table, sine_table, sign):
    half = value_matrix.shape[-1] // 2
    first = value_matrix[..., :half]
    second = value_matrix[..., half:]
    cos_b = cosine_table[:, None, :]
    sin_b = sine_table[:, None, :] * sign
    return jnp.concatenate(
        [first * cos_b - second * sin_b, second * cos_b + first * sin_b], axis=-1
    )


def nn(left, right):
    return jnp.dot(left, right, preferred_element_type=jnp.float32)


def nt(left, right):
    return lax.dot_general(
        left, right, (((1,), (1,)), ((), ())), preferred_element_type=jnp.float32
    )


def tn(left, right):
    return lax.dot_general(
        left, right, (((0,), (0,)), ((), ())), preferred_element_type=jnp.float32
    )


def dense_gates(normed, ids, router):
    logits = nn(normed, router)
    lanes = lax.broadcasted_iota(jnp.int32, logits.shape, 1)
    mask = ids[:, 0:1] == lanes
    for k in range(1, ids.shape[1]):
        mask = mask | (ids[:, k : k + 1] == lanes)
    logits = jnp.where(mask, logits, masked_score)
    weight = jnp.where(mask, jnp.exp(logits - jnp.max(logits, axis=-1, keepdims=True)), 0.0)
    return weight / jnp.sum(weight, axis=-1, keepdims=True)


def gates_kernel(normed_ref, ids_ref, router_ref, gates_ref):
    gates_ref[...] = dense_gates(normed_ref[...], ids_ref[...], router_ref[...])


def gates_call(normed, ids, router):
    rows, width = normed.shape
    experts = router.shape[1]
    tile = 1024
    return pl.pallas_call(
        gates_kernel,
        out_shape=jax.ShapeDtypeStruct((rows, experts), jnp.float32),
        grid=(rows // tile,),
        in_specs=[
            pl.BlockSpec((tile, width), lambda i: (i, 0)),
            pl.BlockSpec((tile, ids.shape[1]), lambda i: (i, 0)),
            pl.BlockSpec((width, experts), lambda i: (0, 0)),
        ],
        out_specs=pl.BlockSpec((tile, experts), lambda i: (i, 0)),
        name="gates_all",
        cost_estimate=pl.CostEstimate(
            flops=2 * rows * width * 128, bytes_accessed=rows * width * 2, transcendentals=0
        ),
    )(normed, ids, router)


def gate_column(gates, expert):
    lanes = lax.broadcasted_iota(jnp.int32, gates.shape, 1)
    return jnp.sum(jnp.where(lanes == expert, gates, 0.0), axis=-1, keepdims=True)


def hidden_terms(normed, cotangent, gate_col, gate_w, up_w, down_w):
    gate_pre = nn(normed, gate_w)
    up_pre = nn(normed, up_w)
    plain = nt(cotangent, down_w)
    sigma = 1.0 / (1.0 + jnp.exp(-gate_pre))
    activated = gate_pre * sigma
    inner = activated * up_pre
    grad_inner = gate_col * plain
    scaled = (gate_col * inner).astype(jnp.bfloat16)
    grad_g = (grad_inner * up_pre * (sigma + activated * (1.0 - sigma))).astype(jnp.bfloat16)
    grad_u = (grad_inner * activated).astype(jnp.bfloat16)
    return inner, plain, scaled, grad_g, grad_u


def own_kernel(
    first_ref,
    normed_ref,
    cot_ref,
    ids_ref,
    router_ref,
    gate_hbm,
    up_hbm,
    down_hbm,
    moe_ref,
    grad_ref,
    router_grad_ref,
    gate_w,
    up_w,
    down_w,
    all_inner,
    all_g,
    all_u,
    gates,
    gate_grads,
    sems,
):
    experts_here = gate_w.shape[0]
    hidden = gate_w.shape[2]
    rows = normed_ref.shape[0]
    tile = 256
    for e in range(experts_here):
        pltpu.make_async_copy(gate_hbm.at[e], gate_w.at[e], sems.at[0, e]).start()
        pltpu.make_async_copy(up_hbm.at[e], up_w.at[e], sems.at[1, e]).start()
        pltpu.make_async_copy(down_hbm.at[e], down_w.at[e], sems.at[2, e]).start()
    first = first_ref[0]

    def route(i, carry):
        at = pl.ds(pl.multiple_of(i * tile, tile), tile)
        gates[at, :] = dense_gates(normed_ref[at, :], ids_ref[at, :], router_ref[...])
        gate_grads[at, :] = jnp.zeros((tile, gates.shape[1]), jnp.float32)
        return carry

    lax.fori_loop(0, rows // tile, route, 0)

    def one_expert(e, carry):
        pltpu.make_async_copy(gate_hbm.at[e], gate_w.at[e], sems.at[0, e]).wait()
        pltpu.make_async_copy(up_hbm.at[e], up_w.at[e], sems.at[1, e]).wait()
        pltpu.make_async_copy(down_hbm.at[e], down_w.at[e], sems.at[2, e]).wait()
        columns = pl.ds(pl.multiple_of(e * hidden, hidden), hidden)

        def one_tile(i, inner_carry):
            at = pl.ds(pl.multiple_of(i * 512, 512), 512)
            gates_tile = gates[at, :]
            inner, plain, scaled, grad_g, grad_u = hidden_terms(
                normed_ref[at, :],
                cot_ref[at, :],
                gate_column(gates_tile, first + e),
                gate_w[e],
                up_w[e],
                down_w[e],
            )
            all_inner[at, columns] = scaled
            all_g[at, columns] = grad_g
            all_u[at, columns] = grad_u
            share = jnp.sum(inner * plain, axis=-1, keepdims=True)
            lanes = lax.broadcasted_iota(jnp.int32, gates_tile.shape, 1)
            gate_grads[at, :] = jnp.where(lanes == first + e, share, gate_grads[at, :])
            return inner_carry

        lax.fori_loop(0, rows // 512, one_tile, 0)
        return carry

    lax.fori_loop(0, experts_here, one_expert, 0)

    router_grad_ref[...] = jnp.zeros_like(router_grad_ref)

    def finish(i, carry):
        at = pl.ds(pl.multiple_of(i * tile, tile), tile)
        gates_tile = gates[at, :]
        grads_tile = gate_grads[at, :]
        mean = jnp.sum(gates_tile * grads_tile, axis=-1, keepdims=True)
        grad_logits = (gates_tile * (grads_tile - mean)).astype(jnp.bfloat16)
        router_grad_ref[...] += tn(normed_ref[at, :], grad_logits)
        down_all = down_w[...].reshape(experts_here * hidden, down_w.shape[2])
        moe_ref[at, :] = nn(all_inner[at, :], down_all).astype(jnp.bfloat16)
        total = nt(grad_logits, router_ref[...])
        for e in range(experts_here):
            columns = slice(e * hidden, (e + 1) * hidden)
            total = total + nt(all_g[at, columns], gate_w[e]) + nt(all_u[at, columns], up_w[e])
        grad_ref[at, :] = total.astype(jnp.bfloat16)
        return carry

    lax.fori_loop(0, rows // tile, finish, 0)


def own_call(first, normed, cotangent, ids, router, gate_w, up_w, down_w):
    rows, width = normed.shape
    experts = router.shape[1]
    here, _, hidden = gate_w.shape
    vmem = pl.BlockSpec(memory_space=pltpu.VMEM)
    anywhere = pl.BlockSpec(memory_space=pl.ANY)
    return pl.pallas_call(
        own_kernel,
        out_shape=(
            jax.ShapeDtypeStruct((rows, width), jnp.bfloat16),
            jax.ShapeDtypeStruct((rows, width), jnp.bfloat16),
            jax.ShapeDtypeStruct((width, experts), jnp.float32),
        ),
        in_specs=[pl.BlockSpec(memory_space=pltpu.SMEM)] + [vmem] * 4 + [anywhere] * 3,
        out_specs=(vmem, vmem, vmem),
        scratch_shapes=[
            pltpu.VMEM(gate_w.shape, jnp.bfloat16),
            pltpu.VMEM(up_w.shape, jnp.bfloat16),
            pltpu.VMEM(down_w.shape, jnp.bfloat16),
            pltpu.VMEM((rows, here * hidden), jnp.bfloat16),
            pltpu.VMEM((rows, here * hidden), jnp.bfloat16),
            pltpu.VMEM((rows, here * hidden), jnp.bfloat16),
            pltpu.VMEM((rows, experts), jnp.float32),
            pltpu.VMEM((rows, experts), jnp.float32),
            pltpu.SemaphoreType.DMA((3, here)),
        ],
        compiler_params=pltpu.CompilerParams(vmem_limit_bytes=62 << 20),
        name="experts_own",
        cost_estimate=pl.CostEstimate(
            flops=12 * rows * width * hidden * here,
            bytes_accessed=6 * here * width * hidden + 8 * rows * width,
            transcendentals=0,
        ),
    )(first, normed, cotangent, ids, router, gate_w, up_w, down_w)


def weights_kernel(first_ref, *refs):
    (normed_ref, cot_ref, gates_ref, gate_w, up_w, down_w) = refs[:6]
    grad_gate_ref, grad_up_ref, grad_down_ref = refs[-3:]
    e = pl.program_id(0)
    normed = normed_ref[...]
    cotangent = cot_ref[...]
    _, _, scaled, grad_g, grad_u = hidden_terms(
        normed,
        cotangent,
        gate_column(gates_ref[...], first_ref[0] + e),
        gate_w[0],
        up_w[0],
        down_w[0],
    )

    @pl.when(pl.program_id(1) == 0)
    def _():
        grad_gate_ref[0] = tn(normed, grad_g)
        grad_up_ref[0] = tn(normed, grad_u)
        grad_down_ref[0] = tn(scaled, cotangent)

    @pl.when(pl.program_id(1) > 0)
    def _():
        grad_gate_ref[0] += tn(normed, grad_g)
        grad_up_ref[0] += tn(normed, grad_u)
        grad_down_ref[0] += tn(scaled, cotangent)


def weights_call(begin, count, first, normed, cotangent, gates, gate_w, up_w, down_w, earlier):
    rows, width = normed.shape
    experts = gates.shape[1]
    hidden = gate_w.shape[2]
    tile = 1024
    pick = lambda e, c: (e + begin, 0, 0)
    in_specs = [
        pl.BlockSpec(memory_space=pltpu.SMEM),
        pl.BlockSpec((tile, width), lambda e, c: (c, 0)),
        pl.BlockSpec((tile, width), lambda e, c: (c, 0)),
        pl.BlockSpec((tile, experts), lambda e, c: (c, 0)),
        pl.BlockSpec((1, width, hidden), pick),
        pl.BlockSpec((1, width, hidden), pick),
        pl.BlockSpec((1, hidden, width), pick),
    ]
    operands = [first + begin, normed, cotangent, gates, gate_w, up_w, down_w]
    aliases = {}
    if earlier is not None:
        in_specs += [pl.BlockSpec(memory_space=pl.ANY)] * 3
        aliases = {7: 0, 8: 1, 9: 2}
        operands += list(earlier)
    return pl.pallas_call(
        weights_kernel,
        out_shape=(
            jax.ShapeDtypeStruct(gate_w.shape, jnp.float32),
            jax.ShapeDtypeStruct(up_w.shape, jnp.float32),
            jax.ShapeDtypeStruct(down_w.shape, jnp.float32),
        ),
        grid=(count, rows // tile),
        in_specs=in_specs,
        out_specs=(
            pl.BlockSpec((1, width, hidden), pick),
            pl.BlockSpec((1, width, hidden), pick),
            pl.BlockSpec((1, hidden, width), pick),
        ),
        input_output_aliases=aliases,
        compiler_params=pltpu.CompilerParams(vmem_limit_bytes=62 << 20),
        name="experts_weights",
        cost_estimate=pl.CostEstimate(
            flops=12 * rows * width * hidden * count,
            bytes_accessed=count * (4 * rows * width + 18 * width * hidden),
            transcendentals=0,
        ),
    )(*operands)


def per_device(
    tokens,
    positions,
    expert_ids,
    norm1_gain,
    w_query,
    key_projection_weight,
    value_projection_weight,
    w_out,
    norm2_gain,
    w_router,
    w_gate,
    w_up,
    w_down,
    grad_output,
):
    weights = (
        lax.all_gather(norm1_gain, "fsdp", axis=0, tiled=True),
        lax.all_gather(w_query, "fsdp", axis=0, tiled=True),
        lax.all_gather(key_projection_weight, "fsdp", axis=0, tiled=True),
        lax.all_gather(value_projection_weight, "fsdp", axis=0, tiled=True),
        lax.all_gather(w_out, "fsdp", axis=1, tiled=True),
        lax.all_gather(norm2_gain, "fsdp", axis=0, tiled=True),
        lax.all_gather(w_router, "fsdp", axis=0, tiled=True),
    )
    gain_one_b, query_w, key_w, value_w, out_w, gain_two_b, router_w = weights
    rows = tokens[0].astype(jnp.float32)
    block_len = rows.shape[0]
    heads_here = query_w.shape[1] // HEAD_DIMENSION
    groups_here = key_w.shape[1] // HEAD_DIMENSION
    group_repeat = heads_here // groups_here
    softmax_scale = 1.0 / math.sqrt(HEAD_DIMENSION)
    scale_one = rms_scale(rows)
    first_normalized = (rows * scale_one * gain_one_b.astype(jnp.float32)).astype(jnp.bfloat16)
    cosine_table, sine_table = rope_tables(positions[0], HEAD_DIMENSION)
    query_rows = apply_rotation(
        jnp.dot(first_normalized, query_w, preferred_element_type=jnp.float32).reshape(
            block_len, heads_here, HEAD_DIMENSION
        ),
        cosine_table,
        sine_table,
        1.0,
    ).astype(jnp.bfloat16)
    key_row_list = (
        apply_rotation(
            jnp.dot(first_normalized, key_w, preferred_element_type=jnp.float32).reshape(
                block_len, groups_here, HEAD_DIMENSION
            ),
            cosine_table,
            sine_table,
            1.0,
        )
        .astype(jnp.bfloat16)
        .reshape(block_len, groups_here * HEAD_DIMENSION)
    )
    value_row_list = jnp.dot(first_normalized, value_w, preferred_element_type=jnp.float32).astype(
        jnp.bfloat16
    )
    query_fourdim = query_rows.reshape(block_len, groups_here, group_repeat, HEAD_DIMENSION)
    query_pos = lax.axis_index("context") * block_len + jnp.arange(block_len, dtype=jnp.int32)
    start_state = (
        jnp.full((groups_here, group_repeat, block_len), masked_score, jnp.float32),
        jnp.zeros((groups_here, group_repeat, block_len), jnp.float32),
        jnp.zeros((block_len, groups_here, group_repeat, HEAD_DIMENSION), jnp.float32),
    )
    state = start_state
    key_piece = lax.all_gather(key_row_list, "context", axis=0, tiled=True)
    value_piece = lax.all_gather(value_row_list, "context", axis=0, tiled=True)
    sequence_length = key_piece.shape[0]
    width = math.gcd(sequence_length, 512)
    key_blocks = key_piece.reshape(sequence_length // width, width, groups_here, HEAD_DIMENSION)
    value_blocks = value_piece.reshape(sequence_length // width, width, groups_here, HEAD_DIMENSION)
    firsts = jnp.arange(sequence_length // width, dtype=jnp.int32) * width

    def attend_inner(carry, item):
        top, total, running_total = carry
        key_block_tile, value_block_tile, first = item
        score_matrix = (
            jnp.einsum(
                "ijzq,pjq->jzip", query_fourdim, key_block_tile, preferred_element_type=jnp.float32
            )
            * softmax_scale
        )
        allowed = (first + jnp.arange(width, dtype=jnp.int32))[None, :] <= query_pos[:, None]
        score_matrix = jnp.where(allowed, score_matrix, masked_score)
        new_top = jnp.maximum(top, jnp.max(score_matrix, axis=-1))
        exponent_values = jnp.where(allowed, jnp.exp(score_matrix - new_top[..., None]), 0.0)
        shrink = jnp.exp(top - new_top)
        total = total * shrink + jnp.sum(exponent_values, axis=-1)
        update = jnp.einsum(
            "hevu,uhw->vhew",
            exponent_values.astype(jnp.bfloat16),
            value_block_tile,
            preferred_element_type=jnp.float32,
        )
        running_total = running_total * jnp.transpose(shrink, (2, 0, 1))[..., None] + update
        return ((new_top, total, running_total), None)

    state, _ = lax.scan(attend_inner, state, (key_blocks, value_blocks, firsts))
    top, total, running_total = state
    attended = running_total / jnp.transpose(total, (2, 0, 1))[..., None]
    logsumexp_total = top + jnp.log(total)
    attended_batch = attended.astype(jnp.bfloat16).reshape(block_len, heads_here * HEAD_DIMENSION)
    mixed = lax.psum(jnp.dot(attended_batch, out_w, preferred_element_type=jnp.float32), "tensor")
    hidden = rows + mixed
    scale_two = rms_scale(hidden)
    normed_two = (hidden * scale_two * gain_two_b.astype(jnp.float32)).astype(jnp.bfloat16)
    experts = router_w.shape[1]
    width_all = rows.shape[1]
    experts_here = w_gate.shape[0]
    first = (lax.axis_index("fsdp") * experts_here).reshape(1)
    cotangent_here = lax.all_gather(grad_output[0], "fsdp", axis=0, tiled=True)
    cotangent_all = lax.all_gather(cotangent_here, "context", axis=0, tiled=True)
    ids_here = lax.all_gather(expert_ids[0], "fsdp", axis=0, tiled=True)
    ids_all = lax.all_gather(ids_here, "context", axis=0, tiled=True)
    grad_rows_out = grad_output[0].astype(jnp.float32)
    normed_here = lax.all_gather(normed_two, "fsdp", axis=0, tiled=True)
    normed_all = lax.all_gather(normed_here, "context", axis=0, tiled=True)
    moe_part, grad_normed_part, grad_router = own_call(
        first, normed_here, cotangent_here, ids_here, router_w, w_gate, w_up, w_down
    )
    both = lax.psum_scatter(
        jnp.stack([grad_normed_part, moe_part], axis=1), "fsdp", scatter_dimension=0, tiled=True
    )
    both = lax.psum(both, "tensor").astype(jnp.float32)
    grad_normed_two, moe = both[:, 0], both[:, 1]
    gates_all = gates_call(normed_all, ids_all, router_w)
    expert_grads = None
    for e in range(experts_here):
        expert_grads = weights_call(
            e, 1, first, normed_all, cotangent_all, gates_all, w_gate, w_up, w_down, expert_grads
        )
    output = (hidden + moe).astype(jnp.bfloat16)
    grad_hidden_n, grad_gain_two = norm_backward(
        hidden, scale_two, gain_two_b.astype(jnp.float32), grad_normed_two
    )
    grad_hidden = grad_rows_out + grad_hidden_n
    grad_hidden_b = grad_hidden.astype(jnp.bfloat16)
    attended_gradient = jnp.dot(grad_hidden_b, out_w.T, preferred_element_type=jnp.float32).astype(
        jnp.bfloat16
    )
    grad_out_w = jnp.dot(attended_batch.T, grad_hidden_b, preferred_element_type=jnp.float32)
    gradient_fourdim = attended_gradient.reshape(
        block_len, groups_here, group_repeat, HEAD_DIMENSION
    )
    delta = jnp.transpose(
        jnp.sum(
            gradient_fourdim.astype(jnp.float32)
            * attended_batch.reshape(block_len, groups_here, group_repeat, HEAD_DIMENSION).astype(
                jnp.float32
            ),
            axis=-1,
        ),
        (1, 2, 0),
    )
    grad_q = jnp.zeros((block_len, groups_here, group_repeat, HEAD_DIMENSION), jnp.float32)
    key_piece = lax.all_gather(key_row_list, "context", axis=0, tiled=True)
    value_piece = lax.all_gather(value_row_list, "context", axis=0, tiled=True)
    sequence_length = key_piece.shape[0]
    back_width = math.gcd(sequence_length, 512)
    key_blocks = key_piece.reshape(
        sequence_length // back_width, back_width, groups_here, HEAD_DIMENSION
    )
    value_blocks = value_piece.reshape(
        sequence_length // back_width, back_width, groups_here, HEAD_DIMENSION
    )
    firsts = jnp.arange(sequence_length // back_width, dtype=jnp.int32) * back_width

    def back_inner(grad_acc, item):
        key_block_tile, value_block_tile, first = item
        score_matrix = (
            jnp.einsum(
                "ijzq,pjq->jzip", query_fourdim, key_block_tile, preferred_element_type=jnp.float32
            )
            * softmax_scale
        )
        allowed = (first + jnp.arange(back_width, dtype=jnp.int32))[None, :] <= query_pos[:, None]
        probabilities = jnp.where(allowed, jnp.exp(score_matrix - logsumexp_total[..., None]), 0.0)
        grad_v_blk = jnp.einsum(
            "ihne,nihf->eif",
            probabilities.astype(jnp.bfloat16),
            gradient_fourdim,
            preferred_element_type=jnp.float32,
        )
        probability_gradient = jnp.einsum(
            "ijzq,pjq->jzip", gradient_fourdim, value_block_tile, preferred_element_type=jnp.float32
        )
        score_gradient = (probabilities * (probability_gradient - delta[..., None])).astype(
            jnp.bfloat16
        )
        grad_acc = (
            grad_acc
            + jnp.einsum(
                "hevu,uhw->vhew", score_gradient, key_block_tile, preferred_element_type=jnp.float32
            )
            * softmax_scale
        )
        grad_k_blk = (
            jnp.einsum(
                "ihne,nihf->eif", score_gradient, query_fourdim, preferred_element_type=jnp.float32
            )
            * softmax_scale
        )
        joined = jnp.concatenate(
            [grad_k_blk.reshape(back_width, -1), grad_v_blk.reshape(back_width, -1)], axis=1
        )
        return (grad_acc, joined)

    grad_q, joined_all = lax.scan(back_inner, grad_q, (key_blocks, value_blocks, firsts))
    grad_kv = joined_all.reshape(sequence_length, -1)
    grad_q, grad_kv = (grad_q, grad_kv)
    own_kv = lax.psum_scatter(
        grad_kv.astype(jnp.bfloat16), "context", scatter_dimension=0, tiled=True
    ).astype(jnp.float32)
    grad_queries = (
        apply_rotation(
            grad_q.reshape(block_len, heads_here, HEAD_DIMENSION), cosine_table, sine_table, -1.0
        )
        .astype(jnp.bfloat16)
        .reshape(block_len, -1)
    )
    key_rows_gradient = (
        apply_rotation(
            own_kv[:, : groups_here * HEAD_DIMENSION].reshape(
                block_len, groups_here, HEAD_DIMENSION
            ),
            cosine_table,
            sine_table,
            -1.0,
        )
        .astype(jnp.bfloat16)
        .reshape(block_len, -1)
    )
    value_rows_gradient = own_kv[:, groups_here * HEAD_DIMENSION :].astype(jnp.bfloat16)
    grad_normed_part_one = jnp.dot(grad_queries, query_w.T, preferred_element_type=jnp.float32)
    grad_normed_part_one = grad_normed_part_one + jnp.dot(
        key_rows_gradient, key_w.T, preferred_element_type=jnp.float32
    )
    grad_normed_part_one = grad_normed_part_one + jnp.dot(
        value_rows_gradient, value_w.T, preferred_element_type=jnp.float32
    )
    grad_normed_one = lax.psum(grad_normed_part_one.astype(jnp.bfloat16), "tensor").astype(
        jnp.float32
    )
    grad_query_w = jnp.dot(first_normalized.T, grad_queries, preferred_element_type=jnp.float32)
    grad_key_w = jnp.dot(first_normalized.T, key_rows_gradient, preferred_element_type=jnp.float32)
    grad_value_w = jnp.dot(
        first_normalized.T, value_rows_gradient, preferred_element_type=jnp.float32
    )
    grad_rows_n, grad_gain_one = norm_backward(
        rows, scale_one, gain_one_b.astype(jnp.float32), grad_normed_one
    )
    grad_tokens = (grad_hidden + grad_rows_n).astype(jnp.bfloat16)
    parts = (
        lax.psum_scatter(
            grad_gain_one.astype(jnp.bfloat16), "fsdp", scatter_dimension=0, tiled=True
        ).astype(jnp.float32),
        lax.psum_scatter(
            grad_query_w.astype(jnp.bfloat16), "fsdp", scatter_dimension=0, tiled=True
        ).astype(jnp.float32),
        lax.psum_scatter(
            grad_key_w.astype(jnp.bfloat16), "fsdp", scatter_dimension=0, tiled=True
        ).astype(jnp.float32),
        lax.psum_scatter(
            grad_value_w.astype(jnp.bfloat16), "fsdp", scatter_dimension=0, tiled=True
        ).astype(jnp.float32),
        lax.psum_scatter(
            grad_out_w.astype(jnp.bfloat16), "fsdp", scatter_dimension=1, tiled=True
        ).astype(jnp.float32),
        lax.psum_scatter(
            grad_gain_two.astype(jnp.bfloat16), "fsdp", scatter_dimension=0, tiled=True
        ).astype(jnp.float32),
        lax.psum_scatter(
            grad_router.astype(jnp.bfloat16), "fsdp", scatter_dimension=0, tiled=True
        ).astype(jnp.float32),
    )
    summed = (
        lax.psum(parts[0].astype(jnp.bfloat16), "context").astype(jnp.float32),
        lax.psum(parts[1].astype(jnp.bfloat16), "context").astype(jnp.float32),
        lax.psum(parts[2].astype(jnp.bfloat16), "context").astype(jnp.float32),
        lax.psum(parts[3].astype(jnp.bfloat16), "context").astype(jnp.float32),
        lax.psum(parts[4].astype(jnp.bfloat16), "context").astype(jnp.float32),
        lax.psum(parts[5].astype(jnp.bfloat16), "context").astype(jnp.float32),
        lax.psum(parts[6].astype(jnp.bfloat16), ("context", "tensor")).astype(jnp.float32),
    )
    return (
        output[None],
        grad_tokens[None],
        summed[0],
        summed[1],
        summed[2],
        summed[3],
        summed[4],
        summed[5],
        summed[6],
        expert_grads[0],
        expert_grads[1],
        expert_grads[2],
    )


def solution(mesh):
    return jax.shard_map(
        per_device,
        mesh=mesh,
        in_specs=(
            P("fsdp", "context", None),
            P("fsdp", "context"),
            P("fsdp", "context", None),
            P("fsdp"),
            P("fsdp", "tensor"),
            P("fsdp", "tensor"),
            P("fsdp", "tensor"),
            P("tensor", "fsdp"),
            P("fsdp"),
            P("fsdp", None),
            P("fsdp", None, "tensor"),
            P("fsdp", None, "tensor"),
            P("fsdp", "tensor", None),
            P("fsdp", "context", None),
        ),
        out_specs=(
            P("fsdp", "context", None),
            P("fsdp", "context", None),
            P("fsdp"),
            P("fsdp", "tensor"),
            P("fsdp", "tensor"),
            P("fsdp", "tensor"),
            P("tensor", "fsdp"),
            P("fsdp"),
            P("fsdp", None),
            P("fsdp", None, "tensor"),
            P("fsdp", None, "tensor"),
            P("fsdp", "tensor", None),
        ),
        check_vma=False,
    )
```

```python
import functools
import math

import jax
import jax.numpy as jnp
from jax import lax
from jax.experimental import pallas as pl
from jax.experimental.pallas import tpu as pltpu
from jax.sharding import PartitionSpec as P

HEAD = 64
LANES = 128
PAD = 32
norm_eps = 1e-06
masked_score = -1e30
BF = jnp.bfloat16
F32 = jnp.float32
VMEM = pl.BlockSpec(memory_space=pltpu.VMEM)
SMEM = pl.BlockSpec(memory_space=pltpu.SMEM)
ANY = pl.BlockSpec(memory_space=pl.ANY)


def nn(left, right):
    return jnp.dot(left, right, preferred_element_type=F32)


def nt(left, right):
    return lax.dot_general(left, right, (((1,), (1,)), ((), ())), preferred_element_type=F32)


def tn(left, right):
    return lax.dot_general(left, right, (((0,), (0,)), ((), ())), preferred_element_type=F32)


def shape(dims, kind):
    return jax.ShapeDtypeStruct(dims, kind)


def call(kernel, outs, specs, out_specs, scratch, flops, moved, name, **more):
    return pl.pallas_call(
        kernel,
        out_shape=outs,
        in_specs=specs,
        out_specs=out_specs,
        scratch_shapes=scratch,
        compiler_params=pltpu.CompilerParams(vmem_limit_bytes=60 << 20),
        name=name,
        cost_estimate=pl.CostEstimate(flops=flops, bytes_accessed=moved, transcendentals=0),
        **more,
    )


def rotate(rows, cos, sin):
    wide = rows.shape[1]
    count = wide // LANES
    after = pltpu.roll(rows, wide - HEAD // 2, 1)
    before = pltpu.roll(rows, HEAD // 2, 1)
    lane = lax.broadcasted_iota(jnp.int32, rows.shape, 1) % HEAD
    partner = jnp.where(lane < HEAD // 2, after, before)
    cos_all = jnp.concatenate([cos] * count, axis=1)
    sin_all = jnp.concatenate([sin] * count, axis=1)
    return rows * cos_all + partner * sin_all


def project_kernel(members, index, rows_ref, cos_ref, sin_ref, *refs):
    small = refs[:members]
    weights = refs[members : 2 * members]
    normed_ref, heads_ref, kv_ref, table_ref, total = refs[2 * members :]
    f = index[0]
    cut = small[0].shape[1]
    for j in range(members):
        at = pl.ds(pl.multiple_of((f ^ j) * cut, LANES), cut)
        table_ref[:, at] = small[j][...]
    rows = rows_ref[...].astype(F32)
    scale = lax.rsqrt(jnp.mean(rows * rows, axis=-1, keepdims=True) + norm_eps)
    gain = table_ref[...].astype(F32)[PAD - 8 : PAD - 7, :]
    normed_ref[...] = (rows * scale * gain).astype(BF)
    acc = None
    for j in range(members):
        at = pl.ds(pl.multiple_of((f ^ j) * cut, LANES), cut)
        term = nn(normed_ref[:, at], weights[j][...])
        acc = term if acc is None else acc + term
    total[...] = acc
    kv_wide = kv_ref.shape[1] // 2
    q_wide = total.shape[1] - 2 * kv_wide
    cos = cos_ref[...]
    sin = sin_ref[...]
    turned = rotate(total[:, :q_wide], cos, sin) * (1.0 / math.sqrt(HEAD))
    turned = turned.astype(BF)
    for h in range(q_wide // HEAD):
        heads_ref[h] = turned[:, h * HEAD : (h + 1) * HEAD]
    kv_ref[:, :kv_wide] = rotate(total[:, q_wide : q_wide + kv_wide], cos, sin).astype(BF)
    kv_ref[:, kv_wide:] = total[:, q_wide + kv_wide :].astype(BF)


def project(index, rows, cos, sin, small, weights, kv_wide):
    members = len(weights)
    tokens, width = rows.shape
    wide = weights[0].shape[1]
    heads = (wide - 2 * kv_wide) // HEAD
    return call(
        functools.partial(project_kernel, members),
        (
            shape((tokens, width), BF),
            shape((heads, tokens, HEAD), BF),
            shape((tokens, 2 * kv_wide), BF),
            shape((PAD, width), BF),
        ),
        [SMEM] + [VMEM] * (3 + 2 * members),
        (VMEM,) * 4,
        [pltpu.VMEM((tokens, wide), F32)],
        2 * tokens * width * wide,
        2 * width * wide,
        "project",
    )(index, rows, cos, sin, *small, *weights)


def attend_kernel(slots, groups, index, heads_ref, *refs):
    kv = refs[:slots]
    att_ref, lse_ref, scores, top, total, acc = refs[slots:]
    place = index[0]
    tokens = heads_ref.shape[1]
    repeat = heads_ref.shape[0] // groups
    half = kv[0].shape[1] // 2
    many = repeat * tokens
    keys = lax.broadcasted_iota(jnp.int32, (tokens, many), 0)
    queries = lax.broadcasted_iota(jnp.int32, (tokens, many), 1) % tokens
    allowed = keys <= queries
    for g in range(groups):
        at = slice(g * HEAD, (g + 1) * HEAD)
        q = heads_ref[g * repeat : (g + 1) * repeat].reshape(many, HEAD)
        for s in range(slots):

            @pl.when(place >= s)
            def _():
                score = nt(kv[s][:, at], q)
                if s == 0:
                    score = jnp.where(allowed, score, masked_score)
                scores[s] = score
                high = jnp.max(score, axis=0, keepdims=True)
                top[...] = high if s == 0 else jnp.maximum(top[...], high)

        for s in range(slots):

            @pl.when(place >= s)
            def _():
                weight = jnp.exp(scores[s] - top[...])
                if s == 0:
                    weight = jnp.where(allowed, weight, 0.0)
                part = jnp.sum(weight, axis=0, keepdims=True)
                value = kv[s][:, half + g * HEAD : half + (g + 1) * HEAD]
                value = jnp.concatenate([value, jnp.ones_like(value)], axis=1)
                out = tn(weight.astype(BF), value)
                total[...] = part if s == 0 else total[...] + part
                acc[...] = out if s == 0 else acc[...] + out

        lse_ref[g] = top[...] + jnp.log(total[...])
        done = (acc[:, :HEAD] / acc[:, HEAD:]).astype(BF)
        for r in range(repeat):
            h = g * repeat + r
            att_ref[:, h * HEAD : (h + 1) * HEAD] = done[r * tokens : (r + 1) * tokens]


def attend(index, heads, kv):
    slots = len(kv)
    count, tokens, _ = heads.shape
    groups = kv[0].shape[1] // (2 * HEAD)
    many = count // groups * tokens
    return call(
        functools.partial(attend_kernel, slots, groups),
        (shape((tokens, count * HEAD), BF), shape((groups, 1, many), F32)),
        [SMEM] + [VMEM] * (1 + slots),
        (VMEM, VMEM),
        [
            pltpu.VMEM((slots, tokens, many), F32),
            pltpu.VMEM((1, many), F32),
            pltpu.VMEM((1, many), F32),
            pltpu.VMEM((many, 2 * HEAD), F32),
        ],
        16 * slots * tokens * many * HEAD,
        4 * tokens * count * HEAD,
        "attend",
    )(index, heads, *kv)


def attend_back_kernel(slots, groups, index, heads_ref, grad_ref, att_ref, lse_ref, cos_ref, sin_ref, *refs):
    kv = refs[:slots]
    grad_q_ref = refs[slots]
    grad_kv = refs[slots + 1 : 2 * slots + 1]
    acc, turned = refs[2 * slots + 1 :]
    place = index[0]
    tokens = heads_ref.shape[1]
    repeat = heads_ref.shape[0] // groups
    half = kv[0].shape[1] // 2
    many = repeat * tokens
    keys = lax.broadcasted_iota(jnp.int32, (tokens, many), 0)
    queries = lax.broadcasted_iota(jnp.int32, (tokens, many), 1) % tokens
    allowed = keys <= queries
    lane = lax.broadcasted_iota(jnp.int32, (many, 2 * HEAD), 1)
    for g in range(groups):
        at = slice(g * HEAD, (g + 1) * HEAD)
        behind = slice(half + g * HEAD, half + (g + 1) * HEAD)
        q = heads_ref[g * repeat : (g + 1) * repeat].reshape(many, HEAD)
        grad = grad_ref[g * repeat : (g + 1) * repeat].reshape(many, HEAD)
        out = jnp.concatenate(
            [
                att_ref[:, (g * repeat + r) * HEAD : (g * repeat + r + 1) * HEAD]
                for r in range(repeat)
            ],
            axis=0,
        )
        delta = jnp.sum(grad.astype(F32) * out.astype(F32), axis=-1, keepdims=True)
        upper = delta.astype(BF).astype(F32)
        lower = delta - upper
        wide = jnp.concatenate([grad.astype(F32), jnp.zeros((many, HEAD), F32)], axis=1)
        wide = jnp.where(lane == HEAD, -upper, jnp.where(lane == HEAD + 1, -lower, wide)).astype(BF)
        lse = lse_ref[g]
        for s in range(slots):

            @pl.when(place >= s)
            def _():
                key = kv[s][:, at]
                value = kv[s][:, behind]
                value = jnp.concatenate([value, jnp.ones_like(value)], axis=1)
                prob = jnp.exp(nt(key, q) - lse)
                if s == 0:
                    prob = jnp.where(allowed, prob, 0.0)
                grad_score = (prob * nt(value, wide)).astype(BF)
                kind = grad_kv[s].dtype
                grad_kv[s][:, at] = nn(grad_score, q).astype(kind)
                grad_kv[s][:, behind] = nn(prob.astype(BF), grad).astype(kind)
                part = tn(grad_score, key)
                acc[...] = part if s == 0 else acc[...] + part

        done = acc[...] * (1.0 / math.sqrt(HEAD))
        for r in range(repeat):
            h = g * repeat + r
            turned[:, h * HEAD : (h + 1) * HEAD] = done[r * tokens : (r + 1) * tokens]
    grad_q_ref[...] = rotate(turned[...], cos_ref[...], -sin_ref[...]).astype(BF)


def attend_back(index, heads, grad, att, lse, cos, sin, kv):
    slots = len(kv)
    count, tokens, _ = heads.shape
    groups = kv[0].shape[1] // (2 * HEAD)
    many = count // groups * tokens
    outs = [shape((tokens, count * HEAD), BF), shape(kv[0].shape, F32)]
    outs += [shape(kv[0].shape, BF)] * (slots - 1)
    return call(
        functools.partial(attend_back_kernel, slots, groups),
        tuple(outs),
        [SMEM] + [VMEM] * (6 + slots),
        (VMEM,) * len(outs),
        [pltpu.VMEM((many, HEAD), F32), pltpu.VMEM((tokens, count * HEAD), F32)],
        40 * slots * tokens * many * HEAD,
        8 * tokens * count * HEAD,
        "attend_back",
    )(index, heads, grad, att, lse, cos, sin, *kv)


def mix_kernel(members, index, rows_ref, att_ref, other_ref, table_ref, ids_ref, *refs):
    mine = refs[:members]
    theirs = refs[members : 2 * members]
    hidden_ref, normed_ref, first, second = refs[2 * members :]
    f = index[0]
    cut = mine[0].shape[1]
    width = rows_ref.shape[1]
    for j in range(members):
        at = pl.ds(pl.multiple_of((f ^ j) * cut, LANES), cut)
        first[:, at] = nn(att_ref[...], mine[j][...])
        second[:, at] = nn(other_ref[...], theirs[j][...])
    hidden = rows_ref[...].astype(F32) + (first[...] + second[...])
    hidden_ref[...] = hidden
    scale = lax.rsqrt(jnp.mean(hidden * hidden, axis=-1, keepdims=True) + norm_eps)
    gain = table_ref[...].astype(F32)[PAD - 7 : PAD - 6, :]
    normed = (hidden * scale * gain).astype(BF)
    normed_ref[:, :width] = normed
    logits = nt(normed, table_ref[...])
    lanes = lax.broadcasted_iota(jnp.int32, logits.shape, 1)
    ids = ids_ref[...]
    mask = ids[:, 0:1] == lanes
    for k in range(1, ids.shape[1]):
        mask = mask | (ids[:, k : k + 1] == lanes)
    logits = jnp.where(mask, logits, masked_score)
    weight = jnp.where(mask, jnp.exp(logits - jnp.max(logits, axis=-1, keepdims=True)), 0.0)
    gates = weight / jnp.sum(weight, axis=-1, keepdims=True)
    upper = gates.astype(BF).astype(F32)
    lower = gates - upper
    blank = jnp.zeros((gates.shape[0], LANES - 2 * PAD), F32)
    normed_ref[:, width:] = jnp.concatenate([upper, lower, blank], axis=1).astype(BF)


def mix(index, rows, att, other, table, ids, mine, theirs):
    members = len(mine)
    tokens, width = rows.shape
    return call(
        functools.partial(mix_kernel, members),
        (shape((tokens, width), F32), shape((tokens, width + LANES), BF)),
        [SMEM] + [VMEM] * (5 + 2 * members),
        (VMEM, VMEM),
        [pltpu.VMEM((tokens, width), F32)] * 2,
        4 * tokens * width * att.shape[1],
        4 * width * att.shape[1],
        "mix",
    )(index, rows, att, other, table, ids, *mine, *theirs)


def gates_of(tail, experts):
    rows = tail.astype(F32)
    both = rows + pltpu.roll(rows, LANES - PAD, 1)
    lane = lax.broadcasted_iota(jnp.int32, both.shape, 1)
    return jnp.where(lane < experts, both, 0.0)


def gate_column(gates, expert):
    lane = lax.broadcasted_iota(jnp.int32, gates.shape, 1)
    return jnp.sum(jnp.where(lane == expert, gates, 0.0), axis=-1, keepdims=True)


def hidden_terms(normed, cotangent, gate_col, gate_w, up_w, down_w):
    gate_pre = nn(normed, gate_w)
    up_pre = nn(normed, up_w)
    plain = nt(cotangent, down_w)
    sigma = 1.0 / (1.0 + jnp.exp(-gate_pre))
    activated = gate_pre * sigma
    inner = activated * up_pre
    grad_inner = gate_col * plain
    scaled = (gate_col * inner).astype(BF)
    grad_g = (grad_inner * up_pre * (sigma + activated * (1.0 - sigma))).astype(BF)
    grad_u = (grad_inner * activated).astype(BF)
    return inner, plain, scaled, grad_g, grad_u


def own_kernel(blocks, experts, index, table_ref, *refs):
    normed_in = refs[:blocks]
    cot_in = refs[blocks : 2 * blocks]
    gate_hbm, up_hbm, down_hbm = refs[2 * blocks : 2 * blocks + 3]
    grad_out = refs[2 * blocks + 3 : 3 * blocks + 3]
    moe_out = refs[3 * blocks + 3 : 4 * blocks + 3]
    router_ref, scaled_ref, grad_g_ref, grad_u_ref = refs[4 * blocks + 3 : 4 * blocks + 7]
    gate_w, up_w, down_w, normed, cot, gates, shares, sems, block_sems = refs[4 * blocks + 7 :]
    here = gate_w.shape[0]
    hidden = gate_w.shape[2]
    tokens = normed_in[0].shape[0]
    width = cot.shape[1]
    rows = blocks * tokens

    def expert_copies(e):
        return (
            pltpu.make_async_copy(gate_hbm.at[e], gate_w.at[e], sems.at[0, e]),
            pltpu.make_async_copy(up_hbm.at[e], up_w.at[e], sems.at[1, e]),
            pltpu.make_async_copy(down_hbm.at[e], down_w.at[e], sems.at[2, e]),
        )

    block_copies = []
    for b in range(blocks):
        at = slice(b * tokens, (b + 1) * tokens)
        block_copies.append(pltpu.make_async_copy(normed_in[b], normed.at[at], block_sems.at[0, b]))
        block_copies.append(pltpu.make_async_copy(cot_in[b], cot.at[at], block_sems.at[1, b]))
    for copy in block_copies:
        copy.start()
    for e in range(here):
        for copy in expert_copies(e):
            copy.start()
    for copy in block_copies:
        copy.wait()
    first = index[0] * here
    gates[...] = gates_of(normed[:, width:], experts)
    shares[...] = jnp.zeros_like(shares)

    def one_expert(e, carry):
        for copy in expert_copies(e):
            copy.wait()
        columns = pl.ds(pl.multiple_of(e * hidden, LANES), hidden)

        def one_tile(i, inner_carry):
            at = pl.ds(pl.multiple_of(i * 256, 256), 256)
            inner, plain, scaled, grad_g, grad_u = hidden_terms(
                normed[at, :width],
                cot[at, :],
                gate_column(gates[at, :], first + e),
                gate_w[e],
                up_w[e],
                down_w[e],
            )
            scaled_ref[at, columns] = scaled
            grad_g_ref[at, columns] = grad_g
            grad_u_ref[at, columns] = grad_u
            share = jnp.sum(inner * plain, axis=-1, keepdims=True)
            lane = lax.broadcasted_iota(jnp.int32, (256, LANES), 1)
            shares[at, :] = jnp.where(lane == first + e, share, shares[at, :])
            return inner_carry

        return lax.fori_loop(0, rows // 256, one_tile, carry)

    lax.fori_loop(0, here, one_expert, 0)

    mean = jnp.sum(gates[...] * shares[...], axis=-1, keepdims=True)
    shares[...] = gates[...] * (shares[...] - mean)
    logits = shares[...].astype(BF)
    router_ref[...] = tn(logits, normed[:, :width])[:PAD]
    for b in range(blocks):
        at = slice(b * tokens, (b + 1) * tokens)
        total = nn(logits[at, :PAD], table_ref[...])
        for e in range(here):
            columns = slice(e * hidden, (e + 1) * hidden)
            total = total + nt(grad_g_ref[at, columns], gate_w[e])
            total = total + nt(grad_u_ref[at, columns], up_w[e])
        grad_out[b][...] = total.astype(BF)
    down_all = down_w[...].reshape(here * hidden, width)
    for b in range(blocks):
        at = slice(b * tokens, (b + 1) * tokens)
        moe_out[b][...] = nn(scaled_ref[at, :], down_all).astype(BF)


def own(index, table, normed, cotangent, gate_w, up_w, down_w, experts):
    blocks = len(normed)
    tokens, width = cotangent[0].shape
    here, _, hidden = gate_w.shape
    rows = blocks * tokens
    outs = [shape((tokens, width), BF)] * (2 * blocks) + [shape((PAD, width), F32)]
    outs += [shape((rows, here * hidden), BF)] * 3
    results = call(
        functools.partial(own_kernel, blocks, experts),
        tuple(outs),
        [SMEM, VMEM] + [ANY] * (2 * blocks + 3),
        (VMEM,) * len(outs),
        [
            pltpu.VMEM(gate_w.shape, BF),
            pltpu.VMEM(up_w.shape, BF),
            pltpu.VMEM(down_w.shape, BF),
            pltpu.VMEM((rows, width + LANES), BF),
            pltpu.VMEM((rows, width), BF),
            pltpu.VMEM((rows, LANES), F32),
            pltpu.VMEM((rows, LANES), F32),
            pltpu.SemaphoreType.DMA((3, here)),
            pltpu.SemaphoreType.DMA((2, blocks)),
        ],
        12 * rows * width * hidden * here,
        6 * here * width * hidden + 8 * rows * width,
        "own",
    )(index, table, *normed, *cotangent, gate_w, up_w, down_w)
    return (
        results[:blocks],
        results[blocks : 2 * blocks],
        results[2 * blocks],
        results[2 * blocks + 1 :],
    )


def first_weights_kernel(sizes, *refs):
    count = sum(sizes)
    normed = refs[:count]
    cot = refs[count : 2 * count]
    saved = refs[2 * count : 2 * count + 3 * len(sizes)]
    grad_gate_ref, grad_up_ref, grad_down_ref = refs[-3:]
    grad_gate = grad_up = grad_down = None
    base = 0
    for part, blocks in enumerate(sizes):
        scaled, grad_g, grad_u = saved[3 * part : 3 * part + 3]
        tokens = normed[0].shape[0]
        for b in range(blocks):
            at = slice(b * tokens, (b + 1) * tokens)
            left = normed[base + b][...]
            terms = (tn(left, grad_g[at, :]), tn(left, grad_u[at, :]), tn(scaled[at, :], cot[base + b][...]))
            if grad_gate is None:
                grad_gate, grad_up, grad_down = terms
            else:
                grad_gate = grad_gate + terms[0]
                grad_up = grad_up + terms[1]
                grad_down = grad_down + terms[2]
        base += blocks
    grad_gate_ref[0] = grad_gate
    grad_up_ref[0] = grad_up
    grad_down_ref[0] = grad_down


def first_weights(normed, cotangent, saved, like):
    sizes = tuple(part[0].shape[0] // cotangent[0].shape[0] for part in saved)
    tokens, width = cotangent[0].shape
    here, _, hidden = like[0].shape
    block = lambda e: (0, 0)
    pick = lambda e: (e, 0, 0)
    specs = [pl.BlockSpec((tokens, width), block)] * (2 * len(normed))
    flat = []
    for part in saved:
        for item in part:
            specs.append(pl.BlockSpec((item.shape[0], hidden), lambda e: (0, e)))
            flat.append(item)
    return call(
        functools.partial(first_weights_kernel, sizes),
        tuple(shape(item.shape, F32) for item in like),
        specs,
        (
            pl.BlockSpec((1, width, hidden), pick),
            pl.BlockSpec((1, width, hidden), pick),
            pl.BlockSpec((1, hidden, width), pick),
        ),
        [],
        6 * len(normed) * tokens * width * hidden * here,
        12 * here * width * hidden,
        "first_weights",
        grid=(here,),
    )(*normed, *cotangent, *flat)


def more_weights_kernel(pieces, experts, begin, index, *refs):
    normed_in = refs[:pieces]
    cot_in = refs[pieces : 2 * pieces]
    gate_w, up_w, down_w, old_gate, old_up, old_down = refs[2 * pieces : 2 * pieces + 6]
    new_gate, new_up, new_down, normed, cot, gates, sems = refs[2 * pieces + 6 :]
    width = cot.shape[1]
    here = index[1]

    @pl.when(pl.program_id(0) == 0)
    def _():
        copies = []
        base = 0
        for p in range(pieces):
            at = pl.ds(base, normed_in[p].shape[0])
            copies.append(pltpu.make_async_copy(normed_in[p], normed.at[at], sems.at[0, p]))
            copies.append(pltpu.make_async_copy(cot_in[p], cot.at[at], sems.at[1, p]))
            base += normed_in[p].shape[0]
        for copy in copies:
            copy.start()
        for copy in copies:
            copy.wait()
        gates[...] = gates_of(normed[:, width:], experts)

    expert = index[0] * here + begin + pl.program_id(0)
    left = normed[:, :width]
    _, _, scaled, grad_g, grad_u = hidden_terms(
        left, cot[...], gate_column(gates[...], expert), gate_w[0], up_w[0], down_w[0]
    )
    new_gate[0] = old_gate[0] + tn(left, grad_g)
    new_up[0] = old_up[0] + tn(left, grad_u)
    new_down[0] = old_down[0] + tn(scaled, cot[...])


def more_weights(begin, count, index, normed, cotangent, gate_w, up_w, down_w, earlier, experts):
    pieces = len(normed)
    width = cotangent[0].shape[1]
    rows = sum(item.shape[0] for item in cotangent)
    hidden = gate_w.shape[2]
    pick = lambda e: (e + begin, 0, 0)
    wide = pl.BlockSpec((1, width, hidden), pick)
    tall = pl.BlockSpec((1, hidden, width), pick)
    return call(
        functools.partial(more_weights_kernel, pieces, experts, begin),
        tuple(shape(item.shape, F32) for item in earlier),
        [SMEM] + [ANY] * (2 * pieces) + [wide, wide, tall] * 2,
        (wide, wide, tall),
        [
            pltpu.VMEM((rows, width + LANES), BF),
            pltpu.VMEM((rows, width), BF),
            pltpu.VMEM((rows, LANES), F32),
            pltpu.SemaphoreType.DMA((2, pieces)),
        ],
        12 * rows * width * hidden * count,
        count * 30 * width * hidden + 4 * rows * width,
        "more_weights",
        grid=(count,),
        input_output_aliases={2 * pieces + 4: 0, 2 * pieces + 5: 1, 2 * pieces + 6: 2},
    )(index, *normed, *cotangent, gate_w, up_w, down_w, *earlier)


def middle_kernel(members, index, hidden_ref, cot_ref, mine_ref, theirs_ref, table_ref, *refs):
    weights = refs[:members]
    grad_ref, grad_b_ref, heads_ref, gain_ref = refs[members:]
    f = index[0]
    cut = weights[0].shape[1]
    hidden = hidden_ref[...]
    normed_grad = mine_ref[...].astype(F32) + theirs_ref[...].astype(F32)
    scale = lax.rsqrt(jnp.mean(hidden * hidden, axis=-1, keepdims=True) + norm_eps)
    gain = table_ref[...].astype(F32)[PAD - 7 : PAD - 6, :]
    weighted = normed_grad * gain
    cubed = scale * scale * scale
    grad = (
        cot_ref[...].astype(F32)
        + scale * weighted
        - hidden * cubed * jnp.mean(weighted * hidden, axis=-1, keepdims=True)
    )
    gain_ref[...] = jnp.sum(normed_grad * hidden * scale, axis=0, keepdims=True)
    grad_ref[...] = grad
    grad_b_ref[...] = grad.astype(BF)
    total = None
    for j in range(members):
        at = pl.ds(pl.multiple_of((f ^ j) * cut, LANES), cut)
        term = nt(grad_b_ref[:, at], weights[j][...])
        total = term if total is None else total + term
    total = total.astype(BF)
    for h in range(heads_ref.shape[0]):
        heads_ref[h] = total[:, h * HEAD : (h + 1) * HEAD]


def middle(index, hidden, cotangent, mine, theirs, table, weights):
    members = len(weights)
    tokens, width = hidden.shape
    heads = weights[0].shape[0] // HEAD
    return call(
        functools.partial(middle_kernel, members),
        (
            shape((tokens, width), F32),
            shape((tokens, width), BF),
            shape((heads, tokens, HEAD), BF),
            shape((1, width), F32),
        ),
        [SMEM] + [VMEM] * (5 + members),
        (VMEM,) * 4,
        [],
        2 * tokens * width * heads * HEAD,
        16 * tokens * width,
        "middle",
    )(index, hidden, cotangent, mine, theirs, table, *weights)


def lower_kernel(members, received, index, grad_q_ref, own_ref, rows_ref, cos_ref, sin_ref, *refs):
    others = refs[:received]
    weights = refs[received : received + members]
    joined_ref, part_ref, gain_ref = refs[received + members :]
    f = index[0]
    cut = weights[0].shape[0]
    total = own_ref[...]
    for item in others:
        total = total + item[...].astype(F32)
    half = total.shape[1] // 2
    q_wide = grad_q_ref.shape[1]
    joined_ref[:, :q_wide] = grad_q_ref[...]
    keys = rotate(total[:, :half], cos_ref[...], -sin_ref[...])
    joined_ref[:, q_wide : q_wide + half] = keys.astype(BF)
    joined_ref[:, q_wide + half :] = total[:, half:].astype(BF)
    rows = rows_ref[...].astype(F32)
    scale = lax.rsqrt(jnp.mean(rows * rows, axis=-1, keepdims=True) + norm_eps)
    for j in range(members):
        at = pl.ds(pl.multiple_of((f ^ j) * cut, LANES), cut)
        part_ref[:, at] = nt(joined_ref[...], weights[j][...]).astype(BF)
    gain_ref[...] = jnp.sum(part_ref[...].astype(F32) * rows * scale, axis=0, keepdims=True)


def lower(index, grad_q, own_kv, others, rows, cos, sin, weights):
    members = len(weights)
    tokens, width = rows.shape
    wide = weights[0].shape[1]
    return call(
        functools.partial(lower_kernel, members, len(others)),
        (shape((tokens, wide), BF), shape((tokens, width), BF), shape((1, width), F32)),
        [SMEM] + [VMEM] * (5 + len(others) + members),
        (VMEM,) * 3,
        [],
        2 * tokens * width * wide,
        2 * width * wide,
        "lower",
    )(index, grad_q, own_kv, rows, cos, sin, *others, *weights)


def last_kernel(rows_ref, grad_ref, mine_ref, theirs_ref, table_ref, out_ref):
    rows = rows_ref[...].astype(F32)
    normed_grad = mine_ref[...].astype(F32) + theirs_ref[...].astype(F32)
    scale = lax.rsqrt(jnp.mean(rows * rows, axis=-1, keepdims=True) + norm_eps)
    gain = table_ref[...].astype(F32)[PAD - 8 : PAD - 7, :]
    weighted = normed_grad * gain
    cubed = scale * scale * scale
    out_ref[...] = (
        grad_ref[...]
        + scale * weighted
        - rows * cubed * jnp.mean(weighted * rows, axis=-1, keepdims=True)
    ).astype(BF)


def last(rows, grad, mine, theirs, table):
    tokens, width = rows.shape
    return call(
        last_kernel,
        shape((tokens, width), BF),
        [VMEM] * 5,
        VMEM,
        [],
        16 * tokens * width,
        12 * tokens * width,
        "last",
    )(rows, grad, mine, theirs, table)


def product_kernel(members, extra, *refs):
    left = refs[:members]
    right = refs[members : 2 * members]
    small = refs[2 * members : 2 * members + extra]
    out_ref = refs[-1]
    total = None
    for j in range(members):
        term = tn(left[j][...], right[j][...])
        total = term if total is None else total + term
    rows, columns = total.shape
    out_ref[:rows, :] = total.astype(BF)
    if extra:
        summed = small[0][...].astype(F32)
        for item in small[1:]:
            summed = summed + item[...].astype(F32)
        out_ref[rows:, :] = jnp.zeros((out_ref.shape[0] - rows, columns), BF)
        out_ref[rows : rows + PAD, : summed.shape[1]] = summed.astype(BF)


def product(left, right, small, extra_rows, name):
    members = len(left)
    rows, columns = left[0].shape[1], right[0].shape[1]
    return call(
        functools.partial(product_kernel, members, len(small)),
        shape((rows + extra_rows, columns), BF),
        [VMEM] * (2 * members + len(small)),
        VMEM,
        [],
        2 * members * left[0].shape[0] * rows * columns,
        4 * rows * columns,
        name,
    )(*left, *right, *small)


def sum_kernel(*refs):
    total = refs[0][...].astype(F32)
    for item in refs[1:-1]:
        total = total + item[...].astype(F32)
    refs[-1][...] = total.astype(BF)


def sum_of(items, name):
    size = items[0].shape[0] * items[0].shape[1]
    return call(
        sum_kernel,
        shape(items[0].shape, BF),
        [VMEM] * len(items),
        VMEM,
        [],
        len(items) * size,
        2 * (len(items) + 1) * size,
        name,
    )(*items)


def spread_kernel(slots, cuts, index, *refs):
    parts = refs[:slots]
    outs = refs[slots:-1]
    whole = refs[-1]
    place = index[0]
    rows = parts[0].shape[0]
    for s in range(slots):
        owner = lax.rem(place + slots - s, slots)
        whole[pl.ds(pl.multiple_of(owner * rows, 16), rows), :] = parts[s][...].astype(F32)
    for out, (row, column) in zip(outs, cuts):
        out[...] = whole[row : row + out.shape[0], column : column + out.shape[1]]


def spread(index, parts, cuts, dims, name):
    rows, columns = parts[0].shape
    slots = len(parts)
    return call(
        functools.partial(spread_kernel, slots, cuts),
        tuple(shape(item, F32) for item in dims),
        [SMEM] + [VMEM] * slots,
        (VMEM,) * len(dims),
        [pltpu.VMEM((slots * rows, columns), F32)],
        slots * rows * columns,
        6 * slots * rows * columns,
        name,
    )(index, *parts)


def build(members, slots):
    def by_fsdp(item, j):
        return lax.ppermute(item, "fsdp", [(i, i ^ j) for i in range(members)])

    def by_tensor(item):
        return lax.ppermute(item, "tensor", [(0, 1), (1, 0)])

    def ring(item, step):
        return lax.ppermute(item, "context", [(i, (i + step) % slots) for i in range(slots)])

    def up(item, step):
        return lax.ppermute(item, "context", [(i, i + step) for i in range(slots - step)])

    def down(item, step):
        return lax.ppermute(item, "context", [(i + step, i) for i in range(slots - step)])

    def across(item):
        return [item] + [by_fsdp(item, j) for j in range(2, members, 2)]

    def with_partner(evens):
        out = []
        for item in evens:
            out += [item, by_fsdp(item, 1)]
        return out

    def gather(item):
        return with_partner(across(item))

    def exchange(pieces):
        return [pieces[0]] + [by_fsdp(pieces[j], j) for j in range(1, members)]

    def column_pieces(item, f):
        cut = item.shape[1] // members
        return [lax.dynamic_slice_in_dim(item, (f ^ j) * cut, cut, 1) for j in range(members)]

    def reduce_to_owner(pieces):
        swapped = [by_fsdp(pieces[j + 1], 1) for j in range(0, members, 2)]
        total = [pieces[0], swapped[0]]
        for j in range(2, members, 2):
            both = (pieces[j].astype(F32) + swapped[j // 2].astype(F32)).astype(BF)
            total.append(by_fsdp(both, j))
        acc = total[0].astype(F32)
        for item in total[1:]:
            acc = acc + item.astype(F32)
        return acc.astype(BF)

    def all_reduce(payload, c, name):
        rows = payload.shape[0] // slots
        chunk = lambda s: lax.dynamic_slice_in_dim(payload, lax.rem(c + s, slots) * rows, rows, 0)
        parts = [chunk(0)] + [ring(chunk(s), s) for s in range(1, slots)]
        total = sum_of(parts, name)
        return [total] + [ring(total, s) for s in range(1, slots)]

    def per_device(
        tokens,
        positions,
        expert_ids,
        norm1_gain,
        w_query,
        w_key,
        w_value,
        w_out,
        norm2_gain,
        w_router,
        w_gate,
        w_up,
        w_down,
        grad_output,
    ):
        rows = tokens[0]
        cotangent = grad_output[0]
        block = rows.shape[0]
        width = rows.shape[1]
        experts = w_router.shape[1]
        here = w_gate.shape[0]
        kv_wide = w_key.shape[1]
        q_wide = w_query.shape[1]
        f = lax.axis_index("fsdp")
        c = lax.axis_index("context")
        t = lax.axis_index("tensor")
        f_index = f.reshape(1)
        c_index = c.reshape(1)
        f_here = jnp.stack([f, jnp.int32(here)])

        small = jnp.zeros((PAD, w_router.shape[0]), BF)
        small = small.at[:experts].set(w_router.T)
        small = small.at[PAD - 8].set(norm1_gain).at[PAD - 7].set(norm2_gain)
        small_all = gather(small)
        qkv_w = gather(jnp.concatenate([w_query, w_key, w_value], axis=1))
        half = HEAD // 2
        freq = jnp.exp(-math.log(10000.0) * 2.0 * jnp.arange(half, dtype=F32) / HEAD)
        angle = positions[0].astype(F32)[:, None] * freq[None, :]
        cos, sin = jnp.cos(angle), jnp.sin(angle)
        cos = jnp.concatenate([cos] * 4, axis=1)
        sin = jnp.concatenate([-sin, sin] * 2, axis=1)
        normed_one, heads, kv, table = project(f_index, rows, cos, sin, small_all, qkv_w, kv_wide)

        kv_slots = [kv] + [up(kv, s) for s in range(1, slots)]
        att, lse = attend(c_index, heads, kv_slots)
        att_other = by_tensor(att)
        out_even = across(w_out)
        out_mine = with_partner(out_even)
        out_theirs = with_partner([by_tensor(item) for item in out_even])
        hidden, normed = mix(
            f_index, rows, att, att_other, table, expert_ids[0], out_mine, out_theirs
        )

        cot_near = gather(cotangent)
        normed_near = gather(normed)
        near = own(
            f_index, table, normed_near[:2], cot_near[:2], w_gate, w_up, w_down, experts
        )
        far = own(
            f_index, table, normed_near[2:], cot_near[2:], w_gate, w_up, w_down, experts
        )
        grad_part = reduce_to_owner(list(near[0]) + list(far[0]))
        grad_other = by_tensor(grad_part)
        moe_part = reduce_to_owner(list(near[1]) + list(far[1]))
        moe = moe_part.astype(F32) + by_tensor(moe_part).astype(F32)
        output = (hidden + moe).astype(BF)

        side = block // 2

        def spread_plane(item):
            mine = lax.dynamic_slice_in_dim(item, t * side, side, 0)
            evens = [item]
            for j in range(2, members, 2):
                got = by_fsdp(mine, j)
                evens += [got, by_tensor(got)]
            return with_partner(evens)

        cot_slots, normed_slots = [], []
        cot_now, normed_now = cotangent, normed
        for s in range(1, slots):
            cot_now = ring(cot_now, 1)
            cot_slots.append(spread_plane(cot_now))
            normed_now = ring(normed_now, 1)
            normed_slots.append(spread_plane(normed_now))

        expert_grads = first_weights(
            normed_near, cot_near, (near[3], far[3]), (w_gate, w_up, w_down)
        )
        parts = 2 if here % 2 == 0 else 1
        for s in range(1, slots):
            for p in range(parts):
                count = here // parts
                expert_grads = more_weights(
                    p * count,
                    count,
                    f_here,
                    normed_slots[s - 1],
                    cot_slots[s - 1],
                    w_gate,
                    w_up,
                    w_down,
                    expert_grads,
                    experts,
                )

        grad_hidden, grad_hidden_b, grad_heads, gain_two = middle(
            f_index, hidden, cotangent, grad_part, grad_other, table, out_mine
        )
        back = attend_back(c_index, heads, grad_heads, att, lse, cos, sin, kv_slots)
        received = [down(back[1 + s], s) for s in range(1, slots)]
        joined, part_one, gain_one = lower(
            f_index, back[0], back[1], received, rows, cos, sin, qkv_w
        )
        other_one = by_tensor(part_one)
        grad_tokens = last(rows, grad_hidden, part_one, other_one, table)

        att_near = gather(att)
        grad_cut = exchange(column_pieces(grad_hidden_b, f))
        out_parts = all_reduce(product(att_near, grad_cut, (), 0, "out_grad"), c, "out_sum")
        (grad_out,) = spread(
            c_index, out_parts, ((0, 0),), (w_out.shape,), "out_spread"
        )
        small_grad = near[2] + far[2]
        small_grad = small_grad.at[PAD - 8].set(gain_one[0]).at[PAD - 7].set(0.5 * gain_two[0])
        small_grad = small_grad.astype(BF)
        small_grad = (small_grad.astype(F32) + by_tensor(small_grad).astype(F32)).astype(BF)
        small_cut = exchange(column_pieces(small_grad, f))
        normed_cut = exchange(column_pieces(normed_one, f))
        joined_near = gather(joined)
        payload = product(normed_cut, joined_near, small_cut, 2 * PAD, "qkv_grad")
        qkv_parts = all_reduce(payload, c, "qkv_sum")
        cut = w_query.shape[0]
        grad_query, grad_key, grad_value, small_done = spread(
            c_index,
            qkv_parts,
            ((0, 0), (0, q_wide), (0, q_wide + kv_wide), (cut, 0)),
            (w_query.shape, w_key.shape, w_value.shape, (PAD, cut)),
            "qkv_spread",
        )
        return (
            output[None],
            grad_tokens[None],
            small_done[PAD - 8],
            grad_query,
            grad_key,
            grad_value,
            grad_out,
            small_done[PAD - 7],
            small_done[:experts].T,
            expert_grads[0],
            expert_grads[1],
            expert_grads[2],
        )

    return per_device


def solution(mesh):
    return jax.shard_map(
        build(mesh.shape["fsdp"], mesh.shape["context"]),
        mesh=mesh,
        in_specs=(
            P("fsdp", "context", None),
            P("fsdp", "context"),
            P("fsdp", "context", None),
            P("fsdp"),
            P("fsdp", "tensor"),
            P("fsdp", "tensor"),
            P("fsdp", "tensor"),
            P("tensor", "fsdp"),
            P("fsdp"),
            P("fsdp", None),
            P("fsdp", None, "tensor"),
            P("fsdp", None, "tensor"),
            P("fsdp", "tensor", None),
            P("fsdp", "context", None),
        ),
        out_specs=(
            P("fsdp", "context", None),
            P("fsdp", "context", None),
            P("fsdp"),
            P("fsdp", "tensor"),
            P("fsdp", "tensor"),
            P("fsdp", "tensor"),
            P("tensor", "fsdp"),
            P("fsdp"),
            P("fsdp", None),
            P("fsdp", None, "tensor"),
            P("fsdp", None, "tensor"),
            P("fsdp", "tensor", None),
        ),
        check_vma=False,
    )
```

```python
import functools
import math

import jax
import jax.numpy as jnp
from jax import lax
from jax.experimental import pallas as pl
from jax.experimental.pallas import tpu as pltpu
from jax.sharding import PartitionSpec as P

HEAD = 64
LANES = 128
PAD = 32
norm_eps = 1e-06
masked_score = -1e30
BF = jnp.bfloat16
F32 = jnp.float32
VMEM = pl.BlockSpec(memory_space=pltpu.VMEM)
SMEM = pl.BlockSpec(memory_space=pltpu.SMEM)
ANY = pl.BlockSpec(memory_space=pl.ANY)


def nn(left, right):
    return jnp.dot(left, right, preferred_element_type=F32)


def nt(left, right):
    return lax.dot_general(left, right, (((1,), (1,)), ((), ())), preferred_element_type=F32)


def tn(left, right):
    return lax.dot_general(left, right, (((0,), (0,)), ((), ())), preferred_element_type=F32)


def partner(f):
    return f + 1 - 2 * lax.rem(f, 2)


def member(f, j, members):
    base = lax.rem(f + members - (j - j % 2), members)
    return base if j % 2 == 0 else partner(base)


def shape(dims, kind):
    return jax.ShapeDtypeStruct(dims, kind)


def call(kernel, outs, specs, out_specs, scratch, flops, moved, name, after=(), **more):
    skip = len(after)

    def body(*refs):
        kernel(*refs[skip:])

    run = pl.pallas_call(
        body,
        out_shape=outs,
        in_specs=[ANY] * skip + list(specs),
        out_specs=out_specs,
        scratch_shapes=scratch,
        compiler_params=pltpu.CompilerParams(vmem_limit_bytes=60 << 20),
        name=name,
        cost_estimate=pl.CostEstimate(flops=flops, bytes_accessed=moved, transcendentals=0),
        **more,
    )
    return lambda *operands: run(*after, *operands)


def rotate(rows, cos, sin):
    wide = rows.shape[1]
    count = wide // LANES
    after = pltpu.roll(rows, wide - HEAD // 2, 1)
    before = pltpu.roll(rows, HEAD // 2, 1)
    lane = lax.broadcasted_iota(jnp.int32, rows.shape, 1) % HEAD
    partner = jnp.where(lane < HEAD // 2, after, before)
    cos_all = jnp.concatenate([cos] * count, axis=1)
    sin_all = jnp.concatenate([sin] * count, axis=1)
    return rows * cos_all + partner * sin_all


def project_kernel(members, index, rows_ref, cos_ref, sin_ref, *refs):
    small = refs[:members]
    weights = refs[members : 2 * members]
    normed_ref, heads_ref, kv_ref, table_ref, total = refs[2 * members :]
    f = index[0]
    cut = small[0].shape[1]
    for j in range(members):
        at = pl.ds(pl.multiple_of(member(f, j, members) * cut, LANES), cut)
        table_ref[:, at] = small[j][...]
    rows = rows_ref[...].astype(F32)
    scale = lax.rsqrt(jnp.mean(rows * rows, axis=-1, keepdims=True) + norm_eps)
    gain = table_ref[...].astype(F32)[PAD - 8 : PAD - 7, :]
    normed_ref[...] = (rows * scale * gain).astype(BF)
    acc = None
    for j in range(members):
        at = pl.ds(pl.multiple_of(member(f, j, members) * cut, LANES), cut)
        term = nn(normed_ref[:, at], weights[j][...])
        acc = term if acc is None else acc + term
    total[...] = acc
    kv_wide = kv_ref.shape[1] // 2
    q_wide = total.shape[1] - 2 * kv_wide
    cos = cos_ref[...]
    sin = sin_ref[...]
    turned = rotate(total[:, :q_wide], cos, sin) * (1.0 / math.sqrt(HEAD))
    turned = turned.astype(BF)
    for h in range(q_wide // HEAD):
        heads_ref[h] = turned[:, h * HEAD : (h + 1) * HEAD]
    kv_ref[:, :kv_wide] = rotate(total[:, q_wide : q_wide + kv_wide], cos, sin).astype(BF)
    kv_ref[:, kv_wide:] = total[:, q_wide + kv_wide :].astype(BF)


def project(index, rows, cos, sin, small, weights, kv_wide):
    members = len(weights)
    tokens, width = rows.shape
    wide = weights[0].shape[1]
    heads = (wide - 2 * kv_wide) // HEAD
    return call(
        functools.partial(project_kernel, members),
        (
            shape((tokens, width), BF),
            shape((heads, tokens, HEAD), BF),
            shape((tokens, 2 * kv_wide), BF),
            shape((PAD, width), BF),
        ),
        [SMEM] + [VMEM] * (3 + 2 * members),
        (VMEM,) * 4,
        [pltpu.VMEM((tokens, wide), F32)],
        2 * tokens * width * wide,
        2 * width * wide,
        "project",
    )(index, rows, cos, sin, *small, *weights)


def attend_kernel(slots, groups, index, heads_ref, *refs):
    kv = refs[:slots]
    att_ref, lse_ref, scores, top, total, acc = refs[slots:]
    place = index[0]
    tokens = heads_ref.shape[1]
    repeat = heads_ref.shape[0] // groups
    half = kv[0].shape[1] // 2
    many = repeat * tokens
    keys = lax.broadcasted_iota(jnp.int32, (tokens, many), 0)
    queries = lax.broadcasted_iota(jnp.int32, (tokens, many), 1) % tokens
    allowed = keys <= queries
    for g in range(groups):
        at = slice(g * HEAD, (g + 1) * HEAD)
        q = heads_ref[g * repeat : (g + 1) * repeat].reshape(many, HEAD)
        for s in range(slots):

            @pl.when(place >= s)
            def _():
                score = nt(kv[s][:, at], q)
                if s == 0:
                    score = jnp.where(allowed, score, masked_score)
                scores[s] = score
                high = jnp.max(score, axis=0, keepdims=True)
                top[...] = high if s == 0 else jnp.maximum(top[...], high)

        for s in range(slots):

            @pl.when(place >= s)
            def _():
                weight = jnp.exp(scores[s] - top[...])
                if s == 0:
                    weight = jnp.where(allowed, weight, 0.0)
                part = jnp.sum(weight, axis=0, keepdims=True)
                value = kv[s][:, half + g * HEAD : half + (g + 1) * HEAD]
                value = jnp.concatenate([value, jnp.ones_like(value)], axis=1)
                out = tn(weight.astype(BF), value)
                total[...] = part if s == 0 else total[...] + part
                acc[...] = out if s == 0 else acc[...] + out

        lse_ref[g] = top[...] + jnp.log(total[...])
        done = (acc[:, :HEAD] / acc[:, HEAD:]).astype(BF)
        for r in range(repeat):
            h = g * repeat + r
            att_ref[:, h * HEAD : (h + 1) * HEAD] = done[r * tokens : (r + 1) * tokens]


def attend(index, heads, kv):
    slots = len(kv)
    count, tokens, _ = heads.shape
    groups = kv[0].shape[1] // (2 * HEAD)
    many = count // groups * tokens
    return call(
        functools.partial(attend_kernel, slots, groups),
        (shape((tokens, count * HEAD), BF), shape((groups, 1, many), F32)),
        [SMEM] + [VMEM] * (1 + slots),
        (VMEM, VMEM),
        [
            pltpu.VMEM((slots, tokens, many), F32),
            pltpu.VMEM((1, many), F32),
            pltpu.VMEM((1, many), F32),
            pltpu.VMEM((many, 2 * HEAD), F32),
        ],
        16 * slots * tokens * many * HEAD,
        4 * tokens * count * HEAD,
        "attend",
    )(index, heads, *kv)


def attend_back_kernel(slots, groups, index, heads_ref, grad_ref, att_ref, lse_ref, cos_ref, sin_ref, *refs):
    kv = refs[:slots]
    grad_q_ref = refs[slots]
    grad_kv = refs[slots + 1 : 2 * slots + 1]
    acc, turned = refs[2 * slots + 1 :]
    place = index[0]
    tokens = heads_ref.shape[1]
    repeat = heads_ref.shape[0] // groups
    half = kv[0].shape[1] // 2
    many = repeat * tokens
    keys = lax.broadcasted_iota(jnp.int32, (tokens, many), 0)
    queries = lax.broadcasted_iota(jnp.int32, (tokens, many), 1) % tokens
    allowed = keys <= queries
    lane = lax.broadcasted_iota(jnp.int32, (many, 2 * HEAD), 1)
    for g in range(groups):
        at = slice(g * HEAD, (g + 1) * HEAD)
        behind = slice(half + g * HEAD, half + (g + 1) * HEAD)
        q = heads_ref[g * repeat : (g + 1) * repeat].reshape(many, HEAD)
        grad = grad_ref[g * repeat : (g + 1) * repeat].reshape(many, HEAD)
        out = jnp.concatenate(
            [
                att_ref[:, (g * repeat + r) * HEAD : (g * repeat + r + 1) * HEAD]
                for r in range(repeat)
            ],
            axis=0,
        )
        delta = jnp.sum(grad.astype(F32) * out.astype(F32), axis=-1, keepdims=True)
        upper = delta.astype(BF).astype(F32)
        lower = delta - upper
        wide = jnp.concatenate([grad.astype(F32), jnp.zeros((many, HEAD), F32)], axis=1)
        wide = jnp.where(lane == HEAD, -upper, jnp.where(lane == HEAD + 1, -lower, wide)).astype(BF)
        lse = lse_ref[g]
        for s in range(slots):

            @pl.when(place >= s)
            def _():
                key = kv[s][:, at]
                value = kv[s][:, behind]
                value = jnp.concatenate([value, jnp.ones_like(value)], axis=1)
                prob = jnp.exp(nt(key, q) - lse)
                if s == 0:
                    prob = jnp.where(allowed, prob, 0.0)
                grad_score = (prob * nt(value, wide)).astype(BF)
                kind = grad_kv[s].dtype
                grad_kv[s][:, at] = nn(grad_score, q).astype(kind)
                grad_kv[s][:, behind] = nn(prob.astype(BF), grad).astype(kind)
                part = tn(grad_score, key)
                acc[...] = part if s == 0 else acc[...] + part

        done = acc[...] * (1.0 / math.sqrt(HEAD))
        for r in range(repeat):
            h = g * repeat + r
            turned[:, h * HEAD : (h + 1) * HEAD] = done[r * tokens : (r + 1) * tokens]
    grad_q_ref[...] = rotate(turned[...], cos_ref[...], -sin_ref[...]).astype(BF)


def attend_back(index, heads, grad, att, lse, cos, sin, kv, after=()):
    slots = len(kv)
    count, tokens, _ = heads.shape
    groups = kv[0].shape[1] // (2 * HEAD)
    many = count // groups * tokens
    outs = [shape((tokens, count * HEAD), BF), shape(kv[0].shape, F32)]
    outs += [shape(kv[0].shape, BF)] * (slots - 1)
    return call(
        functools.partial(attend_back_kernel, slots, groups),
        tuple(outs),
        [SMEM] + [VMEM] * (6 + slots),
        (VMEM,) * len(outs),
        [pltpu.VMEM((many, HEAD), F32), pltpu.VMEM((tokens, count * HEAD), F32)],
        40 * slots * tokens * many * HEAD,
        8 * tokens * count * HEAD,
        "attend_back",
        after,
    )(index, heads, grad, att, lse, cos, sin, *kv)


def mix_kernel(members, index, rows_ref, att_ref, other_ref, table_ref, ids_ref, *refs):
    mine = refs[:members]
    theirs = refs[members : 2 * members]
    hidden_ref, normed_ref, first, second = refs[2 * members :]
    f = index[0]
    cut = mine[0].shape[1]
    width = rows_ref.shape[1]
    for j in range(members):
        at = pl.ds(pl.multiple_of(member(f, j, members) * cut, LANES), cut)
        first[:, at] = nn(att_ref[...], mine[j][...])
        second[:, at] = nn(other_ref[...], theirs[j][...])
    hidden = rows_ref[...].astype(F32) + (first[...] + second[...])
    hidden_ref[...] = hidden
    scale = lax.rsqrt(jnp.mean(hidden * hidden, axis=-1, keepdims=True) + norm_eps)
    gain = table_ref[...].astype(F32)[PAD - 7 : PAD - 6, :]
    normed = (hidden * scale * gain).astype(BF)
    normed_ref[:, :width] = normed
    logits = nt(normed, table_ref[...])
    lanes = lax.broadcasted_iota(jnp.int32, logits.shape, 1)
    ids = ids_ref[...]
    mask = ids[:, 0:1] == lanes
    for k in range(1, ids.shape[1]):
        mask = mask | (ids[:, k : k + 1] == lanes)
    logits = jnp.where(mask, logits, masked_score)
    weight = jnp.where(mask, jnp.exp(logits - jnp.max(logits, axis=-1, keepdims=True)), 0.0)
    gates = weight / jnp.sum(weight, axis=-1, keepdims=True)
    upper = gates.astype(BF).astype(F32)
    lower = gates - upper
    blank = jnp.zeros((gates.shape[0], LANES - 2 * PAD), F32)
    normed_ref[:, width:] = jnp.concatenate([upper, lower, blank], axis=1).astype(BF)


def mix(index, rows, att, other, table, ids, mine, theirs, after=()):
    members = len(mine)
    tokens, width = rows.shape
    return call(
        functools.partial(mix_kernel, members),
        (shape((tokens, width), F32), shape((tokens, width + LANES), BF)),
        [SMEM] + [VMEM] * (5 + 2 * members),
        (VMEM, VMEM),
        [pltpu.VMEM((tokens, width), F32)] * 2,
        4 * tokens * width * att.shape[1],
        4 * width * att.shape[1],
        "mix",
        after,
    )(index, rows, att, other, table, ids, *mine, *theirs)


def gates_of(tail, experts):
    rows = tail.astype(F32)
    both = rows + pltpu.roll(rows, LANES - PAD, 1)
    lane = lax.broadcasted_iota(jnp.int32, both.shape, 1)
    return jnp.where(lane < experts, both, 0.0)


def gate_column(gates, expert):
    lane = lax.broadcasted_iota(jnp.int32, gates.shape, 1)
    return jnp.sum(jnp.where(lane == expert, gates, 0.0), axis=-1, keepdims=True)


def hidden_terms(normed, cotangent, gate_col, gate_w, up_w, down_w):
    gate_pre = nn(normed, gate_w)
    up_pre = nn(normed, up_w)
    plain = nt(cotangent, down_w)
    sigma = 1.0 / (1.0 + jnp.exp(-gate_pre))
    activated = gate_pre * sigma
    inner = activated * up_pre
    grad_inner = gate_col * plain
    scaled = (gate_col * inner).astype(BF)
    grad_g = (grad_inner * up_pre * (sigma + activated * (1.0 - sigma))).astype(BF)
    grad_u = (grad_inner * activated).astype(BF)
    return inner, plain, scaled, grad_g, grad_u


class Sender:
    def __init__(self, sems):
        self.sems = sems
        self.used = 0
        self.made = []

    def add(self, source, target, device):
        copy = pltpu.make_async_remote_copy(
            src_ref=source,
            dst_ref=target,
            send_sem=self.sems.at[0, self.used],
            recv_sem=self.sems.at[1, self.used],
            device_id=device,
            device_id_type=pl.DeviceIdType.MESH,
        )
        self.used += 1
        self.made.append(copy)
        return copy


def greet(devices):
    barrier = pltpu.get_barrier_semaphore()
    for device in devices:
        pl.semaphore_signal(
            barrier, inc=1, device_id=device, device_id_type=pl.DeviceIdType.MESH
        )
    pl.semaphore_wait(barrier, len(devices))


def own_kernel(members, slots, experts, table_ref, normed_in, *refs):
    cot_in = refs[:members]
    gate_hbm, up_hbm, down_hbm = refs[members : members + 3]
    (
        far_ref,
        moe_ref,
        mine_ref,
        router_ref,
        grad_gate_ref,
        grad_up_ref,
        grad_down_ref,
        gate_w,
        up_w,
        down_w,
        normed,
        cot,
        all_inner,
        all_g,
        all_u,
        parts,
        swapped,
        joined,
        arrived,
        stage_gate,
        stage_up,
        stage_down,
        gates,
        shares,
        sems,
        weight_sems,
        local_sems,
        stage_sems,
        moe_stage,
        moe_sems,
    ) = refs[members + 3 :]
    f = lax.axis_index("fsdp")
    c = lax.axis_index("context")
    t = lax.axis_index("tensor")
    here = gate_w.shape[0]
    hidden = gate_w.shape[2]
    tokens = normed_in.shape[0]
    side = tokens // 2
    width = cot.shape[2]
    evens = range(2, members, 2)
    beside = {"fsdp": partner(f)}
    opposite = {"tensor": 1 - t}
    ahead = {"context": lax.rem(c + 1, slots)}
    behind = {"context": lax.rem(c + slots - 1, slots)}
    apart = {j: {"fsdp": lax.rem(f + j, members)} for j in evens}
    owner = {j: {"fsdp": lax.rem(f + members - j, members)} for j in evens}

    net = Sender(sems)
    near_core = net.add(normed_in, normed.at[1], beside)
    near_far = {j: net.add(normed_in, normed.at[j], apart[j]) for j in evens}
    near_relay = {j: net.add(normed.at[j], normed.at[j + 1], beside) for j in evens}
    hop, whole, half, cross, relay_half, relay_cross = {}, {}, {}, {}, {}, {}
    lower_half, upper_half = pl.ds(0, side), pl.ds(side, side)
    for s in range(1, slots):
        origin = normed_in if s == 1 else far_ref.at[s - 2, 0]
        now = far_ref.at[s - 1]
        hop[s] = net.add(origin, now.at[0], ahead)
        whole[s] = net.add(now.at[0], now.at[1], beside)
        piece = pl.ds(pl.multiple_of(t * side, side), side)
        for j in evens:
            half[s, j] = net.add(now.at[0, piece], now.at[j, lower_half], apart[j])
            cross[s, j] = net.add(now.at[j, lower_half], now.at[j, upper_half], opposite)
            relay_half[s, j] = net.add(now.at[j, lower_half], now.at[j + 1, lower_half], beside)
            relay_cross[s, j] = net.add(now.at[j, upper_half], now.at[j + 1, upper_half], beside)
    swap = {
        j: net.add(parts.at[j + 1], swapped.at[j // 2], beside) for j in range(0, members, 2)
    }
    home = {j: net.add(joined.at[j // 2], arrived.at[j // 2], owner[j]) for j in evens}

    weight_copies = [
        (
            pltpu.make_async_copy(gate_hbm.at[e], gate_w.at[e], weight_sems.at[0, e]),
            pltpu.make_async_copy(up_hbm.at[e], up_w.at[e], weight_sems.at[1, e]),
            pltpu.make_async_copy(down_hbm.at[e], down_w.at[e], weight_sems.at[2, e]),
        )
        for e in range(here)
    ]
    local = [pltpu.make_async_copy(normed_in, normed.at[0], local_sems.at[0])]
    for j in range(members):
        local.append(pltpu.make_async_copy(cot_in[j], cot.at[j], local_sems.at[1 + j]))
    for copy in local + list(weight_copies[0]):
        copy.start()
    greet([beside, opposite, ahead, behind] + [apart[j] for j in evens])
    near_core.start()
    for j in evens:
        near_far[j].start()
    hop[1].start()
    for e in range(1, here):
        for copy in weight_copies[e]:
            copy.start()
    for copy in local:
        copy.wait()
    near_core.wait_recv()

    def prepare(first, count):
        for b in range(first, first + count):
            at = slice(b * tokens, (b + 1) * tokens)
            gates[at, :] = gates_of(normed[b, :, width:], experts)
            shares[at, :] = jnp.zeros((tokens, LANES), F32)

    def one_tile(b, e):
        step = 2 * tokens
        at = pl.ds(b * tokens, step)
        pair = slice(b, b + 2)
        columns = pl.ds(pl.multiple_of(e * hidden, LANES), hidden)
        inner, plain, scaled, grad_g, grad_u = hidden_terms(
            normed[pair, :, :width].reshape(step, width),
            cot[pair].reshape(step, width),
            gate_column(gates[at, :], f * here + e),
            gate_w[e],
            up_w[e],
            down_w[e],
        )
        all_inner[at, columns] = scaled
        all_g[at, columns] = grad_g
        all_u[at, columns] = grad_u
        share = jnp.sum(inner * plain, axis=-1, keepdims=True)
        lane = lax.broadcasted_iota(jnp.int32, (step, LANES), 1)
        shares[at, :] = jnp.where(lane == f * here + e, share, shares[at, :])

    def hidden_pass(first, count, hooks, fresh):
        def one_expert(e, carry):
            if fresh:
                pltpu.make_async_copy(gate_hbm.at[e], gate_w.at[e], weight_sems.at[0, e]).wait()
                pltpu.make_async_copy(up_hbm.at[e], up_w.at[e], weight_sems.at[1, e]).wait()
                pltpu.make_async_copy(down_hbm.at[e], down_w.at[e], weight_sems.at[2, e]).wait()

            for b in range(first, first + count, 2):
                one_tile(b, e)
            for at, hook in hooks.items():
                pl.when(e == at)(hook)
            return carry

        lax.fori_loop(0, here, one_expert, 0)

    def grad_pass(first, count):
        def one_block(b, carry):
            at = pl.ds(pl.multiple_of(b * tokens, tokens), tokens)
            mean = jnp.sum(gates[at, :] * shares[at, :], axis=-1, keepdims=True)
            logits = (gates[at, :] * (shares[at, :] - mean)).astype(BF)
            added = tn(logits, normed[b, :, :width])[:PAD]
            router_ref[...] += added
            total = nn(logits[:, :PAD], table_ref[...])
            for e in range(here):
                columns = slice(e * hidden, (e + 1) * hidden)
                total = total + nt(all_g[at, columns], gate_w[e])
                total = total + nt(all_u[at, columns], up_w[e])
            parts[b] = total.astype(BF)
            return carry

        lax.fori_loop(first, first + count, one_block, 0)

    def slot_arrived(s):
        hop[s].wait_recv()
        if s + 1 < slots:
            hop[s + 1].start()
        whole[s].start()
        for j in evens:
            half[s, j].start()

    def half_arrived(s):
        for j in evens:
            half[s, j].wait_recv()
            cross[s, j].start()
            relay_half[s, j].start()

    def cross_arrived(s):
        for j in evens:
            cross[s, j].wait_recv()
            relay_cross[s, j].start()

    router_ref[...] = jnp.zeros_like(router_ref)
    prepare(0, 2)
    hidden_pass(0, 2, {}, True)
    for j in evens:
        near_far[j].wait_recv()
        near_relay[j].start()
    slot_arrived(1)
    grad_pass(0, 2)
    swap[0].start()
    for j in evens:
        near_relay[j].wait_recv()
    prepare(2, members - 2)
    rest = list(range(2, slots))
    middle_hook = max(here // 2 - 1, 0)

    def first_hook():
        if slots > 2:
            slot_arrived(2)
        half_arrived(1)

    hidden_pass(2, members - 2, {middle_hook: first_hook}, False)
    cross_arrived(1)
    if slots > 2:
        half_arrived(2)
    grad_pass(2, members - 2)
    for j in evens:
        swap[j].start()
    for j in evens:
        swap[j].wait_recv()
        joined[j // 2] = (parts[j].astype(F32) + swapped[j // 2].astype(F32)).astype(BF)
        home[j].start()
    for s in range(3, slots):
        slot_arrived(s)

    down_all = down_w[...].reshape(here * hidden, width)

    def one_moe(b, carry):
        at = pl.ds(pl.multiple_of(b * tokens, tokens), tokens)
        slot = lax.rem(b, 2)
        copy = pltpu.make_async_copy(moe_stage.at[slot], moe_ref.at[b], moe_sems.at[slot])
        pl.when(b >= 2)(copy.wait)
        moe_stage[slot] = nn(all_inner[at, :], down_all).astype(BF)
        copy.start()
        return carry

    lax.fori_loop(0, members, one_moe, 0)
    for slot in range(2):
        pltpu.make_async_copy(moe_stage.at[slot], moe_ref.at[slot], moe_sems.at[slot]).wait()
    if slots > 2:
        cross_arrived(2)

    buffers = stage_gate.shape[0]

    def stage_copies(e, b):
        return (
            pltpu.make_async_copy(stage_gate.at[b], grad_gate_ref.at[e], stage_sems.at[0, b]),
            pltpu.make_async_copy(stage_up.at[b], grad_up_ref.at[e], stage_sems.at[1, b]),
            pltpu.make_async_copy(stage_down.at[b], grad_down_ref.at[e], stage_sems.at[2, b]),
        )

    def sum_home():
        swap[0].wait_recv()
        total = parts[0].astype(F32) + swapped[0].astype(F32)
        for j in evens:
            home[j].wait_recv()
            total = total + arrived[j // 2].astype(F32)
        mine_ref[...] = total.astype(BF)

    def late_half():
        for s in range(3, slots):
            half_arrived(s)

    def weights_of(e, carry):
        b = lax.rem(e, buffers)

        @pl.when(e >= buffers)
        def _():
            for copy in stage_copies(e, b):
                copy.wait()

        columns = pl.ds(pl.multiple_of(e * hidden, LANES), hidden)
        rows = members * tokens
        left = normed[:, :, :width].reshape(rows, width)
        stage_gate[b] = tn(left, all_g[:, columns])
        stage_up[b] = tn(left, all_u[:, columns])
        stage_down[b] = tn(all_inner[:, columns], cot[...].reshape(rows, width))
        for copy in stage_copies(e, b):
            copy.start()
        pl.when(e == here // 2)(sum_home)
        pl.when(e == here - 2)(late_half)
        return carry

    lax.fori_loop(0, here, weights_of, 0)
    for s in range(3, slots):
        cross_arrived(s)
    for e in range(max(here - buffers, 0), here):
        for copy in stage_copies(e, e % buffers):
            copy.wait()
    for s in range(1, slots):
        whole[s].wait_recv()
        for j in evens:
            relay_half[s, j].wait_recv()
            relay_cross[s, j].wait_recv()
    for copy in net.made:
        copy.wait_send()


def own(table, normed, cotangent, gate_w, up_w, down_w, experts, slots):
    members = len(cotangent)
    tokens, width = cotangent[0].shape
    here, _, hidden = gate_w.shape
    rows = members * tokens
    halves = members // 2
    buffers = 2 if members <= 4 else 1
    copies = 1 + 2 * (halves - 1) + (slots - 1) * (2 + 4 * (halves - 1)) + halves + (halves - 1)
    token_block = (tokens, width)
    return pl.pallas_call(
        functools.partial(own_kernel, members, slots, experts),
        out_shape=(
            shape((slots - 1, members, tokens, width + LANES), BF),
            shape((members, tokens, width), BF),
            shape(token_block, BF),
            shape((PAD, width), F32),
            shape(gate_w.shape, F32),
            shape(up_w.shape, F32),
            shape(down_w.shape, F32),
        ),
        in_specs=[VMEM, ANY] + [ANY] * (members + 3),
        out_specs=(ANY, ANY, VMEM, VMEM, ANY, ANY, ANY),
        scratch_shapes=[
            pltpu.VMEM(gate_w.shape, BF),
            pltpu.VMEM(up_w.shape, BF),
            pltpu.VMEM(down_w.shape, BF),
            pltpu.VMEM((members, tokens, width + LANES), BF),
            pltpu.VMEM((members, tokens, width), BF),
            pltpu.VMEM((rows, here * hidden), BF),
            pltpu.VMEM((rows, here * hidden), BF),
            pltpu.VMEM((rows, here * hidden), BF),
            pltpu.VMEM((members,) + token_block, BF),
            pltpu.VMEM((halves,) + token_block, BF),
            pltpu.VMEM((halves,) + token_block, BF),
            pltpu.VMEM((halves,) + token_block, BF),
            pltpu.VMEM((buffers, width, hidden), F32),
            pltpu.VMEM((buffers, width, hidden), F32),
            pltpu.VMEM((buffers, hidden, width), F32),
            pltpu.VMEM((rows, LANES), F32),
            pltpu.VMEM((rows, LANES), F32),
            pltpu.SemaphoreType.DMA((2, copies)),
            pltpu.SemaphoreType.DMA((3, here)),
            pltpu.SemaphoreType.DMA((1 + members,)),
            pltpu.SemaphoreType.DMA((3, buffers)),
            pltpu.VMEM((2,) + token_block, BF),
            pltpu.SemaphoreType.DMA((2,)),
        ],
        compiler_params=pltpu.CompilerParams(
            vmem_limit_bytes=63 << 20, collective_id=1, has_side_effects=True
        ),
        name="own",
        cost_estimate=pl.CostEstimate(
            flops=18 * rows * width * hidden * here,
            bytes_accessed=18 * here * width * hidden,
            transcendentals=0,
        ),
    )(table, normed, *cotangent, gate_w, up_w, down_w)


def more_weights_kernel(slot, layout, experts, begin, index, normed_in, *refs):
    pieces = len(layout)
    cot_in = refs[:pieces]
    gate_w, up_w, down_w, old_gate, old_up, old_down = refs[pieces : pieces + 6]
    new_gate, new_up, new_down, token, normed, cot, gates, all_inner, all_g, all_u, sems = refs[
        pieces + 6 :
    ]
    members, tokens, width = cot.shape
    rows = members * tokens
    here = index[1]

    @pl.when(pl.program_id(0) == 0)
    def _():
        copies = [pltpu.make_async_copy(normed_in.at[slot], normed, sems.at[0])]
        for p, (block, first, count) in enumerate(layout):
            place = cot.at[block, pl.ds(first, count)]
            copies.append(pltpu.make_async_copy(cot_in[p].at[slot], place, sems.at[1 + p]))
        for copy in copies:
            copy.start()
        for copy in copies:
            copy.wait()
        gates[...] = gates_of(normed[:, :, width:].reshape(rows, LANES), experts)

    expert = index[0] * here + begin + pl.program_id(0)
    step = 2 * tokens
    for b in range(rows // step):
        at = pl.ds(b * step, step)
        pair = slice(2 * b, 2 * b + 2)
        _, _, scaled, grad_g, grad_u = hidden_terms(
            normed[pair, :, :width].reshape(step, width),
            cot[pair].reshape(step, width),
            gate_column(gates[at, :], expert),
            gate_w[0],
            up_w[0],
            down_w[0],
        )
        all_inner[at, :] = scaled
        all_g[at, :] = grad_g
        all_u[at, :] = grad_u
    left = normed[:, :, :width].reshape(rows, width)
    new_gate[0] = old_gate[0] + tn(left, all_g[...])
    new_up[0] = old_up[0] + tn(left, all_u[...])
    new_down[0] = old_down[0] + tn(all_inner[...], cot[...].reshape(rows, width))
    token[...] = jnp.zeros_like(token)


def more_weights(
    slot, begin, count, index, normed, cotangent, layout, weights, earlier, experts, after
):
    pieces = len(layout)
    _, members, tokens, _ = normed.shape
    width = cotangent[0].shape[2]
    rows = members * tokens
    here, _, hidden = weights[0].shape
    pick = lambda e: (e + begin, 0, 0)
    wide = pl.BlockSpec((1, width, hidden), pick)
    tall = pl.BlockSpec((1, hidden, width), pick)
    base = len(after) + pieces + 5
    *grads, token = call(
        functools.partial(more_weights_kernel, slot, layout, experts, begin),
        tuple(shape(item.shape, F32) for item in earlier) + (shape((8, LANES), F32),),
        [SMEM] + [ANY] * (1 + pieces) + [wide, wide, tall] * 2,
        (wide, wide, tall, pl.BlockSpec((8, LANES), lambda e: (0, 0))),
        [
            pltpu.VMEM((members, tokens, width + LANES), BF),
            pltpu.VMEM((members, tokens, width), BF),
            pltpu.VMEM((rows, LANES), F32),
            pltpu.VMEM((rows, hidden), BF),
            pltpu.VMEM((rows, hidden), BF),
            pltpu.VMEM((rows, hidden), BF),
            pltpu.SemaphoreType.DMA((1 + pieces,)),
        ],
        12 * rows * width * hidden * count,
        count * 30 * width * hidden + 4 * rows * width,
        "more_weights",
        after,
        grid=(count,),
        input_output_aliases={base + i: i for i in range(3)} if count < here else {},
    )(index, normed, *cotangent, *weights, *earlier)
    return grads, token


def middle_kernel(members, index, hidden_ref, cot_ref, mine_ref, theirs_ref, table_ref, *refs):
    weights = refs[:members]
    grad_ref, grad_b_ref, heads_ref, gain_ref = refs[members:]
    f = index[0]
    cut = weights[0].shape[1]
    hidden = hidden_ref[...]
    normed_grad = mine_ref[...].astype(F32) + theirs_ref[...].astype(F32)
    scale = lax.rsqrt(jnp.mean(hidden * hidden, axis=-1, keepdims=True) + norm_eps)
    gain = table_ref[...].astype(F32)[PAD - 7 : PAD - 6, :]
    weighted = normed_grad * gain
    cubed = scale * scale * scale
    grad = (
        cot_ref[...].astype(F32)
        + scale * weighted
        - hidden * cubed * jnp.mean(weighted * hidden, axis=-1, keepdims=True)
    )
    gain_ref[...] = jnp.sum(normed_grad * hidden * scale, axis=0, keepdims=True)
    grad_ref[...] = grad
    grad_b_ref[...] = grad.astype(BF)
    total = None
    for j in range(members):
        at = pl.ds(pl.multiple_of(member(f, j, members) * cut, LANES), cut)
        term = nt(grad_b_ref[:, at], weights[j][...])
        total = term if total is None else total + term
    total = total.astype(BF)
    for h in range(heads_ref.shape[0]):
        heads_ref[h] = total[:, h * HEAD : (h + 1) * HEAD]


def middle(index, hidden, cotangent, mine, theirs, table, weights, after=()):
    members = len(weights)
    tokens, width = hidden.shape
    heads = weights[0].shape[0] // HEAD
    return call(
        functools.partial(middle_kernel, members),
        (
            shape((tokens, width), F32),
            shape((tokens, width), BF),
            shape((heads, tokens, HEAD), BF),
            shape((1, width), F32),
        ),
        [SMEM] + [VMEM] * (5 + members),
        (VMEM,) * 4,
        [],
        2 * tokens * width * heads * HEAD,
        16 * tokens * width,
        "middle",
        after,
    )(index, hidden, cotangent, mine, theirs, table, *weights)


def lower_kernel(members, received, index, grad_q_ref, own_ref, rows_ref, cos_ref, sin_ref, *refs):
    others = refs[:received]
    weights = refs[received : received + members]
    joined_ref, part_ref, gain_ref = refs[received + members :]
    f = index[0]
    cut = weights[0].shape[0]
    total = own_ref[...]
    for item in others:
        total = total + item[...].astype(F32)
    half = total.shape[1] // 2
    q_wide = grad_q_ref.shape[1]
    joined_ref[:, :q_wide] = grad_q_ref[...]
    keys = rotate(total[:, :half], cos_ref[...], -sin_ref[...])
    joined_ref[:, q_wide : q_wide + half] = keys.astype(BF)
    joined_ref[:, q_wide + half :] = total[:, half:].astype(BF)
    rows = rows_ref[...].astype(F32)
    scale = lax.rsqrt(jnp.mean(rows * rows, axis=-1, keepdims=True) + norm_eps)
    for j in range(members):
        at = pl.ds(pl.multiple_of(member(f, j, members) * cut, LANES), cut)
        part_ref[:, at] = nt(joined_ref[...], weights[j][...]).astype(BF)
    gain_ref[...] = jnp.sum(part_ref[...].astype(F32) * rows * scale, axis=0, keepdims=True)


def lower(index, grad_q, own_kv, others, rows, cos, sin, weights, after=()):
    members = len(weights)
    tokens, width = rows.shape
    wide = weights[0].shape[1]
    return call(
        functools.partial(lower_kernel, members, len(others)),
        (shape((tokens, wide), BF), shape((tokens, width), BF), shape((1, width), F32)),
        [SMEM] + [VMEM] * (5 + len(others) + members),
        (VMEM,) * 3,
        [],
        2 * tokens * width * wide,
        2 * width * wide,
        "lower",
        after,
    )(index, grad_q, own_kv, rows, cos, sin, *others, *weights)


def last_kernel(rows_ref, grad_ref, mine_ref, theirs_ref, table_ref, out_ref):
    rows = rows_ref[...].astype(F32)
    normed_grad = mine_ref[...].astype(F32) + theirs_ref[...].astype(F32)
    scale = lax.rsqrt(jnp.mean(rows * rows, axis=-1, keepdims=True) + norm_eps)
    gain = table_ref[...].astype(F32)[PAD - 8 : PAD - 7, :]
    weighted = normed_grad * gain
    cubed = scale * scale * scale
    out_ref[...] = (
        grad_ref[...]
        + scale * weighted
        - rows * cubed * jnp.mean(weighted * rows, axis=-1, keepdims=True)
    ).astype(BF)


def last(rows, grad, mine, theirs, table, after=()):
    tokens, width = rows.shape
    return call(
        last_kernel,
        shape((tokens, width), BF),
        [VMEM] * 5,
        VMEM,
        [],
        16 * tokens * width,
        12 * tokens * width,
        "last",
        after,
    )(rows, grad, mine, theirs, table)


def product_kernel(members, extra, *refs):
    left = refs[:members]
    right = refs[members : 2 * members]
    small = refs[2 * members : 2 * members + extra]
    out_ref = refs[-1]
    total = None
    for j in range(members):
        term = tn(left[j][...], right[j][...])
        total = term if total is None else total + term
    rows, columns = total.shape
    out_ref[:rows, :] = total.astype(BF)
    if extra:
        summed = small[0][...].astype(F32)
        for item in small[1:]:
            summed = summed + item[...].astype(F32)
        out_ref[rows:, :] = jnp.zeros((out_ref.shape[0] - rows, columns), BF)
        out_ref[rows : rows + PAD, : summed.shape[1]] = summed.astype(BF)


def product(left, right, small, extra_rows, name, after=()):
    members = len(left)
    rows, columns = left[0].shape[1], right[0].shape[1]
    return call(
        functools.partial(product_kernel, members, len(small)),
        shape((rows + extra_rows, columns), BF),
        [VMEM] * (2 * members + len(small)),
        VMEM,
        [],
        2 * members * left[0].shape[0] * rows * columns,
        4 * rows * columns,
        name,
        after,
    )(*left, *right, *small)


def sum_kernel(*refs):
    total = refs[0][...].astype(F32)
    for item in refs[1:-1]:
        total = total + item[...].astype(F32)
    refs[-1][...] = total.astype(BF)


def sum_of(items, name, after=()):
    size = items[0].shape[0] * items[0].shape[1]
    return call(
        sum_kernel,
        shape(items[0].shape, BF),
        [VMEM] * len(items),
        VMEM,
        [],
        len(items) * size,
        2 * (len(items) + 1) * size,
        name,
        after,
    )(*items)


def spread_kernel(slots, cuts, index, *refs):
    parts = refs[:slots]
    outs = refs[slots:-1]
    whole = refs[-1]
    place = index[0]
    rows = parts[0].shape[0]
    for s in range(slots):
        owner = lax.rem(place + slots - s, slots)
        whole[pl.ds(pl.multiple_of(owner * rows, 16), rows), :] = parts[s][...].astype(F32)
    for out, (row, column) in zip(outs, cuts):
        out[...] = whole[row : row + out.shape[0], column : column + out.shape[1]]


def spread(index, parts, cuts, dims, name, after=()):
    rows, columns = parts[0].shape
    slots = len(parts)
    return call(
        functools.partial(spread_kernel, slots, cuts),
        tuple(shape(item, F32) for item in dims),
        [SMEM] + [VMEM] * slots,
        (VMEM,) * len(dims),
        [pltpu.VMEM((slots * rows, columns), F32)],
        slots * rows * columns,
        6 * slots * rows * columns,
        name,
        after,
    )(index, *parts)


def build(members, slots):
    def source_of(i, j):
        base = (i - (j - j % 2)) % members
        return base if j % 2 == 0 else base ^ 1

    def by_fsdp(item, j):
        return lax.ppermute(item, "fsdp", [(source_of(i, j), i) for i in range(members)])

    def by_tensor(item):
        return lax.ppermute(item, "tensor", [(0, 1), (1, 0)])

    def ring(item, step):
        return lax.ppermute(item, "context", [(i, (i + step) % slots) for i in range(slots)])

    def up(item, step):
        return lax.ppermute(item, "context", [(i, i + step) for i in range(slots - step)])

    def down(item, step):
        return lax.ppermute(item, "context", [(i + step, i) for i in range(slots - step)])

    def across(item):
        return [item] + [by_fsdp(item, j) for j in range(2, members, 2)]

    def with_partner(evens):
        out = []
        for item in evens:
            out += [item, by_fsdp(item, 1)]
        return out

    def gather(item):
        return with_partner(across(item))

    def exchange(pieces):
        return [pieces[0]] + [by_fsdp(pieces[j], j) for j in range(1, members)]

    def column_pieces(item, f):
        cut = item.shape[1] // members

        def target(j):
            start = f if j % 2 == 0 else partner(f)
            return lax.rem(start + j - j % 2, members)

        return [lax.dynamic_slice_in_dim(item, target(j) * cut, cut, 1) for j in range(members)]

    def reduce_to_owner(pieces):
        swapped = [by_fsdp(pieces[j + 1], 1) for j in range(0, members, 2)]
        total = [pieces[0], swapped[0]]
        for j in range(2, members, 2):
            both = (pieces[j].astype(F32) + swapped[j // 2].astype(F32)).astype(BF)
            total.append(by_fsdp(both, members - j))
        acc = total[0].astype(F32)
        for item in total[1:]:
            acc = acc + item.astype(F32)
        return acc.astype(BF)

    def reduce_parts(payload, c):
        rows = payload.shape[0] // slots
        chunk = lambda s: lax.dynamic_slice_in_dim(payload, lax.rem(c + s, slots) * rows, rows, 0)
        return [chunk(0)] + [ring(chunk(s), s) for s in range(1, slots)]

    def share_parts(total):
        return [total] + [ring(total, s) for s in range(1, slots)]

    def per_device(
        tokens,
        positions,
        expert_ids,
        norm1_gain,
        w_query,
        w_key,
        w_value,
        w_out,
        norm2_gain,
        w_router,
        w_gate,
        w_up,
        w_down,
        grad_output,
    ):
        rows = tokens[0]
        cotangent = grad_output[0]
        block = rows.shape[0]
        width = rows.shape[1]
        experts = w_router.shape[1]
        here = w_gate.shape[0]
        kv_wide = w_key.shape[1]
        q_wide = w_query.shape[1]
        f = lax.axis_index("fsdp")
        c = lax.axis_index("context")
        t = lax.axis_index("tensor")
        f_index = f.reshape(1)
        c_index = c.reshape(1)
        f_here = jnp.stack([f, jnp.int32(here)])

        small = jnp.zeros((PAD, w_router.shape[0]), BF)
        small = small.at[:experts].set(w_router.T)
        small = small.at[PAD - 8].set(norm1_gain).at[PAD - 7].set(norm2_gain)
        small_all = gather(small)
        qkv_w = gather(jnp.concatenate([w_query, w_key, w_value], axis=1))
        half = HEAD // 2
        freq = jnp.exp(-math.log(10000.0) * 2.0 * jnp.arange(half, dtype=F32) / HEAD)
        angle = positions[0].astype(F32)[:, None] * freq[None, :]
        cos, sin = jnp.cos(angle), jnp.sin(angle)
        cos = jnp.concatenate([cos] * 4, axis=1)
        sin = jnp.concatenate([-sin, sin] * 2, axis=1)
        normed_one, heads, kv, table = project(f_index, rows, cos, sin, small_all, qkv_w, kv_wide)

        kv_slots = [kv] + [up(kv, s) for s in range(1, slots)]
        att, lse = attend(c_index, heads, kv_slots)
        att_other = by_tensor(att)
        out_even = across(w_out)
        out_mine = with_partner(out_even)
        out_theirs = with_partner([by_tensor(item) for item in out_even])
        hidden, normed = mix(
            f_index, rows, att, att_other, table, expert_ids[0], out_mine, out_theirs
        )

        cot_near = gather(cotangent)
        side = block // 2
        cot_now, cot_slots = cotangent, []
        for s in range(1, slots):
            cot_now = ring(cot_now, 1)
            cot_slots.append(cot_now)
        cot_all = jnp.stack(cot_slots)
        cot_half = lax.dynamic_slice_in_dim(cot_all, t * side, side, 1)
        cot_pieces = [cot_all, by_fsdp(cot_all, 1)]
        layout = [(0, 0, block), (1, 0, block)]
        for j in range(2, members, 2):
            got = by_fsdp(cot_half, j)
            crossed = by_tensor(got)
            cot_pieces += [got, crossed, by_fsdp(got, 1), by_fsdp(crossed, 1)]
            layout += [(j, 0, side), (j, side, side), (j + 1, 0, side), (j + 1, side, side)]

        normed_slots, moe_parts, grad_part, router_grad, *expert_grads = own(
            table, normed, cot_near, w_gate, w_up, w_down, experts, slots
        )
        grad_other = by_tensor(grad_part)
        parts = 2 if here % 2 == 0 else 1
        queue = []
        for s in range(1, slots):
            split = parts if s + 1 < slots else 1
            queue += [(s - 1, p * (here // split), here // split) for p in range(split)]

        def fill(count, after):
            nonlocal expert_grads
            token = after
            for _ in range(count):
                if not queue:
                    break
                slot, begin, many = queue.pop(0)
                expert_grads, token = more_weights(
                    slot,
                    begin,
                    many,
                    f_here,
                    normed_slots,
                    cot_pieces,
                    tuple(layout),
                    (w_gate, w_up, w_down),
                    expert_grads,
                    experts,
                    (token,),
                )
            return token

        token = fill(1, router_grad)

        grad_hidden, grad_hidden_b, grad_heads, gain_two = middle(
            f_index, hidden, cotangent, grad_part, grad_other, table, out_mine, (token,)
        )
        back = attend_back(c_index, heads, grad_heads, att, lse, cos, sin, kv_slots)
        received = [down(back[1 + s], s) for s in range(1, slots)]
        att_near = gather(att)
        grad_cut = exchange(column_pieces(grad_hidden_b, f))
        moe_part = reduce_to_owner([moe_parts[j] for j in range(members)])
        moe = moe_part.astype(F32) + by_tensor(moe_part).astype(F32)
        output = (hidden + moe).astype(BF)

        token = fill(1, back[0])
        out_payload = product(att_near, grad_cut, (), 0, "out_grad", (token,))
        joined, part_one, gain_one = lower(
            f_index, back[0], back[1], received, rows, cos, sin, qkv_w, (token,)
        )
        other_one = by_tensor(part_one)
        small_grad = router_grad
        small_grad = small_grad.at[PAD - 8].set(gain_one[0]).at[PAD - 7].set(0.5 * gain_two[0])
        small_grad = small_grad.astype(BF)
        small_grad = (small_grad.astype(F32) + by_tensor(small_grad).astype(F32)).astype(BF)
        small_cut = exchange(column_pieces(small_grad, f))
        normed_cut = exchange(column_pieces(normed_one, f))
        joined_near = gather(joined)

        token = fill(1, part_one)
        payload = product(normed_cut, joined_near, small_cut, 2 * PAD, "qkv_grad", (token,))
        out_parts = reduce_parts(out_payload, c)
        out_total = sum_of(out_parts, "out_sum", (token,))
        out_parts = share_parts(out_total)
        qkv_parts = reduce_parts(payload, c)
        grad_tokens = last(rows, grad_hidden, part_one, other_one, table, (token,))

        token = fill(1, payload)
        qkv_total = sum_of(qkv_parts, "qkv_sum", (token,))
        qkv_parts = share_parts(qkv_total)
        (grad_out,) = spread(
            c_index, out_parts, ((0, 0),), (w_out.shape,), "out_spread", (token,)
        )
        token = fill(len(queue), qkv_total)
        cut = w_query.shape[0]
        grad_query, grad_key, grad_value, small_done = spread(
            c_index,
            qkv_parts,
            ((0, 0), (0, q_wide), (0, q_wide + kv_wide), (cut, 0)),
            (w_query.shape, w_key.shape, w_value.shape, (PAD, cut)),
            "qkv_spread",
            (token,),
        )
        return (
            output[None],
            grad_tokens[None],
            small_done[PAD - 8],
            grad_query,
            grad_key,
            grad_value,
            grad_out,
            small_done[PAD - 7],
            small_done[:experts].T,
            expert_grads[0],
            expert_grads[1],
            expert_grads[2],
        )

    return per_device


def solution(mesh):
    return jax.shard_map(
        build(mesh.shape["fsdp"], mesh.shape["context"]),
        mesh=mesh,
        in_specs=(
            P("fsdp", "context", None),
            P("fsdp", "context"),
            P("fsdp", "context", None),
            P("fsdp"),
            P("fsdp", "tensor"),
            P("fsdp", "tensor"),
            P("fsdp", "tensor"),
            P("tensor", "fsdp"),
            P("fsdp"),
            P("fsdp", None),
            P("fsdp", None, "tensor"),
            P("fsdp", None, "tensor"),
            P("fsdp", "tensor", None),
            P("fsdp", "context", None),
        ),
        out_specs=(
            P("fsdp", "context", None),
            P("fsdp", "context", None),
            P("fsdp"),
            P("fsdp", "tensor"),
            P("fsdp", "tensor"),
            P("fsdp", "tensor"),
            P("tensor", "fsdp"),
            P("fsdp"),
            P("fsdp", None),
            P("fsdp", None, "tensor"),
            P("fsdp", None, "tensor"),
            P("fsdp", "tensor", None),
        ),
        check_vma=False,
    )
```

```python
import functools
import math

import jax
import jax.numpy as jnp
from jax import lax
from jax.experimental import pallas as pl
from jax.experimental.pallas import tpu as pltpu
from jax.sharding import PartitionSpec as P

HEAD = 64
LANES = 128
PAD = 32
norm_eps = 1e-06
masked_score = -1e30
BF = jnp.bfloat16
F32 = jnp.float32
VMEM = pl.BlockSpec(memory_space=pltpu.VMEM)
SMEM = pl.BlockSpec(memory_space=pltpu.SMEM)
ANY = pl.BlockSpec(memory_space=pl.ANY)


def nn(left, right):
    return jnp.dot(left, right, preferred_element_type=F32)


def nt(left, right):
    return lax.dot_general(left, right, (((1,), (1,)), ((), ())), preferred_element_type=F32)


def tn(left, right):
    return lax.dot_general(left, right, (((0,), (0,)), ((), ())), preferred_element_type=F32)


def partner(f):
    return f + 1 - 2 * lax.rem(f, 2)


def member(f, j, members):
    base = lax.rem(f + members - (j - j % 2), members)
    return base if j % 2 == 0 else partner(base)


def columns_of(ref, owner, cut):
    if cut % LANES == 0:
        return ref[:, pl.ds(pl.multiple_of(owner * cut, LANES), cut)]
    pair = ref[:, pl.ds(pl.multiple_of(lax.div(owner, 2) * (2 * cut), LANES), 2 * cut)]
    return jnp.where(lax.rem(owner, 2) == 0, pair[:, :cut], pair[:, cut:])


def put_columns(ref, owner, first, second):
    cut = first.shape[1]
    if cut % LANES == 0:
        ref[:, pl.ds(pl.multiple_of(owner * cut, LANES), cut)] = first
        ref[:, pl.ds(pl.multiple_of(partner(owner) * cut, LANES), cut)] = second
    else:
        even = lax.rem(owner, 2) == 0
        both = [jnp.where(even, first, second), jnp.where(even, second, first)]
        at = pl.ds(pl.multiple_of(lax.div(owner, 2) * (2 * cut), LANES), 2 * cut)
        ref[:, at] = jnp.concatenate(both, axis=1)


def shape(dims, kind):
    return jax.ShapeDtypeStruct(dims, kind)


def call(kernel, outs, specs, out_specs, scratch, flops, moved, name, after=(), **more):
    skip = len(after)

    def body(*refs):
        kernel(*refs[skip:])

    run = pl.pallas_call(
        body,
        out_shape=outs,
        in_specs=[ANY] * skip + list(specs),
        out_specs=out_specs,
        scratch_shapes=scratch,
        compiler_params=pltpu.CompilerParams(vmem_limit_bytes=60 << 20),
        name=name,
        cost_estimate=pl.CostEstimate(flops=flops, bytes_accessed=moved, transcendentals=0),
        **more,
    )
    return lambda *operands: run(*after, *operands)


def rotate(rows, cos, sin):
    wide = rows.shape[1]
    count = wide // LANES
    after = pltpu.roll(rows, wide - HEAD // 2, 1)
    before = pltpu.roll(rows, HEAD // 2, 1)
    lane = lax.broadcasted_iota(jnp.int32, rows.shape, 1) % HEAD
    partner = jnp.where(lane < HEAD // 2, after, before)
    cos_all = jnp.concatenate([cos] * count, axis=1)
    sin_all = jnp.concatenate([sin] * count, axis=1)
    return rows * cos_all + partner * sin_all


class Sender:
    def __init__(self, sems):
        self.sems = sems
        self.used = 0
        self.made = []

    def add(self, source, target, device):
        copy = pltpu.make_async_remote_copy(
            src_ref=source,
            dst_ref=target,
            send_sem=self.sems.at[0, self.used],
            recv_sem=self.sems.at[1, self.used],
            device_id=device,
            device_id_type=pl.DeviceIdType.MESH,
        )
        self.used += 1
        self.made.append(copy)
        return copy


def greet(devices):
    barrier = pltpu.get_barrier_semaphore()
    for device in devices:
        pl.semaphore_signal(
            barrier, inc=1, device_id=device, device_id_type=pl.DeviceIdType.MESH
        )
    pl.semaphore_wait(barrier, len(devices))


def target(f, j, members):
    start = f if j % 2 == 0 else partner(f)
    return lax.rem(start + j - j % 2, members)


def attend_slot(s, diagonal, heads_ref, kv, top, sums, acc):
    groups = top.shape[0]
    tokens = heads_ref.shape[1]
    repeat = heads_ref.shape[0] // groups
    half = kv.shape[2] // 2
    many = repeat * tokens
    if diagonal:
        keys = lax.broadcasted_iota(jnp.int32, (tokens, many), 0)
        queries = lax.broadcasted_iota(jnp.int32, (tokens, many), 1) % tokens
        allowed = keys <= queries
    for g in range(groups):
        q = heads_ref[g * repeat : (g + 1) * repeat].reshape(many, HEAD)
        score = nt(kv[s, :, g * HEAD : (g + 1) * HEAD], q)
        value = kv[s, :, half + g * HEAD : half + (g + 1) * HEAD]
        if diagonal:
            score = jnp.where(allowed, score, masked_score)
            high = jnp.max(score, axis=0, keepdims=True)
            weight = jnp.where(allowed, jnp.exp(score - high), 0.0)
            sums[g] = jnp.sum(weight, axis=0, keepdims=True)
            acc[g] = tn(value, weight.astype(BF))
        else:
            old = top[g]
            high = jnp.maximum(old, jnp.max(score, axis=0, keepdims=True))
            shrink = jnp.exp(old - high)
            weight = jnp.exp(score - high)
            sums[g] = sums[g] * shrink + jnp.sum(weight, axis=0, keepdims=True)
            acc[g] = acc[g] * shrink + tn(value, weight.astype(BF))
        top[g] = high


def attend_end(att_ref, lse_ref, top, sums, acc):
    groups, _, many = top.shape
    tokens = att_ref.shape[0]
    repeat = many // tokens
    for g in range(groups):
        lse_ref[g] = top[g] + jnp.log(sums[g])
        done = jnp.transpose(acc[g] / sums[g]).astype(BF)
        for r in range(repeat):
            h = g * repeat + r
            att_ref[:, h * HEAD : (h + 1) * HEAD] = done[r * tokens : (r + 1) * tokens]


def forward_kernel(members, slots, small_in, qkv_in, wout_in, rows_ref, cos_ref, sin_ref, ids_ref, cot_in, *refs):
    (
        table_ref,
        normed_one_ref,
        heads_ref,
        kv_out,
        att_ref,
        lse_ref,
        hidden_ref,
        normed_ref,
        qkv_out,
        wout_out,
        cot_near,
        cot_done,
        cot_hops,
        att_near,
        cut_near,
        small,
        qkv,
        mine,
        theirs,
        kv,
        total,
        first,
        second,
        other,
        top,
        sums,
        acc,
        stage,
        sems,
        local_sems,
    ) = refs
    f = lax.axis_index("fsdp")
    c = lax.axis_index("context")
    t = lax.axis_index("tensor")
    tokens, width = rows_ref.shape
    side = tokens // 2
    cut = small_in.shape[1]
    evens = range(2, members, 2)
    beside = {"fsdp": partner(f)}
    opposite = {"tensor": 1 - t}
    ahead = {"context": lax.rem(c + 1, slots)}
    apart = {j: {"fsdp": lax.rem(f + j, members)} for j in evens}
    lower_half, upper_half = pl.ds(0, side), pl.ds(side, side)
    piece = pl.ds(pl.multiple_of(t * side, side), side)

    net = Sender(sems)
    small_sent = [
        net.add(small_in, small.at[j], {"fsdp": target(f, j, members)}) for j in range(1, members)
    ]

    def family(source, place):
        return (
            net.add(source, place.at[1], beside),
            {j: net.add(source, place.at[j], apart[j]) for j in evens},
            {j: net.add(place.at[j], place.at[j + 1], beside) for j in evens},
        )

    qkv_core, qkv_far, qkv_relay = family(qkv_in, qkv)
    out_core, out_far, out_relay = family(wout_in, mine)
    out_cross = {j: net.add(wout_in if j == 0 else mine.at[j], theirs.at[j], opposite) for j in range(0, members, 2)}
    out_cross_relay = {j: net.add(theirs.at[j], theirs.at[j + 1], beside) for j in range(0, members, 2)}
    cot_core, cot_far, cot_relay = family(cot_in, cot_near)
    done = cot_done.shape[0]
    hop, whole, half, cross, relay_half, relay_cross = {}, {}, {}, {}, {}, {}
    place = lambda s: cot_done.at[s - 1, 0] if s <= done else cot_hops.at[s - done - 1]
    for s in range(1, slots):
        hop[s] = net.add(cot_in if s == 1 else place(s - 1), place(s), ahead)
    for s in range(1, done + 1):
        now = cot_done.at[s - 1]
        whole[s] = net.add(now.at[0], now.at[1], beside)
        for j in evens:
            half[s, j] = net.add(now.at[0, piece], now.at[j, lower_half], apart[j])
            cross[s, j] = net.add(now.at[j, lower_half], now.at[j, upper_half], opposite)
            relay_half[s, j] = net.add(now.at[j, lower_half], now.at[j + 1, lower_half], beside)
            relay_cross[s, j] = net.add(now.at[j, upper_half], now.at[j + 1, upper_half], beside)
    att_core, att_far, att_relay = family(att_ref, att_near)
    cuts = []
    for j in range(1, members):
        cuts.append(net.add(stage.at[j], cut_near.at[j], {"fsdp": target(f, j, members)}))
    plain = len(net.made)
    later = {
        s: net.add(kv.at[0], kv.at[s], {"context": lax.rem(c + s, slots)}) for s in range(1, slots)
    }
    plain_made = net.made[:plain]
    att_sent = net.add(att_ref, other, opposite)

    locals_in = [
        pltpu.make_async_copy(small_in, small.at[0], local_sems.at[0]),
        pltpu.make_async_copy(qkv_in, qkv.at[0], local_sems.at[1]),
        pltpu.make_async_copy(wout_in, mine.at[0], local_sems.at[2]),
    ]
    qkv_saved = pltpu.make_async_copy(qkv, qkv_out, local_sems.at[3])
    out_saved = pltpu.make_async_copy(mine, wout_out, local_sems.at[4])
    cut_saved = pltpu.make_async_copy(stage.at[0], cut_near.at[0], local_sems.at[5 + slots])
    kv_saved = [
        pltpu.make_async_copy(kv.at[s], kv_out.at[s], local_sems.at[5 + s]) for s in range(slots)
    ]
    for copy in locals_in:
        copy.start()
    greet(
        [{"fsdp": target(f, j, members)} for j in range(1, members)]
        + [opposite]
        + [{"context": lax.rem(c + s, slots)} for s in range(1, slots)]
    )
    for copy in small_sent:
        copy.start()
    for copy in [qkv_core] + [qkv_far[j] for j in evens]:
        copy.start()
    for copy in [out_core, out_cross[0]] + [out_far[j] for j in evens]:
        copy.start()
    hop[1].start()
    cot_core.start()

    rows = rows_ref[...].astype(F32)
    scale = lax.rsqrt(jnp.mean(rows * rows, axis=-1, keepdims=True) + norm_eps)
    hidden_ref[...] = rows * scale
    for copy in locals_in:
        copy.wait()
    for copy in small_sent:
        copy.wait_recv()

    def columns(j):
        return columns_of(normed_one_ref, member(f, j, members), cut)

    for j in range(0, members, 2):
        put_columns(table_ref, member(f, j, members), small[j], small[j + 1])
    gain = table_ref[...].astype(F32)[PAD - 8 : PAD - 7, :]
    normed_one_ref[...] = (hidden_ref[...] * gain).astype(BF)
    total[...] = nn(columns(0), qkv[0])
    qkv_core.wait_recv()
    total[...] += nn(columns(1), qkv[1])

    def slot_arrived(s):
        hop[s].wait_recv()
        if s + 1 < slots:
            hop[s + 1].start()
        if s <= done:
            whole[s].start()
            for j in evens:
                half[s, j].start()

    slot_arrived(1)
    for j in range(members):
        stage[j] = columns_of(normed_one_ref, target(f, j, members), cut)
    cut_saved.start()
    for copy in cuts:
        copy.start()
    for j in evens:
        qkv_far[j].wait_recv()
        qkv_relay[j].start()
        total[...] += nn(columns(j), qkv[j])
    for j in evens:
        qkv_relay[j].wait_recv()
        total[...] += nn(columns(j + 1), qkv[j + 1])
    qkv_saved.start()
    kv_wide = kv.shape[2] // 2
    q_wide = total.shape[1] - 2 * kv_wide
    cos = cos_ref[...]
    sin = sin_ref[...]
    kv[0, :, :kv_wide] = rotate(total[:, q_wide : q_wide + kv_wide], cos, sin).astype(BF)
    kv[0, :, kv_wide:] = total[:, q_wide + kv_wide :].astype(BF)
    for s in range(1, slots):
        pl.when(c + s < slots)(later[s].start)
    turned = (rotate(total[:, :q_wide], cos, sin) * (1.0 / math.sqrt(HEAD))).astype(BF)
    for h in range(q_wide // HEAD):
        heads_ref[h] = turned[:, h * HEAD : (h + 1) * HEAD]
    attend_slot(0, True, heads_ref, kv, top, sums, acc)
    for j in evens:
        out_far[j].wait_recv()
        out_relay[j].start()
        out_cross[j].start()
    out_cross[0].wait_recv()
    out_cross_relay[0].start()

    def half_arrived(s):
        for j in evens:
            half[s, j].wait_recv()
            relay_half[s, j].start()
            cross[s, j].start()

    def keys_arrived(s):
        later[s].wait_recv()
        attend_slot(s, False, heads_ref, kv, top, sums, acc)

    for s in range(1, slots):
        pl.when(c >= s)(functools.partial(keys_arrived, s))
        if s == 1:
            half_arrived(1)
    if slots > 2:
        slot_arrived(2)
    for j in evens:
        cot_far[j].start()
    kv_saved[0].start()
    for s in range(1, slots):
        pl.when(c >= s)(kv_saved[s].start)
    attend_end(att_ref, lse_ref, top, sums, acc)
    att_sent.start()
    att_core.start()
    for j in evens:
        att_far[j].start()

    out_core.wait_recv()
    for j in evens:
        out_relay[j].wait_recv()
    out_saved.start()
    for j in range(0, members, 2):
        pair = nn(att_ref[...], mine[j]), nn(att_ref[...], mine[j + 1])
        put_columns(first, member(f, j, members), *pair)
    for j in evens:
        out_cross[j].wait_recv()
        out_cross_relay[j].start()
    for j in evens:
        cross[1, j].wait_recv()
        relay_cross[1, j].start()
    if done > 1:
        half_arrived(2)
    for j in range(0, members, 2):
        out_cross_relay[j].wait_recv()
    att_sent.wait_recv()
    for j in range(0, members, 2):
        pair = nn(other[...], theirs[j]), nn(other[...], theirs[j + 1])
        put_columns(second, member(f, j, members), *pair)

    hidden = rows_ref[...].astype(F32) + (first[...] + second[...])
    hidden_ref[...] = hidden
    scale = lax.rsqrt(jnp.mean(hidden * hidden, axis=-1, keepdims=True) + norm_eps)
    gain = table_ref[...].astype(F32)[PAD - 7 : PAD - 6, :]
    normed = (hidden * scale * gain).astype(BF)
    normed_ref[:, :width] = normed
    logits = nt(normed, table_ref[...])
    lanes = lax.broadcasted_iota(jnp.int32, logits.shape, 1)
    ids = ids_ref[...]
    mask = ids[:, 0:1] == lanes
    for k in range(1, ids.shape[1]):
        mask = mask | (ids[:, k : k + 1] == lanes)
    logits = jnp.where(mask, logits, masked_score)
    weight = jnp.where(mask, jnp.exp(logits - jnp.max(logits, axis=-1, keepdims=True)), 0.0)
    gates = weight / jnp.sum(weight, axis=-1, keepdims=True)
    upper = gates.astype(BF).astype(F32)
    lower = gates - upper
    blank = jnp.zeros((gates.shape[0], LANES - 2 * PAD), F32)
    normed_ref[:, width:] = jnp.concatenate([upper, lower, blank], axis=1).astype(BF)

    for j in evens:
        cot_far[j].wait_recv()
        cot_relay[j].start()
    for s in range(2, done + 1):
        for j in evens:
            cross[s, j].wait_recv()
            relay_cross[s, j].start()
    for s in range(3, slots):
        slot_arrived(s)
    for j in evens:
        att_far[j].wait_recv()
        att_relay[j].start()
    cot_core.wait_recv()
    att_core.wait_recv()
    for copy in cuts:
        copy.wait_recv()
    for j in evens:
        cot_relay[j].wait_recv()
        att_relay[j].wait_recv()
    for s in range(1, done + 1):
        whole[s].wait_recv()
        for j in evens:
            relay_half[s, j].wait_recv()
            relay_cross[s, j].wait_recv()
    qkv_saved.wait()
    out_saved.wait()
    cut_saved.wait()
    kv_saved[0].wait()
    for s in range(1, slots):
        pl.when(c >= s)(kv_saved[s].wait)
    for copy in plain_made:
        copy.wait_send()
    for s in range(1, slots):
        pl.when(c + s < slots)(later[s].wait_send)
    att_sent.wait_send()


def forward(small, qkv, wout, rows, cos, sin, ids, cotangent, kv_wide, members, slots):
    tokens, width = rows.shape
    wide = qkv.shape[1]
    q_wide = wide - 2 * kv_wide
    heads = q_wide // HEAD
    groups = kv_wide // HEAD
    many = heads // groups * tokens
    halves = members // 2
    far = halves - 1
    done = min(2, slots - 1)
    copies = 2 * (members - 1) + 4 * (1 + 2 * far) + 2 * halves + 2 * (slots - 1) + 1 + done * (1 + 4 * far)
    return pl.pallas_call(
        functools.partial(forward_kernel, members, slots),
        out_shape=(
            shape((PAD, width), BF),
            shape((tokens, width), BF),
            shape((heads, tokens, HEAD), BF),
            shape((slots, tokens, 2 * kv_wide), BF),
            shape((tokens, q_wide), BF),
            shape((groups, 1, many), F32),
            shape((tokens, width), F32),
            shape((tokens, width + LANES), BF),
            shape((members,) + qkv.shape, BF),
            shape((members,) + wout.shape, BF),
            shape((members, tokens, width), BF),
            shape((done, members, tokens, width), BF),
            shape((max(slots - 1 - done, 1), tokens, width), BF),
            shape((members, tokens, q_wide), BF),
            shape((members, tokens, width // members), BF),
        ),
        in_specs=[ANY] * 3 + [VMEM] * 4 + [ANY],
        out_specs=(VMEM, VMEM, VMEM, ANY, VMEM, VMEM, VMEM, VMEM) + (ANY,) * 7,
        scratch_shapes=[
            pltpu.VMEM((members,) + small.shape, BF),
            pltpu.VMEM((members,) + qkv.shape, BF),
            pltpu.VMEM((members,) + wout.shape, BF),
            pltpu.VMEM((members,) + wout.shape, BF),
            pltpu.VMEM((slots, tokens, 2 * kv_wide), BF),
            pltpu.VMEM((tokens, wide), F32),
            pltpu.VMEM((tokens, width), F32),
            pltpu.VMEM((tokens, width), F32),
            pltpu.VMEM((tokens, q_wide), BF),
            pltpu.VMEM((groups, 1, many), F32),
            pltpu.VMEM((groups, 1, many), F32),
            pltpu.VMEM((groups, HEAD, many), F32),
            pltpu.VMEM((members, tokens, width // members), BF),
            pltpu.SemaphoreType.DMA((2, copies)),
            pltpu.SemaphoreType.DMA((6 + slots,)),
        ],
        compiler_params=pltpu.CompilerParams(
            vmem_limit_bytes=60 << 20, collective_id=0, has_side_effects=True
        ),
        name="forward",
        cost_estimate=pl.CostEstimate(
            flops=8 * tokens * width * wide, bytes_accessed=8 * width * wide, transcendentals=0
        ),
    )(small, qkv, wout, rows, cos, sin, ids, cotangent)


def attend_back_kernel(slots, groups, index, heads_ref, grad_ref, att_ref, lse_ref, cos_ref, sin_ref, kv_ref, *refs):
    kv = [kv_ref.at[s] for s in range(slots)]
    grad_q_ref = refs[0]
    grad_kv = refs[1 : slots + 1]
    acc, turned = refs[slots + 1 :]
    place = index[0]
    tokens = heads_ref.shape[1]
    repeat = heads_ref.shape[0] // groups
    half = kv[0].shape[1] // 2
    many = repeat * tokens
    keys = lax.broadcasted_iota(jnp.int32, (tokens, many), 0)
    queries = lax.broadcasted_iota(jnp.int32, (tokens, many), 1) % tokens
    allowed = keys <= queries
    lane = lax.broadcasted_iota(jnp.int32, (many, 2 * HEAD), 1)
    for g in range(groups):
        at = slice(g * HEAD, (g + 1) * HEAD)
        behind = slice(half + g * HEAD, half + (g + 1) * HEAD)
        q = heads_ref[g * repeat : (g + 1) * repeat].reshape(many, HEAD)
        grad = grad_ref[g * repeat : (g + 1) * repeat].reshape(many, HEAD)
        out = jnp.concatenate(
            [
                att_ref[:, (g * repeat + r) * HEAD : (g * repeat + r + 1) * HEAD]
                for r in range(repeat)
            ],
            axis=0,
        )
        delta = jnp.sum(grad.astype(F32) * out.astype(F32), axis=-1, keepdims=True)
        upper = delta.astype(BF).astype(F32)
        lower = delta - upper
        wide = jnp.concatenate([grad.astype(F32), jnp.zeros((many, HEAD), F32)], axis=1)
        wide = jnp.where(lane == HEAD, -upper, jnp.where(lane == HEAD + 1, -lower, wide)).astype(BF)
        lse = lse_ref[g]
        for s in range(slots):

            @pl.when(place >= s)
            def _():
                key = kv[s][:, at]
                value = kv[s][:, behind]
                value = jnp.concatenate([value, jnp.ones_like(value)], axis=1)
                prob = jnp.exp(nt(key, q) - lse)
                if s == 0:
                    prob = jnp.where(allowed, prob, 0.0)
                grad_score = (prob * nt(value, wide)).astype(BF)
                kind = grad_kv[s].dtype
                grad_kv[s][:, at] = nn(grad_score, q).astype(kind)
                grad_kv[s][:, behind] = nn(prob.astype(BF), grad).astype(kind)
                part = tn(grad_score, key)
                acc[...] = part if s == 0 else acc[...] + part

        done = acc[...] * (1.0 / math.sqrt(HEAD))
        for r in range(repeat):
            h = g * repeat + r
            turned[:, h * HEAD : (h + 1) * HEAD] = done[r * tokens : (r + 1) * tokens]
    grad_q_ref[...] = rotate(turned[...], cos_ref[...], -sin_ref[...]).astype(BF)


def attend_back(index, heads, grad, att, lse, cos, sin, kv, after=()):
    slots = kv.shape[0]
    count, tokens, _ = heads.shape
    groups = kv.shape[2] // (2 * HEAD)
    many = count // groups * tokens
    outs = [shape((tokens, count * HEAD), BF), shape(kv.shape[1:], F32)]
    outs += [shape(kv.shape[1:], BF)] * (slots - 1)
    return call(
        functools.partial(attend_back_kernel, slots, groups),
        tuple(outs),
        [SMEM] + [VMEM] * 7,
        (VMEM,) * len(outs),
        [pltpu.VMEM((many, HEAD), F32), pltpu.VMEM((tokens, count * HEAD), F32)],
        40 * slots * tokens * many * HEAD,
        8 * tokens * count * HEAD,
        "attend_back",
        after,
    )(index, heads, grad, att, lse, cos, sin, kv)


def gates_of(tail, experts):
    rows = tail.astype(F32)
    both = rows + pltpu.roll(rows, LANES - PAD, 1)
    lane = lax.broadcasted_iota(jnp.int32, both.shape, 1)
    return jnp.where(lane < experts, both, 0.0)


def gate_column(gates, expert):
    lane = lax.broadcasted_iota(jnp.int32, gates.shape, 1)
    return jnp.sum(jnp.where(lane == expert, gates, 0.0), axis=-1, keepdims=True)


def hidden_terms(normed, cotangent, gate_col, gate_w, up_w, down_w):
    gate_pre = nn(normed, gate_w)
    up_pre = nn(normed, up_w)
    plain = nt(cotangent, down_w)
    sigma = 1.0 / (1.0 + jnp.exp(-gate_pre))
    activated = gate_pre * sigma
    inner = activated * up_pre
    grad_inner = gate_col * plain
    scaled = (gate_col * inner).astype(BF)
    grad_g = (grad_inner * up_pre * (sigma + activated * (1.0 - sigma))).astype(BF)
    grad_u = (grad_inner * activated).astype(BF)
    return inner, plain, scaled, grad_g, grad_u


def own_kernel(members, slots, experts, table_ref, normed_in, cot_own, cot_near, cot_hops, *refs):
    cot_in = [cot_own] + [cot_near.at[j] for j in range(1, members)]
    gate_hbm, up_hbm, down_hbm = refs[:3]
    (
        far_ref,
        last_ref,
        cot_far,
        moe_ref,
        mine_ref,
        router_ref,
        grad_gate_ref,
        grad_up_ref,
        grad_down_ref,
        gate_w,
        up_w,
        down_w,
        normed,
        cot,
        all_inner,
        all_g,
        all_u,
        parts,
        swapped,
        joined,
        arrived,
        stage_gate,
        stage_up,
        stage_down,
        gates,
        shares,
        sems,
        weight_sems,
        local_sems,
        stage_sems,
        moe_stage,
        moe_sems,
    ) = refs[3:]
    f = lax.axis_index("fsdp")
    c = lax.axis_index("context")
    t = lax.axis_index("tensor")
    here = gate_w.shape[0]
    hidden = gate_w.shape[2]
    tokens = normed_in.shape[0]
    side = tokens // 2
    width = cot.shape[2]
    evens = range(2, members, 2)
    beside = {"fsdp": partner(f)}
    opposite = {"tensor": 1 - t}
    ahead = {"context": lax.rem(c + 1, slots)}
    behind = {"context": lax.rem(c + slots - 1, slots)}
    apart = {j: {"fsdp": lax.rem(f + j, members)} for j in evens}
    owner = {j: {"fsdp": lax.rem(f + members - j, members)} for j in evens}

    net = Sender(sems)
    near_core = net.add(normed_in, normed.at[1], beside)
    near_far = {j: net.add(normed_in, normed.at[j], apart[j]) for j in evens}
    near_relay = {j: net.add(normed.at[j], normed.at[j + 1], beside) for j in evens}
    hop, whole, half, cross, relay_half, relay_cross = {}, {}, {}, {}, {}, {}
    lower_half, upper_half = pl.ds(0, side), pl.ds(side, side)
    piece = pl.ds(pl.multiple_of(t * side, side), side)
    whole_slots = range(1, slots - 1)
    for s in range(1, slots):
        origin = normed_in if s == 1 else far_ref.at[s - 2, 0]
        hop[s] = net.add(origin, far_ref.at[s - 1, 0] if s < slots - 1 else last_ref, ahead)
    for s in whole_slots:
        now = far_ref.at[s - 1]
        whole[s] = net.add(now.at[0], now.at[1], beside)
        for j in evens:
            half[s, j] = net.add(now.at[0, piece], now.at[j, lower_half], apart[j])
            cross[s, j] = net.add(now.at[j, lower_half], now.at[j, upper_half], opposite)
            relay_half[s, j] = net.add(now.at[j, lower_half], now.at[j + 1, lower_half], beside)
            relay_cross[s, j] = net.add(now.at[j, upper_half], now.at[j + 1, upper_half], beside)
    count = cot_hops.shape[0] if slots > 3 else 0
    later = range(slots - count, slots)
    late_whole, late_half, late_cross, late_relay_half, late_relay_cross = {}, {}, {}, {}, {}
    for s in later:
        origin = cot_hops.at[s - slots + count]
        now = cot_far.at[s - slots + count]
        late_whole[s] = net.add(origin, now.at[0], beside)
        for j in evens:
            late_half[s, j] = net.add(origin.at[piece], now.at[j - 1, lower_half], apart[j])
            late_cross[s, j] = net.add(now.at[j - 1, lower_half], now.at[j - 1, upper_half], opposite)
            late_relay_half[s, j] = net.add(now.at[j - 1, lower_half], now.at[j, lower_half], beside)
            late_relay_cross[s, j] = net.add(now.at[j - 1, upper_half], now.at[j, upper_half], beside)
    swap = {
        j: net.add(parts.at[j + 1], swapped.at[j // 2], beside) for j in range(0, members, 2)
    }
    home = {j: net.add(joined.at[j // 2], arrived.at[j // 2], owner[j]) for j in evens}

    weight_copies = [
        (
            pltpu.make_async_copy(gate_hbm.at[e], gate_w.at[e], weight_sems.at[0, e]),
            pltpu.make_async_copy(up_hbm.at[e], up_w.at[e], weight_sems.at[1, e]),
            pltpu.make_async_copy(down_hbm.at[e], down_w.at[e], weight_sems.at[2, e]),
        )
        for e in range(here)
    ]
    local = [pltpu.make_async_copy(normed_in, normed.at[0], local_sems.at[0])]
    for j in range(members):
        local.append(pltpu.make_async_copy(cot_in[j], cot.at[j], local_sems.at[1 + j]))
    for copy in local + list(weight_copies[0]):
        copy.start()
    greet([beside, opposite, ahead, behind] + [apart[j] for j in evens])
    near_core.start()
    for j in evens:
        near_far[j].start()
    hop[1].start()
    for s in later:
        late_whole[s].start()
        for j in evens:
            late_half[s, j].start()
    for e in range(1, here):
        for copy in weight_copies[e]:
            copy.start()
    for copy in local:
        copy.wait()
    near_core.wait_recv()

    def prepare(first, count):
        for b in range(first, first + count):
            at = slice(b * tokens, (b + 1) * tokens)
            gates[at, :] = gates_of(normed[b, :, width:], experts)
            shares[at, :] = jnp.zeros((tokens, LANES), F32)

    def one_tile(b, e):
        step = 2 * tokens
        at = pl.ds(b * tokens, step)
        pair = slice(b, b + 2)
        columns = pl.ds(pl.multiple_of(e * hidden, LANES), hidden)
        inner, plain, scaled, grad_g, grad_u = hidden_terms(
            normed[pair, :, :width].reshape(step, width),
            cot[pair].reshape(step, width),
            gate_column(gates[at, :], f * here + e),
            gate_w[e],
            up_w[e],
            down_w[e],
        )
        all_inner[at, columns] = scaled
        all_g[at, columns] = grad_g
        all_u[at, columns] = grad_u
        share = jnp.sum(inner * plain, axis=-1, keepdims=True)
        lane = lax.broadcasted_iota(jnp.int32, (step, LANES), 1)
        shares[at, :] = jnp.where(lane == f * here + e, share, shares[at, :])

    def hidden_pass(first, count, hooks, fresh):
        def one_expert(e, carry):
            if fresh:
                pltpu.make_async_copy(gate_hbm.at[e], gate_w.at[e], weight_sems.at[0, e]).wait()
                pltpu.make_async_copy(up_hbm.at[e], up_w.at[e], weight_sems.at[1, e]).wait()
                pltpu.make_async_copy(down_hbm.at[e], down_w.at[e], weight_sems.at[2, e]).wait()

            for b in range(first, first + count, 2):
                one_tile(b, e)
            for at, hook in hooks.items():
                pl.when(e == at)(hook)
            return carry

        lax.fori_loop(0, here, one_expert, 0)

    def grad_pass(first, count):
        def one_block(b, carry):
            at = pl.ds(pl.multiple_of(b * tokens, tokens), tokens)
            mean = jnp.sum(gates[at, :] * shares[at, :], axis=-1, keepdims=True)
            logits = (gates[at, :] * (shares[at, :] - mean)).astype(BF)
            added = tn(logits, normed[b, :, :width])[:PAD]
            router_ref[...] += added
            total = nn(logits[:, :PAD], table_ref[...])
            for e in range(here):
                columns = slice(e * hidden, (e + 1) * hidden)
                total = total + nt(all_g[at, columns], gate_w[e])
                total = total + nt(all_u[at, columns], up_w[e])
            parts[b] = total.astype(BF)
            return carry

        lax.fori_loop(first, first + count, one_block, 0)

    def slot_arrived(s):
        hop[s].wait_recv()
        if s + 1 < slots:
            hop[s + 1].start()
        if s in whole_slots:
            whole[s].start()
            for j in evens:
                half[s, j].start()

    def half_arrived(s):
        if s in whole_slots:
            for j in evens:
                half[s, j].wait_recv()
                cross[s, j].start()
                relay_half[s, j].start()

    def cross_arrived(s):
        if s in whole_slots:
            for j in evens:
                cross[s, j].wait_recv()
                relay_cross[s, j].start()

    down_all = lambda: down_w[...].reshape(here * hidden, width)

    def moe_pass(first, count):
        def one_moe(b, carry):
            at = pl.ds(pl.multiple_of(b * tokens, tokens), tokens)
            slot = lax.rem(b, 2)
            copy = pltpu.make_async_copy(moe_stage.at[slot], moe_ref.at[b], moe_sems.at[slot])
            pl.when(b >= 2)(copy.wait)
            moe_stage[slot] = nn(all_inner[at, :], down_all()).astype(BF)
            copy.start()
            return carry

        lax.fori_loop(first, first + count, one_moe, 0)

    router_ref[...] = jnp.zeros_like(router_ref)
    prepare(0, 2)
    hidden_pass(0, 2, {}, True)
    grad_pass(0, 2)
    swap[0].start()
    for j in evens:
        near_far[j].wait_recv()
        near_relay[j].start()
    slot_arrived(1)
    moe_pass(0, 2)
    for j in evens:
        near_relay[j].wait_recv()
    prepare(2, members - 2)
    hidden_pass(2, members - 2, {}, False)
    half_arrived(1)
    for s in later:
        for j in evens:
            late_half[s, j].wait_recv()
            late_cross[s, j].start()
            late_relay_half[s, j].start()
    grad_pass(2, members - 2)
    for j in evens:
        swap[j].start()
    if slots > 2:
        slot_arrived(2)
    for j in evens:
        swap[j].wait_recv()
        joined[j // 2] = (parts[j].astype(F32) + swapped[j // 2].astype(F32)).astype(BF)
        home[j].start()
    cross_arrived(1)
    moe_pass(2, members - 2)
    for slot in range(2):
        pltpu.make_async_copy(moe_stage.at[slot], moe_ref.at[slot], moe_sems.at[slot]).wait()
    half_arrived(2)
    for s in later:
        for j in evens:
            late_cross[s, j].wait_recv()
            late_relay_cross[s, j].start()

    buffers = stage_gate.shape[0]

    def stage_copies(e, b):
        return (
            pltpu.make_async_copy(stage_gate.at[b], grad_gate_ref.at[e], stage_sems.at[0, b]),
            pltpu.make_async_copy(stage_up.at[b], grad_up_ref.at[e], stage_sems.at[1, b]),
            pltpu.make_async_copy(stage_down.at[b], grad_down_ref.at[e], stage_sems.at[2, b]),
        )

    def sum_home():
        swap[0].wait_recv()
        total = parts[0].astype(F32) + swapped[0].astype(F32)
        for j in evens:
            home[j].wait_recv()
            total = total + arrived[j // 2].astype(F32)
        mine_ref[...] = total.astype(BF)

    def middle_slots():
        cross_arrived(2)
        for s in range(3, slots):
            slot_arrived(s)
            half_arrived(s)
            cross_arrived(s)

    def weights_of(e, carry):
        b = lax.rem(e, buffers)

        @pl.when(e >= buffers)
        def _():
            for copy in stage_copies(e, b):
                copy.wait()

        columns = pl.ds(pl.multiple_of(e * hidden, LANES), hidden)
        rows = members * tokens
        left = normed[:, :, :width].reshape(rows, width)
        stage_gate[b] = tn(left, all_g[:, columns])
        stage_up[b] = tn(left, all_u[:, columns])
        stage_down[b] = tn(all_inner[:, columns], cot[...].reshape(rows, width))
        for copy in stage_copies(e, b):
            copy.start()
        pl.when(e == here // 2)(middle_slots)
        pl.when(e == here - 1)(sum_home)
        return carry

    lax.fori_loop(0, here, weights_of, 0)
    for e in range(max(here - buffers, 0), here):
        for copy in stage_copies(e, e % buffers):
            copy.wait()
    for s in whole_slots:
        whole[s].wait_recv()
        for j in evens:
            relay_half[s, j].wait_recv()
            relay_cross[s, j].wait_recv()
    for s in later:
        late_whole[s].wait_recv()
        for j in evens:
            late_relay_half[s, j].wait_recv()
            late_relay_cross[s, j].wait_recv()
    for copy in net.made:
        copy.wait_send()


def own(table, normed, cotangent, cot_near, cot_hops, gate_w, up_w, down_w, experts, slots):
    members = cot_near.shape[0]
    tokens, width = cotangent.shape
    here, _, hidden = gate_w.shape
    rows = members * tokens
    halves = members // 2
    buffers = 2 if members <= 4 else 1
    far = halves - 1
    late = cot_hops.shape[0]
    copies = 1 + 2 * far + (slots - 1) * (2 + 4 * far) + late * (1 + 4 * far) + halves + far
    token_block = (tokens, width)
    return pl.pallas_call(
        functools.partial(own_kernel, members, slots, experts),
        out_shape=(
            shape((slots - 2, members, tokens, width + LANES), BF),
            shape((tokens, width + LANES), BF),
            shape((late, members - 1, tokens, width), BF),
            shape((members, tokens, width), BF),
            shape(token_block, BF),
            shape((PAD, width), F32),
            shape(gate_w.shape, F32),
            shape(up_w.shape, F32),
            shape(down_w.shape, F32),
        ),
        in_specs=[VMEM] + [ANY] * 7,
        out_specs=(ANY, ANY, ANY, ANY, VMEM, VMEM, ANY, ANY, ANY),
        scratch_shapes=[
            pltpu.VMEM(gate_w.shape, BF),
            pltpu.VMEM(up_w.shape, BF),
            pltpu.VMEM(down_w.shape, BF),
            pltpu.VMEM((members, tokens, width + LANES), BF),
            pltpu.VMEM((members, tokens, width), BF),
            pltpu.VMEM((rows, here * hidden), BF),
            pltpu.VMEM((rows, here * hidden), BF),
            pltpu.VMEM((rows, here * hidden), BF),
            pltpu.VMEM((members,) + token_block, BF),
            pltpu.VMEM((halves,) + token_block, BF),
            pltpu.VMEM((halves,) + token_block, BF),
            pltpu.VMEM((halves,) + token_block, BF),
            pltpu.VMEM((buffers, width, hidden), F32),
            pltpu.VMEM((buffers, width, hidden), F32),
            pltpu.VMEM((buffers, hidden, width), F32),
            pltpu.VMEM((rows, LANES), F32),
            pltpu.VMEM((rows, LANES), F32),
            pltpu.SemaphoreType.DMA((2, copies)),
            pltpu.SemaphoreType.DMA((3, here)),
            pltpu.SemaphoreType.DMA((1 + members,)),
            pltpu.SemaphoreType.DMA((3, buffers)),
            pltpu.VMEM((2,) + token_block, BF),
            pltpu.SemaphoreType.DMA((2,)),
        ],
        compiler_params=pltpu.CompilerParams(
            vmem_limit_bytes=63 << 20, collective_id=1, has_side_effects=True
        ),
        name="own",
        cost_estimate=pl.CostEstimate(
            flops=18 * rows * width * hidden * here,
            bytes_accessed=18 * here * width * hidden,
            transcendentals=0,
        ),
    )(table, normed, cotangent, cot_near, cot_hops, gate_w, up_w, down_w)


class Plan:
    def __init__(self, number, ins, outs, scratch, copies, build):
        self.number = number
        self.ins = ins
        self.outs = outs
        self.scratch = scratch
        self.copies = copies
        self.build = build


def more_weights_kernel(sources, counts, plan, experts, begin, index, *refs):
    in_normed, in_cot = counts
    refs = list(refs)

    def take(number):
        front = refs[:number]
        del refs[:number]
        return front

    normed_in = take(in_normed)
    cot_in = take(in_cot)
    gate_w, up_w, down_w, old_gate, old_up, old_down = take(6)
    plan_in = take(len(plan.ins))
    new_gate, new_up, new_down = take(3)
    plan_out = take(len(plan.outs))
    normed, cot, gates, all_inner, all_g, all_u, sems, remote_sems = take(8)
    plan_scratch = refs
    members, tokens, width = cot.shape
    rows = members * tokens
    here = index[1]
    step_at = pl.program_id(0)
    net = Sender(remote_sems)
    devices, begin_plan, ready, after, finish = plan.build(net, plan_in, plan_out, plan_scratch)
    last = pl.num_programs(0) - 1

    @pl.when(step_at == 0)
    def _():
        copies = []
        for group, refs_in, whole in ((0, normed_in, normed), (1, cot_in, cot)):
            for number, lead, first, count in sources[group]:
                ref = refs_in[number]
                ref = ref if lead is None else ref.at[lead]
                place = whole.at[first] if count == 1 else whole.at[pl.ds(first, count)]
                copies.append(pltpu.make_async_copy(ref, place, sems.at[len(copies)]))
        for copy in copies:
            copy.start()
        if devices:
            greet(devices)
        begin_plan()
        for copy in copies:
            copy.wait()
        gates[...] = gates_of(normed[:, :, width:].reshape(rows, LANES), experts)
        ready()

    expert = index[0] * here + begin + step_at
    step = 2 * tokens
    for b in range(rows // step):
        at = pl.ds(b * step, step)
        pair = slice(2 * b, 2 * b + 2)
        _, _, scaled, grad_g, grad_u = hidden_terms(
            normed[pair, :, :width].reshape(step, width),
            cot[pair].reshape(step, width),
            gate_column(gates[at, :], expert),
            gate_w[0],
            up_w[0],
            down_w[0],
        )
        all_inner[at, :] = scaled
        all_g[at, :] = grad_g
        all_u[at, :] = grad_u
    left = normed[:, :, :width].reshape(rows, width)
    new_gate[0] = old_gate[0] + tn(left, all_g[...])
    new_up[0] = old_up[0] + tn(left, all_u[...])
    new_down[0] = old_down[0] + tn(all_inner[...], cot[...].reshape(rows, width))
    for number, hook in enumerate(after):
        pl.when(step_at == jnp.minimum(number, last))(hook)
    pl.when(step_at == last)(finish)


def more_weights(begin, count, index, normed, cotangent, sources, weights, earlier, experts, plan):
    here, width, hidden = weights[0].shape
    tokens = cotangent[0].shape[-2]
    members = max(first + many for _, _, first, many in sources[1])
    rows = members * tokens
    pick = lambda e: (e + begin, 0, 0)
    wide = pl.BlockSpec((1, width, hidden), pick)
    tall = pl.BlockSpec((1, hidden, width), pick)
    base = 1 + len(normed) + len(cotangent) + 3
    results = pl.pallas_call(
        functools.partial(
            more_weights_kernel,
            sources,
            (len(normed), len(cotangent)),
            plan,
            experts,
            begin,
        ),
        out_shape=tuple(shape(item.shape, F32) for item in earlier)
        + tuple(item for item, _ in plan.outs),
        grid=(count,),
        in_specs=[SMEM]
        + [ANY] * (len(normed) + len(cotangent))
        + [wide, wide, tall] * 2
        + [spec for _, spec in plan.ins],
        out_specs=(wide, wide, tall) + tuple(spec for _, spec in plan.outs),
        scratch_shapes=[
            pltpu.VMEM((members, tokens, width + LANES), BF),
            pltpu.VMEM((members, tokens, width), BF),
            pltpu.VMEM((rows, LANES), F32),
            pltpu.VMEM((rows, hidden), BF),
            pltpu.VMEM((rows, hidden), BF),
            pltpu.VMEM((rows, hidden), BF),
            pltpu.SemaphoreType.DMA((4,)),
            pltpu.SemaphoreType.DMA((2, plan.copies)),
        ]
        + list(plan.scratch),
        input_output_aliases={base + i: i for i in range(3)} if count < here else {},
        compiler_params=pltpu.CompilerParams(
            vmem_limit_bytes=63 << 20,
            collective_id=plan.number,
            has_side_effects=plan.number is not None,
        ),
        name="weights_" + str(plan.number),
        cost_estimate=pl.CostEstimate(
            flops=12 * rows * width * hidden * count,
            bytes_accessed=count * 30 * width * hidden + 4 * rows * width,
            transcendentals=0,
        ),
    )(index, *normed, *cotangent, *weights, *earlier, *[item for item, _ in plan.ins])
    return results[:3], results[3:]


def places(members, slots):
    f = lax.axis_index("fsdp")
    c = lax.axis_index("context")
    t = lax.axis_index("tensor")
    fsdp = {j: {"fsdp": target(f, j, members)} for j in range(1, members)}
    return f, c, t, fsdp, {"tensor": 1 - t}


def nothing():
    pass


def home_plan(number, members, slots, grad_part, moe_parts):
    tokens, width = grad_part.shape
    halves = members // 2
    evens = range(2, members, 2)

    def build(net, ins, outs, scratch):
        part, moe_in = ins
        other, moe_mine = outs
        own_part, swapped, joined, arrived, local = scratch
        f, c, t, fsdp, opposite = places(members, slots)
        cross_part = net.add(part, other, opposite)
        swap = [net.add(moe_in.at[2 * i + 1], swapped.at[i], fsdp[1]) for i in range(halves)]
        home = {
            j: net.add(
                joined.at[j // 2], arrived.at[j // 2], {"fsdp": lax.rem(f + members - j, members)}
            )
            for j in evens
        }
        loads = [
            pltpu.make_async_copy(moe_in.at[2 * i], own_part.at[i], local.at[i])
            for i in range(halves)
        ]

        def start():
            for copy in [cross_part] + swap[1:] + swap[:1] + loads:
                copy.start()

        def ready():
            for copy in loads:
                copy.wait()
            for j in evens:
                swap[j // 2].wait_recv()
                joined[j // 2] = (
                    own_part[j // 2].astype(F32) + swapped[j // 2].astype(F32)
                ).astype(BF)
                home[j].start()

        def finish():
            swap[0].wait_recv()
            total = own_part[0].astype(F32) + swapped[0].astype(F32)
            for j in evens:
                home[j].wait_recv()
                total = total + arrived[j // 2].astype(F32)
            moe_mine[...] = total.astype(BF)
            cross_part.wait_recv()
            for copy in net.made:
                copy.wait_send()

        devices = [fsdp[1], opposite] + [fsdp[j] for j in evens]
        return devices, start, ready, [], finish

    block = (halves, tokens, width)
    return Plan(
        number,
        [(grad_part, ANY), (moe_parts, ANY)],
        [(shape((tokens, width), BF), ANY), (shape((tokens, width), BF), VMEM)],
        [pltpu.VMEM(block, BF)] * 4 + [pltpu.SemaphoreType.DMA((halves,))],
        1 + halves + halves - 1,
        build,
    )


def keys_plan(number, members, slots, grad_kv, grad_b, normed_last):
    _, tokens, cut = grad_b.shape
    wide = normed_last.shape[1]
    side = tokens // 2
    evens = range(2, members, 2)

    def build(net, ins, outs, scratch):
        kv_in = ins[: slots - 1]
        grad_in, last_in = ins[slots - 1 :]
        received, grad_near, spread_out = outs
        f, c, t, fsdp, opposite = places(members, slots)
        piece = pl.ds(pl.multiple_of(t * side, side), side)
        lower_half, upper_half = pl.ds(0, side), pl.ds(side, side)
        back = [
            net.add(kv_in[s - 1], received.at[s - 1], {"context": lax.rem(c + slots - s, slots)})
            for s in range(1, slots)
        ]
        plain = len(net.made)
        cuts = []
        for j in range(1, members):
            cuts.append(net.add(grad_in.at[j], grad_near.at[j], fsdp[j]))
        whole = net.add(last_in, spread_out.at[0], fsdp[1])
        half, cross, relay, relay_cross = {}, {}, {}, {}
        for j in evens:
            low, high = spread_out.at[j - 1, lower_half], spread_out.at[j - 1, upper_half]
            half[j] = net.add(last_in.at[piece], low, fsdp[j])
            cross[j] = net.add(low, high, opposite)
            relay[j] = net.add(low, spread_out.at[j, lower_half], fsdp[1])
            relay_cross[j] = net.add(high, spread_out.at[j, upper_half], fsdp[1])

        def start():
            for s in range(1, slots):
                pl.when(c >= s)(back[s - 1].start)
            for copy in [half[j] for j in evens] + cuts + [whole]:
                copy.start()

        def first():
            for j in evens:
                half[j].wait_recv()
                cross[j].start()
                relay[j].start()

        def finish():
            for j in evens:
                cross[j].wait_recv()
                relay_cross[j].start()
            for s in range(1, slots):
                pl.when(c + s < slots)(back[s - 1].wait_recv)
                pl.when(c >= s)(back[s - 1].wait_send)
            for copy in cuts + [whole]:
                copy.wait_recv()
            for j in evens:
                relay[j].wait_recv()
                relay_cross[j].wait_recv()
            for copy in net.made[plain:]:
                copy.wait_send()

        devices = list(fsdp.values()) + [opposite]
        devices += [{"context": lax.rem(c + s, slots)} for s in range(1, slots)]
        return devices, start, nothing, [nothing, first], finish

    far = members // 2 - 1
    return Plan(
        number,
        [(item, ANY) for item in grad_kv] + [(grad_b, ANY), (normed_last, ANY)],
        [
            (shape((slots - 1,) + grad_kv[0].shape, BF), ANY),
            (shape((members, tokens, cut), BF), ANY),
            (shape((members - 1, tokens, wide), BF), ANY),
        ],
        [],
        (slots - 1) + (members - 1) + 1 + 4 * far,
        build,
    )


def rows_plan(number, members, slots, part_one, joined, router, gain_one, gain_two, payload):
    tokens, width = part_one.shape
    cut = width // members
    evens = range(2, members, 2)
    rows = payload.shape[0] // slots

    def build(net, ins, outs, scratch):
        part_in, joined_in, router_ref, one_ref, two_ref, payload_in = ins
        other, joined_near, small_near, chunks = outs
        small_mine, small_other, small_sum, small_got, small_cut = scratch
        f, c, t, fsdp, opposite = places(members, slots)
        part_sent = net.add(part_in, other, opposite)
        small_sent = net.add(small_mine, small_other, opposite)
        core = net.add(joined_in, joined_near.at[1], fsdp[1])
        far_copy = {j: net.add(joined_in, joined_near.at[j], fsdp[j]) for j in evens}
        relay = {j: net.add(joined_near.at[j], joined_near.at[j + 1], fsdp[1]) for j in evens}
        small_cuts = []
        for j in range(1, members):
            small_cuts.append(net.add(small_cut.at[j], small_got.at[j], fsdp[j]))
        shares = []
        for s in range(1, slots):
            owner = lax.rem(c + s, slots)
            at = pl.ds(pl.multiple_of(owner * rows, 16), rows)
            shares.append(net.add(payload_in.at[at], chunks.at[s], {"context": owner}))

        def start():
            small = router_ref[...]
            row = lax.broadcasted_iota(jnp.int32, small.shape, 0)
            small = jnp.where(row == PAD - 8, one_ref[...], small)
            small = jnp.where(row == PAD - 7, 0.5 * two_ref[...], small)
            small_mine[...] = small.astype(BF)
            small_sent.start()
            for copy in [part_sent, core] + [far_copy[j] for j in evens] + shares:
                copy.start()

        def ready():
            small_sent.wait_recv()
            small_sum[...] = (small_mine[...].astype(F32) + small_other[...].astype(F32)).astype(BF)
            small_got[0] = columns_of(small_sum, f, cut)
            for j in range(1, members):
                small_cut[j] = columns_of(small_sum, target(f, j, members), cut)
            for copy in small_cuts:
                copy.start()

        def second():
            for j in evens:
                far_copy[j].wait_recv()
                relay[j].start()

        def finish():
            for copy in [part_sent, core] + [relay[j] for j in evens] + small_cuts + shares:
                copy.wait_recv()
            small_near[...] = small_got[...]
            for copy in net.made:
                copy.wait_send()

        devices = list(fsdp.values()) + [opposite]
        devices += [{"context": lax.rem(c + s, slots)} for s in range(1, slots)]
        return devices, start, ready, [nothing, second], finish

    far = members // 2 - 1
    small = (PAD, width)
    return Plan(
        number,
        [(part_one, ANY), (joined, ANY)]
        + [(router, VMEM), (gain_one, VMEM), (gain_two, VMEM), (payload, ANY)],
        [
            (shape((tokens, width), BF), ANY),
            (shape((members,) + joined.shape, BF), ANY),
            (shape((members, PAD, cut), BF), VMEM),
            (shape((slots, rows, payload.shape[1]), BF), ANY),
        ],
        [pltpu.VMEM(small, BF)] * 3 + [pltpu.VMEM((members, PAD, cut), BF)] * 2,
        2 + 1 + 2 * far + (members - 1) + (slots - 1),
        build,
    )


def chunk_plan(number, members, slots, payload, moe_mine):
    rows = payload.shape[0] // slots

    def build(net, ins, outs, scratch):
        f, c, t, fsdp, opposite = places(members, slots)
        copies = [net.add(ins[1], outs[1], opposite)]
        for s in range(1, slots):
            owner = lax.rem(c + s, slots)
            at = pl.ds(pl.multiple_of(owner * rows, 16), rows)
            copies.append(net.add(ins[0].at[at], outs[0].at[s], {"context": owner}))

        def start():
            for copy in copies:
                copy.start()

        def finish():
            for copy in copies:
                copy.wait_recv()
                copy.wait_send()

        devices = [{"context": lax.rem(c + s, slots)} for s in range(1, slots)]
        return devices + [opposite], start, nothing, [], finish

    return Plan(
        number,
        [(payload, ANY), (moe_mine, ANY)],
        [
            (shape((slots, rows, payload.shape[1]), BF), ANY),
            (shape(moe_mine.shape, BF), ANY),
        ],
        [],
        slots,
        build,
    )


def middle_kernel(members, index, hidden_ref, cot_ref, mine_ref, theirs_ref, table_ref, weights_ref, *refs):
    weights = [weights_ref.at[j] for j in range(members)]
    grad_ref, grad_b_ref, heads_ref, gain_ref, rounded = refs
    f = index[0]
    cut = weights[0].shape[1]
    hidden = hidden_ref[...]
    normed_grad = mine_ref[...].astype(F32) + theirs_ref[...].astype(F32)
    scale = lax.rsqrt(jnp.mean(hidden * hidden, axis=-1, keepdims=True) + norm_eps)
    gain = table_ref[...].astype(F32)[PAD - 7 : PAD - 6, :]
    weighted = normed_grad * gain
    cubed = scale * scale * scale
    grad = (
        cot_ref[...].astype(F32)
        + scale * weighted
        - hidden * cubed * jnp.mean(weighted * hidden, axis=-1, keepdims=True)
    )
    gain_ref[...] = jnp.sum(normed_grad * hidden * scale, axis=0, keepdims=True)
    grad_ref[...] = grad
    rounded[...] = grad.astype(BF)
    total = None
    for j in range(members):
        grad_b_ref[j] = columns_of(rounded, target(f, j, members), cut)
        term = nt(columns_of(rounded, member(f, j, members), cut), weights[j][...])
        total = term if total is None else total + term
    total = total.astype(BF)
    for h in range(heads_ref.shape[0]):
        heads_ref[h] = total[:, h * HEAD : (h + 1) * HEAD]


def middle(index, hidden, cotangent, mine, theirs, table, weights, after=()):
    members = weights.shape[0]
    tokens, width = hidden.shape
    heads = weights[0].shape[0] // HEAD
    return call(
        functools.partial(middle_kernel, members),
        (
            shape((tokens, width), F32),
            shape((members, tokens, width // members), BF),
            shape((heads, tokens, HEAD), BF),
            shape((1, width), F32),
        ),
        [SMEM] + [VMEM] * 6,
        (VMEM,) * 4,
        [pltpu.VMEM((tokens, width), BF)],
        2 * tokens * width * heads * HEAD,
        16 * tokens * width,
        "middle",
        after,
    )(index, hidden, cotangent, mine, theirs, table, weights)


def lower_kernel(members, slots, index, grad_q_ref, own_ref, rows_ref, cos_ref, sin_ref, *refs):
    others = refs[0]
    weights = [refs[1].at[j] for j in range(members)]
    joined_ref, part_ref, gain_ref = refs[2:]
    f = index[0]
    cut = weights[0].shape[0]
    total = own_ref[...]
    for s in range(1, slots):
        total = total + jnp.where(index[1] + s < slots, others[s - 1].astype(F32), 0.0)
    half = total.shape[1] // 2
    q_wide = grad_q_ref.shape[1]
    joined_ref[:, :q_wide] = grad_q_ref[...]
    keys = rotate(total[:, :half], cos_ref[...], -sin_ref[...])
    joined_ref[:, q_wide : q_wide + half] = keys.astype(BF)
    joined_ref[:, q_wide + half :] = total[:, half:].astype(BF)
    rows = rows_ref[...].astype(F32)
    scale = lax.rsqrt(jnp.mean(rows * rows, axis=-1, keepdims=True) + norm_eps)
    for j in range(0, members, 2):
        first = nt(joined_ref[...], weights[j][...]).astype(BF)
        second = nt(joined_ref[...], weights[j + 1][...]).astype(BF)
        put_columns(part_ref, member(f, j, members), first, second)
    gain_ref[...] = jnp.sum(part_ref[...].astype(F32) * rows * scale, axis=0, keepdims=True)


def lower(index, grad_q, own_kv, others, rows, cos, sin, weights, after=()):
    members = len(weights)
    tokens, width = rows.shape
    wide = weights[0].shape[1]
    return call(
        functools.partial(lower_kernel, members, others.shape[0] + 1),
        (shape((tokens, wide), BF), shape((tokens, width), BF), shape((1, width), F32)),
        [SMEM] + [VMEM] * 7,
        (VMEM,) * 3,
        [],
        2 * tokens * width * wide,
        2 * width * wide,
        "lower",
        after,
    )(index, grad_q, own_kv, rows, cos, sin, others, weights)


def last_kernel(rows_ref, grad_ref, mine_ref, theirs_ref, table_ref, out_ref):
    rows = rows_ref[...].astype(F32)
    normed_grad = mine_ref[...].astype(F32) + theirs_ref[...].astype(F32)
    scale = lax.rsqrt(jnp.mean(rows * rows, axis=-1, keepdims=True) + norm_eps)
    gain = table_ref[...].astype(F32)[PAD - 8 : PAD - 7, :]
    weighted = normed_grad * gain
    cubed = scale * scale * scale
    out_ref[...] = (
        grad_ref[...]
        + scale * weighted
        - rows * cubed * jnp.mean(weighted * rows, axis=-1, keepdims=True)
    ).astype(BF)


def last(rows, grad, mine, theirs, table, after=()):
    tokens, width = rows.shape
    return call(
        last_kernel,
        shape((tokens, width), BF),
        [VMEM] * 5,
        VMEM,
        [],
        16 * tokens * width,
        12 * tokens * width,
        "last",
        after,
    )(rows, grad, mine, theirs, table)


def product_kernel(extra, left_own, left, right_own, right, *refs):
    members = left.shape[0]
    out_ref = refs[-1]
    mine = [ref[0] if len(ref.shape) == 3 else ref[...] for ref in (left_own, right_own)]
    total = tn(*mine)
    for j in range(1, members):
        total = total + tn(left[j], right[j])
    rows, columns = total.shape
    out_ref[:rows, :] = total.astype(BF)
    if extra:
        small = refs[0]
        summed = small[0].astype(F32)
        for j in range(1, members):
            summed = summed + small[j].astype(F32)
        out_ref[rows:, :] = jnp.zeros((out_ref.shape[0] - rows, columns), BF)
        out_ref[rows : rows + PAD, : summed.shape[1]] = summed.astype(BF)


def product(left_own, left, right_own, right, small, extra_rows, name):
    members, tokens, rows = left.shape
    columns = right.shape[2]
    return call(
        functools.partial(product_kernel, len(small)),
        shape((rows + extra_rows, columns), BF),
        [VMEM] * (4 + len(small)),
        VMEM,
        [],
        2 * members * tokens * rows * columns,
        4 * rows * columns,
        name,
    )(left_own, left, right_own, right, *small)


def sum_kernel(index, whole_ref, parts_ref, out_ref):
    slots, rows, _ = parts_ref.shape
    at = pl.ds(pl.multiple_of(index[1] * rows, 16), rows)
    total = whole_ref[at, :].astype(F32)
    for s in range(1, slots):
        total = total + parts_ref[s].astype(F32)
    out_ref[...] = total.astype(BF)


def sum_of(index, whole, parts, name):
    slots, rows, columns = parts.shape
    return call(
        sum_kernel,
        shape((rows, columns), BF),
        [SMEM, VMEM, VMEM],
        VMEM,
        [],
        slots * rows * columns,
        2 * (slots + 1) * rows * columns,
        name,
    )(index, whole, parts)


def joint_sum_kernel(index, whole_ref, parts_ref, more_ref, out_ref):
    slots, rows, wide = parts_ref.shape
    at = pl.ds(pl.multiple_of(index[1] * rows, 16), rows)
    total = whole_ref[at, :].astype(F32)
    for s in range(1, slots):
        total = total + parts_ref[s].astype(F32)
    out_ref[:rows, :] = total.astype(BF)
    many, columns = more_ref.shape
    fold = wide // columns
    each = many // fold
    out_ref[rows:, :] = jnp.zeros((each, wide), BF)
    for k in range(fold):
        out_ref[rows:, k * columns : (k + 1) * columns] = more_ref[k * each : (k + 1) * each, :]


def joint_sum(index, whole, parts, more):
    slots, rows, columns = parts.shape
    extra = more.shape[0] // (columns // more.shape[1])
    return call(
        joint_sum_kernel,
        shape((rows + extra, columns), BF),
        [SMEM, VMEM, VMEM, VMEM],
        VMEM,
        [],
        slots * rows * columns,
        2 * (slots + 1) * rows * columns,
        "joint_sum",
    )(index, whole, parts, more)


def spread_kernel(slots, experts, index, *refs):
    parts = refs[:slots]
    query_ref, key_ref, value_ref, out_ref, one_ref, two_ref, router_ref, whole = refs[slots:]
    place = index[1]
    cut, q_wide = query_ref.shape
    kv_wide = key_ref.shape[1]
    rows = whole.shape[0] // slots
    many, columns = out_ref.shape
    each = parts[0].shape[0] - rows
    fold = parts[0].shape[1] // columns
    for s in range(slots):
        owner = lax.rem(place + slots - s, slots)
        whole[pl.ds(pl.multiple_of(owner * rows, 16), rows), :] = parts[s][:rows, :].astype(F32)
        for k in range(fold):
            base = owner * (many // slots) + k * each
            out_ref[pl.ds(pl.multiple_of(base, 16), each), :] = parts[s][
                rows:, k * columns : (k + 1) * columns
            ].astype(F32)
    query_ref[...] = whole[:cut, :q_wide]
    key_ref[...] = whole[:cut, q_wide : q_wide + kv_wide]
    value_ref[...] = whole[:cut, q_wide + kv_wide :]
    small = whole[cut : cut + PAD, :cut]
    one_ref[...] = small[PAD - 8 : PAD - 7, :]
    two_ref[...] = small[PAD - 7 : PAD - 6, :]
    router_ref[...] = jnp.transpose(small)[:, :experts]


def spread(index, parts, rows, dims, experts):
    slots = len(parts)
    columns = parts[0].shape[1]
    return call(
        functools.partial(spread_kernel, slots, experts),
        tuple(shape(item, F32) for item in dims),
        [SMEM] + [VMEM] * slots,
        (VMEM,) * len(dims),
        [pltpu.VMEM((slots * rows, columns), F32)],
        slots * rows * columns,
        6 * slots * rows * columns,
        "spread",
    )(index, *parts)


def build(members, slots):
    def ring(item, step):
        return lax.ppermute(item, "context", [(i, (i + step) % slots) for i in range(slots)])

    def per_device(
        tokens,
        positions,
        expert_ids,
        norm1_gain,
        w_query,
        w_key,
        w_value,
        w_out,
        norm2_gain,
        w_router,
        w_gate,
        w_up,
        w_down,
        grad_output,
    ):
        rows = tokens[0]
        cotangent = grad_output[0]
        block = rows.shape[0]
        width = rows.shape[1]
        experts = w_router.shape[1]
        here = w_gate.shape[0]
        kv_wide = w_key.shape[1]
        q_wide = w_query.shape[1]
        f = lax.axis_index("fsdp")
        c = lax.axis_index("context")
        c_index = c.reshape(1)
        index = jnp.stack([f, c])
        f_here = jnp.stack([f, jnp.int32(here)])

        small = jnp.zeros((PAD, w_router.shape[0]), BF)
        small = small.at[:experts].set(w_router.T)
        small = small.at[PAD - 8].set(norm1_gain).at[PAD - 7].set(norm2_gain)
        qkv_own = jnp.concatenate([w_query, w_key, w_value], axis=1)
        half = HEAD // 2
        freq = jnp.exp(-math.log(10000.0) * 2.0 * jnp.arange(half, dtype=F32) / HEAD)
        angle = positions[0].astype(F32)[:, None] * freq[None, :]
        cos, sin = jnp.cos(angle), jnp.sin(angle)
        cos = jnp.concatenate([cos] * 4, axis=1)
        sin = jnp.concatenate([-sin, sin] * 2, axis=1)
        (
            table,
            normed_one,
            heads,
            kv_slots,
            att,
            lse,
            hidden,
            normed,
            qkv_w,
            out_mine,
            cot_near,
            cot_done,
            cot_hops,
            att_near,
            normed_near,
        ) = forward(
            small,
            qkv_own,
            w_out,
            rows,
            cos,
            sin,
            expert_ids[0],
            cotangent,
            kv_wide,
            members,
            slots,
        )

        normed_slots, normed_last, cot_far, moe_parts, grad_part, router_grad, *expert_grads = own(
            table, normed, cotangent, cot_near, cot_hops, w_gate, w_up, w_down, experts, slots
        )

        parts = 2 if here % 2 == 0 else 1
        queue = []
        for s in range(1, slots - 1):
            queue += [(s, p * (here // parts), here // parts) for p in range(parts)]
        done = cot_done.shape[0]

        def fill(plan, item, grads, normed_far=None):
            s, begin, many = item
            if s < slots - 1:
                normed_refs, normed_from = [normed_slots], ((0, s - 1, 0, members),)
            else:
                normed_refs = [normed_last, normed_far]
                normed_from = ((0, None, 0, 1), (1, None, 1, members - 1))
            if s <= done:
                cot_refs, cot_from = [cot_done], ((0, s - 1, 0, members),)
            else:
                cot_refs = [cot_hops, cot_far]
                cot_from = ((0, s - done - 1, 0, 1), (1, s - done - 1, 1, members - 1))
            return more_weights(
                begin,
                many,
                f_here,
                normed_refs,
                cot_refs,
                (normed_from, cot_from),
                (w_gate, w_up, w_down),
                grads,
                experts,
                plan,
            )

        plan = home_plan(2, members, slots, grad_part, moe_parts)
        expert_grads, (grad_other, moe_mine) = fill(plan, queue[0], expert_grads)

        grad_hidden, grad_hidden_b, grad_heads, gain_two = middle(
            index, hidden, cotangent, grad_part, grad_other, table, out_mine
        )
        back = attend_back(c_index, heads, grad_heads, att, lse, cos, sin, kv_slots)
        plan = keys_plan(3, members, slots, list(back[2:]), grad_hidden_b, normed_last)
        expert_grads, (received, grad_near, normed_far) = fill(plan, queue[1], expert_grads)
        out_payload = product(att, att_near, grad_hidden_b, grad_near, (), 0, "out_grad")
        joined, part_one, gain_one = lower(
            index, back[0], back[1], received, rows, cos, sin, qkv_w
        )
        plan = rows_plan(
            4, members, slots, part_one, joined, router_grad, gain_one, gain_two, out_payload
        )
        expert_grads, (other_one, joined_near, small_near, out_chunks) = fill(
            plan, queue[2], expert_grads
        )
        payload = product(
            normed_near, normed_near, joined, joined_near, (small_near,), 2 * PAD, "qkv_grad"
        )
        out_total = sum_of(index, out_payload, out_chunks, "out_sum")
        plan = chunk_plan(5, members, slots, payload, moe_mine)
        expert_grads, (qkv_chunks, moe_other) = fill(plan, queue[3], expert_grads)
        total = joint_sum(index, payload, qkv_chunks, out_total)
        shared = [total] + [ring(total, s) for s in range(1, slots)]
        grad_tokens = last(rows, grad_hidden, part_one, other_one, table)
        moe = moe_mine.astype(F32) + moe_other.astype(F32)
        output = (hidden + moe).astype(BF)
        none = Plan(None, [], [], [], 1, lambda *_: ([], nothing, nothing, [], nothing))
        for item in queue[4:] + [(slots - 1, 0, here)]:
            expert_grads, _ = fill(none, item, expert_grads, normed_far)
        cut = w_query.shape[0]
        grad_query, grad_key, grad_value, grad_out, grad_one, grad_two, grad_router = spread(
            index,
            shared,
            payload.shape[0] // slots,
            (
                w_query.shape,
                w_key.shape,
                w_value.shape,
                w_out.shape,
                (1, cut),
                (1, cut),
                (cut, experts),
            ),
            experts,
        )
        return (
            output[None],
            grad_tokens[None],
            grad_one[0],
            grad_query,
            grad_key,
            grad_value,
            grad_out,
            grad_two[0],
            grad_router,
            expert_grads[0],
            expert_grads[1],
            expert_grads[2],
        )

    return per_device


def solution(mesh):
    return jax.shard_map(
        build(mesh.shape["fsdp"], mesh.shape["context"]),
        mesh=mesh,
        in_specs=(
            P("fsdp", "context", None),
            P("fsdp", "context"),
            P("fsdp", "context", None),
            P("fsdp"),
            P("fsdp", "tensor"),
            P("fsdp", "tensor"),
            P("fsdp", "tensor"),
            P("tensor", "fsdp"),
            P("fsdp"),
            P("fsdp", None),
            P("fsdp", None, "tensor"),
            P("fsdp", None, "tensor"),
            P("fsdp", "tensor", None),
            P("fsdp", "context", None),
        ),
        out_specs=(
            P("fsdp", "context", None),
            P("fsdp", "context", None),
            P("fsdp"),
            P("fsdp", "tensor"),
            P("fsdp", "tensor"),
            P("fsdp", "tensor"),
            P("tensor", "fsdp"),
            P("fsdp"),
            P("fsdp", None),
            P("fsdp", None, "tensor"),
            P("fsdp", None, "tensor"),
            P("fsdp", "tensor", None),
        ),
        check_vma=False,
    )
```

```python
import functools
import math

import jax
import jax.numpy as jnp
import numpy as np
from jax import lax
from jax.experimental import pallas as pl
from jax.experimental.pallas import tpu as pltpu
from jax.sharding import PartitionSpec as P

HEAD = 64
LANES = 128
PAD = 32
norm_eps = 1e-06
masked_score = -1e30
BF = jnp.bfloat16
F32 = jnp.float32
VMEM = pl.BlockSpec(memory_space=pltpu.VMEM)
SMEM = pl.BlockSpec(memory_space=pltpu.SMEM)
ANY = pl.BlockSpec(memory_space=pl.ANY)


def nn(left, right):
    return jnp.dot(left, right, preferred_element_type=F32)


def nt(left, right):
    return lax.dot_general(left, right, (((1,), (1,)), ((), ())), preferred_element_type=F32)


def tn(left, right):
    return lax.dot_general(left, right, (((0,), (0,)), ((), ())), preferred_element_type=F32)


def partner(f):
    return f + 1 - 2 * lax.rem(f, 2)


def member(f, j, members):
    base = lax.rem(f + members - (j - j % 2), members)
    return base if j % 2 == 0 else partner(base)


def columns_of(ref, owner, cut):
    if cut % LANES == 0:
        return ref[:, pl.ds(pl.multiple_of(owner * cut, LANES), cut)]
    pair = ref[:, pl.ds(pl.multiple_of(lax.div(owner, 2) * (2 * cut), LANES), 2 * cut)]
    return jnp.where(lax.rem(owner, 2) == 0, pair[:, :cut], pair[:, cut:])


def put_columns(ref, owner, first, second):
    cut = first.shape[1]
    if cut % LANES == 0:
        ref[:, pl.ds(pl.multiple_of(owner * cut, LANES), cut)] = first
        ref[:, pl.ds(pl.multiple_of(partner(owner) * cut, LANES), cut)] = second
    else:
        even = lax.rem(owner, 2) == 0
        both = [jnp.where(even, first, second), jnp.where(even, second, first)]
        at = pl.ds(pl.multiple_of(lax.div(owner, 2) * (2 * cut), LANES), 2 * cut)
        ref[:, at] = jnp.concatenate(both, axis=1)


def shape(dims, kind):
    return jax.ShapeDtypeStruct(dims, kind)


def call(kernel, outs, specs, out_specs, scratch, flops, moved, name, after=(), **more):
    skip = len(after)

    def body(*refs):
        kernel(*refs[skip:])

    run = pl.pallas_call(
        body,
        out_shape=outs,
        in_specs=[ANY] * skip + list(specs),
        out_specs=out_specs,
        scratch_shapes=scratch,
        compiler_params=pltpu.CompilerParams(vmem_limit_bytes=60 << 20),
        name=name,
        cost_estimate=pl.CostEstimate(flops=flops, bytes_accessed=moved, transcendentals=0),
        **more,
    )
    return lambda *operands: run(*after, *operands)


def rotate(rows, cos, sin):
    wide = rows.shape[1]
    count = wide // LANES
    after = pltpu.roll(rows, wide - HEAD // 2, 1)
    before = pltpu.roll(rows, HEAD // 2, 1)
    lane = lax.broadcasted_iota(jnp.int32, rows.shape, 1) % HEAD
    partner = jnp.where(lane < HEAD // 2, after, before)
    cos_all = jnp.concatenate([cos] * count, axis=1)
    sin_all = jnp.concatenate([sin] * count, axis=1)
    return rows * cos_all + partner * sin_all


class Sender:
    def __init__(self, sems):
        self.sems = sems
        self.used = 0
        self.made = []

    def add(self, source, target, device):
        copy = pltpu.make_async_remote_copy(
            src_ref=source,
            dst_ref=target,
            send_sem=self.sems.at[0, self.used],
            recv_sem=self.sems.at[1, self.used],
            device_id=device,
            device_id_type=pl.DeviceIdType.MESH,
        )
        self.used += 1
        self.made.append(copy)
        return copy


def greet(devices):
    barrier = pltpu.get_barrier_semaphore()
    for device in devices:
        pl.semaphore_signal(
            barrier, inc=1, device_id=device, device_id_type=pl.DeviceIdType.MESH
        )
    pl.semaphore_wait(barrier, len(devices))


def target(f, j, members):
    start = f if j % 2 == 0 else partner(f)
    return lax.rem(start + j - j % 2, members)


def attend_slot(s, heads_ref, kv, top, sums, acc):
    groups = top.shape[0]
    tokens = heads_ref.shape[1]
    repeat = heads_ref.shape[0] // groups
    half = kv.shape[2] // 2
    many = repeat * tokens
    keys = lax.broadcasted_iota(jnp.int32, (tokens, many), 0)
    queries = lax.broadcasted_iota(jnp.int32, (tokens, many), 1) % tokens
    allowed = keys <= queries + jnp.where(s == 0, 0, tokens)
    for g in range(groups):
        q = heads_ref[g * repeat : (g + 1) * repeat].reshape(many, HEAD)
        score = jnp.where(allowed, nt(kv[s, :, g * HEAD : (g + 1) * HEAD], q), masked_score)
        value = kv[s, :, half + g * HEAD : half + (g + 1) * HEAD]
        old = top[g]
        high = jnp.maximum(old, jnp.max(score, axis=0, keepdims=True))
        shrink = jnp.exp(old - high)
        weight = jnp.where(allowed, jnp.exp(score - high), 0.0)
        sums[g] = sums[g] * shrink + jnp.sum(weight, axis=0, keepdims=True)
        acc[g] = acc[g] * shrink + tn(value, weight.astype(BF))
        top[g] = high


def attend_end(att_ref, lse_ref, top, sums, acc):
    groups, _, many = top.shape
    tokens = att_ref.shape[0]
    repeat = many // tokens
    for g in range(groups):
        lse_ref[g] = top[g] + jnp.log(sums[g])
        done = jnp.transpose(acc[g] / sums[g]).astype(BF)
        for r in range(repeat):
            h = g * repeat + r
            att_ref[:, h * HEAD : (h + 1) * HEAD] = done[r * tokens : (r + 1) * tokens]


def forward_kernel(
    members,
    slots,
    query_in,
    key_in,
    value_in,
    wout_in,
    cot_in,
    router_ref,
    one_ref,
    two_ref,
    rows_ref,
    turns_ref,
    ids_ref,
    *refs,
):
    (
        table_ref,
        normed_one_ref,
        heads_ref,
        kv_out,
        att_ref,
        lse_ref,
        hidden_ref,
        normed_ref,
        qkv_out,
        wout_out,
        cot_near,
        cot_done,
        cot_two,
        cut_near,
        cut_ref,
        small,
        qkv,
        mine,
        theirs,
        kv,
        total,
        first,
        second,
        other,
        top,
        sums,
        acc,
        sems,
        local_sems,
    ) = refs
    f = lax.axis_index("fsdp")
    c = lax.axis_index("context")
    t = lax.axis_index("tensor")
    tokens, width = rows_ref.shape
    side = tokens // 2
    experts, cut = router_ref.shape
    evens = range(2, members, 2)
    beside = {"fsdp": partner(f)}
    opposite = {"tensor": 1 - t}
    ahead = {"context": lax.rem(c + 1, slots)}
    apart = {j: {"fsdp": lax.rem(f + j, members)} for j in evens}
    lower_half, upper_half = pl.ds(0, side), pl.ds(side, side)
    piece = pl.ds(pl.multiple_of(t * side, side), side)

    net = Sender(sems)
    small_sent = [
        net.add(small.at[0], small.at[j], {"fsdp": target(f, j, members)}) for j in range(1, members)
    ]

    def family(source, place):
        return (
            net.add(source, place.at[1], beside),
            {j: net.add(source, place.at[j], apart[j]) for j in evens},
            {j: net.add(place.at[j], place.at[j + 1], beside) for j in evens},
        )

    q_wide, kv_wide = query_in.shape[1], key_in.shape[1]
    bounds = (0, q_wide, q_wide + kv_wide, q_wide + 2 * kv_wide)
    projections = [
        (source, pl.ds(low, high - low))
        for source, low, high in zip((query_in, key_in, value_in), bounds, bounds[1:])
    ]
    groups_of = {"query": projections[:1], "keys": projections[1:]}
    spans = {"query": pl.ds(0, q_wide), "keys": pl.ds(q_wide, 2 * kv_wide)}
    qkv_core, qkv_far, qkv_relay = {}, {}, {}
    for name in ("keys", "query"):
        qkv_core[name] = [net.add(source, qkv.at[1, :, at], beside) for source, at in groups_of[name]]
        qkv_far[name] = {
            j: [net.add(source, qkv.at[j, :, at], apart[j]) for source, at in groups_of[name]]
            for j in evens
        }
        span = spans[name]
        qkv_relay[name] = {
            j: net.add(qkv.at[j, :, span], qkv.at[j + 1, :, span], beside) for j in evens
        }
    out_core, out_far, out_relay = family(wout_in, mine)
    out_cross = {j: net.add(wout_in if j == 0 else mine.at[j], theirs.at[j], opposite) for j in range(0, members, 2)}
    out_cross_relay = {j: net.add(theirs.at[j], theirs.at[j + 1], beside) for j in range(0, members, 2)}
    cot_core, cot_far, cot_relay = family(cot_in, cot_near)
    done = cot_done.shape[0]
    hop, whole, half, cross, relay_half, relay_cross = {}, {}, {}, {}, {}, {}
    hop[1] = net.add(cot_in, cot_done.at[0, 0], ahead)
    if slots > 2:
        hop[2] = net.add(cot_done.at[0, 0], cot_two, ahead)
    for s in range(1, done + 1):
        now = cot_done.at[s - 1]
        whole[s] = net.add(now.at[0], now.at[1], beside)
        for j in evens:
            half[s, j] = net.add(now.at[0, piece], now.at[j, lower_half], apart[j])
            cross[s, j] = net.add(now.at[j, lower_half], now.at[j, upper_half], opposite)
            relay_half[s, j] = net.add(now.at[j, lower_half], now.at[j + 1, lower_half], beside)
            relay_cross[s, j] = net.add(now.at[j, upper_half], now.at[j + 1, upper_half], beside)
    cuts = [
        net.add(cut_ref.at[j], cut_near.at[j], {"fsdp": target(f, j, members)})
        for j in range(1, members)
    ]
    plain = len(net.made)
    first_later = net.used
    net.used += slots - 1

    def later(s):
        at = first_later + s - 1
        return pltpu.make_async_remote_copy(
            src_ref=kv.at[s - 1],
            dst_ref=kv.at[s],
            send_sem=sems.at[0, at],
            recv_sem=sems.at[1, at],
            device_id=ahead,
            device_id_type=pl.DeviceIdType.MESH,
        )

    plain_made = net.made[:plain]
    att_sent = net.add(att_ref, other, opposite)

    locals_in = [
        pltpu.make_async_copy(source, qkv.at[0, :, at], sem)
        for (source, at), sem in zip(projections, [local_sems.at[i] for i in (0, 1, 2)])
    ]
    locals_in.append(pltpu.make_async_copy(wout_in, mine.at[0], local_sems.at[5 + slots]))
    qkv_saved = pltpu.make_async_copy(qkv, qkv_out, local_sems.at[3])
    out_saved = pltpu.make_async_copy(mine, wout_out, local_sems.at[4])
    kv_saved = [
        pltpu.make_async_copy(kv.at[s], kv_out.at[s], local_sems.at[5 + s]) for s in range(slots)
    ]
    for copy in locals_in:
        copy.start()
    small[0] = jnp.zeros((PAD, cut), BF)
    small[0, :experts, :] = router_ref[...]
    small[0, PAD - 8, :] = one_ref[...]
    small[0, PAD - 7, :] = two_ref[...]
    greet(
        [{"fsdp": target(f, j, members)} for j in range(1, members)]
        + [opposite]
        + [ahead, {"context": lax.rem(c + slots - 1, slots)}]
    )
    for copy in small_sent:
        copy.start()
    for name in ("keys", "query"):
        for copies in [qkv_core[name]] + [qkv_far[name][j] for j in evens]:
            for copy in copies:
                copy.start()
    for copy in [out_core, out_cross[0]] + [out_far[j] for j in evens]:
        copy.start()
    hop[1].start()
    cot_core.start()

    rows = rows_ref[...].astype(F32)
    scale = lax.rsqrt(jnp.mean(rows * rows, axis=-1, keepdims=True) + norm_eps)
    hidden_ref[...] = rows * scale
    for copy in locals_in:
        copy.wait()
    for copy in small_sent:
        copy.wait_recv()

    for j in range(0, members, 2):
        put_columns(table_ref, member(f, j, members), small[j], small[j + 1])
    gain = table_ref[...].astype(F32)[PAD - 8 : PAD - 7, :]
    normed_one_ref[...] = (hidden_ref[...] * gain).astype(BF)
    for j in range(members):
        cut_ref[j] = columns_of(normed_one_ref, target(f, j, members), cut)

    total[...] = jnp.zeros(total.shape, F32)

    def product_of(name):
        span = spans[name]

        def far_arrived(j):
            for copy in qkv_far[name][j]:
                copy.wait_recv()
            qkv_relay[name][j].start()

        def core_arrived():
            for copy in qkv_core[name]:
                copy.wait_recv()

        def one_pair(p, carry):
            owner = lax.rem(f + members - 2 * p, members)
            for j in evens:
                pl.when(2 * p == j)(functools.partial(far_arrived, j))
            left = columns_of(normed_one_ref, owner, cut)
            total[:, span] += nn(left, qkv[2 * p, :, span])
            pl.when(p == 0)(core_arrived)
            for j in evens:
                pl.when(2 * p == j)(qkv_relay[name][j].wait_recv)
            left = columns_of(normed_one_ref, partner(owner), cut)
            total[:, span] += nn(left, qkv[2 * p + 1, :, span])
            return carry

        lax.fori_loop(0, members // 2, one_pair, 0)

    cos = turns_ref[:, :LANES]
    sin = turns_ref[:, LANES:]
    product_of("keys")
    kv[0, :, :kv_wide] = rotate(total[:, q_wide : q_wide + kv_wide], cos, sin).astype(BF)
    kv[0, :, kv_wide:] = total[:, q_wide + kv_wide :].astype(BF)
    pl.when(c + 1 < slots)(later(1).start)
    hop[1].wait_recv()
    whole[1].start()
    for j in evens:
        half[1, j].start()
    for copy in [cot_far[j] for j in evens] + cuts:
        copy.start()
    product_of("query")
    qkv_saved.start()
    turned = (rotate(total[:, :q_wide], cos, sin) * (1.0 / math.sqrt(HEAD))).astype(BF)
    for h in range(q_wide // HEAD):
        heads_ref[h] = turned[:, h * HEAD : (h + 1) * HEAD]
    top[...] = jnp.full(top.shape, masked_score, F32)
    sums[...] = jnp.zeros(sums.shape, F32)
    acc[...] = jnp.zeros(acc.shape, F32)
    def weights_arrived():
        for j in evens:
            out_far[j].wait_recv()
            out_relay[j].start()
            out_cross[j].start()
        out_cross[0].wait_recv()
        out_cross_relay[0].start()


    def half_arrived(s):
        for j in evens:
            half[s, j].wait_recv()
            relay_half[s, j].start()
            cross[s, j].start()

    def keys_arrived(s, carry):
        @pl.when(c >= s)
        def _():
            @pl.when(s > 0)
            def _():
                later(s).wait_recv()

                @pl.when((c + 1 < slots) & (s + 1 < slots))
                def _():
                    later(s + 1).start()

            attend_slot(s, heads_ref, kv, top, sums, acc)

        pl.when(s == 0)(weights_arrived)
        pl.when(s == 1)(functools.partial(half_arrived, 1))
        return carry

    lax.fori_loop(0, slots, keys_arrived, 0)
    if slots > 2:
        hop[2].start()
    kv_saved[0].start()
    for s in range(1, slots):
        pl.when(c >= s)(kv_saved[s].start)
    attend_end(att_ref, lse_ref, top, sums, acc)
    att_sent.start()

    out_core.wait_recv()
    for j in evens:
        out_relay[j].wait_recv()
    out_saved.start()
    def mixed(left, weights, place):
        def one_pair(p, carry):
            owner = lax.rem(f + members - 2 * p, members)
            pair = nn(left[...], weights[2 * p]), nn(left[...], weights[2 * p + 1])
            put_columns(place, owner, *pair)
            return carry

        lax.fori_loop(0, members // 2, one_pair, 0)

    mixed(att_ref, mine, first)
    for j in evens:
        out_cross[j].wait_recv()
        out_cross_relay[j].start()
    for j in evens:
        cross[1, j].wait_recv()
        relay_cross[1, j].start()
    for j in range(0, members, 2):
        out_cross_relay[j].wait_recv()
    att_sent.wait_recv()
    mixed(other, theirs, second)

    hidden = rows_ref[...].astype(F32) + (first[...] + second[...])
    hidden_ref[...] = hidden
    scale = lax.rsqrt(jnp.mean(hidden * hidden, axis=-1, keepdims=True) + norm_eps)
    gain = table_ref[...].astype(F32)[PAD - 7 : PAD - 6, :]
    normed = (hidden * scale * gain).astype(BF)
    normed_ref[:, :width] = normed
    logits = nt(normed, table_ref[...])
    lanes = lax.broadcasted_iota(jnp.int32, logits.shape, 1)
    ids = jnp.transpose(ids_ref[...].astype(F32)).astype(jnp.int32)
    mask = ids[:, 0:1] == lanes
    for k in range(1, ids.shape[1]):
        mask = mask | (ids[:, k : k + 1] == lanes)
    logits = jnp.where(mask, logits, masked_score)
    weight = jnp.where(mask, jnp.exp(logits - jnp.max(logits, axis=-1, keepdims=True)), 0.0)
    gates = weight / jnp.sum(weight, axis=-1, keepdims=True)
    upper = gates.astype(BF).astype(F32)
    lower = gates - upper
    blank = jnp.zeros((gates.shape[0], LANES - 2 * PAD), F32)
    normed_ref[:, width:] = jnp.concatenate([upper, lower, blank], axis=1).astype(BF)

    for j in evens:
        cot_far[j].wait_recv()
        cot_relay[j].start()
    if slots > 2:
        hop[2].wait_recv()
    for copy in [cot_core] + cuts:
        copy.wait_recv()
    for j in evens:
        cot_relay[j].wait_recv()
    for s in range(1, done + 1):
        whole[s].wait_recv()
        for j in evens:
            relay_half[s, j].wait_recv()
            relay_cross[s, j].wait_recv()
    qkv_saved.wait()
    out_saved.wait()
    kv_saved[0].wait()
    for s in range(1, slots):
        pl.when(c >= s)(kv_saved[s].wait)
    for copy in plain_made:
        copy.wait_send()
    for s in range(1, slots):
        pl.when((c >= s - 1) & (c + 1 < slots))(later(s).wait_send)
    att_sent.wait_send()


def forward(projections, wout, cotangent, small, rows, turns, ids, members, slots):
    tokens, width = rows.shape
    cut, q_wide = projections[0].shape
    kv_wide = projections[1].shape[1]
    wide = q_wide + 2 * kv_wide
    heads = q_wide // HEAD
    groups = kv_wide // HEAD
    many = heads // groups * tokens
    halves = members // 2
    far = halves - 1
    done = 1
    copies = (members - 1) + 2 * (1 + 2 * far) + 3 * (1 + far) + 2 * far + 2 * halves
    copies += (slots - 1) + 1 + done * (1 + 4 * far) + 2 + (members - 1)
    return pl.pallas_call(
        functools.partial(forward_kernel, members, slots),
        out_shape=(
            shape((PAD, width), BF),
            shape((tokens, width), BF),
            shape((heads, tokens, HEAD), BF),
            shape((slots, tokens, 2 * kv_wide), BF),
            shape((tokens, q_wide), BF),
            shape((groups, 1, many), F32),
            shape((tokens, width), F32),
            shape((tokens, width + LANES), BF),
            shape((members, cut, wide), BF),
            shape((members,) + wout.shape, BF),
            shape((members, tokens, width), BF),
            shape((done, members, tokens, width), BF),
            shape((tokens, width), BF),
            shape((members, tokens, width // members), BF),
            shape((members, tokens, width // members), BF),
        ),
        in_specs=[ANY] * 5 + [VMEM] * 6,
        out_specs=(VMEM, VMEM, VMEM, ANY, VMEM, VMEM, VMEM, VMEM) + (ANY,) * 6 + (VMEM,),
        scratch_shapes=[
            pltpu.VMEM((members, PAD, cut), BF),
            pltpu.VMEM((members, cut, wide), BF),
            pltpu.VMEM((members,) + wout.shape, BF),
            pltpu.VMEM((members,) + wout.shape, BF),
            pltpu.VMEM((slots, tokens, 2 * kv_wide), BF),
            pltpu.VMEM((tokens, wide), F32),
            pltpu.VMEM((tokens, width), F32),
            pltpu.VMEM((tokens, width), F32),
            pltpu.VMEM((tokens, q_wide), BF),
            pltpu.VMEM((groups, 1, many), F32),
            pltpu.VMEM((groups, 1, many), F32),
            pltpu.VMEM((groups, HEAD, many), F32),
            pltpu.SemaphoreType.DMA((2, copies)),
            pltpu.SemaphoreType.DMA((7 + slots,)),
        ],
        compiler_params=pltpu.CompilerParams(
            vmem_limit_bytes=60 << 20, collective_id=0, has_side_effects=True
        ),
        name="forward",
        cost_estimate=pl.CostEstimate(
            flops=8 * tokens * width * wide, bytes_accessed=8 * width * wide, transcendentals=0
        ),
    )(*projections, wout, cotangent, *small, rows, turns, ids)


def attend_back_start(heads_ref, grad_ref, att_ref, wide, acc):
    groups, many, _ = wide.shape
    repeat = heads_ref.shape[0] // groups
    lane = lax.broadcasted_iota(jnp.int32, (many, 2 * HEAD), 1)
    for g in range(groups):
        grad = grad_ref[g * repeat : (g + 1) * repeat].reshape(many, HEAD).astype(F32)
        out = jnp.concatenate(
            [
                att_ref[:, (g * repeat + r) * HEAD : (g * repeat + r + 1) * HEAD]
                for r in range(repeat)
            ],
            axis=0,
        )
        delta = jnp.sum(grad * out.astype(F32), axis=-1, keepdims=True)
        upper = delta.astype(BF).astype(F32)
        both = jnp.concatenate([grad, jnp.zeros((many, HEAD), F32)], axis=1)
        both = jnp.where(lane == HEAD, -upper, jnp.where(lane == HEAD + 1, upper - delta, both))
        wide[g] = both.astype(BF)
        acc[g] = jnp.zeros((many, HEAD), F32)


def attend_back_slot(s, heads_ref, grad_ref, lse_ref, kv, wide, acc, grad_kv):
    groups, many, _ = wide.shape
    tokens = heads_ref.shape[1]
    repeat = heads_ref.shape[0] // groups
    half = kv.shape[2] // 2
    keys = lax.broadcasted_iota(jnp.int32, (tokens, many), 0)
    queries = lax.broadcasted_iota(jnp.int32, (tokens, many), 1) % tokens
    allowed = keys <= queries + jnp.where(s == 0, 0, tokens)
    for g in range(groups):
        at = slice(g * HEAD, (g + 1) * HEAD)
        behind = slice(half + g * HEAD, half + (g + 1) * HEAD)
        q = heads_ref[g * repeat : (g + 1) * repeat].reshape(many, HEAD)
        grad = grad_ref[g * repeat : (g + 1) * repeat].reshape(many, HEAD)
        key = kv[s, :, at]
        value = kv[s, :, behind]
        value = jnp.concatenate([value, jnp.ones_like(value)], axis=1)
        prob = jnp.where(allowed, jnp.exp(nt(key, q) - lse_ref[g]), 0.0)
        grad_score = (prob * nt(value, wide[g])).astype(BF)
        grad_kv[:, at] = nn(grad_score, q)
        grad_kv[:, behind] = nn(prob.astype(BF), grad)
        acc[g] += tn(grad_score, key)


def attend_back_end(turns_ref, acc, turned, grad_q_ref):
    groups, many, _ = acc.shape
    tokens = turned.shape[0]
    repeat = many // tokens
    for g in range(groups):
        done = acc[g] * (1.0 / math.sqrt(HEAD))
        for r in range(repeat):
            h = g * repeat + r
            turned[:, h * HEAD : (h + 1) * HEAD] = done[r * tokens : (r + 1) * tokens]
    grad_q_ref[...] = rotate(turned[...], turns_ref[:, :LANES], -turns_ref[:, LANES:]).astype(BF)


def gates_of(tail, experts):
    rows = tail.astype(F32)
    both = rows + pltpu.roll(rows, LANES - PAD, 1)
    lane = lax.broadcasted_iota(jnp.int32, both.shape, 1)
    return jnp.where(lane < experts, both, 0.0)


def gate_column(gates, expert):
    lane = lax.broadcasted_iota(jnp.int32, gates.shape, 1)
    return jnp.sum(jnp.where(lane == expert, gates, 0.0), axis=-1, keepdims=True)


def hidden_terms(normed, cotangent, gate_col, gate_w, up_w, down_w):
    gate_pre = nn(normed, gate_w)
    up_pre = nn(normed, up_w)
    plain = nt(cotangent, down_w)
    sigma = 1.0 / (1.0 + jnp.exp(-gate_pre))
    activated = gate_pre * sigma
    inner = activated * up_pre
    grad_inner = gate_col * plain
    scaled = (gate_col * inner).astype(BF)
    grad_g = (grad_inner * up_pre * (sigma + activated * (1.0 - sigma))).astype(BF)
    grad_u = (grad_inner * activated).astype(BF)
    return inner, plain, scaled, grad_g, grad_u


def own_kernel(members, slots, experts, table_ref, normed_in, cot_own, cot_near, cot_two, *refs):
    cot_in = [cot_own] + [cot_near.at[j] for j in range(1, members)]
    gate_hbm, up_hbm, down_hbm = refs[:3]
    (
        far_ref,
        last_ref,
        cot_hops,
        two_out,
        moe_ref,
        mine_ref,
        router_ref,
        grad_gate_ref,
        grad_up_ref,
        grad_down_ref,
        gate_w,
        up_w,
        down_w,
        normed,
        cot,
        all_inner,
        all_g,
        all_u,
        parts,
        swapped,
        joined,
        arrived,
        stage_gate,
        stage_up,
        stage_down,
        gates,
        shares,
        sems,
        weight_sems,
        local_sems,
        stage_sems,
        moe_stage,
        moe_sems,
    ) = refs[3:]
    f = lax.axis_index("fsdp")
    c = lax.axis_index("context")
    t = lax.axis_index("tensor")
    here = gate_w.shape[0]
    hidden = gate_w.shape[2]
    tokens = normed_in.shape[0]
    side = tokens // 2
    width = cot.shape[2]
    evens = range(2, members, 2)
    beside = {"fsdp": partner(f)}
    opposite = {"tensor": 1 - t}
    ahead = {"context": lax.rem(c + 1, slots)}
    behind = {"context": lax.rem(c + slots - 1, slots)}
    apart = {j: {"fsdp": lax.rem(f + j, members)} for j in evens}
    owner = {j: {"fsdp": lax.rem(f + members - j, members)} for j in evens}

    net = Sender(sems)
    near_core = net.add(normed_in, normed.at[1], beside)
    near_far = {j: net.add(normed_in, normed.at[j], apart[j]) for j in evens}
    near_relay = {j: net.add(normed.at[j], normed.at[j + 1], beside) for j in evens}
    hop, whole, half, cross, relay_half, relay_cross = {}, {}, {}, {}, {}, {}
    lower_half, upper_half = pl.ds(0, side), pl.ds(side, side)
    piece = pl.ds(pl.multiple_of(t * side, side), side)
    whole_slots = range(1, slots - 1)
    for s in range(1, slots):
        origin = normed_in if s == 1 else far_ref.at[s - 2, 0]
        hop[s] = net.add(origin, far_ref.at[s - 1, 0] if s < slots - 1 else last_ref, ahead)
    for s in whole_slots:
        now = far_ref.at[s - 1]
        whole[s] = net.add(now.at[0], now.at[1], beside)
        for j in evens:
            half[s, j] = net.add(now.at[0, piece], now.at[j, lower_half], apart[j])
            cross[s, j] = net.add(now.at[j, lower_half], now.at[j, upper_half], opposite)
            relay_half[s, j] = net.add(now.at[j, lower_half], now.at[j + 1, lower_half], beside)
            relay_cross[s, j] = net.add(now.at[j, upper_half], now.at[j + 1, upper_half], beside)
    done = 2
    late = {}
    for s in range(done + 1, slots):
        origin = cot_two if s == done + 1 else cot_hops.at[s - done - 2]
        late[s] = net.add(origin, cot_hops.at[s - done - 1], ahead)
    two_whole = net.add(cot_two, two_out.at[0], beside)
    two_half, two_cross, two_relay, two_relay_cross = {}, {}, {}, {}
    for j in evens:
        low, high = two_out.at[j - 1, lower_half], two_out.at[j - 1, upper_half]
        two_half[j] = net.add(cot_two.at[piece], low, apart[j])
        two_cross[j] = net.add(low, high, opposite)
        two_relay[j] = net.add(low, two_out.at[j, lower_half], beside)
        two_relay_cross[j] = net.add(high, two_out.at[j, upper_half], beside)
    swap = {
        j: net.add(parts.at[j + 1], swapped.at[j // 2], beside) for j in range(0, members, 2)
    }
    home = {j: net.add(joined.at[j // 2], arrived.at[j // 2], owner[j]) for j in evens}

    weight_copies = [
        (
            pltpu.make_async_copy(gate_hbm.at[e], gate_w.at[e], weight_sems.at[0, e]),
            pltpu.make_async_copy(up_hbm.at[e], up_w.at[e], weight_sems.at[1, e]),
            pltpu.make_async_copy(down_hbm.at[e], down_w.at[e], weight_sems.at[2, e]),
        )
        for e in range(here)
    ]
    local = [pltpu.make_async_copy(normed_in, normed.at[0], local_sems.at[0])]
    for j in range(members):
        local.append(pltpu.make_async_copy(cot_in[j], cot.at[j], local_sems.at[1 + j]))
    for copy in local + list(weight_copies[0]):
        copy.start()
    greet([beside, opposite, ahead, behind] + [apart[j] for j in evens])
    near_core.start()
    for j in evens:
        near_far[j].start()
    hop[1].start()
    for e in range(1, here):
        for copy in weight_copies[e]:
            copy.start()
    for copy in local:
        copy.wait()
    near_core.wait_recv()

    chunk = width // 3
    step = 2 * tokens

    def prepare(pair):
        at = pl.ds(pl.multiple_of(pair * step, step), step)
        tail = normed[pl.ds(2 * pair, 2), :, width:].reshape(step, LANES)
        gates[at, :] = gates_of(tail, experts)
        shares[at, :] = jnp.zeros((step, LANES), F32)

    def hidden_pass(pair):
        def one_expert(e, carry):
            @pl.when(pair == 0)
            def _():
                pltpu.make_async_copy(gate_hbm.at[e], gate_w.at[e], weight_sems.at[0, e]).wait()
                pltpu.make_async_copy(up_hbm.at[e], up_w.at[e], weight_sems.at[1, e]).wait()
                pltpu.make_async_copy(down_hbm.at[e], down_w.at[e], weight_sems.at[2, e]).wait()

            at = pl.ds(pl.multiple_of(pair * step, step), step)
            both = pl.ds(2 * pair, 2)
            columns = pl.ds(pl.multiple_of(e * hidden, LANES), hidden)
            inner, plain, scaled, grad_g, grad_u = hidden_terms(
                normed[both, :, :width].reshape(step, width),
                cot[both].reshape(step, width),
                gate_column(gates[at, :], f * here + e),
                gate_w[e],
                up_w[e],
                down_w[e],
            )
            all_inner[at, columns] = scaled
            all_g[at, columns] = grad_g
            all_u[at, columns] = grad_u
            share = jnp.sum(inner * plain, axis=-1, keepdims=True)
            lane = lax.broadcasted_iota(jnp.int32, (step, LANES), 1)
            shares[at, :] = jnp.where(lane == f * here + e, share, shares[at, :])
            return carry

        lax.fori_loop(0, here, one_expert, 0)

    def grad_pass(pair):
        def one_block(b, carry):
            at = pl.ds(pl.multiple_of(b * tokens, tokens), tokens)
            mean = jnp.sum(gates[at, :] * shares[at, :], axis=-1, keepdims=True)
            logits = (gates[at, :] * (shares[at, :] - mean)).astype(BF)
            router_ref[...] += tn(logits, normed[b, :, :width])[:PAD]

            def one_chunk(k, inner_carry):
                part = pl.ds(pl.multiple_of(k * chunk, LANES), chunk)
                total = nn(logits[:, :PAD], table_ref[:, part])
                for e in range(here):
                    columns = slice(e * hidden, (e + 1) * hidden)
                    total = total + nt(all_g[at, columns], gate_w[e, part, :])
                    total = total + nt(all_u[at, columns], up_w[e, part, :])
                parts[b, :, part] = total.astype(BF)
                return inner_carry

            return lax.fori_loop(0, 3, one_chunk, carry)

        lax.fori_loop(2 * pair, 2 * pair + 2, one_block, 0)

    def slot_arrived(s):
        hop[s].wait_recv()
        if s + 1 < slots:
            hop[s + 1].start()
        if s in whole_slots:
            whole[s].start()
            for j in evens:
                half[s, j].start()

    def half_arrived(s):
        if s in whole_slots:
            for j in evens:
                half[s, j].wait_recv()
                cross[s, j].start()
                relay_half[s, j].start()

    def cross_arrived(s):
        if s in whole_slots:
            for j in evens:
                cross[s, j].wait_recv()
                relay_cross[s, j].start()

    def moe_pass(pair):
        def one_moe(b, carry):
            at = pl.ds(pl.multiple_of(b * tokens, tokens), tokens)
            slot = lax.rem(b, 2)
            copy = pltpu.make_async_copy(moe_stage.at[slot], moe_ref.at[b], moe_sems.at[slot])
            pl.when(b >= 2)(copy.wait)

            def one_chunk(k, inner_carry):
                part = pl.ds(pl.multiple_of(k * chunk, LANES), chunk)
                down = down_w[:, :, part].reshape(here * hidden, chunk)
                moe_stage[slot, :, part] = nn(all_inner[at, :], down).astype(BF)
                return inner_carry

            lax.fori_loop(0, 3, one_chunk, 0)
            copy.start()
            return carry

        lax.fori_loop(2 * pair, 2 * pair + 2, one_moe, 0)

    def far_ready():
        for j in evens:
            near_relay[j].wait_recv()

    def near_done():
        swap[0].start()
        for j in evens:
            near_far[j].wait_recv()
            near_relay[j].start()
        slot_arrived(1)
        if done + 1 < slots:
            late[done + 1].start()
        for copy in [two_whole] + [two_half[j] for j in evens]:
            copy.start()

    def all_done():
        for j in evens:
            swap[j].start()
        if slots > 2:
            slot_arrived(2)
        for j in evens:
            swap[j].wait_recv()
            joined[j // 2] = (parts[j].astype(F32) + swapped[j // 2].astype(F32)).astype(BF)
            home[j].start()
        cross_arrived(1)
        for j in evens:
            two_half[j].wait_recv()
            two_cross[j].start()
            two_relay[j].start()

    router_ref[...] = jnp.zeros_like(router_ref)

    def one_pair(pair, carry):
        pl.when(pair == 1)(far_ready)
        prepare(pair)
        hidden_pass(pair)
        pl.when(pair == 1)(functools.partial(half_arrived, 1))
        grad_pass(pair)
        pl.when(pair == 0)(near_done)
        pl.when(pair == members // 2 - 1)(all_done)
        moe_pass(pair)
        return carry

    lax.fori_loop(0, members // 2, one_pair, 0)
    for slot in range(2):
        pltpu.make_async_copy(moe_stage.at[slot], moe_ref.at[slot], moe_sems.at[slot]).wait()
    half_arrived(2)

    buffers = stage_gate.shape[0]

    def stage_copies(e, b):
        return (
            pltpu.make_async_copy(stage_gate.at[b], grad_gate_ref.at[e], stage_sems.at[0, b]),
            pltpu.make_async_copy(stage_up.at[b], grad_up_ref.at[e], stage_sems.at[1, b]),
            pltpu.make_async_copy(stage_down.at[b], grad_down_ref.at[e], stage_sems.at[2, b]),
        )

    def sum_home():
        swap[0].wait_recv()
        total = parts[0].astype(F32) + swapped[0].astype(F32)
        for j in evens:
            home[j].wait_recv()
            total = total + arrived[j // 2].astype(F32)
        mine_ref[...] = total.astype(BF)

    def middle_slots():
        for j in evens:
            two_cross[j].wait_recv()
            two_relay_cross[j].start()
        cross_arrived(2)
        for s in range(3, slots - 1):
            slot_arrived(s)
            half_arrived(s)
            cross_arrived(s)

    def weights_of(e, carry):
        b = lax.rem(e, buffers)

        @pl.when(e >= buffers)
        def _():
            for copy in stage_copies(e, b):
                copy.wait()

        columns = pl.ds(pl.multiple_of(e * hidden, LANES), hidden)
        rows = members * tokens

        def one_chunk(k, inner_carry):
            part = pl.ds(pl.multiple_of(k * chunk, LANES), chunk)
            left = normed[:, :, part].reshape(rows, chunk)
            right = cot[:, :, part].reshape(rows, chunk)
            stage_gate[b, part, :] = tn(left, all_g[:, columns])
            stage_up[b, part, :] = tn(left, all_u[:, columns])
            stage_down[b, :, part] = tn(all_inner[:, columns], right)
            return inner_carry

        lax.fori_loop(0, 3, one_chunk, 0)
        for copy in stage_copies(e, b):
            copy.start()
        pl.when(e == here // 2)(middle_slots)
        pl.when(e == here - 1)(sum_home)
        return carry

    lax.fori_loop(0, here, weights_of, 0)
    for e in range(max(here - buffers, 0), here):
        for copy in stage_copies(e, e % buffers):
            copy.wait()
    for s in whole_slots:
        whole[s].wait_recv()
        for j in evens:
            relay_half[s, j].wait_recv()
            relay_cross[s, j].wait_recv()
    for s in range(done + 1, slots):
        late[s].wait_recv()
        if s + 1 < slots:
            late[s + 1].start()
    hop[slots - 1].wait_recv()
    two_whole.wait_recv()
    for j in evens:
        two_relay[j].wait_recv()
        two_relay_cross[j].wait_recv()
    for copy in net.made:
        copy.wait_send()


def own(table, normed, cotangent, cot_near, cot_two, gate_w, up_w, down_w, experts, slots):
    members = cot_near.shape[0]
    tokens, width = cotangent.shape
    here, _, hidden = gate_w.shape
    rows = members * tokens
    halves = members // 2
    buffers = 2 if members <= 4 else 1
    far = halves - 1
    late = max(slots - 3, 0)
    copies = 1 + 2 * far + (slots - 1) * (2 + 4 * far) + late + halves + far + 1 + 4 * far
    token_block = (tokens, width)
    return pl.pallas_call(
        functools.partial(own_kernel, members, slots, experts),
        out_shape=(
            shape((slots - 2, members, tokens, width + LANES), BF),
            shape((tokens, width + LANES), BF),
            shape((max(late, 1), tokens, width), BF),
            shape((members - 1, tokens, width), BF),
            shape((members, tokens, width), BF),
            shape(token_block, BF),
            shape((PAD, width), F32),
            shape(gate_w.shape, F32),
            shape(up_w.shape, F32),
            shape(down_w.shape, F32),
        ),
        in_specs=[VMEM] + [ANY] * 7,
        out_specs=(ANY, ANY, ANY, ANY, ANY, VMEM, VMEM, ANY, ANY, ANY),
        scratch_shapes=[
            pltpu.VMEM(gate_w.shape, BF),
            pltpu.VMEM(up_w.shape, BF),
            pltpu.VMEM(down_w.shape, BF),
            pltpu.VMEM((members, tokens, width + LANES), BF),
            pltpu.VMEM((members, tokens, width), BF),
            pltpu.VMEM((rows, here * hidden), BF),
            pltpu.VMEM((rows, here * hidden), BF),
            pltpu.VMEM((rows, here * hidden), BF),
            pltpu.VMEM((members,) + token_block, BF),
            pltpu.VMEM((halves,) + token_block, BF),
            pltpu.VMEM((halves,) + token_block, BF),
            pltpu.VMEM((halves,) + token_block, BF),
            pltpu.VMEM((buffers, width, hidden), F32),
            pltpu.VMEM((buffers, width, hidden), F32),
            pltpu.VMEM((buffers, hidden, width), F32),
            pltpu.VMEM((rows, LANES), F32),
            pltpu.VMEM((rows, LANES), F32),
            pltpu.SemaphoreType.DMA((2, copies)),
            pltpu.SemaphoreType.DMA((3, here)),
            pltpu.SemaphoreType.DMA((1 + members,)),
            pltpu.SemaphoreType.DMA((3, buffers)),
            pltpu.VMEM((2,) + token_block, BF),
            pltpu.SemaphoreType.DMA((2,)),
        ],
        compiler_params=pltpu.CompilerParams(
            vmem_limit_bytes=63 << 20, collective_id=1, has_side_effects=True
        ),
        name="own",
        cost_estimate=pl.CostEstimate(
            flops=18 * rows * width * hidden * here,
            bytes_accessed=18 * here * width * hidden,
            transcendentals=0,
        ),
    )(table, normed, cotangent, cot_near, cot_two, gate_w, up_w, down_w)


class Plan:
    def __init__(self, number, ins, outs, scratch, copies, build):
        self.number = number
        self.ins = ins
        self.outs = outs
        self.scratch = scratch
        self.copies = copies
        self.build = build


def more_weights_kernel(sources, counts, plan, experts, begin, index, *refs):
    in_normed, in_cot = counts
    refs = list(refs)

    def take(number):
        front = refs[:number]
        del refs[:number]
        return front

    normed_in = take(in_normed)
    cot_in = take(in_cot)
    gate_w, up_w, down_w, old_gate, old_up, old_down = take(6)
    plan_in = take(len(plan.ins))
    new_gate, new_up, new_down = take(3)
    plan_out = take(len(plan.outs))
    normed, cot, gates, all_inner, all_g, all_u, sems, remote_sems = take(8)
    plan_scratch = refs
    members, tokens, width = cot.shape
    rows = members * tokens
    here = index[1]
    step_at = pl.program_id(0)
    net = Sender(remote_sems)
    devices, begin_plan, ready, after, finish = plan.build(net, plan_in, plan_out, plan_scratch)
    last = pl.num_programs(0) - 1

    @pl.when(step_at == 0)
    def _():
        copies = []
        for group, refs_in, whole in ((0, normed_in, normed), (1, cot_in, cot)):
            for number, lead, first, count in sources[group]:
                ref = refs_in[number]
                ref = ref if lead is None else ref.at[lead]
                place = whole.at[first] if count == 1 else whole.at[pl.ds(first, count)]
                copies.append(pltpu.make_async_copy(ref, place, sems.at[len(copies)]))
        for copy in copies:
            copy.start()
        if devices:
            greet(devices)
        begin_plan()
        for copy in copies:
            copy.wait()
        gates[...] = gates_of(normed[:, :, width:].reshape(rows, LANES), experts)
        ready()

    expert = index[0] * here + begin + step_at
    step = 2 * tokens

    def one_tile(b, carry):
        at = pl.ds(pl.multiple_of(b * step, step), step)
        pair = pl.ds(2 * b, 2)
        _, _, scaled, grad_g, grad_u = hidden_terms(
            normed[pair, :, :width].reshape(step, width),
            cot[pair].reshape(step, width),
            gate_column(gates[at, :], expert),
            gate_w[0],
            up_w[0],
            down_w[0],
        )
        all_inner[at, :] = scaled
        all_g[at, :] = grad_g
        all_u[at, :] = grad_u
        return carry

    straight = plan.number is None and rows <= 1024
    if straight:
        for b in range(rows // step):
            one_tile(b, 0)
    else:
        lax.fori_loop(0, rows // step, one_tile, 0)
    chunk = width // 3

    def one_chunk(k, carry):
        at = pl.ds(pl.multiple_of(k * chunk, LANES), chunk)
        left = normed[:, :, at].reshape(rows, chunk)
        right = cot[:, :, at].reshape(rows, chunk)
        new_gate[0, at, :] = old_gate[0, at, :] + tn(left, all_g[...])
        new_up[0, at, :] = old_up[0, at, :] + tn(left, all_u[...])
        new_down[0, :, at] = old_down[0, :, at] + tn(all_inner[...], right)
        return carry

    lax.fori_loop(0, 3, one_chunk, 0)
    for number, hook in enumerate(after):
        pl.when(step_at == jnp.minimum(number, last))(hook)
    pl.when(step_at == last)(finish)


def more_weights(begin, count, index, normed, cotangent, sources, weights, earlier, experts, plan):
    here, width, hidden = weights[0].shape
    tokens = cotangent[0].shape[-2]
    members = max(first + many for _, _, first, many in sources[1])
    rows = members * tokens
    pick = lambda e: (e + begin, 0, 0)
    wide = pl.BlockSpec((1, width, hidden), pick)
    tall = pl.BlockSpec((1, hidden, width), pick)
    base = 1 + len(normed) + len(cotangent) + 3
    results = pl.pallas_call(
        functools.partial(
            more_weights_kernel,
            sources,
            (len(normed), len(cotangent)),
            plan,
            experts,
            begin,
        ),
        out_shape=tuple(shape(item.shape, F32) for item in earlier)
        + tuple(item for item, _ in plan.outs),
        grid=(count,),
        in_specs=[SMEM]
        + [ANY] * (len(normed) + len(cotangent))
        + [wide, wide, tall] * 2
        + [spec for _, spec in plan.ins],
        out_specs=(wide, wide, tall) + tuple(spec for _, spec in plan.outs),
        scratch_shapes=[
            pltpu.VMEM((members, tokens, width + LANES), BF),
            pltpu.VMEM((members, tokens, width), BF),
            pltpu.VMEM((rows, LANES), F32),
            pltpu.VMEM((rows, hidden), BF),
            pltpu.VMEM((rows, hidden), BF),
            pltpu.VMEM((rows, hidden), BF),
            pltpu.SemaphoreType.DMA((4,)),
            pltpu.SemaphoreType.DMA((2, plan.copies)),
        ]
        + list(plan.scratch),
        input_output_aliases={base + i: i for i in range(3)} if count < here else {},
        compiler_params=pltpu.CompilerParams(
            vmem_limit_bytes=63 << 20,
            collective_id=plan.number,
            has_side_effects=plan.number is not None,
        ),
        name="weights_" + str(plan.number),
        cost_estimate=pl.CostEstimate(
            flops=12 * rows * width * hidden * count,
            bytes_accessed=count * 30 * width * hidden + 4 * rows * width,
            transcendentals=0,
        ),
    )(index, *normed, *cotangent, *weights, *earlier, *[item for item, _ in plan.ins])
    return results[:3], results[3:]


def places(members, slots):
    f = lax.axis_index("fsdp")
    c = lax.axis_index("context")
    t = lax.axis_index("tensor")
    fsdp = {j: {"fsdp": target(f, j, members)} for j in range(1, members)}
    return f, c, t, fsdp, {"tensor": 1 - t}


def nothing():
    pass


def home_plan(number, members, slots, grad_part, moe_parts):
    tokens, width = grad_part.shape
    halves = members // 2
    evens = range(2, members, 2)

    def build(net, ins, outs, scratch):
        part, moe_in = ins
        other, moe_mine = outs
        own_part, swapped, joined, arrived, local = scratch
        f, c, t, fsdp, opposite = places(members, slots)
        cross_part = net.add(part, other, opposite)
        swap = [net.add(moe_in.at[2 * i + 1], swapped.at[i], fsdp[1]) for i in range(halves)]
        home = {
            j: net.add(
                joined.at[j // 2], arrived.at[j // 2], {"fsdp": lax.rem(f + members - j, members)}
            )
            for j in evens
        }
        loads = [
            pltpu.make_async_copy(moe_in.at[2 * i], own_part.at[i], local.at[i])
            for i in range(halves)
        ]

        def start():
            for copy in [cross_part] + swap[1:] + swap[:1] + loads:
                copy.start()

        def ready():
            for copy in loads:
                copy.wait()
            for j in evens:
                swap[j // 2].wait_recv()
                joined[j // 2] = (
                    own_part[j // 2].astype(F32) + swapped[j // 2].astype(F32)
                ).astype(BF)
                home[j].start()

        def finish():
            swap[0].wait_recv()
            total = own_part[0].astype(F32) + swapped[0].astype(F32)
            for j in evens:
                home[j].wait_recv()
                total = total + arrived[j // 2].astype(F32)
            moe_mine[...] = total.astype(BF)
            cross_part.wait_recv()
            for copy in net.made:
                copy.wait_send()

        devices = [fsdp[1], opposite] + [fsdp[j] for j in evens]
        return devices, start, ready, [], finish

    block = (halves, tokens, width)
    return Plan(
        number,
        [(grad_part, ANY), (moe_parts, ANY)],
        [
            (shape((tokens, width), BF), ANY),
            (shape((tokens, width), BF), VMEM),
        ],
        [pltpu.VMEM(block, BF)] * 4 + [pltpu.SemaphoreType.DMA((halves,))],
        1 + halves + halves - 1,
        build,
    )


def keys_plan(number, members, slots, attention, grad_b, normed_last, cot_hops, late):
    heads, grad_heads, att, lse, turns, kv = attention
    _, tokens, cut = grad_b.shape
    wide = normed_last.shape[1]
    width = cot_hops.shape[2]
    side = tokens // 2
    evens = range(2, members, 2)
    groups = lse.shape[0]
    many = lse.shape[2]
    far = members // 2 - 1

    def build(net, ins, outs, scratch):
        heads_ref, grad_ref, att_ref, lse_ref, turns_ref, kv_ref = ins[:6]
        grad_in, last_in, hops_in, att_in = ins[6:]
        grad_q, own_kv, received, grad_near, spread_out, cot_out, att_near = outs
        grad_kv, wide_ref, acc, turned = scratch
        f, c, t, fsdp, opposite = places(members, slots)
        piece = pl.ds(pl.multiple_of(t * side, side), side)
        lower_half, upper_half = pl.ds(0, side), pl.ds(side, side)
        first_back = net.used
        net.used += slots - 1

        def back(s):
            at = first_back + s - 1
            return pltpu.make_async_remote_copy(
                src_ref=grad_kv.at[s - 1],
                dst_ref=received.at[s - 1],
                send_sem=net.sems.at[0, at],
                recv_sem=net.sems.at[1, at],
                device_id={"context": lax.rem(c + slots - s, slots)},
                device_id_type=pl.DeviceIdType.MESH,
            )

        cuts = []
        for j in range(1, members):
            cuts.append(net.add(grad_in.at[j], grad_near.at[j], fsdp[j]))
        sources = [(last_in, spread_out)]
        sources += [(hops_in.at[i], cot_out.at[i]) for i in range(late)]
        att_core = net.add(att_in, att_near.at[1], fsdp[1])
        att_far = [net.add(att_in, att_near.at[j], fsdp[j]) for j in evens]
        att_relay = [net.add(att_near.at[j], att_near.at[j + 1], fsdp[1]) for j in evens]
        whole, half, cross, relay, relay_cross = [], [], [], [], []
        for source, place in sources:
            whole.append(net.add(source, place.at[0], fsdp[1]))
            for j in evens:
                low, high = place.at[j - 1, lower_half], place.at[j - 1, upper_half]
                half.append(net.add(source.at[piece], low, fsdp[j]))
                cross.append(net.add(low, high, opposite))
                relay.append(net.add(low, place.at[j, lower_half], fsdp[1]))
                relay_cross.append(net.add(high, place.at[j, upper_half], fsdp[1]))

        def through(i, carry):
            s = slots - 1 - i

            @pl.when(c >= s)
            def _():
                attend_back_slot(s, heads_ref, grad_ref, lse_ref, kv_ref, wide_ref, acc, own_kv)

                @pl.when(s > 0)
                def _():
                    grad_kv[s - 1] = own_kv[...].astype(BF)
                    back(s).start()

            return carry

        def start():
            for copy in half + att_far + cuts + whole + [att_core]:
                copy.start()
            attend_back_start(heads_ref, grad_ref, att_ref, wide_ref, acc)
            lax.fori_loop(0, slots, through, 0)
            pass_on(0, far)
            attend_back_end(turns_ref, acc, turned, grad_q)

        def pass_on(low, high):
            for copy, following, other in list(zip(half, cross, relay))[low:high]:
                copy.wait_recv()
                following.start()
                other.start()

        def first():
            pass_on(far, len(half))

        def second():
            for copy, following in zip(att_far, att_relay):
                copy.wait_recv()
                following.start()

        def finish():
            for copy, following in zip(cross, relay_cross):
                copy.wait_recv()
                following.start()
            for s in range(1, slots):
                pl.when(c + s < slots)(back(s).wait_recv)
                pl.when(c >= s)(back(s).wait_send)
            for copy in cuts + whole + relay + relay_cross + att_relay + [att_core]:
                copy.wait_recv()
            for copy in net.made:
                copy.wait_send()

        devices = list(fsdp.values()) + [opposite]
        devices += [{"context": lax.rem(c + s, slots)} for s in range(1, slots)]
        return devices, start, nothing, [first, second], finish

    far = members // 2 - 1
    return Plan(
        number,
        [(item, VMEM) for item in attention]
        + [(grad_b, ANY), (normed_last, ANY), (cot_hops, ANY), (att, ANY)],
        [
            (shape(att.shape, BF), VMEM),
            (shape(kv.shape[1:], F32), VMEM),
            (shape((slots - 1,) + kv.shape[1:], BF), ANY),
            (shape((members, tokens, cut), BF), ANY),
            (shape((members - 1, tokens, wide), BF), ANY),
            (shape((max(late, 1), members - 1, tokens, width), BF), ANY),
            (shape((members,) + att.shape, BF), ANY),
        ],
        [
            pltpu.VMEM((slots - 1,) + kv.shape[1:], BF),
            pltpu.VMEM((groups, many, 2 * HEAD), BF),
            pltpu.VMEM((groups, many, HEAD), F32),
            pltpu.VMEM(att.shape, F32),
        ],
        (slots - 1) + (members - 1) + (1 + late) * (1 + 4 * far) + 1 + 2 * far,
        build,
    )


def rows_plan(
    number, members, slots, part_one, joined, router, gain_one, gain_two, payload
):
    tokens, width = part_one.shape
    cut = width // members
    evens = range(2, members, 2)
    rows = payload.shape[0] // slots

    def build(net, ins, outs, scratch):
        part_in, joined_in, router_ref, one_ref, two_ref, payload_in = ins
        other, joined_near, small_near, chunks = outs
        small_mine, small_other, small_sum, small_got, small_cut = scratch
        f, c, t, fsdp, opposite = places(members, slots)
        part_sent = net.add(part_in, other, opposite)
        small_sent = net.add(small_mine, small_other, opposite)
        core = net.add(joined_in, joined_near.at[1], fsdp[1])
        far_copy = {j: net.add(joined_in, joined_near.at[j], fsdp[j]) for j in evens}
        relay = {j: net.add(joined_near.at[j], joined_near.at[j + 1], fsdp[1]) for j in evens}
        small_cuts = []
        for j in range(1, members):
            small_cuts.append(net.add(small_cut.at[j], small_got.at[j], fsdp[j]))
        shares = []
        for s in range(1, slots):
            owner = lax.rem(c + s, slots)
            at = pl.ds(pl.multiple_of(owner * rows, 16), rows)
            shares.append(net.add(payload_in.at[at], chunks.at[s], {"context": owner}))

        def start():
            small = router_ref[...]
            row = lax.broadcasted_iota(jnp.int32, small.shape, 0)
            small = jnp.where(row == PAD - 8, one_ref[...], small)
            small = jnp.where(row == PAD - 7, 0.5 * two_ref[...], small)
            small_mine[...] = small.astype(BF)
            small_sent.start()
            for copy in [part_sent, core] + [far_copy[j] for j in evens] + shares:
                copy.start()

        def ready():
            small_sent.wait_recv()
            small_sum[...] = (small_mine[...].astype(F32) + small_other[...].astype(F32)).astype(BF)
            small_got[0] = columns_of(small_sum, f, cut)
            for j in range(1, members):
                small_cut[j] = columns_of(small_sum, target(f, j, members), cut)
            for copy in small_cuts:
                copy.start()

        def second():
            for j in evens:
                far_copy[j].wait_recv()
                relay[j].start()

        def finish():
            for copy in [part_sent, core] + [relay[j] for j in evens] + small_cuts + shares:
                copy.wait_recv()
            small_near[...] = small_got[...]
            for copy in net.made:
                copy.wait_send()

        devices = list(fsdp.values()) + [opposite]
        devices += [{"context": lax.rem(c + s, slots)} for s in range(1, slots)]
        return devices, start, ready, [nothing, second], finish

    far = members // 2 - 1
    small = (PAD, width)
    return Plan(
        number,
        [(part_one, ANY), (joined, ANY)]
        + [(router, VMEM), (gain_one, VMEM), (gain_two, VMEM), (payload, ANY)],
        [
            (shape((tokens, width), BF), ANY),
            (shape((members,) + joined.shape, BF), ANY),
            (shape((members, PAD, cut), BF), VMEM),
            (shape((slots, rows, payload.shape[1]), BF), ANY),
        ],
        [pltpu.VMEM(small, BF)] * 3 + [pltpu.VMEM((members, PAD, cut), BF)] * 2,
        2 + 1 + 2 * far + (members - 1) + (slots - 1),
        build,
    )


def chunk_plan(number, members, slots, payload, moe_mine):
    rows = payload.shape[0] // slots

    def build(net, ins, outs, scratch):
        f, c, t, fsdp, opposite = places(members, slots)
        copies = [net.add(ins[1], outs[1], opposite)]
        for s in range(1, slots):
            owner = lax.rem(c + s, slots)
            at = pl.ds(pl.multiple_of(owner * rows, 16), rows)
            copies.append(net.add(ins[0].at[at], outs[0].at[s], {"context": owner}))

        def start():
            for copy in copies:
                copy.start()

        def finish():
            for copy in copies:
                copy.wait_recv()
                copy.wait_send()

        devices = [{"context": lax.rem(c + s, slots)} for s in range(1, slots)]
        return devices + [opposite], start, nothing, [], finish

    return Plan(
        number,
        [(payload, ANY), (moe_mine, ANY)],
        [
            (shape((slots, rows, payload.shape[1]), BF), ANY),
            (shape(moe_mine.shape, BF), ANY),
        ],
        [],
        slots,
        build,
    )


def middle_kernel(members, index, hidden_ref, cot_ref, mine_ref, theirs_ref, table_ref, weights_ref, *refs):
    grad_ref, grad_b_ref, heads_ref, gain_ref, rounded, columns, summed = refs
    f = index[0]
    cut = weights_ref.shape[2]
    hidden = hidden_ref[...]
    normed_grad = mine_ref[...].astype(F32) + theirs_ref[...].astype(F32)
    scale = lax.rsqrt(jnp.mean(hidden * hidden, axis=-1, keepdims=True) + norm_eps)
    gain = table_ref[...].astype(F32)[PAD - 7 : PAD - 6, :]
    weighted = normed_grad * gain
    cubed = scale * scale * scale
    grad = (
        cot_ref[...].astype(F32)
        + scale * weighted
        - hidden * cubed * jnp.mean(weighted * hidden, axis=-1, keepdims=True)
    )
    gain_ref[...] = jnp.sum(normed_grad * hidden * scale, axis=0, keepdims=True)
    grad_ref[...] = grad
    rounded[...] = grad.astype(BF)
    for j in range(members):
        grad_b_ref[j] = columns_of(rounded, target(f, j, members), cut)
        columns[j] = columns_of(rounded, member(f, j, members), cut)
    summed[...] = nt(columns[0], weights_ref[0])

    def one_member(j, carry):
        summed[...] += nt(columns[j], weights_ref[j])
        return carry

    lax.fori_loop(1, members, one_member, 0)
    total = summed[...].astype(BF)
    for h in range(heads_ref.shape[0]):
        heads_ref[h] = total[:, h * HEAD : (h + 1) * HEAD]


def middle(index, hidden, cotangent, mine, theirs, table, weights, after=()):
    members = weights.shape[0]
    tokens, width = hidden.shape
    heads = weights[0].shape[0] // HEAD
    return call(
        functools.partial(middle_kernel, members),
        (
            shape((tokens, width), F32),
            shape((members, tokens, width // members), BF),
            shape((heads, tokens, HEAD), BF),
            shape((1, width), F32),
        ),
        [SMEM] + [VMEM] * 6,
        (VMEM,) * 4,
        [
            pltpu.VMEM((tokens, width), BF),
            pltpu.VMEM((members, tokens, width // members), BF),
            pltpu.VMEM((tokens, heads * HEAD), F32),
        ],
        2 * tokens * width * heads * HEAD,
        16 * tokens * width,
        "middle",
        after,
    )(index, hidden, cotangent, mine, theirs, table, weights)


def lower_kernel(members, slots, index, grad_q_ref, own_ref, rows_ref, turns_ref, *refs):
    others = refs[0]
    weights = refs[1]
    joined_ref, part_ref, gain_ref = refs[2:]
    f = index[0]
    cut = weights.shape[1]
    total = own_ref[...]
    for s in range(1, slots):
        total = total + jnp.where(index[1] + s < slots, others[s - 1].astype(F32), 0.0)
    half = total.shape[1] // 2
    q_wide = grad_q_ref.shape[1]
    joined_ref[:, :q_wide] = grad_q_ref[...]
    keys = rotate(total[:, :half], turns_ref[:, :LANES], -turns_ref[:, LANES:])
    joined_ref[:, q_wide : q_wide + half] = keys.astype(BF)
    joined_ref[:, q_wide + half :] = total[:, half:].astype(BF)
    rows = rows_ref[...].astype(F32)
    scale = lax.rsqrt(jnp.mean(rows * rows, axis=-1, keepdims=True) + norm_eps)

    def one_pair(p, carry):
        owner = lax.rem(f + members - 2 * p, members)
        first = nt(joined_ref[...], weights[2 * p]).astype(BF)
        second = nt(joined_ref[...], weights[2 * p + 1]).astype(BF)
        put_columns(part_ref, owner, first, second)
        return carry

    lax.fori_loop(0, members // 2, one_pair, 0)
    gain_ref[...] = jnp.sum(part_ref[...].astype(F32) * rows * scale, axis=0, keepdims=True)


def lower(index, grad_q, own_kv, others, rows, turns, weights, after=()):
    members = len(weights)
    tokens, width = rows.shape
    wide = weights[0].shape[1]
    return call(
        functools.partial(lower_kernel, members, others.shape[0] + 1),
        (shape((tokens, wide), BF), shape((tokens, width), BF), shape((1, width), F32)),
        [SMEM] + [VMEM] * 6,
        (VMEM,) * 3,
        [],
        2 * tokens * width * wide,
        2 * width * wide,
        "lower",
        after,
    )(index, grad_q, own_kv, rows, turns, others, weights)


def last_kernel(
    rows_ref, grad_ref, mine_ref, theirs_ref, table_ref, hidden_ref, moe_ref, other_ref, out_ref, result_ref
):
    moe = moe_ref[...].astype(F32) + other_ref[...].astype(F32)
    result_ref[...] = (hidden_ref[...] + moe).astype(BF)
    rows = rows_ref[...].astype(F32)
    normed_grad = mine_ref[...].astype(F32) + theirs_ref[...].astype(F32)
    scale = lax.rsqrt(jnp.mean(rows * rows, axis=-1, keepdims=True) + norm_eps)
    gain = table_ref[...].astype(F32)[PAD - 8 : PAD - 7, :]
    weighted = normed_grad * gain
    cubed = scale * scale * scale
    out_ref[...] = (
        grad_ref[...]
        + scale * weighted
        - rows * cubed * jnp.mean(weighted * rows, axis=-1, keepdims=True)
    ).astype(BF)


def last(rows, grad, mine, theirs, table, hidden, moe, other):
    tokens, width = rows.shape
    return call(
        last_kernel,
        (shape((tokens, width), BF), shape((tokens, width), BF)),
        [VMEM] * 8,
        (VMEM, VMEM),
        [],
        16 * tokens * width,
        20 * tokens * width,
        "last",
    )(rows, grad, mine, theirs, table, hidden, moe, other)


def product_kernel(extra, left_own, left, right_own, right, *refs):
    members = left.shape[0]
    out_ref = refs[-2]
    mine = [ref[0] if len(ref.shape) == 3 else ref[...] for ref in (left_own, right_own)]
    summed = refs[-1]
    summed[...] = tn(*mine)

    def one_member(j, carry):
        summed[...] += tn(left[j], right[j])
        return carry

    lax.fori_loop(1, members, one_member, 0)
    total = summed[...]
    rows, columns = total.shape
    out_ref[:rows, :] = total.astype(BF)
    if extra:
        small = refs[0]
        summed = small[0].astype(F32)
        for j in range(1, members):
            summed = summed + small[j].astype(F32)
        out_ref[rows:, :] = jnp.zeros((out_ref.shape[0] - rows, columns), BF)
        out_ref[rows : rows + PAD, : summed.shape[1]] = summed.astype(BF)


def product(left_own, left, right_own, right, small, extra_rows, name):
    members, tokens, rows = left.shape
    columns = right.shape[2]
    return call(
        functools.partial(product_kernel, len(small)),
        shape((rows + extra_rows, columns), BF),
        [VMEM] * (4 + len(small)),
        VMEM,
        [pltpu.VMEM((rows, columns), F32)],
        2 * members * tokens * rows * columns,
        4 * rows * columns,
        name,
    )(left_own, left, right_own, right, *small)


def sum_kernel(index, whole_ref, parts_ref, out_ref):
    slots, rows, _ = parts_ref.shape
    at = pl.ds(pl.multiple_of(index[1] * rows, 16), rows)
    total = whole_ref[at, :].astype(F32)
    for s in range(1, slots):
        total = total + parts_ref[s].astype(F32)
    out_ref[...] = total.astype(BF)


def sum_of(index, whole, parts, name):
    slots, rows, columns = parts.shape
    return call(
        sum_kernel,
        shape((rows, columns), BF),
        [SMEM, VMEM, VMEM],
        VMEM,
        [],
        slots * rows * columns,
        2 * (slots + 1) * rows * columns,
        name,
    )(index, whole, parts)


def joint_sum_kernel(index, whole_ref, parts_ref, more_ref, out_ref):
    slots, rows, wide = parts_ref.shape
    at = pl.ds(pl.multiple_of(index[1] * rows, 16), rows)
    total = whole_ref[at, :].astype(F32)
    for s in range(1, slots):
        total = total + parts_ref[s].astype(F32)
    out_ref[:rows, :] = total.astype(BF)
    many, columns = more_ref.shape
    fold = wide // columns
    each = many // fold
    out_ref[rows:, :] = jnp.zeros((each, wide), BF)
    for k in range(fold):
        out_ref[rows:, k * columns : (k + 1) * columns] = more_ref[k * each : (k + 1) * each, :]


def joint_sum(index, whole, parts, more):
    slots, rows, columns = parts.shape
    extra = more.shape[0] // (columns // more.shape[1])
    return call(
        joint_sum_kernel,
        shape((rows + extra, columns), BF),
        [SMEM, VMEM, VMEM, VMEM],
        VMEM,
        [],
        slots * rows * columns,
        2 * (slots + 1) * rows * columns,
        "joint_sum",
    )(index, whole, parts, more)


def spread_kernel(slots, experts, index, *refs):
    parts = refs[:slots]
    query_ref, key_ref, value_ref, out_ref, one_ref, two_ref, router_ref, whole = refs[slots:]
    place = index[1]
    cut, q_wide = query_ref.shape
    kv_wide = key_ref.shape[1]
    rows = whole.shape[0] // slots
    many, columns = out_ref.shape
    each = parts[0].shape[0] - rows
    fold = parts[0].shape[1] // columns
    for s in range(slots):
        owner = lax.rem(place + slots - s, slots)
        whole[pl.ds(pl.multiple_of(owner * rows, 16), rows), :] = parts[s][:rows, :].astype(F32)
        for k in range(fold):
            base = owner * (many // slots) + k * each
            out_ref[pl.ds(pl.multiple_of(base, 16), each), :] = parts[s][
                rows:, k * columns : (k + 1) * columns
            ].astype(F32)
    query_ref[...] = whole[:cut, :q_wide]
    key_ref[...] = whole[:cut, q_wide : q_wide + kv_wide]
    value_ref[...] = whole[:cut, q_wide + kv_wide :]
    small = whole[cut : cut + PAD, :cut]
    one_ref[...] = small[PAD - 8]
    two_ref[...] = small[PAD - 7]
    router_ref[...] = small[:experts]


def spread(index, parts, rows, dims, experts):
    slots = len(parts)
    columns = parts[0].shape[1]
    return call(
        functools.partial(spread_kernel, slots, experts),
        tuple(shape(item, F32) for item in dims),
        [SMEM] + [VMEM] * slots,
        (VMEM,) * len(dims),
        [pltpu.VMEM((slots * rows, columns), F32)],
        slots * rows * columns,
        6 * slots * rows * columns,
        "spread",
    )(index, *parts)


def build(members, slots):
    def ring(item, step):
        return lax.ppermute(item, "context", [(i, (i + step) % slots) for i in range(slots)])

    def per_device(
        tokens,
        positions,
        expert_ids,
        norm1_gain,
        w_query,
        w_key,
        w_value,
        w_out,
        norm2_gain,
        w_router,
        w_gate,
        w_up,
        w_down,
        grad_output,
    ):
        rows = tokens[0]
        cotangent = grad_output[0]
        block = rows.shape[0]
        width = rows.shape[1]
        experts = w_router.shape[1]
        here = w_gate.shape[0]
        kv_wide = w_key.shape[1]
        q_wide = w_query.shape[1]
        f = lax.axis_index("fsdp")
        c = lax.axis_index("context")
        c_index = c.reshape(1)
        index = jnp.stack([f, c])
        f_here = jnp.stack([f, jnp.int32(here)])

        half = HEAD // 2
        lane = np.arange(2 * LANES)
        freq = np.exp(-math.log(10000.0) * 2.0 * np.arange(half, dtype=np.float32) / HEAD)
        sign = np.where(lane % HEAD < half, -1.0, 1.0).astype(np.float32)
        angle = positions[0].astype(F32)[:, None] * freq.astype(np.float32)[lane % half][None, :]
        turns = jnp.where((lane < LANES)[None, :], jnp.cos(angle), jnp.sin(angle) * sign[None, :])

        (
            table,
            normed_one,
            heads,
            kv_slots,
            att,
            lse,
            hidden,
            normed,
            qkv_w,
            out_mine,
            cot_near,
            cot_done,
            cot_two,
            normed_near,
            normed_cut,
        ) = forward(
            (w_query, w_key, w_value),
            w_out,
            cotangent,
            (w_router.T, norm1_gain, norm2_gain),
            rows,
            turns,
            expert_ids[0].T,
            members,
            slots,
        )

        results = own(
            table, normed, cotangent, cot_near, cot_two, w_gate, w_up, w_down, experts, slots
        )
        normed_slots, normed_last, cot_hops, two_far, moe_parts = results[:5]
        grad_part, router_grad, *expert_grads = results[5:]


        parts = 2 if here % 2 == 0 else here
        queue = []
        for s in range(1, slots - 1):
            queue += [(s, p * (here // parts), here // parts) for p in range(parts)]

        def fill(plan, item, grads, normed_far=None, cot_far=None):
            s, begin, many = item
            if s < slots - 1:
                normed_refs, normed_from = [normed_slots], ((0, s - 1, 0, members),)
            else:
                normed_refs = [normed_last, normed_far]
                normed_from = ((0, None, 0, 1), (1, None, 1, members - 1))
            if s == 1:
                cot_refs, cot_from = [cot_done], ((0, 0, 0, members),)
            else:
                cot_refs = [cot_two, two_far] if s == 2 else [cot_hops, cot_far]
                lead = None if s == 2 else s - 3
                cot_from = ((0, lead, 0, 1), (1, lead, 1, members - 1))
            return more_weights(
                begin,
                many,
                f_here,
                normed_refs,
                cot_refs,
                (normed_from, cot_from),
                (w_gate, w_up, w_down),
                grads,
                experts,
                plan,
            )

        plan = home_plan(2, members, slots, grad_part, moe_parts)
        expert_grads, (grad_other, moe_mine) = fill(plan, queue[0], expert_grads)

        grad_hidden, grad_hidden_b, grad_heads, gain_two = middle(
            index, hidden, cotangent, grad_part, grad_other, table, out_mine
        )
        attention = (heads, grad_heads, att, lse, turns, kv_slots)
        plan = keys_plan(
            3, members, slots, attention, grad_hidden_b, normed_last, cot_hops, max(slots - 3, 0)
        )
        expert_grads, results = fill(plan, queue[1], expert_grads)
        grad_q, own_kv, received, grad_near, normed_far, cot_far, att_near = results
        out_payload = product(att, att_near, grad_hidden_b, grad_near, (), 0, "out_grad")
        joined, part_one, gain_one = lower(
            index, grad_q, own_kv, received, rows, turns, qkv_w
        )
        plan = rows_plan(
            4,
            members,
            slots,
            part_one,
            joined,
            router_grad,
            gain_one,
            gain_two,
            out_payload,
        )
        expert_grads, results = fill(plan, queue[2], expert_grads, normed_far, cot_far)
        other_one, joined_near, small_near, out_chunks = results
        payload = product(
            normed_cut, normed_near, joined, joined_near, (small_near,), 2 * PAD, "qkv_grad"
        )
        out_total = sum_of(index, out_payload, out_chunks, "out_sum")
        plan = chunk_plan(5, members, slots, payload, moe_mine)
        expert_grads, (qkv_chunks, moe_other) = fill(
            plan, queue[3], expert_grads, normed_far, cot_far
        )
        total = joint_sum(index, payload, qkv_chunks, out_total)
        shared = [total] + [ring(total, s) for s in range(1, slots)]
        grad_tokens, output = last(
            rows, grad_hidden, part_one, other_one, table, hidden, moe_mine, moe_other
        )
        none = Plan(None, [], [], [], 1, lambda *_: ([], nothing, nothing, [], nothing))
        for item in queue[4:] + [(slots - 1, 0, here)]:
            expert_grads, _ = fill(none, item, expert_grads, normed_far, cot_far)
        cut = w_query.shape[0]
        grad_query, grad_key, grad_value, grad_out, grad_one, grad_two, grad_router = spread(
            index,
            shared,
            payload.shape[0] // slots,
            (
                w_query.shape,
                w_key.shape,
                w_value.shape,
                w_out.shape,
                (cut,),
                (cut,),
                (experts, cut),
            ),
            experts,
        )
        return (
            output[None],
            grad_tokens[None],
            grad_one,
            grad_query,
            grad_key,
            grad_value,
            grad_out,
            grad_two,
            grad_router.T,
            expert_grads[0],
            expert_grads[1],
            expert_grads[2],
        )

    return per_device


def solution(mesh):
    return jax.shard_map(
        build(mesh.shape["fsdp"], mesh.shape["context"]),
        mesh=mesh,
        in_specs=(
            P("fsdp", "context", None),
            P("fsdp", "context"),
            P("fsdp", "context", None),
            P("fsdp"),
            P("fsdp", "tensor"),
            P("fsdp", "tensor"),
            P("fsdp", "tensor"),
            P("tensor", "fsdp"),
            P("fsdp"),
            P("fsdp", None),
            P("fsdp", None, "tensor"),
            P("fsdp", None, "tensor"),
            P("fsdp", "tensor", None),
            P("fsdp", "context", None),
        ),
        out_specs=(
            P("fsdp", "context", None),
            P("fsdp", "context", None),
            P("fsdp"),
            P("fsdp", "tensor"),
            P("fsdp", "tensor"),
            P("fsdp", "tensor"),
            P("tensor", "fsdp"),
            P("fsdp"),
            P("fsdp", None),
            P("fsdp", None, "tensor"),
            P("fsdp", None, "tensor"),
            P("fsdp", "tensor", None),
        ),
        check_vma=False,
    )
```

```python
import functools
import math

import jax
import jax.numpy as jnp
import numpy as np
from jax import lax
from jax.experimental import pallas as pl
from jax.experimental.pallas import tpu as pltpu
from jax.sharding import PartitionSpec as P

HEAD = 64
LANES = 128
PAD = 32
norm_eps = 1e-06
masked_score = -1e30
BF = jnp.bfloat16
F32 = jnp.float32
VMEM = pl.BlockSpec(memory_space=pltpu.VMEM)
SMEM = pl.BlockSpec(memory_space=pltpu.SMEM)
ANY = pl.BlockSpec(memory_space=pl.ANY)


def nn(left, right):
    return jnp.dot(left, right, preferred_element_type=F32)


def nt(left, right):
    return lax.dot_general(left, right, (((1,), (1,)), ((), ())), preferred_element_type=F32)


def tn(left, right):
    return lax.dot_general(left, right, (((0,), (0,)), ((), ())), preferred_element_type=F32)


def partner(f):
    return f + 1 - 2 * lax.rem(f, 2)


def member(f, j, members):
    base = lax.rem(f + members - (j - j % 2), members)
    return base if j % 2 == 0 else partner(base)


def columns_of(ref, owner, cut):
    if cut % LANES == 0:
        return ref[:, pl.ds(pl.multiple_of(owner * cut, LANES), cut)]
    pair = ref[:, pl.ds(pl.multiple_of(lax.div(owner, 2) * (2 * cut), LANES), 2 * cut)]
    return jnp.where(lax.rem(owner, 2) == 0, pair[:, :cut], pair[:, cut:])


def put_columns(ref, owner, first, second):
    cut = first.shape[1]
    if cut % LANES == 0:
        ref[:, pl.ds(pl.multiple_of(owner * cut, LANES), cut)] = first
        ref[:, pl.ds(pl.multiple_of(partner(owner) * cut, LANES), cut)] = second
    else:
        even = lax.rem(owner, 2) == 0
        both = [jnp.where(even, first, second), jnp.where(even, second, first)]
        at = pl.ds(pl.multiple_of(lax.div(owner, 2) * (2 * cut), LANES), 2 * cut)
        ref[:, at] = jnp.concatenate(both, axis=1)


def shape(dims, kind):
    return jax.ShapeDtypeStruct(dims, kind)


def call(kernel, outs, specs, out_specs, scratch, flops, moved, name, after=(), **more):
    skip = len(after)

    def body(*refs):
        kernel(*refs[skip:])

    run = pl.pallas_call(
        body,
        out_shape=outs,
        in_specs=[ANY] * skip + list(specs),
        out_specs=out_specs,
        scratch_shapes=scratch,
        compiler_params=pltpu.CompilerParams(vmem_limit_bytes=60 << 20),
        name=name,
        cost_estimate=pl.CostEstimate(flops=flops, bytes_accessed=moved, transcendentals=0),
        **more,
    )
    return lambda *operands: run(*after, *operands)


def rotate(rows, cos, sin):
    wide = rows.shape[1]
    count = wide // LANES
    after = pltpu.roll(rows, wide - HEAD // 2, 1)
    before = pltpu.roll(rows, HEAD // 2, 1)
    lane = lax.broadcasted_iota(jnp.int32, rows.shape, 1) % HEAD
    partner = jnp.where(lane < HEAD // 2, after, before)
    cos_all = jnp.concatenate([cos] * count, axis=1)
    sin_all = jnp.concatenate([sin] * count, axis=1)
    return rows * cos_all + partner * sin_all


class Sender:
    def __init__(self, sems):
        self.sems = sems
        self.used = 0
        self.made = []

    def add(self, source, target, device):
        copy = pltpu.make_async_remote_copy(
            src_ref=source,
            dst_ref=target,
            send_sem=self.sems.at[0, self.used],
            recv_sem=self.sems.at[1, self.used],
            device_id=device,
            device_id_type=pl.DeviceIdType.MESH,
        )
        self.used += 1
        self.made.append(copy)
        return copy


def greet(devices):
    barrier = pltpu.get_barrier_semaphore()
    for device in devices:
        pl.semaphore_signal(
            barrier, inc=1, device_id=device, device_id_type=pl.DeviceIdType.MESH
        )
    pl.semaphore_wait(barrier, len(devices))


def target(f, j, members):
    start = f if j % 2 == 0 else partner(f)
    return lax.rem(start + j - j % 2, members)


def attend_slot(s, heads_ref, kv, top, sums, acc):
    groups = top.shape[0]
    tokens = heads_ref.shape[1]
    repeat = heads_ref.shape[0] // groups
    half = kv.shape[2] // 2
    many = repeat * tokens
    keys = lax.broadcasted_iota(jnp.int32, (tokens, many), 0)
    queries = lax.broadcasted_iota(jnp.int32, (tokens, many), 1) % tokens
    allowed = keys <= queries + jnp.where(s == 0, 0, tokens)
    for g in range(groups):
        q = heads_ref[g * repeat : (g + 1) * repeat].reshape(many, HEAD)
        score = jnp.where(allowed, nt(kv[s, :, g * HEAD : (g + 1) * HEAD], q), masked_score)
        value = kv[s, :, half + g * HEAD : half + (g + 1) * HEAD]
        old = top[g]
        high = jnp.maximum(old, jnp.max(score, axis=0, keepdims=True))
        shrink = jnp.exp(old - high)
        weight = jnp.where(allowed, jnp.exp(score - high), 0.0)
        sums[g] = sums[g] * shrink + jnp.sum(weight, axis=0, keepdims=True)
        acc[g] = acc[g] * shrink + tn(value, weight.astype(BF))
        top[g] = high


def attend_end(att_ref, lse_ref, top, sums, acc):
    groups, _, many = top.shape
    tokens = att_ref.shape[0]
    repeat = many // tokens
    for g in range(groups):
        lse_ref[g] = top[g] + jnp.log(sums[g])
        done = jnp.transpose(acc[g] / sums[g]).astype(BF)
        for r in range(repeat):
            h = g * repeat + r
            att_ref[:, h * HEAD : (h + 1) * HEAD] = done[r * tokens : (r + 1) * tokens]


def forward_kernel(
    members,
    slots,
    query_in,
    key_in,
    value_in,
    wout_in,
    cot_in,
    router_ref,
    one_ref,
    two_ref,
    rows_ref,
    turns_ref,
    ids_ref,
    *refs,
):
    (
        table_ref,
        normed_one_ref,
        heads_ref,
        kv_out,
        att_ref,
        lse_ref,
        hidden_ref,
        normed_ref,
        qkv_out,
        wout_out,
        cot_near,
        cot_done,
        cot_two,
        cut_ref,
        small,
        qkv,
        mine,
        theirs,
        kv,
        total,
        first,
        second,
        other,
        top,
        sums,
        acc,
        sems,
        local_sems,
    ) = refs
    f = lax.axis_index("fsdp")
    c = lax.axis_index("context")
    t = lax.axis_index("tensor")
    tokens, width = rows_ref.shape
    side = tokens // 2
    experts, cut = router_ref.shape
    evens = range(2, members, 2)
    beside = {"fsdp": partner(f)}
    opposite = {"tensor": 1 - t}
    ahead = {"context": lax.rem(c + 1, slots)}
    apart = {j: {"fsdp": lax.rem(f + j, members)} for j in evens}
    lower_half, upper_half = pl.ds(0, side), pl.ds(side, side)
    piece = pl.ds(pl.multiple_of(t * side, side), side)

    net = Sender(sems)
    small_sent = [
        net.add(small.at[0], small.at[j], {"fsdp": target(f, j, members)}) for j in range(1, members)
    ]

    def family(source, place):
        return (
            net.add(source, place.at[1], beside),
            {j: net.add(source, place.at[j], apart[j]) for j in evens},
            {j: net.add(place.at[j], place.at[j + 1], beside) for j in evens},
        )

    q_wide, kv_wide = query_in.shape[1], key_in.shape[1]
    bounds = (0, q_wide, q_wide + kv_wide, q_wide + 2 * kv_wide)
    projections = [
        (source, pl.ds(low, high - low))
        for source, low, high in zip((query_in, key_in, value_in), bounds, bounds[1:])
    ]
    groups_of = {"query": projections[:1], "keys": projections[1:]}
    spans = {"query": pl.ds(0, q_wide), "keys": pl.ds(q_wide, 2 * kv_wide)}
    qkv_core, qkv_far, qkv_relay = {}, {}, {}
    for name in ("keys", "query"):
        qkv_core[name] = [net.add(source, qkv.at[1, :, at], beside) for source, at in groups_of[name]]
        qkv_far[name] = {
            j: [net.add(source, qkv.at[j, :, at], apart[j]) for source, at in groups_of[name]]
            for j in evens
        }
        span = spans[name]
        qkv_relay[name] = {
            j: net.add(qkv.at[j, :, span], qkv.at[j + 1, :, span], beside) for j in evens
        }
    out_core, out_far, out_relay = family(wout_in, mine)
    out_cross = {j: net.add(wout_in if j == 0 else mine.at[j], theirs.at[j], opposite) for j in range(0, members, 2)}
    out_cross_relay = {j: net.add(theirs.at[j], theirs.at[j + 1], beside) for j in range(0, members, 2)}
    cot_core, cot_far, cot_relay = family(cot_in, cot_near)
    done = cot_done.shape[0]
    hop, whole, half, cross, relay_half, relay_cross = {}, {}, {}, {}, {}, {}
    hop[1] = net.add(cot_in, cot_done.at[0, 0], ahead)
    if slots > 2:
        hop[2] = net.add(cot_done.at[0, 0], cot_two, ahead)
    for s in range(1, done + 1):
        now = cot_done.at[s - 1]
        whole[s] = net.add(now.at[0], now.at[1], beside)
        for j in evens:
            half[s, j] = net.add(now.at[0, piece], now.at[j, lower_half], apart[j])
            cross[s, j] = net.add(now.at[j, lower_half], now.at[j, upper_half], opposite)
            relay_half[s, j] = net.add(now.at[j, lower_half], now.at[j + 1, lower_half], beside)
            relay_cross[s, j] = net.add(now.at[j, upper_half], now.at[j + 1, upper_half], beside)
    plain = len(net.made)
    first_later = net.used
    net.used += slots - 1

    def later(s):
        at = first_later + s - 1
        return pltpu.make_async_remote_copy(
            src_ref=kv.at[s - 1],
            dst_ref=kv.at[s],
            send_sem=sems.at[0, at],
            recv_sem=sems.at[1, at],
            device_id=ahead,
            device_id_type=pl.DeviceIdType.MESH,
        )

    plain_made = net.made[:plain]
    att_sent = net.add(att_ref, other, opposite)

    locals_in = [
        pltpu.make_async_copy(source, qkv.at[0, :, at], sem)
        for (source, at), sem in zip(projections, [local_sems.at[i] for i in (0, 1, 2)])
    ]
    locals_in.append(pltpu.make_async_copy(wout_in, mine.at[0], local_sems.at[5 + slots]))
    qkv_saved = pltpu.make_async_copy(qkv, qkv_out, local_sems.at[3])
    out_saved = pltpu.make_async_copy(mine, wout_out, local_sems.at[4])
    kv_saved = [
        pltpu.make_async_copy(kv.at[s], kv_out.at[s], local_sems.at[5 + s]) for s in range(slots)
    ]
    for copy in locals_in:
        copy.start()
    small[0] = jnp.zeros((PAD, cut), BF)
    small[0, :experts, :] = router_ref[...]
    small[0, PAD - 8, :] = one_ref[...]
    small[0, PAD - 7, :] = two_ref[...]
    greet(
        [{"fsdp": target(f, j, members)} for j in range(1, members)]
        + [opposite]
        + [ahead, {"context": lax.rem(c + slots - 1, slots)}]
    )
    for copy in small_sent:
        copy.start()
    for name in ("keys", "query"):
        for copies in [qkv_core[name]] + [qkv_far[name][j] for j in evens]:
            for copy in copies:
                copy.start()
    for copy in [out_core, out_cross[0]] + [out_far[j] for j in evens]:
        copy.start()
    hop[1].start()
    cot_core.start()

    rows = rows_ref[...].astype(F32)
    scale = lax.rsqrt(jnp.mean(rows * rows, axis=-1, keepdims=True) + norm_eps)
    hidden_ref[...] = rows * scale
    for copy in locals_in:
        copy.wait()
    for copy in small_sent:
        copy.wait_recv()

    for j in range(0, members, 2):
        put_columns(table_ref, member(f, j, members), small[j], small[j + 1])
    gain = table_ref[...].astype(F32)[PAD - 8 : PAD - 7, :]
    normed_one_ref[...] = (hidden_ref[...] * gain).astype(BF)
    for j in range(members):
        cut_ref[j] = columns_of(normed_one_ref, target(f, j, members), cut)

    total[...] = jnp.zeros(total.shape, F32)

    def product_of(name):
        span = spans[name]

        def far_arrived(j):
            for copy in qkv_far[name][j]:
                copy.wait_recv()
            qkv_relay[name][j].start()

        def core_arrived():
            for copy in qkv_core[name]:
                copy.wait_recv()

        def one_pair(p, carry):
            owner = lax.rem(f + members - 2 * p, members)
            for j in evens:
                pl.when(2 * p == j)(functools.partial(far_arrived, j))
            left = columns_of(normed_one_ref, owner, cut)
            total[:, span] += nn(left, qkv[2 * p, :, span])
            pl.when(p == 0)(core_arrived)
            for j in evens:
                pl.when(2 * p == j)(qkv_relay[name][j].wait_recv)
            left = columns_of(normed_one_ref, partner(owner), cut)
            total[:, span] += nn(left, qkv[2 * p + 1, :, span])
            return carry

        lax.fori_loop(0, members // 2, one_pair, 0)

    cos = turns_ref[:, :LANES]
    sin = turns_ref[:, LANES:]
    product_of("keys")
    kv[0, :, :kv_wide] = rotate(total[:, q_wide : q_wide + kv_wide], cos, sin).astype(BF)
    kv[0, :, kv_wide:] = total[:, q_wide + kv_wide :].astype(BF)
    pl.when(c + 1 < slots)(later(1).start)
    hop[1].wait_recv()
    if slots > 2:
        pl.when(c == slots - 1)(hop[2].start)
    whole[1].start()
    for j in evens:
        half[1, j].start()
    for j in evens:
        cot_far[j].start()
    product_of("query")
    qkv_saved.start()
    turned = (rotate(total[:, :q_wide], cos, sin) * (1.0 / math.sqrt(HEAD))).astype(BF)
    for h in range(q_wide // HEAD):
        heads_ref[h] = turned[:, h * HEAD : (h + 1) * HEAD]
    top[...] = jnp.full(top.shape, masked_score, F32)
    sums[...] = jnp.zeros(sums.shape, F32)
    acc[...] = jnp.zeros(acc.shape, F32)
    def weights_arrived():
        for j in evens:
            out_far[j].wait_recv()
            out_relay[j].start()
            out_cross[j].start()
        out_cross[0].wait_recv()
        out_cross_relay[0].start()


    def half_arrived(s):
        for j in evens:
            half[s, j].wait_recv()
            relay_half[s, j].start()
            cross[s, j].start()

    def keys_arrived(s, carry):
        @pl.when(c >= s)
        def _():
            @pl.when(s > 0)
            def _():
                later(s).wait_recv()

                @pl.when((c + 1 < slots) & (s + 1 < slots))
                def _():
                    later(s + 1).start()

            if slots > 2:
                pl.when((s == c) & (c + 1 < slots))(hop[2].start)
            attend_slot(s, heads_ref, kv, top, sums, acc)

        pl.when(s == 0)(weights_arrived)
        pl.when(s == 1)(functools.partial(half_arrived, 1))
        return carry

    lax.fori_loop(0, slots, keys_arrived, 0)
    kv_saved[0].start()
    for s in range(1, slots):
        pl.when(c >= s)(kv_saved[s].start)
    attend_end(att_ref, lse_ref, top, sums, acc)
    att_sent.start()

    out_core.wait_recv()
    for j in evens:
        out_relay[j].wait_recv()
    out_saved.start()
    def mixed(left, weights, place):
        def one_pair(p, carry):
            owner = lax.rem(f + members - 2 * p, members)
            pair = nn(left[...], weights[2 * p]), nn(left[...], weights[2 * p + 1])
            put_columns(place, owner, *pair)
            return carry

        lax.fori_loop(0, members // 2, one_pair, 0)

    mixed(att_ref, mine, first)
    for j in evens:
        out_cross[j].wait_recv()
        out_cross_relay[j].start()
    for j in evens:
        cross[1, j].wait_recv()
        relay_cross[1, j].start()
    for j in range(0, members, 2):
        out_cross_relay[j].wait_recv()
    att_sent.wait_recv()
    mixed(other, theirs, second)

    hidden = rows_ref[...].astype(F32) + (first[...] + second[...])
    hidden_ref[...] = hidden
    scale = lax.rsqrt(jnp.mean(hidden * hidden, axis=-1, keepdims=True) + norm_eps)
    gain = table_ref[...].astype(F32)[PAD - 7 : PAD - 6, :]
    normed = (hidden * scale * gain).astype(BF)
    normed_ref[:, :width] = normed
    logits = nt(normed, table_ref[...])
    lanes = lax.broadcasted_iota(jnp.int32, logits.shape, 1)
    ids = jnp.transpose(ids_ref[...].astype(F32)).astype(jnp.int32)
    mask = ids[:, 0:1] == lanes
    for k in range(1, ids.shape[1]):
        mask = mask | (ids[:, k : k + 1] == lanes)
    logits = jnp.where(mask, logits, masked_score)
    weight = jnp.where(mask, jnp.exp(logits - jnp.max(logits, axis=-1, keepdims=True)), 0.0)
    gates = weight / jnp.sum(weight, axis=-1, keepdims=True)
    upper = gates.astype(BF).astype(F32)
    lower = gates - upper
    blank = jnp.zeros((gates.shape[0], LANES - 2 * PAD), F32)
    normed_ref[:, width:] = jnp.concatenate([upper, lower, blank], axis=1).astype(BF)

    for j in evens:
        cot_far[j].wait_recv()
        cot_relay[j].start()
    if slots > 2:
        hop[2].wait_recv()
    cot_core.wait_recv()
    for j in evens:
        cot_relay[j].wait_recv()
    for s in range(1, done + 1):
        whole[s].wait_recv()
        for j in evens:
            relay_half[s, j].wait_recv()
            relay_cross[s, j].wait_recv()
    qkv_saved.wait()
    out_saved.wait()
    kv_saved[0].wait()
    for s in range(1, slots):
        pl.when(c >= s)(kv_saved[s].wait)
    for copy in plain_made:
        copy.wait_send()
    for s in range(1, slots):
        pl.when((c >= s - 1) & (c + 1 < slots))(later(s).wait_send)
    att_sent.wait_send()


def forward(projections, wout, cotangent, small, rows, turns, ids, members, slots):
    tokens, width = rows.shape
    cut, q_wide = projections[0].shape
    kv_wide = projections[1].shape[1]
    wide = q_wide + 2 * kv_wide
    heads = q_wide // HEAD
    groups = kv_wide // HEAD
    many = heads // groups * tokens
    halves = members // 2
    far = halves - 1
    done = 1
    copies = (members - 1) + 2 * (1 + 2 * far) + 3 * (1 + far) + 2 * far + 2 * halves
    copies += (slots - 1) + 1 + done * (1 + 4 * far) + 2
    return pl.pallas_call(
        functools.partial(forward_kernel, members, slots),
        out_shape=(
            shape((PAD, width), BF),
            shape((tokens, width), BF),
            shape((heads, tokens, HEAD), BF),
            shape((slots, tokens, 2 * kv_wide), BF),
            shape((tokens, q_wide), BF),
            shape((groups, 1, many), F32),
            shape((tokens, width), F32),
            shape((tokens, width + LANES), BF),
            shape((members, cut, wide), BF),
            shape((members,) + wout.shape, BF),
            shape((members, tokens, width), BF),
            shape((done, members, tokens, width), BF),
            shape((tokens, width), BF),
            shape((members, tokens, width // members), BF),
        ),
        in_specs=[ANY] * 5 + [VMEM] * 6,
        out_specs=(VMEM, VMEM, VMEM, ANY, VMEM, VMEM, VMEM, VMEM) + (ANY,) * 5 + (VMEM,),
        scratch_shapes=[
            pltpu.VMEM((members, PAD, cut), BF),
            pltpu.VMEM((members, cut, wide), BF),
            pltpu.VMEM((members,) + wout.shape, BF),
            pltpu.VMEM((members,) + wout.shape, BF),
            pltpu.VMEM((slots, tokens, 2 * kv_wide), BF),
            pltpu.VMEM((tokens, wide), F32),
            pltpu.VMEM((tokens, width), F32),
            pltpu.VMEM((tokens, width), F32),
            pltpu.VMEM((tokens, q_wide), BF),
            pltpu.VMEM((groups, 1, many), F32),
            pltpu.VMEM((groups, 1, many), F32),
            pltpu.VMEM((groups, HEAD, many), F32),
            pltpu.SemaphoreType.DMA((2, copies)),
            pltpu.SemaphoreType.DMA((7 + slots,)),
        ],
        compiler_params=pltpu.CompilerParams(
            vmem_limit_bytes=60 << 20, collective_id=0, has_side_effects=True
        ),
        name="forward",
        cost_estimate=pl.CostEstimate(
            flops=8 * tokens * width * wide, bytes_accessed=8 * width * wide, transcendentals=0
        ),
    )(*projections, wout, cotangent, *small, rows, turns, ids)


def attend_back_start(heads_ref, grad_ref, att_ref, wide, acc):
    groups, many, _ = wide.shape
    repeat = heads_ref.shape[0] // groups
    lane = lax.broadcasted_iota(jnp.int32, (many, 2 * HEAD), 1)
    for g in range(groups):
        grad = grad_ref[g * repeat : (g + 1) * repeat].reshape(many, HEAD).astype(F32)
        out = jnp.concatenate(
            [
                att_ref[:, (g * repeat + r) * HEAD : (g * repeat + r + 1) * HEAD]
                for r in range(repeat)
            ],
            axis=0,
        )
        delta = jnp.sum(grad * out.astype(F32), axis=-1, keepdims=True)
        upper = delta.astype(BF).astype(F32)
        both = jnp.concatenate([grad, jnp.zeros((many, HEAD), F32)], axis=1)
        both = jnp.where(lane == HEAD, -upper, jnp.where(lane == HEAD + 1, upper - delta, both))
        wide[g] = both.astype(BF)
        acc[g] = jnp.zeros((many, HEAD), F32)


def attend_back_slot(s, heads_ref, grad_ref, lse_ref, kv, wide, acc, grad_kv):
    groups, many, _ = wide.shape
    tokens = heads_ref.shape[1]
    repeat = heads_ref.shape[0] // groups
    half = kv.shape[2] // 2
    keys = lax.broadcasted_iota(jnp.int32, (tokens, many), 0)
    queries = lax.broadcasted_iota(jnp.int32, (tokens, many), 1) % tokens
    allowed = keys <= queries + jnp.where(s == 0, 0, tokens)
    for g in range(groups):
        at = slice(g * HEAD, (g + 1) * HEAD)
        behind = slice(half + g * HEAD, half + (g + 1) * HEAD)
        q = heads_ref[g * repeat : (g + 1) * repeat].reshape(many, HEAD)
        grad = grad_ref[g * repeat : (g + 1) * repeat].reshape(many, HEAD)
        key = kv[s, :, at]
        value = kv[s, :, behind]
        value = jnp.concatenate([value, jnp.ones_like(value)], axis=1)
        prob = jnp.where(allowed, jnp.exp(nt(key, q) - lse_ref[g]), 0.0)
        grad_score = (prob * nt(value, wide[g])).astype(BF)
        grad_kv[:, at] = nn(grad_score, q)
        grad_kv[:, behind] = nn(prob.astype(BF), grad)
        acc[g] += tn(grad_score, key)


def attend_back_end(turns_ref, acc, turned, grad_q_ref):
    groups, many, _ = acc.shape
    tokens = turned.shape[0]
    repeat = many // tokens
    for g in range(groups):
        done = acc[g] * (1.0 / math.sqrt(HEAD))
        for r in range(repeat):
            h = g * repeat + r
            turned[:, h * HEAD : (h + 1) * HEAD] = done[r * tokens : (r + 1) * tokens]
    grad_q_ref[...] = rotate(turned[...], turns_ref[:, :LANES], -turns_ref[:, LANES:]).astype(BF)


def gates_of(tail, experts):
    rows = tail.astype(F32)
    both = rows + pltpu.roll(rows, LANES - PAD, 1)
    lane = lax.broadcasted_iota(jnp.int32, both.shape, 1)
    return jnp.where(lane < experts, both, 0.0)


def gate_column(gates, expert):
    lane = lax.broadcasted_iota(jnp.int32, gates.shape, 1)
    return jnp.sum(jnp.where(lane == expert, gates, 0.0), axis=-1, keepdims=True)


def hidden_terms(normed, cotangent, gate_col, gate_w, up_w, down_w):
    gate_pre = nn(normed, gate_w)
    up_pre = nn(normed, up_w)
    plain = nt(cotangent, down_w)
    sigma = 1.0 / (1.0 + jnp.exp(-gate_pre))
    activated = gate_pre * sigma
    inner = activated * up_pre
    grad_inner = gate_col * plain
    scaled = (gate_col * inner).astype(BF)
    grad_g = (grad_inner * up_pre * (sigma + activated * (1.0 - sigma))).astype(BF)
    grad_u = (grad_inner * activated).astype(BF)
    return inner, plain, scaled, grad_g, grad_u


def own_kernel(members, slots, experts, table_ref, normed_in, cot_own, cot_near, cot_two, cut_in, *refs):
    cot_in = [cot_own] + [cot_near.at[j] for j in range(1, members)]
    gate_hbm, up_hbm, down_hbm = refs[:3]
    (
        far_ref,
        last_ref,
        cut_near,
        two_out,
        moe_ref,
        mine_ref,
        router_ref,
        grad_gate_ref,
        grad_up_ref,
        grad_down_ref,
        gate_w,
        up_w,
        down_w,
        normed,
        cot,
        all_inner,
        all_g,
        all_u,
        parts,
        swapped,
        joined,
        arrived,
        stage_gate,
        stage_up,
        stage_down,
        gates,
        shares,
        sems,
        weight_sems,
        local_sems,
        stage_sems,
        moe_stage,
        moe_sems,
    ) = refs[3:]
    f = lax.axis_index("fsdp")
    c = lax.axis_index("context")
    t = lax.axis_index("tensor")
    here = gate_w.shape[0]
    hidden = gate_w.shape[2]
    tokens = normed_in.shape[0]
    side = tokens // 2
    width = cot.shape[2]
    evens = range(2, members, 2)
    beside = {"fsdp": partner(f)}
    opposite = {"tensor": 1 - t}
    ahead = {"context": lax.rem(c + 1, slots)}
    behind = {"context": lax.rem(c + slots - 1, slots)}
    apart = {j: {"fsdp": lax.rem(f + j, members)} for j in evens}
    owner = {j: {"fsdp": lax.rem(f + members - j, members)} for j in evens}

    net = Sender(sems)
    near_core = net.add(normed_in, normed.at[1], beside)
    near_far = {j: net.add(normed_in, normed.at[j], apart[j]) for j in evens}
    near_relay = {j: net.add(normed.at[j], normed.at[j + 1], beside) for j in evens}
    hop, whole, half, cross, relay_half, relay_cross = {}, {}, {}, {}, {}, {}
    lower_half, upper_half = pl.ds(0, side), pl.ds(side, side)
    piece = pl.ds(pl.multiple_of(t * side, side), side)
    whole_slots = range(1, slots - 1)
    for s in range(1, slots):
        origin = normed_in if s == 1 else far_ref.at[s - 2, 0]
        hop[s] = net.add(origin, far_ref.at[s - 1, 0] if s < slots - 1 else last_ref, ahead)
    for s in whole_slots:
        now = far_ref.at[s - 1]
        whole[s] = net.add(now.at[0], now.at[1], beside)
        for j in evens:
            half[s, j] = net.add(now.at[0, piece], now.at[j, lower_half], apart[j])
            cross[s, j] = net.add(now.at[j, lower_half], now.at[j, upper_half], opposite)
            relay_half[s, j] = net.add(now.at[j, lower_half], now.at[j + 1, lower_half], beside)
            relay_cross[s, j] = net.add(now.at[j, upper_half], now.at[j + 1, upper_half], beside)
    cuts = [
        net.add(cut_in.at[j], cut_near.at[j], {"fsdp": target(f, j, members)})
        for j in range(1, members)
    ]
    two_whole = net.add(cot_two, two_out.at[0], beside)
    two_half, two_cross, two_relay, two_relay_cross = {}, {}, {}, {}
    for j in evens:
        low, high = two_out.at[j - 1, lower_half], two_out.at[j - 1, upper_half]
        two_half[j] = net.add(cot_two.at[piece], low, apart[j])
        two_cross[j] = net.add(low, high, opposite)
        two_relay[j] = net.add(low, two_out.at[j, lower_half], beside)
        two_relay_cross[j] = net.add(high, two_out.at[j, upper_half], beside)
    swap = {
        j: net.add(parts.at[j + 1], swapped.at[j // 2], beside) for j in range(0, members, 2)
    }
    home = {j: net.add(joined.at[j // 2], arrived.at[j // 2], owner[j]) for j in evens}

    weight_copies = [
        (
            pltpu.make_async_copy(gate_hbm.at[e], gate_w.at[e], weight_sems.at[0, e]),
            pltpu.make_async_copy(up_hbm.at[e], up_w.at[e], weight_sems.at[1, e]),
            pltpu.make_async_copy(down_hbm.at[e], down_w.at[e], weight_sems.at[2, e]),
        )
        for e in range(here)
    ]
    local = [pltpu.make_async_copy(normed_in, normed.at[0], local_sems.at[0])]
    for j in range(members):
        local.append(pltpu.make_async_copy(cot_in[j], cot.at[j], local_sems.at[1 + j]))
    for copy in local + list(weight_copies[0]):
        copy.start()
    greet(
        [{"fsdp": target(f, j, members)} for j in range(1, members)] + [opposite, ahead, behind]
    )
    near_core.start()
    for j in evens:
        near_far[j].start()
    hop[1].start()
    for e in range(1, here):
        for copy in weight_copies[e]:
            copy.start()
    for copy in local:
        copy.wait()
    near_core.wait_recv()

    chunk = width // 3
    thin = width // 6
    step = 2 * tokens

    def prepare(pair):
        at = pl.ds(pl.multiple_of(pair * step, step), step)
        tail = normed[pl.ds(2 * pair, 2), :, width:].reshape(step, LANES)
        gates[at, :] = gates_of(tail, experts)
        shares[at, :] = jnp.zeros((step, LANES), F32)

    def hidden_pass(pair):
        def one_expert(e, carry):
            @pl.when(pair == 0)
            def _():
                pltpu.make_async_copy(gate_hbm.at[e], gate_w.at[e], weight_sems.at[0, e]).wait()
                pltpu.make_async_copy(up_hbm.at[e], up_w.at[e], weight_sems.at[1, e]).wait()
                pltpu.make_async_copy(down_hbm.at[e], down_w.at[e], weight_sems.at[2, e]).wait()

            at = pl.ds(pl.multiple_of(pair * step, step), step)
            both = pl.ds(2 * pair, 2)
            columns = pl.ds(pl.multiple_of(e * hidden, LANES), hidden)
            inner, plain, scaled, grad_g, grad_u = hidden_terms(
                normed[both, :, :width].reshape(step, width),
                cot[both].reshape(step, width),
                gate_column(gates[at, :], f * here + e),
                gate_w[e],
                up_w[e],
                down_w[e],
            )
            all_inner[at, columns] = scaled
            all_g[at, columns] = grad_g
            all_u[at, columns] = grad_u
            share = jnp.sum(inner * plain, axis=-1, keepdims=True)
            lane = lax.broadcasted_iota(jnp.int32, (step, LANES), 1)
            shares[at, :] = jnp.where(lane == f * here + e, share, shares[at, :])
            return carry

        lax.fori_loop(0, here, one_expert, 0)

    def grad_pass(pair):
        def one_block(b, carry):
            at = pl.ds(pl.multiple_of(b * tokens, tokens), tokens)
            mean = jnp.sum(gates[at, :] * shares[at, :], axis=-1, keepdims=True)
            logits = (gates[at, :] * (shares[at, :] - mean)).astype(BF)
            router_ref[...] += tn(logits, normed[b, :, :width])[:PAD]

            def one_chunk(k, inner_carry):
                part = pl.ds(pl.multiple_of(k * thin, LANES), thin)
                total = nn(logits[:, :PAD], table_ref[:, part])
                for e in range(here):
                    columns = slice(e * hidden, (e + 1) * hidden)
                    total = total + nt(all_g[at, columns], gate_w[e, part, :])
                    total = total + nt(all_u[at, columns], up_w[e, part, :])
                parts[b, :, part] = total.astype(BF)
                return inner_carry

            return lax.fori_loop(0, width // thin, one_chunk, carry)

        lax.fori_loop(2 * pair, 2 * pair + 2, one_block, 0)

    def slot_arrived(s):
        hop[s].wait_recv()
        if s + 1 < slots:
            hop[s + 1].start()
        if s in whole_slots:
            whole[s].start()
            for j in evens:
                half[s, j].start()

    def half_arrived(s):
        if s in whole_slots:
            for j in evens:
                half[s, j].wait_recv()
                cross[s, j].start()
                relay_half[s, j].start()

    def cross_arrived(s):
        if s in whole_slots:
            for j in evens:
                cross[s, j].wait_recv()
                relay_cross[s, j].start()

    def moe_pass(pair):
        def one_moe(b, carry):
            at = pl.ds(pl.multiple_of(b * tokens, tokens), tokens)
            slot = lax.rem(b, 2)
            copy = pltpu.make_async_copy(moe_stage.at[slot], moe_ref.at[b], moe_sems.at[slot])
            pl.when(b >= 2)(copy.wait)

            def one_chunk(k, inner_carry):
                part = pl.ds(pl.multiple_of(k * thin, LANES), thin)
                down = down_w[:, :, part].reshape(here * hidden, thin)
                moe_stage[slot, :, part] = nn(all_inner[at, :], down).astype(BF)
                return inner_carry

            lax.fori_loop(0, width // thin, one_chunk, 0)
            copy.start()
            return carry

        lax.fori_loop(2 * pair, 2 * pair + 2, one_moe, 0)

    def far_ready():
        for j in evens:
            near_relay[j].wait_recv()

    def near_done():
        swap[0].start()
        for j in evens:
            near_far[j].wait_recv()
            near_relay[j].start()
        slot_arrived(1)
        for copy in [two_whole] + [two_half[j] for j in evens]:
            copy.start()

    def all_done():
        for j in evens:
            swap[j].start()
        if slots > 2:
            slot_arrived(2)
        for j in evens:
            swap[j].wait_recv()
            joined[j // 2] = (parts[j].astype(F32) + swapped[j // 2].astype(F32)).astype(BF)
            home[j].start()
        for copy in cuts:
            copy.start()
        cross_arrived(1)
        for j in evens:
            two_half[j].wait_recv()
            two_cross[j].start()
            two_relay[j].start()

    router_ref[...] = jnp.zeros_like(router_ref)

    def one_pair(pair, carry):
        pl.when(pair == 1)(far_ready)
        prepare(pair)
        hidden_pass(pair)
        pl.when(pair == 1)(functools.partial(half_arrived, 1))
        grad_pass(pair)
        pl.when(pair == 0)(near_done)
        pl.when(pair == members // 2 - 1)(all_done)
        moe_pass(pair)
        return carry

    lax.fori_loop(0, members // 2, one_pair, 0)
    for slot in range(2):
        pltpu.make_async_copy(moe_stage.at[slot], moe_ref.at[slot], moe_sems.at[slot]).wait()
    buffers = stage_gate.shape[0]

    def stage_copies(e, b):
        return (
            pltpu.make_async_copy(stage_gate.at[b], grad_gate_ref.at[e], stage_sems.at[0, b]),
            pltpu.make_async_copy(stage_up.at[b], grad_up_ref.at[e], stage_sems.at[1, b]),
            pltpu.make_async_copy(stage_down.at[b], grad_down_ref.at[e], stage_sems.at[2, b]),
        )

    def sum_home():
        swap[0].wait_recv()
        total = parts[0].astype(F32) + swapped[0].astype(F32)
        for j in evens:
            home[j].wait_recv()
            total = total + arrived[j // 2].astype(F32)
        mine_ref[...] = total.astype(BF)

    def middle_slots():
        half_arrived(2)
        for j in evens:
            two_cross[j].wait_recv()
            two_relay_cross[j].start()

    def later_slots():
        cross_arrived(2)
        for s in range(3, slots - 1):
            slot_arrived(s)
            half_arrived(s)
            cross_arrived(s)

    def weights_of(e, carry):
        b = lax.rem(e, buffers)

        @pl.when(e >= buffers)
        def _():
            for copy in stage_copies(e, b):
                copy.wait()

        columns = pl.ds(pl.multiple_of(e * hidden, LANES), hidden)
        rows = members * tokens

        def one_chunk(k, inner_carry):
            part = pl.ds(pl.multiple_of(k * chunk, LANES), chunk)
            left = normed[:, :, part].reshape(rows, chunk)
            right = cot[:, :, part].reshape(rows, chunk)
            stage_gate[b, part, :] = tn(left, all_g[:, columns])
            stage_up[b, part, :] = tn(left, all_u[:, columns])
            stage_down[b, :, part] = tn(all_inner[:, columns], right)
            return inner_carry

        lax.fori_loop(0, 3, one_chunk, 0)
        for copy in stage_copies(e, b):
            copy.start()
        pl.when(e == min(1, here - 1))(middle_slots)
        pl.when(e == here - 1)(sum_home)
        pl.when(e == here - 1)(later_slots)
        return carry

    lax.fori_loop(0, here, weights_of, 0)
    for e in range(max(here - buffers, 0), here):
        for copy in stage_copies(e, e % buffers):
            copy.wait()
    for s in whole_slots:
        whole[s].wait_recv()
        for j in evens:
            relay_half[s, j].wait_recv()
            relay_cross[s, j].wait_recv()
    for copy in cuts:
        copy.wait_recv()
    hop[slots - 1].wait_recv()
    two_whole.wait_recv()
    for j in evens:
        two_relay[j].wait_recv()
        two_relay_cross[j].wait_recv()
    for copy in net.made:
        copy.wait_send()


def own(table, normed, cotangent, cot_near, cot_two, normed_cut, gate_w, up_w, down_w, experts, slots):
    members = cot_near.shape[0]
    tokens, width = cotangent.shape
    here, _, hidden = gate_w.shape
    rows = members * tokens
    halves = members // 2
    buffers = 2 if members <= 4 else 1
    far = halves - 1
    copies = 1 + 2 * far + (slots - 1) * (2 + 4 * far) + halves + far + 1 + 4 * far + members - 1
    token_block = (tokens, width)
    return pl.pallas_call(
        functools.partial(own_kernel, members, slots, experts),
        out_shape=(
            shape((slots - 2, members, tokens, width + LANES), BF),
            shape((tokens, width + LANES), BF),
            shape(normed_cut.shape, BF),
            shape((members - 1, tokens, width), BF),
            shape((members, tokens, width), BF),
            shape(token_block, BF),
            shape((PAD, width), F32),
            shape(gate_w.shape, F32),
            shape(up_w.shape, F32),
            shape(down_w.shape, F32),
        ),
        in_specs=[VMEM] + [ANY] * 8,
        out_specs=(ANY, ANY, ANY, ANY, ANY, VMEM, VMEM, ANY, ANY, ANY),
        scratch_shapes=[
            pltpu.VMEM(gate_w.shape, BF),
            pltpu.VMEM(up_w.shape, BF),
            pltpu.VMEM(down_w.shape, BF),
            pltpu.VMEM((members, tokens, width + LANES), BF),
            pltpu.VMEM((members, tokens, width), BF),
            pltpu.VMEM((rows, here * hidden), BF),
            pltpu.VMEM((rows, here * hidden), BF),
            pltpu.VMEM((rows, here * hidden), BF),
            pltpu.VMEM((members,) + token_block, BF),
            pltpu.VMEM((halves,) + token_block, BF),
            pltpu.VMEM((halves,) + token_block, BF),
            pltpu.VMEM((halves,) + token_block, BF),
            pltpu.VMEM((buffers, width, hidden), F32),
            pltpu.VMEM((buffers, width, hidden), F32),
            pltpu.VMEM((buffers, hidden, width), F32),
            pltpu.VMEM((rows, LANES), F32),
            pltpu.VMEM((rows, LANES), F32),
            pltpu.SemaphoreType.DMA((2, copies)),
            pltpu.SemaphoreType.DMA((3, here)),
            pltpu.SemaphoreType.DMA((1 + members,)),
            pltpu.SemaphoreType.DMA((3, buffers)),
            pltpu.VMEM((2,) + token_block, BF),
            pltpu.SemaphoreType.DMA((2,)),
        ],
        compiler_params=pltpu.CompilerParams(
            vmem_limit_bytes=63 << 20, collective_id=1, has_side_effects=True
        ),
        name="own",
        cost_estimate=pl.CostEstimate(
            flops=18 * rows * width * hidden * here,
            bytes_accessed=18 * here * width * hidden,
            transcendentals=0,
        ),
    )(table, normed, cotangent, cot_near, cot_two, normed_cut, gate_w, up_w, down_w)


class Plan:
    def __init__(self, number, ins, outs, scratch, copies, build):
        self.number = number
        self.ins = ins
        self.outs = outs
        self.scratch = scratch
        self.copies = copies
        self.build = build


def more_weights_kernel(sources, counts, plan, experts, begin, index, *refs):
    in_normed, in_cot = counts
    refs = list(refs)

    def take(number):
        front = refs[:number]
        del refs[:number]
        return front

    normed_in = take(in_normed)
    cot_in = take(in_cot)
    gate_w, up_w, down_w, old_gate, old_up, old_down = take(6)
    plan_in = take(len(plan.ins))
    new_gate, new_up, new_down = take(3)
    plan_out = take(len(plan.outs))
    normed, cot, gates, all_inner, all_g, all_u, sems, remote_sems = take(8)
    plan_scratch = refs
    members, tokens, width = cot.shape
    rows = members * tokens
    here = index[1]
    step_at = pl.program_id(0)
    net = Sender(remote_sems)
    devices, begin_plan, ready, after, finish = plan.build(net, plan_in, plan_out, plan_scratch)
    last = pl.num_programs(0) - 1

    @pl.when(step_at == 0)
    def _():
        copies = []
        for group, refs_in, whole in ((0, normed_in, normed), (1, cot_in, cot)):
            for number, lead, first, count in sources[group]:
                ref = refs_in[number]
                ref = ref if lead is None else ref.at[lead]
                place = whole.at[first] if count == 1 else whole.at[pl.ds(first, count)]
                copies.append(pltpu.make_async_copy(ref, place, sems.at[len(copies)]))
        for copy in copies:
            copy.start()
        if devices:
            greet(devices)
        begin_plan()
        for copy in copies:
            copy.wait()
        gates[...] = gates_of(normed[:, :, width:].reshape(rows, LANES), experts)
        ready()

    expert = index[0] * here + begin + step_at
    many = 1 if plan.number in (2, 3, 4, 5) else 2
    step = many * tokens

    def one_tile(b, carry):
        at = pl.ds(pl.multiple_of(b * step, step), step)
        pair = pl.ds(many * b, many)
        _, _, scaled, grad_g, grad_u = hidden_terms(
            normed[pair, :, :width].reshape(step, width),
            cot[pair].reshape(step, width),
            gate_column(gates[at, :], expert),
            gate_w[0],
            up_w[0],
            down_w[0],
        )
        all_inner[at, :] = scaled
        all_g[at, :] = grad_g
        all_u[at, :] = grad_u
        return carry

    straight = plan.number is None and rows <= 1024
    if straight:
        for b in range(rows // step):
            one_tile(b, 0)
    else:
        lax.fori_loop(0, rows // step, one_tile, 0)
    pieces = 1 if straight else 6 if plan.number in (3, 4, 5) else 3
    chunk = width // pieces

    def one_chunk(k, carry):
        at = pl.ds(pl.multiple_of(k * chunk, LANES), chunk)
        left = normed[:, :, at].reshape(rows, chunk)
        right = cot[:, :, at].reshape(rows, chunk)
        new_gate[0, at, :] = old_gate[0, at, :] + tn(left, all_g[...])
        new_up[0, at, :] = old_up[0, at, :] + tn(left, all_u[...])
        new_down[0, :, at] = old_down[0, :, at] + tn(all_inner[...], right)
        return carry

    if straight:
        one_chunk(0, 0)
    else:
        lax.fori_loop(0, pieces, one_chunk, 0)
    for number, hook in enumerate(after):
        pl.when(step_at == jnp.minimum(number, last))(hook)
    pl.when(step_at == last)(finish)


def more_weights(begin, count, index, normed, cotangent, sources, weights, earlier, experts, plan):
    here, width, hidden = weights[0].shape
    tokens = cotangent[0].shape[-2]
    members = max(first + many for _, _, first, many in sources[1])
    rows = members * tokens
    pick = lambda e: (e + begin, 0, 0)
    wide = pl.BlockSpec((1, width, hidden), pick)
    tall = pl.BlockSpec((1, hidden, width), pick)
    base = 1 + len(normed) + len(cotangent) + 3
    results = pl.pallas_call(
        functools.partial(
            more_weights_kernel,
            sources,
            (len(normed), len(cotangent)),
            plan,
            experts,
            begin,
        ),
        out_shape=tuple(shape(item.shape, F32) for item in earlier)
        + tuple(item for item, _ in plan.outs),
        grid=(count,),
        in_specs=[SMEM]
        + [ANY] * (len(normed) + len(cotangent))
        + [wide, wide, tall] * 2
        + [spec for _, spec in plan.ins],
        out_specs=(wide, wide, tall) + tuple(spec for _, spec in plan.outs),
        scratch_shapes=[
            pltpu.VMEM((members, tokens, width + LANES), BF),
            pltpu.VMEM((members, tokens, width), BF),
            pltpu.VMEM((rows, LANES), F32),
            pltpu.VMEM((rows, hidden), BF),
            pltpu.VMEM((rows, hidden), BF),
            pltpu.VMEM((rows, hidden), BF),
            pltpu.SemaphoreType.DMA((4,)),
            pltpu.SemaphoreType.DMA((2, plan.copies)),
        ]
        + list(plan.scratch),
        input_output_aliases={base + i: i for i in range(3)} if count < here else {},
        compiler_params=pltpu.CompilerParams(
            vmem_limit_bytes=63 << 20,
            collective_id=plan.number,
            has_side_effects=plan.number is not None,
        ),
        name="weights_" + str(plan.number),
        cost_estimate=pl.CostEstimate(
            flops=12 * rows * width * hidden * count,
            bytes_accessed=count * 30 * width * hidden + 4 * rows * width,
            transcendentals=0,
        ),
    )(index, *normed, *cotangent, *weights, *earlier, *[item for item, _ in plan.ins])
    return results[:3], results[3:]


def places(members, slots):
    f = lax.axis_index("fsdp")
    c = lax.axis_index("context")
    t = lax.axis_index("tensor")
    fsdp = {j: {"fsdp": target(f, j, members)} for j in range(1, members)}
    return f, c, t, fsdp, {"tensor": 1 - t}


def nothing():
    pass


def home_plan(number, members, slots, grad_part, moe_parts, cot_two):
    tokens, width = grad_part.shape
    halves = members // 2
    evens = range(2, members, 2)

    def build(net, ins, outs, scratch):
        part, moe_in, two_in = ins
        other, moe_mine, hops = outs
        own_part, swapped, joined, arrived, local = scratch
        f, c, t, fsdp, opposite = places(members, slots)
        cross_part = net.add(part, other, opposite)
        ahead = {"context": lax.rem(c + 1, slots)}
        behind = {"context": lax.rem(c + slots - 1, slots)}
        late = [
            net.add(two_in if i == 0 else hops.at[i - 1], hops.at[i], ahead)
            for i in range(slots - 3)
        ]
        swap = [net.add(moe_in.at[2 * i + 1], swapped.at[i], fsdp[1]) for i in range(halves)]
        home = {
            j: net.add(
                joined.at[j // 2], arrived.at[j // 2], {"fsdp": lax.rem(f + members - j, members)}
            )
            for j in evens
        }
        loads = [
            pltpu.make_async_copy(moe_in.at[2 * i], own_part.at[i], local.at[i])
            for i in range(halves)
        ]

        def start():
            for copy in [cross_part] + swap[1:] + swap[:1] + loads + late[:1]:
                copy.start()

        def ready():
            for copy in loads:
                copy.wait()
            for j in evens:
                swap[j // 2].wait_recv()
                joined[j // 2] = (
                    own_part[j // 2].astype(F32) + swapped[j // 2].astype(F32)
                ).astype(BF)
                home[j].start()

        def finish():
            swap[0].wait_recv()
            total = own_part[0].astype(F32) + swapped[0].astype(F32)
            for j in evens:
                home[j].wait_recv()
                total = total + arrived[j // 2].astype(F32)
            moe_mine[...] = total.astype(BF)
            cross_part.wait_recv()
            for i, copy in enumerate(late):
                copy.wait_recv()
                for following in late[i + 1 : i + 2]:
                    following.start()
            for copy in net.made:
                copy.wait_send()

        devices = [fsdp[1], opposite, ahead, behind] + [fsdp[j] for j in evens]
        return devices, start, ready, [], finish

    block = (halves, tokens, width)
    return Plan(
        number,
        [(grad_part, ANY), (moe_parts, ANY), (cot_two, ANY)],
        [
            (shape((tokens, width), BF), ANY),
            (shape((tokens, width), BF), VMEM),
            (shape((max(slots - 3, 1), tokens, width), BF), ANY),
        ],
        [pltpu.VMEM(block, BF)] * 4 + [pltpu.SemaphoreType.DMA((halves,))],
        1 + halves + halves - 1 + slots - 3,
        build,
    )


def keys_plan(number, members, slots, attention, grad_b, normed_last, cot_hops, late):
    heads, grad_heads, att, lse, turns, kv = attention
    _, tokens, cut = grad_b.shape
    wide = normed_last.shape[1]
    width = cot_hops.shape[2]
    side = tokens // 2
    evens = range(2, members, 2)
    groups = lse.shape[0]
    many = lse.shape[2]
    far = members // 2 - 1

    def build(net, ins, outs, scratch):
        heads_ref, grad_ref, att_ref, lse_ref, turns_ref, kv_ref = ins[:6]
        grad_in, last_in, hops_in, att_in = ins[6:]
        grad_q, own_kv, received, grad_near, spread_out, cot_out, att_near = outs
        grad_kv, wide_ref, acc, turned = scratch
        f, c, t, fsdp, opposite = places(members, slots)
        piece = pl.ds(pl.multiple_of(t * side, side), side)
        lower_half, upper_half = pl.ds(0, side), pl.ds(side, side)
        first_back = net.used
        net.used += slots - 1

        def back(s):
            at = first_back + s - 1
            return pltpu.make_async_remote_copy(
                src_ref=grad_kv.at[s - 1],
                dst_ref=received.at[s - 1],
                send_sem=net.sems.at[0, at],
                recv_sem=net.sems.at[1, at],
                device_id={"context": lax.rem(c + slots - s, slots)},
                device_id_type=pl.DeviceIdType.MESH,
            )

        cuts = []
        for j in range(1, members):
            cuts.append(net.add(grad_in.at[j], grad_near.at[j], fsdp[j]))
        sources = [(last_in, spread_out)]
        sources += [(hops_in.at[i], cot_out.at[i]) for i in range(late)]
        att_core = net.add(att_in, att_near.at[1], fsdp[1])
        att_far = [net.add(att_in, att_near.at[j], fsdp[j]) for j in evens]
        att_relay = [net.add(att_near.at[j], att_near.at[j + 1], fsdp[1]) for j in evens]
        whole, half, cross, relay, relay_cross = [], [], [], [], []
        for source, place in sources:
            whole.append(net.add(source, place.at[0], fsdp[1]))
            for j in evens:
                low, high = place.at[j - 1, lower_half], place.at[j - 1, upper_half]
                half.append(net.add(source.at[piece], low, fsdp[j]))
                cross.append(net.add(low, high, opposite))
                relay.append(net.add(low, place.at[j, lower_half], fsdp[1]))
                relay_cross.append(net.add(high, place.at[j, upper_half], fsdp[1]))

        def through(i, carry):
            s = slots - 1 - i

            @pl.when(c >= s)
            def _():
                attend_back_slot(s, heads_ref, grad_ref, lse_ref, kv_ref, wide_ref, acc, own_kv)

                @pl.when(s > 0)
                def _():
                    grad_kv[s - 1] = own_kv[...].astype(BF)
                    back(s).start()

            return carry

        def start():
            for copy in half + att_far + cuts + whole + [att_core]:
                copy.start()
            attend_back_start(heads_ref, grad_ref, att_ref, wide_ref, acc)
            lax.fori_loop(0, slots, through, 0)
            pass_on(0, far)
            attend_back_end(turns_ref, acc, turned, grad_q)

        def pass_on(low, high):
            for copy, following, other in list(zip(half, cross, relay))[low:high]:
                copy.wait_recv()
                following.start()
                other.start()

        def first():
            pass_on(far, len(half))

        def second():
            for copy, following in zip(att_far, att_relay):
                copy.wait_recv()
                following.start()

        def finish():
            for copy, following in zip(cross, relay_cross):
                copy.wait_recv()
                following.start()
            for s in range(1, slots):
                pl.when(c + s < slots)(back(s).wait_recv)
                pl.when(c >= s)(back(s).wait_send)
            for copy in cuts + whole + relay + relay_cross + att_relay + [att_core]:
                copy.wait_recv()
            for copy in net.made:
                copy.wait_send()

        devices = list(fsdp.values()) + [opposite]
        devices += [{"context": lax.rem(c + s, slots)} for s in range(1, slots)]
        return devices, start, nothing, [first, second], finish

    far = members // 2 - 1
    return Plan(
        number,
        [(item, VMEM) for item in attention]
        + [(grad_b, ANY), (normed_last, ANY), (cot_hops, ANY), (att, ANY)],
        [
            (shape(att.shape, BF), VMEM),
            (shape(kv.shape[1:], F32), VMEM),
            (shape((slots - 1,) + kv.shape[1:], BF), ANY),
            (shape((members, tokens, cut), BF), ANY),
            (shape((members - 1, tokens, wide), BF), ANY),
            (shape((max(late, 1), members - 1, tokens, width), BF), ANY),
            (shape((members,) + att.shape, BF), ANY),
        ],
        [
            pltpu.VMEM((slots - 1,) + kv.shape[1:], BF),
            pltpu.VMEM((groups, many, 2 * HEAD), BF),
            pltpu.VMEM((groups, many, HEAD), F32),
            pltpu.VMEM(att.shape, F32),
        ],
        (slots - 1) + (members - 1) + (1 + late) * (1 + 4 * far) + 1 + 2 * far,
        build,
    )


def rows_plan(
    number, members, slots, part_one, joined, router, gain_one, gain_two, payload
):
    tokens, width = part_one.shape
    cut = width // members
    evens = range(2, members, 2)
    rows = payload.shape[0] // slots

    def build(net, ins, outs, scratch):
        part_in, joined_in, router_ref, one_ref, two_ref, payload_in = ins
        other, joined_near, small_near, chunks = outs
        small_mine, small_other, small_sum, small_got, small_cut = scratch
        f, c, t, fsdp, opposite = places(members, slots)
        part_sent = net.add(part_in, other, opposite)
        small_sent = net.add(small_mine, small_other, opposite)
        core = net.add(joined_in, joined_near.at[1], fsdp[1])
        far_copy = {j: net.add(joined_in, joined_near.at[j], fsdp[j]) for j in evens}
        relay = {j: net.add(joined_near.at[j], joined_near.at[j + 1], fsdp[1]) for j in evens}
        small_cuts = []
        for j in range(1, members):
            small_cuts.append(net.add(small_cut.at[j], small_got.at[j], fsdp[j]))
        shares = []
        for s in range(1, slots):
            owner = lax.rem(c + s, slots)
            at = pl.ds(pl.multiple_of(owner * rows, 16), rows)
            shares.append(net.add(payload_in.at[at], chunks.at[s], {"context": owner}))

        def start():
            small = router_ref[...]
            row = lax.broadcasted_iota(jnp.int32, small.shape, 0)
            small = jnp.where(row == PAD - 8, one_ref[...], small)
            small = jnp.where(row == PAD - 7, 0.5 * two_ref[...], small)
            small_mine[...] = small.astype(BF)
            small_sent.start()
            for copy in [part_sent, core] + [far_copy[j] for j in evens] + shares:
                copy.start()

        def ready():
            small_sent.wait_recv()
            small_sum[...] = (small_mine[...].astype(F32) + small_other[...].astype(F32)).astype(BF)
            small_got[0] = columns_of(small_sum, f, cut)
            for j in range(1, members):
                small_cut[j] = columns_of(small_sum, target(f, j, members), cut)
            for copy in small_cuts:
                copy.start()

        def second():
            for j in evens:
                far_copy[j].wait_recv()
                relay[j].start()

        def finish():
            for copy in [part_sent, core] + [relay[j] for j in evens] + small_cuts + shares:
                copy.wait_recv()
            small_near[...] = small_got[...]
            for copy in net.made:
                copy.wait_send()

        devices = list(fsdp.values()) + [opposite]
        devices += [{"context": lax.rem(c + s, slots)} for s in range(1, slots)]
        return devices, start, ready, [nothing, second], finish

    far = members // 2 - 1
    small = (PAD, width)
    return Plan(
        number,
        [(part_one, ANY), (joined, ANY)]
        + [(router, VMEM), (gain_one, VMEM), (gain_two, VMEM), (payload, ANY)],
        [
            (shape((tokens, width), BF), ANY),
            (shape((members,) + joined.shape, BF), ANY),
            (shape((members, PAD, cut), BF), VMEM),
            (shape((slots, rows, payload.shape[1]), BF), ANY),
        ],
        [pltpu.VMEM(small, BF)] * 3 + [pltpu.VMEM((members, PAD, cut), BF)] * 2,
        2 + 1 + 2 * far + (members - 1) + (slots - 1),
        build,
    )


def chunk_plan(number, members, slots, payload, moe_mine):
    rows = payload.shape[0] // slots

    def build(net, ins, outs, scratch):
        f, c, t, fsdp, opposite = places(members, slots)
        copies = [net.add(ins[1], outs[1], opposite)]
        for s in range(1, slots):
            owner = lax.rem(c + s, slots)
            at = pl.ds(pl.multiple_of(owner * rows, 16), rows)
            copies.append(net.add(ins[0].at[at], outs[0].at[s], {"context": owner}))

        def start():
            for copy in copies:
                copy.start()

        def finish():
            for copy in copies:
                copy.wait_recv()
                copy.wait_send()

        devices = [{"context": lax.rem(c + s, slots)} for s in range(1, slots)]
        return devices + [opposite], start, nothing, [], finish

    return Plan(
        number,
        [(payload, ANY), (moe_mine, ANY)],
        [
            (shape((slots, rows, payload.shape[1]), BF), ANY),
            (shape(moe_mine.shape, BF), ANY),
        ],
        [],
        slots,
        build,
    )


def middle_kernel(members, index, hidden_ref, cot_ref, mine_ref, theirs_ref, table_ref, weights_ref, *refs):
    grad_ref, grad_b_ref, heads_ref, gain_ref, rounded, columns, summed = refs
    f = index[0]
    cut = weights_ref.shape[2]
    hidden = hidden_ref[...]
    normed_grad = mine_ref[...].astype(F32) + theirs_ref[...].astype(F32)
    scale = lax.rsqrt(jnp.mean(hidden * hidden, axis=-1, keepdims=True) + norm_eps)
    gain = table_ref[...].astype(F32)[PAD - 7 : PAD - 6, :]
    weighted = normed_grad * gain
    cubed = scale * scale * scale
    grad = (
        cot_ref[...].astype(F32)
        + scale * weighted
        - hidden * cubed * jnp.mean(weighted * hidden, axis=-1, keepdims=True)
    )
    gain_ref[...] = jnp.sum(normed_grad * hidden * scale, axis=0, keepdims=True)
    grad_ref[...] = grad
    rounded[...] = grad.astype(BF)
    for j in range(members):
        grad_b_ref[j] = columns_of(rounded, target(f, j, members), cut)
        columns[j] = columns_of(rounded, member(f, j, members), cut)
    summed[...] = nt(columns[0], weights_ref[0])

    def one_member(j, carry):
        summed[...] += nt(columns[j], weights_ref[j])
        return carry

    lax.fori_loop(1, members, one_member, 0)
    total = summed[...].astype(BF)
    for h in range(heads_ref.shape[0]):
        heads_ref[h] = total[:, h * HEAD : (h + 1) * HEAD]


def middle(index, hidden, cotangent, mine, theirs, table, weights, after=()):
    members = weights.shape[0]
    tokens, width = hidden.shape
    heads = weights[0].shape[0] // HEAD
    return call(
        functools.partial(middle_kernel, members),
        (
            shape((tokens, width), F32),
            shape((members, tokens, width // members), BF),
            shape((heads, tokens, HEAD), BF),
            shape((1, width), F32),
        ),
        [SMEM] + [VMEM] * 6,
        (VMEM,) * 4,
        [
            pltpu.VMEM((tokens, width), BF),
            pltpu.VMEM((members, tokens, width // members), BF),
            pltpu.VMEM((tokens, heads * HEAD), F32),
        ],
        2 * tokens * width * heads * HEAD,
        16 * tokens * width,
        "middle",
        after,
    )(index, hidden, cotangent, mine, theirs, table, weights)


def lower_kernel(members, slots, index, grad_q_ref, own_ref, rows_ref, turns_ref, *refs):
    others = refs[0]
    weights = refs[1]
    joined_ref, part_ref, gain_ref = refs[2:]
    f = index[0]
    cut = weights.shape[1]
    total = own_ref[...]
    for s in range(1, slots):
        total = total + jnp.where(index[1] + s < slots, others[s - 1].astype(F32), 0.0)
    half = total.shape[1] // 2
    q_wide = grad_q_ref.shape[1]
    joined_ref[:, :q_wide] = grad_q_ref[...]
    keys = rotate(total[:, :half], turns_ref[:, :LANES], -turns_ref[:, LANES:])
    joined_ref[:, q_wide : q_wide + half] = keys.astype(BF)
    joined_ref[:, q_wide + half :] = total[:, half:].astype(BF)
    rows = rows_ref[...].astype(F32)
    scale = lax.rsqrt(jnp.mean(rows * rows, axis=-1, keepdims=True) + norm_eps)

    def one_pair(p, carry):
        owner = lax.rem(f + members - 2 * p, members)
        first = nt(joined_ref[...], weights[2 * p]).astype(BF)
        second = nt(joined_ref[...], weights[2 * p + 1]).astype(BF)
        put_columns(part_ref, owner, first, second)
        return carry

    lax.fori_loop(0, members // 2, one_pair, 0)
    gain_ref[...] = jnp.sum(part_ref[...].astype(F32) * rows * scale, axis=0, keepdims=True)


def lower(index, grad_q, own_kv, others, rows, turns, weights, after=()):
    members = len(weights)
    tokens, width = rows.shape
    wide = weights[0].shape[1]
    return call(
        functools.partial(lower_kernel, members, others.shape[0] + 1),
        (shape((tokens, wide), BF), shape((tokens, width), BF), shape((1, width), F32)),
        [SMEM] + [VMEM] * 6,
        (VMEM,) * 3,
        [],
        2 * tokens * width * wide,
        2 * width * wide,
        "lower",
        after,
    )(index, grad_q, own_kv, rows, turns, others, weights)


def last_kernel(
    rows_ref, grad_ref, mine_ref, theirs_ref, table_ref, hidden_ref, moe_ref, other_ref, out_ref, result_ref
):
    moe = moe_ref[...].astype(F32) + other_ref[...].astype(F32)
    result_ref[...] = (hidden_ref[...] + moe).astype(BF)
    rows = rows_ref[...].astype(F32)
    normed_grad = mine_ref[...].astype(F32) + theirs_ref[...].astype(F32)
    scale = lax.rsqrt(jnp.mean(rows * rows, axis=-1, keepdims=True) + norm_eps)
    gain = table_ref[...].astype(F32)[PAD - 8 : PAD - 7, :]
    weighted = normed_grad * gain
    cubed = scale * scale * scale
    out_ref[...] = (
        grad_ref[...]
        + scale * weighted
        - rows * cubed * jnp.mean(weighted * rows, axis=-1, keepdims=True)
    ).astype(BF)


def last(rows, grad, mine, theirs, table, hidden, moe, other):
    tokens, width = rows.shape
    return call(
        last_kernel,
        (shape((tokens, width), BF), shape((tokens, width), BF)),
        [VMEM] * 8,
        (VMEM, VMEM),
        [],
        16 * tokens * width,
        20 * tokens * width,
        "last",
    )(rows, grad, mine, theirs, table, hidden, moe, other)


def product_kernel(extra, left_own, left, right_own, right, *refs):
    members = left.shape[0]
    out_ref = refs[-2]
    mine = [ref[0] if len(ref.shape) == 3 else ref[...] for ref in (left_own, right_own)]
    summed = refs[-1]
    summed[...] = tn(*mine)

    def one_member(j, carry):
        summed[...] += tn(left[j], right[j])
        return carry

    lax.fori_loop(1, members, one_member, 0)
    total = summed[...]
    rows, columns = total.shape
    out_ref[:rows, :] = total.astype(BF)
    if extra:
        small = refs[0]
        summed = small[0].astype(F32)
        for j in range(1, members):
            summed = summed + small[j].astype(F32)
        out_ref[rows:, :] = jnp.zeros((out_ref.shape[0] - rows, columns), BF)
        out_ref[rows : rows + PAD, : summed.shape[1]] = summed.astype(BF)


def product(left_own, left, right_own, right, small, extra_rows, name):
    members, tokens, rows = left.shape
    columns = right.shape[2]
    return call(
        functools.partial(product_kernel, len(small)),
        shape((rows + extra_rows, columns), BF),
        [VMEM] * (4 + len(small)),
        VMEM,
        [pltpu.VMEM((rows, columns), F32)],
        2 * members * tokens * rows * columns,
        4 * rows * columns,
        name,
    )(left_own, left, right_own, right, *small)


def sum_kernel(index, whole_ref, parts_ref, out_ref):
    slots, rows, _ = parts_ref.shape
    at = pl.ds(pl.multiple_of(index[1] * rows, 16), rows)
    total = whole_ref[at, :].astype(F32)
    for s in range(1, slots):
        total = total + parts_ref[s].astype(F32)
    out_ref[...] = total.astype(BF)


def sum_of(index, whole, parts, name):
    slots, rows, columns = parts.shape
    return call(
        sum_kernel,
        shape((rows, columns), BF),
        [SMEM, VMEM, VMEM],
        VMEM,
        [],
        slots * rows * columns,
        2 * (slots + 1) * rows * columns,
        name,
    )(index, whole, parts)


def joint_sum_kernel(index, whole_ref, parts_ref, more_ref, out_ref):
    slots, rows, wide = parts_ref.shape
    at = pl.ds(pl.multiple_of(index[1] * rows, 16), rows)
    total = whole_ref[at, :].astype(F32)
    for s in range(1, slots):
        total = total + parts_ref[s].astype(F32)
    out_ref[:rows, :] = total.astype(BF)
    many, columns = more_ref.shape
    fold = wide // columns
    each = many // fold
    out_ref[rows:, :] = jnp.zeros((each, wide), BF)
    for k in range(fold):
        out_ref[rows:, k * columns : (k + 1) * columns] = more_ref[k * each : (k + 1) * each, :]


def joint_sum(index, whole, parts, more):
    slots, rows, columns = parts.shape
    extra = more.shape[0] // (columns // more.shape[1])
    return call(
        joint_sum_kernel,
        shape((rows + extra, columns), BF),
        [SMEM, VMEM, VMEM, VMEM],
        VMEM,
        [],
        slots * rows * columns,
        2 * (slots + 1) * rows * columns,
        "joint_sum",
    )(index, whole, parts, more)


def spread_kernel(slots, experts, index, *refs):
    parts = refs[:slots]
    query_ref, key_ref, value_ref, out_ref, one_ref, two_ref, router_ref, whole = refs[slots:]
    place = index[1]
    cut, q_wide = query_ref.shape
    kv_wide = key_ref.shape[1]
    rows = whole.shape[0] // slots
    many, columns = out_ref.shape
    each = parts[0].shape[0] - rows
    fold = parts[0].shape[1] // columns
    for s in range(slots):
        owner = lax.rem(place + slots - s, slots)
        whole[pl.ds(pl.multiple_of(owner * rows, 16), rows), :] = parts[s][:rows, :].astype(F32)
        for k in range(fold):
            base = owner * (many // slots) + k * each
            out_ref[pl.ds(pl.multiple_of(base, 16), each), :] = parts[s][
                rows:, k * columns : (k + 1) * columns
            ].astype(F32)
    query_ref[...] = whole[:cut, :q_wide]
    key_ref[...] = whole[:cut, q_wide : q_wide + kv_wide]
    value_ref[...] = whole[:cut, q_wide + kv_wide :]
    small = whole[cut : cut + PAD, :cut]
    one_ref[...] = small[PAD - 8]
    two_ref[...] = small[PAD - 7]
    router_ref[...] = small[:experts]


def spread(index, parts, rows, dims, experts):
    slots = len(parts)
    columns = parts[0].shape[1]
    return call(
        functools.partial(spread_kernel, slots, experts),
        tuple(shape(item, F32) for item in dims),
        [SMEM] + [VMEM] * slots,
        (VMEM,) * len(dims),
        [pltpu.VMEM((slots * rows, columns), F32)],
        slots * rows * columns,
        6 * slots * rows * columns,
        "spread",
    )(index, *parts)


def build(members, slots):
    def ring(item, step):
        return lax.ppermute(item, "context", [(i, (i + step) % slots) for i in range(slots)])

    def per_device(
        tokens,
        positions,
        expert_ids,
        norm1_gain,
        w_query,
        w_key,
        w_value,
        w_out,
        norm2_gain,
        w_router,
        w_gate,
        w_up,
        w_down,
        grad_output,
    ):
        rows = tokens[0]
        cotangent = grad_output[0]
        block = rows.shape[0]
        width = rows.shape[1]
        experts = w_router.shape[1]
        here = w_gate.shape[0]
        kv_wide = w_key.shape[1]
        q_wide = w_query.shape[1]
        f = lax.axis_index("fsdp")
        c = lax.axis_index("context")
        c_index = c.reshape(1)
        index = jnp.stack([f, c])
        f_here = jnp.stack([f, jnp.int32(here)])

        half = HEAD // 2
        lane = np.arange(2 * LANES)
        freq = np.exp(-math.log(10000.0) * 2.0 * np.arange(half, dtype=np.float32) / HEAD)
        sign = np.where(lane % HEAD < half, -1.0, 1.0).astype(np.float32)
        angle = positions[0].astype(F32)[:, None] * freq.astype(np.float32)[lane % half][None, :]
        turns = jnp.where((lane < LANES)[None, :], jnp.cos(angle), jnp.sin(angle) * sign[None, :])

        (
            table,
            normed_one,
            heads,
            kv_slots,
            att,
            lse,
            hidden,
            normed,
            qkv_w,
            out_mine,
            cot_near,
            cot_done,
            cot_two,
            normed_cut,
        ) = forward(
            (w_query, w_key, w_value),
            w_out,
            cotangent,
            (w_router.T, norm1_gain, norm2_gain),
            rows,
            turns,
            expert_ids[0].T,
            members,
            slots,
        )

        results = own(
            table,
            normed,
            cotangent,
            cot_near,
            cot_two,
            normed_cut,
            w_gate,
            w_up,
            w_down,
            experts,
            slots,
        )
        normed_slots, normed_last, normed_near, two_far, moe_parts = results[:5]
        grad_part, router_grad, *expert_grads = results[5:]


        parts = 2 if here % 2 == 0 else here
        queue = []
        for s in range(1, slots - 1):
            queue += [(s, p * (here // parts), here // parts) for p in range(parts)]

        def fill(plan, item, grads, normed_far=None, cot_far=None):
            s, begin, many = item
            if s < slots - 1:
                normed_refs, normed_from = [normed_slots], ((0, s - 1, 0, members),)
            else:
                normed_refs = [normed_last, normed_far]
                normed_from = ((0, None, 0, 1), (1, None, 1, members - 1))
            if s == 1:
                cot_refs, cot_from = [cot_done], ((0, 0, 0, members),)
            else:
                cot_refs = [cot_two, two_far] if s == 2 else [cot_hops, cot_far]
                lead = None if s == 2 else s - 3
                cot_from = ((0, lead, 0, 1), (1, lead, 1, members - 1))
            return more_weights(
                begin,
                many,
                f_here,
                normed_refs,
                cot_refs,
                (normed_from, cot_from),
                (w_gate, w_up, w_down),
                grads,
                experts,
                plan,
            )

        plan = home_plan(2, members, slots, grad_part, moe_parts, cot_two)
        expert_grads, (grad_other, moe_mine, cot_hops) = fill(plan, queue[0], expert_grads)

        grad_hidden, grad_hidden_b, grad_heads, gain_two = middle(
            index, hidden, cotangent, grad_part, grad_other, table, out_mine
        )
        attention = (heads, grad_heads, att, lse, turns, kv_slots)
        plan = keys_plan(
            3, members, slots, attention, grad_hidden_b, normed_last, cot_hops, max(slots - 3, 0)
        )
        expert_grads, results = fill(plan, queue[1], expert_grads)
        grad_q, own_kv, received, grad_near, normed_far, cot_far, att_near = results
        out_payload = product(att, att_near, grad_hidden_b, grad_near, (), 0, "out_grad")
        joined, part_one, gain_one = lower(
            index, grad_q, own_kv, received, rows, turns, qkv_w
        )
        plan = rows_plan(
            4,
            members,
            slots,
            part_one,
            joined,
            router_grad,
            gain_one,
            gain_two,
            out_payload,
        )
        expert_grads, results = fill(plan, queue[2], expert_grads, normed_far, cot_far)
        other_one, joined_near, small_near, out_chunks = results
        payload = product(
            normed_cut, normed_near, joined, joined_near, (small_near,), 2 * PAD, "qkv_grad"
        )
        out_total = sum_of(index, out_payload, out_chunks, "out_sum")
        plan = chunk_plan(5, members, slots, payload, moe_mine)
        expert_grads, (qkv_chunks, moe_other) = fill(
            plan, queue[3], expert_grads, normed_far, cot_far
        )
        total = joint_sum(index, payload, qkv_chunks, out_total)
        shared = [total] + [ring(total, s) for s in range(1, slots)]
        grad_tokens, output = last(
            rows, grad_hidden, part_one, other_one, table, hidden, moe_mine, moe_other
        )
        none = Plan(None, [], [], [], 1, lambda *_: ([], nothing, nothing, [], nothing))
        for item in queue[4:] + [(slots - 1, 0, here)]:
            expert_grads, _ = fill(none, item, expert_grads, normed_far, cot_far)
        cut = w_query.shape[0]
        grad_query, grad_key, grad_value, grad_out, grad_one, grad_two, grad_router = spread(
            index,
            shared,
            payload.shape[0] // slots,
            (
                w_query.shape,
                w_key.shape,
                w_value.shape,
                w_out.shape,
                (cut,),
                (cut,),
                (experts, cut),
            ),
            experts,
        )
        return (
            output[None],
            grad_tokens[None],
            grad_one,
            grad_query,
            grad_key,
            grad_value,
            grad_out,
            grad_two,
            grad_router.T,
            expert_grads[0],
            expert_grads[1],
            expert_grads[2],
        )

    return per_device


def solution(mesh):
    return jax.shard_map(
        build(mesh.shape["fsdp"], mesh.shape["context"]),
        mesh=mesh,
        in_specs=(
            P("fsdp", "context", None),
            P("fsdp", "context"),
            P("fsdp", "context", None),
            P("fsdp"),
            P("fsdp", "tensor"),
            P("fsdp", "tensor"),
            P("fsdp", "tensor"),
            P("tensor", "fsdp"),
            P("fsdp"),
            P("fsdp", None),
            P("fsdp", None, "tensor"),
            P("fsdp", None, "tensor"),
            P("fsdp", "tensor", None),
            P("fsdp", "context", None),
        ),
        out_specs=(
            P("fsdp", "context", None),
            P("fsdp", "context", None),
            P("fsdp"),
            P("fsdp", "tensor"),
            P("fsdp", "tensor"),
            P("fsdp", "tensor"),
            P("tensor", "fsdp"),
            P("fsdp"),
            P("fsdp", None),
            P("fsdp", None, "tensor"),
            P("fsdp", None, "tensor"),
            P("fsdp", "tensor", None),
        ),
        check_vma=False,
    )
```

```python
import functools
import math

import jax
import jax.numpy as jnp
import numpy as np
from jax import lax
from jax.experimental import pallas as pl
from jax.experimental.pallas import tpu as pltpu
from jax.sharding import PartitionSpec as P

HEAD = 64
LANES = 128
PAD = 32
norm_eps = 1e-06
masked_score = -1e30
BF = jnp.bfloat16
F32 = jnp.float32
TILE_ONE = (5,)
CHUNK_SIX = (5,)
VMEM = pl.BlockSpec(memory_space=pltpu.VMEM)
SMEM = pl.BlockSpec(memory_space=pltpu.SMEM)
ANY = pl.BlockSpec(memory_space=pl.ANY)


def nn(left, right):
    return jnp.dot(left, right, preferred_element_type=F32)


def nt(left, right):
    return lax.dot_general(left, right, (((1,), (1,)), ((), ())), preferred_element_type=F32)


def tn(left, right):
    return lax.dot_general(left, right, (((0,), (0,)), ((), ())), preferred_element_type=F32)


def partner(f):
    return f + 1 - 2 * lax.rem(f, 2)


def member(f, j, members):
    base = lax.rem(f + members - (j - j % 2), members)
    return base if j % 2 == 0 else partner(base)


def columns_of(ref, owner, cut):
    if cut % LANES == 0:
        return ref[:, pl.ds(pl.multiple_of(owner * cut, LANES), cut)]
    pair = ref[:, pl.ds(pl.multiple_of(lax.div(owner, 2) * (2 * cut), LANES), 2 * cut)]
    return jnp.where(lax.rem(owner, 2) == 0, pair[:, :cut], pair[:, cut:])


def put_columns(ref, owner, first, second):
    cut = first.shape[1]
    if cut % LANES == 0:
        ref[:, pl.ds(pl.multiple_of(owner * cut, LANES), cut)] = first
        ref[:, pl.ds(pl.multiple_of(partner(owner) * cut, LANES), cut)] = second
    else:
        even = lax.rem(owner, 2) == 0
        both = [jnp.where(even, first, second), jnp.where(even, second, first)]
        at = pl.ds(pl.multiple_of(lax.div(owner, 2) * (2 * cut), LANES), 2 * cut)
        ref[:, at] = jnp.concatenate(both, axis=1)


def shape(dims, kind):
    return jax.ShapeDtypeStruct(dims, kind)


def call(kernel, outs, specs, out_specs, scratch, flops, moved, name, after=(), **more):
    skip = len(after)

    def body(*refs):
        kernel(*refs[skip:])

    run = pl.pallas_call(
        body,
        out_shape=outs,
        in_specs=[ANY] * skip + list(specs),
        out_specs=out_specs,
        scratch_shapes=scratch,
        compiler_params=pltpu.CompilerParams(vmem_limit_bytes=60 << 20),
        name=name,
        cost_estimate=pl.CostEstimate(flops=flops, bytes_accessed=moved, transcendentals=0),
        **more,
    )
    return lambda *operands: run(*after, *operands)


def rotate(rows, cos, sin):
    wide = rows.shape[1]
    count = wide // LANES
    after = pltpu.roll(rows, wide - HEAD // 2, 1)
    before = pltpu.roll(rows, HEAD // 2, 1)
    lane = lax.broadcasted_iota(jnp.int32, rows.shape, 1) % HEAD
    partner = jnp.where(lane < HEAD // 2, after, before)
    cos_all = jnp.concatenate([cos] * count, axis=1)
    sin_all = jnp.concatenate([sin] * count, axis=1)
    return rows * cos_all + partner * sin_all


class Sender:
    def __init__(self, sems):
        self.sems = sems
        self.used = 0
        self.made = []

    def add(self, source, target, device):
        copy = pltpu.make_async_remote_copy(
            src_ref=source,
            dst_ref=target,
            send_sem=self.sems.at[0, self.used],
            recv_sem=self.sems.at[1, self.used],
            device_id=device,
            device_id_type=pl.DeviceIdType.MESH,
        )
        self.used += 1
        self.made.append(copy)
        return copy


def greet(devices):
    barrier = pltpu.get_barrier_semaphore()
    for device in devices:
        pl.semaphore_signal(
            barrier, inc=1, device_id=device, device_id_type=pl.DeviceIdType.MESH
        )
    pl.semaphore_wait(barrier, len(devices))


def target(f, j, members):
    start = f if j % 2 == 0 else partner(f)
    return lax.rem(start + j - j % 2, members)


def attend_slot(s, heads_ref, kv, top, sums, acc):
    groups = top.shape[0]
    tokens = heads_ref.shape[1]
    repeat = heads_ref.shape[0] // groups
    half = kv.shape[2] // 2
    many = repeat * tokens
    keys = lax.broadcasted_iota(jnp.int32, (tokens, many), 0)
    queries = lax.broadcasted_iota(jnp.int32, (tokens, many), 1) % tokens
    allowed = keys <= queries + jnp.where(s == 0, 0, tokens)
    for g in range(groups):
        q = heads_ref[g * repeat : (g + 1) * repeat].reshape(many, HEAD)
        score = jnp.where(allowed, nt(kv[s, :, g * HEAD : (g + 1) * HEAD], q), masked_score)
        value = kv[s, :, half + g * HEAD : half + (g + 1) * HEAD]
        old = top[g]
        high = jnp.maximum(old, jnp.max(score, axis=0, keepdims=True))
        shrink = jnp.exp(old - high)
        weight = jnp.where(allowed, jnp.exp(score - high), 0.0)
        sums[g] = sums[g] * shrink + jnp.sum(weight, axis=0, keepdims=True)
        acc[g] = acc[g] * shrink + tn(value, weight.astype(BF))
        top[g] = high


def attend_end(att_ref, lse_ref, top, sums, acc):
    groups, _, many = top.shape
    tokens = att_ref.shape[0]
    repeat = many // tokens
    for g in range(groups):
        lse_ref[g] = top[g] + jnp.log(sums[g])
        done = jnp.transpose(acc[g] / sums[g]).astype(BF)
        for r in range(repeat):
            h = g * repeat + r
            att_ref[:, h * HEAD : (h + 1) * HEAD] = done[r * tokens : (r + 1) * tokens]


def forward_kernel(
    members,
    slots,
    query_in,
    key_in,
    value_in,
    wout_in,
    cot_in,
    router_ref,
    one_ref,
    two_ref,
    rows_ref,
    turns_ref,
    ids_ref,
    *refs,
):
    (
        table_ref,
        normed_one_ref,
        heads_ref,
        kv_out,
        att_ref,
        lse_ref,
        hidden_ref,
        normed_ref,
        qkv_out,
        wout_out,
        cot_near,
        cot_done,
        cot_two,
        cut_ref,
        small,
        qkv,
        mine,
        theirs,
        kv,
        total,
        first,
        second,
        other,
        top,
        sums,
        acc,
        sems,
        local_sems,
    ) = refs
    f = lax.axis_index("fsdp")
    c = lax.axis_index("context")
    t = lax.axis_index("tensor")
    tokens, width = rows_ref.shape
    side = tokens // 2
    experts, cut = router_ref.shape
    evens = range(2, members, 2)
    beside = {"fsdp": partner(f)}
    opposite = {"tensor": 1 - t}
    ahead = {"context": lax.rem(c + 1, slots)}
    apart = {j: {"fsdp": lax.rem(f + j, members)} for j in evens}
    lower_half, upper_half = pl.ds(0, side), pl.ds(side, side)
    piece = pl.ds(pl.multiple_of(t * side, side), side)

    net = Sender(sems)
    small_sent = [
        net.add(small.at[0], small.at[j], {"fsdp": target(f, j, members)}) for j in range(1, members)
    ]

    def family(source, place):
        return (
            net.add(source, place.at[1], beside),
            {j: net.add(source, place.at[j], apart[j]) for j in evens},
            {j: net.add(place.at[j], place.at[j + 1], beside) for j in evens},
        )

    q_wide, kv_wide = query_in.shape[1], key_in.shape[1]
    bounds = (0, q_wide, q_wide + kv_wide, q_wide + 2 * kv_wide)
    projections = [
        (source, pl.ds(low, high - low))
        for source, low, high in zip((query_in, key_in, value_in), bounds, bounds[1:])
    ]
    groups_of = {"query": projections[:1], "keys": projections[1:]}
    spans = {"query": pl.ds(0, q_wide), "keys": pl.ds(q_wide, 2 * kv_wide)}
    qkv_core, qkv_far, qkv_relay = {}, {}, {}
    for name in ("keys", "query"):
        qkv_core[name] = [net.add(source, qkv.at[1, :, at], beside) for source, at in groups_of[name]]
        qkv_far[name] = {
            j: [net.add(source, qkv.at[j, :, at], apart[j]) for source, at in groups_of[name]]
            for j in evens
        }
        span = spans[name]
        qkv_relay[name] = {
            j: net.add(qkv.at[j, :, span], qkv.at[j + 1, :, span], beside) for j in evens
        }
    out_core, out_far, out_relay = family(wout_in, mine)
    out_cross = {j: net.add(wout_in if j == 0 else mine.at[j], theirs.at[j], opposite) for j in range(0, members, 2)}
    out_cross_relay = {j: net.add(theirs.at[j], theirs.at[j + 1], beside) for j in range(0, members, 2)}
    cot_core, cot_far, cot_relay = family(cot_in, cot_near)
    done = cot_done.shape[0]
    hop, whole, half, cross, relay_half, relay_cross = {}, {}, {}, {}, {}, {}
    hop[1] = net.add(cot_in, cot_done.at[0, 0], ahead)
    if slots > 2:
        hop[2] = net.add(cot_done.at[0, 0], cot_two, ahead)
    for s in range(1, done + 1):
        now = cot_done.at[s - 1]
        whole[s] = net.add(now.at[0], now.at[1], beside)
        for j in evens:
            half[s, j] = net.add(now.at[0, piece], now.at[j, lower_half], apart[j])
            cross[s, j] = net.add(now.at[j, lower_half], now.at[j, upper_half], opposite)
            relay_half[s, j] = net.add(now.at[j, lower_half], now.at[j + 1, lower_half], beside)
            relay_cross[s, j] = net.add(now.at[j, upper_half], now.at[j + 1, upper_half], beside)
    plain = len(net.made)
    first_later = net.used
    net.used += slots - 1

    def later(s):
        at = first_later + s - 1
        return pltpu.make_async_remote_copy(
            src_ref=kv.at[s - 1],
            dst_ref=kv.at[s],
            send_sem=sems.at[0, at],
            recv_sem=sems.at[1, at],
            device_id=ahead,
            device_id_type=pl.DeviceIdType.MESH,
        )

    plain_made = net.made[:plain]
    att_sent = net.add(att_ref, other, opposite)

    locals_in = [
        pltpu.make_async_copy(source, qkv.at[0, :, at], sem)
        for (source, at), sem in zip(projections, [local_sems.at[i] for i in (0, 1, 2)])
    ]
    locals_in.append(pltpu.make_async_copy(wout_in, mine.at[0], local_sems.at[5 + slots]))
    qkv_saved = pltpu.make_async_copy(qkv, qkv_out, local_sems.at[3])
    out_saved = pltpu.make_async_copy(mine, wout_out, local_sems.at[4])
    kv_saved = [
        pltpu.make_async_copy(kv.at[s], kv_out.at[s], local_sems.at[5 + s]) for s in range(slots)
    ]
    for copy in locals_in:
        copy.start()
    small[0] = jnp.zeros((PAD, cut), BF)
    small[0, :experts, :] = router_ref[...]
    small[0, PAD - 8, :] = one_ref[...]
    small[0, PAD - 7, :] = two_ref[...]
    greet(
        [{"fsdp": target(f, j, members)} for j in range(1, members)]
        + [opposite]
        + [ahead, {"context": lax.rem(c + slots - 1, slots)}]
    )
    for copy in small_sent:
        copy.start()
    for name in ("keys", "query"):
        for copies in [qkv_core[name]] + [qkv_far[name][j] for j in evens]:
            for copy in copies:
                copy.start()
    for copy in [out_core, out_cross[0]] + [out_far[j] for j in evens]:
        copy.start()
    hop[1].start()
    cot_core.start()

    rows = rows_ref[...].astype(F32)
    scale = lax.rsqrt(jnp.mean(rows * rows, axis=-1, keepdims=True) + norm_eps)
    hidden_ref[...] = rows * scale
    for copy in locals_in:
        copy.wait()
    for copy in small_sent:
        copy.wait_recv()

    for j in range(0, members, 2):
        put_columns(table_ref, member(f, j, members), small[j], small[j + 1])
    gain = table_ref[...].astype(F32)[PAD - 8 : PAD - 7, :]
    normed_one_ref[...] = (hidden_ref[...] * gain).astype(BF)
    for j in range(members):
        cut_ref[j] = columns_of(normed_one_ref, target(f, j, members), cut)

    total[...] = jnp.zeros(total.shape, F32)

    def product_of(name):
        span = spans[name]

        def far_arrived(j):
            for copy in qkv_far[name][j]:
                copy.wait_recv()
            qkv_relay[name][j].start()

        def core_arrived():
            for copy in qkv_core[name]:
                copy.wait_recv()

        def one_pair(p, carry):
            owner = lax.rem(f + members - 2 * p, members)
            for j in evens:
                pl.when(2 * p == j)(functools.partial(far_arrived, j))
            left = columns_of(normed_one_ref, owner, cut)
            total[:, span] += nn(left, qkv[2 * p, :, span])
            pl.when(p == 0)(core_arrived)
            for j in evens:
                pl.when(2 * p == j)(qkv_relay[name][j].wait_recv)
            left = columns_of(normed_one_ref, partner(owner), cut)
            total[:, span] += nn(left, qkv[2 * p + 1, :, span])
            return carry

        lax.fori_loop(0, members // 2, one_pair, 0)

    cos = turns_ref[:, :LANES]
    sin = turns_ref[:, LANES:]
    product_of("keys")
    kv[0, :, :kv_wide] = rotate(total[:, q_wide : q_wide + kv_wide], cos, sin).astype(BF)
    kv[0, :, kv_wide:] = total[:, q_wide + kv_wide :].astype(BF)
    pl.when(c + 1 < slots)(later(1).start)
    hop[1].wait_recv()
    if slots > 2:
        pl.when(c == slots - 1)(hop[2].start)
    whole[1].start()
    for j in evens:
        half[1, j].start()
    for j in evens:
        cot_far[j].start()
    product_of("query")
    qkv_saved.start()
    turned = (rotate(total[:, :q_wide], cos, sin) * (1.0 / math.sqrt(HEAD))).astype(BF)
    for h in range(q_wide // HEAD):
        heads_ref[h] = turned[:, h * HEAD : (h + 1) * HEAD]
    top[...] = jnp.full(top.shape, masked_score, F32)
    sums[...] = jnp.zeros(sums.shape, F32)
    acc[...] = jnp.zeros(acc.shape, F32)
    def weights_arrived():
        for j in evens:
            out_far[j].wait_recv()
            out_relay[j].start()
            out_cross[j].start()
        out_cross[0].wait_recv()
        out_cross_relay[0].start()


    def half_arrived(s):
        for j in evens:
            half[s, j].wait_recv()
            relay_half[s, j].start()
            cross[s, j].start()

    def keys_arrived(s, carry):
        @pl.when(c >= s)
        def _():
            @pl.when(s > 0)
            def _():
                later(s).wait_recv()

                @pl.when((c + 1 < slots) & (s + 1 < slots))
                def _():
                    later(s + 1).start()

            if slots > 2:
                pl.when((s == c) & (c + 1 < slots))(hop[2].start)
            attend_slot(s, heads_ref, kv, top, sums, acc)

        pl.when(s == 0)(weights_arrived)
        pl.when(s == 1)(functools.partial(half_arrived, 1))
        return carry

    lax.fori_loop(0, slots, keys_arrived, 0)
    kv_saved[0].start()
    for s in range(1, slots):
        pl.when(c >= s)(kv_saved[s].start)
    attend_end(att_ref, lse_ref, top, sums, acc)
    att_sent.start()

    out_core.wait_recv()
    for j in evens:
        out_relay[j].wait_recv()
    out_saved.start()
    def mixed(left, weights, place):
        def one_pair(p, carry):
            owner = lax.rem(f + members - 2 * p, members)
            pair = nn(left[...], weights[2 * p]), nn(left[...], weights[2 * p + 1])
            put_columns(place, owner, *pair)
            return carry

        lax.fori_loop(0, members // 2, one_pair, 0)

    mixed(att_ref, mine, first)
    for j in evens:
        out_cross[j].wait_recv()
        out_cross_relay[j].start()
    for j in evens:
        cross[1, j].wait_recv()
        relay_cross[1, j].start()
    for j in range(0, members, 2):
        out_cross_relay[j].wait_recv()
    att_sent.wait_recv()
    mixed(other, theirs, second)

    gain_two = table_ref[...].astype(F32)[PAD - 7 : PAD - 6, :]
    tile = 64

    def one_tile(i, carry):
        at = pl.ds(pl.multiple_of(i * tile, tile), tile)
        hidden = rows_ref[at, :].astype(F32) + (first[at, :] + second[at, :])
        hidden_ref[at, :] = hidden
        scale = lax.rsqrt(jnp.mean(hidden * hidden, axis=-1, keepdims=True) + norm_eps)
        normed_ref[at, :width] = (hidden * scale * gain_two).astype(BF)
        return carry

    lax.fori_loop(0, tokens // tile, one_tile, 0)
    logits = nt(normed_ref[:, :width], table_ref[...])
    lanes = lax.broadcasted_iota(jnp.int32, logits.shape, 1)
    ids = jnp.transpose(ids_ref[...].astype(F32)).astype(jnp.int32)
    mask = ids[:, 0:1] == lanes
    for k in range(1, ids.shape[1]):
        mask = mask | (ids[:, k : k + 1] == lanes)
    logits = jnp.where(mask, logits, masked_score)
    weight = jnp.where(mask, jnp.exp(logits - jnp.max(logits, axis=-1, keepdims=True)), 0.0)
    gates = weight / jnp.sum(weight, axis=-1, keepdims=True)
    upper = gates.astype(BF).astype(F32)
    lower = gates - upper
    blank = jnp.zeros((gates.shape[0], LANES - 2 * PAD), F32)
    normed_ref[:, width:] = jnp.concatenate([upper, lower, blank], axis=1).astype(BF)

    for j in evens:
        cot_far[j].wait_recv()
        cot_relay[j].start()
    if slots > 2:
        hop[2].wait_recv()
    cot_core.wait_recv()
    for j in evens:
        cot_relay[j].wait_recv()
    for s in range(1, done + 1):
        whole[s].wait_recv()
        for j in evens:
            relay_half[s, j].wait_recv()
            relay_cross[s, j].wait_recv()
    qkv_saved.wait()
    out_saved.wait()
    kv_saved[0].wait()
    for s in range(1, slots):
        pl.when(c >= s)(kv_saved[s].wait)
    for copy in plain_made:
        copy.wait_send()
    for s in range(1, slots):
        pl.when((c >= s - 1) & (c + 1 < slots))(later(s).wait_send)
    att_sent.wait_send()


def forward(projections, wout, cotangent, small, rows, turns, ids, members, slots):
    tokens, width = rows.shape
    cut, q_wide = projections[0].shape
    kv_wide = projections[1].shape[1]
    wide = q_wide + 2 * kv_wide
    heads = q_wide // HEAD
    groups = kv_wide // HEAD
    many = heads // groups * tokens
    halves = members // 2
    far = halves - 1
    done = 1
    copies = (members - 1) + 2 * (1 + 2 * far) + 3 * (1 + far) + 2 * far + 2 * halves
    copies += (slots - 1) + 1 + done * (1 + 4 * far) + 2
    return pl.pallas_call(
        functools.partial(forward_kernel, members, slots),
        out_shape=(
            shape((PAD, width), BF),
            shape((tokens, width), BF),
            shape((heads, tokens, HEAD), BF),
            shape((slots, tokens, 2 * kv_wide), BF),
            shape((tokens, q_wide), BF),
            shape((groups, 1, many), F32),
            shape((tokens, width), F32),
            shape((tokens, width + LANES), BF),
            shape((members, cut, wide), BF),
            shape((members,) + wout.shape, BF),
            shape((members, tokens, width), BF),
            shape((done, members, tokens, width), BF),
            shape((tokens, width), BF),
            shape((members, tokens, width // members), BF),
        ),
        in_specs=[ANY] * 5 + [VMEM] * 6,
        out_specs=(VMEM, VMEM, VMEM, ANY, VMEM, VMEM, VMEM, VMEM) + (ANY,) * 5 + (VMEM,),
        scratch_shapes=[
            pltpu.VMEM((members, PAD, cut), BF),
            pltpu.VMEM((members, cut, wide), BF),
            pltpu.VMEM((members,) + wout.shape, BF),
            pltpu.VMEM((members,) + wout.shape, BF),
            pltpu.VMEM((slots, tokens, 2 * kv_wide), BF),
            pltpu.VMEM((tokens, wide), F32),
            pltpu.VMEM((tokens, width), F32),
            pltpu.VMEM((tokens, width), F32),
            pltpu.VMEM((tokens, q_wide), BF),
            pltpu.VMEM((groups, 1, many), F32),
            pltpu.VMEM((groups, 1, many), F32),
            pltpu.VMEM((groups, HEAD, many), F32),
            pltpu.SemaphoreType.DMA((2, copies)),
            pltpu.SemaphoreType.DMA((7 + slots,)),
        ],
        compiler_params=pltpu.CompilerParams(
            vmem_limit_bytes=60 << 20, collective_id=0, has_side_effects=True
        ),
        name="forward",
        cost_estimate=pl.CostEstimate(
            flops=8 * tokens * width * wide, bytes_accessed=8 * width * wide, transcendentals=0
        ),
    )(*projections, wout, cotangent, *small, rows, turns, ids)


def attend_back_start(heads_ref, grad_ref, att_ref, wide, acc):
    groups, many, _ = wide.shape
    repeat = heads_ref.shape[0] // groups
    lane = lax.broadcasted_iota(jnp.int32, (many, 2 * HEAD), 1)
    for g in range(groups):
        grad = grad_ref[g * repeat : (g + 1) * repeat].reshape(many, HEAD).astype(F32)
        out = jnp.concatenate(
            [
                att_ref[:, (g * repeat + r) * HEAD : (g * repeat + r + 1) * HEAD]
                for r in range(repeat)
            ],
            axis=0,
        )
        delta = jnp.sum(grad * out.astype(F32), axis=-1, keepdims=True)
        upper = delta.astype(BF).astype(F32)
        both = jnp.concatenate([grad, jnp.zeros((many, HEAD), F32)], axis=1)
        both = jnp.where(lane == HEAD, -upper, jnp.where(lane == HEAD + 1, upper - delta, both))
        wide[g] = both.astype(BF)
        acc[g] = jnp.zeros((many, HEAD), F32)


def attend_back_slot(s, heads_ref, grad_ref, lse_ref, kv, wide, acc, grad_kv):
    groups, many, _ = wide.shape
    tokens = heads_ref.shape[1]
    repeat = heads_ref.shape[0] // groups
    half = kv.shape[2] // 2
    keys = lax.broadcasted_iota(jnp.int32, (tokens, many), 0)
    queries = lax.broadcasted_iota(jnp.int32, (tokens, many), 1) % tokens
    allowed = keys <= queries + jnp.where(s == 0, 0, tokens)
    for g in range(groups):
        at = slice(g * HEAD, (g + 1) * HEAD)
        behind = slice(half + g * HEAD, half + (g + 1) * HEAD)
        q = heads_ref[g * repeat : (g + 1) * repeat].reshape(many, HEAD)
        grad = grad_ref[g * repeat : (g + 1) * repeat].reshape(many, HEAD)
        key = kv[s, :, at]
        value = kv[s, :, behind]
        value = jnp.concatenate([value, jnp.ones_like(value)], axis=1)
        prob = jnp.where(allowed, jnp.exp(nt(key, q) - lse_ref[g]), 0.0)
        grad_score = (prob * nt(value, wide[g])).astype(BF)
        grad_kv[:, at] = nn(grad_score, q)
        grad_kv[:, behind] = nn(prob.astype(BF), grad)
        acc[g] += tn(grad_score, key)


def attend_back_end(turns_ref, acc, turned, grad_q_ref):
    groups, many, _ = acc.shape
    tokens = turned.shape[0]
    repeat = many // tokens
    for g in range(groups):
        done = acc[g] * (1.0 / math.sqrt(HEAD))
        for r in range(repeat):
            h = g * repeat + r
            turned[:, h * HEAD : (h + 1) * HEAD] = done[r * tokens : (r + 1) * tokens]
    grad_q_ref[...] = rotate(turned[...], turns_ref[:, :LANES], -turns_ref[:, LANES:]).astype(BF)


def gates_of(tail, experts):
    rows = tail.astype(F32)
    both = rows + pltpu.roll(rows, LANES - PAD, 1)
    lane = lax.broadcasted_iota(jnp.int32, both.shape, 1)
    return jnp.where(lane < experts, both, 0.0)


def gate_column(gates, expert):
    lane = lax.broadcasted_iota(jnp.int32, gates.shape, 1)
    return jnp.sum(jnp.where(lane == expert, gates, 0.0), axis=-1, keepdims=True)


def hidden_terms(normed, cotangent, gate_col, gate_w, up_w, down_w):
    gate_pre = nn(normed, gate_w)
    up_pre = nn(normed, up_w)
    plain = nt(cotangent, down_w)
    sigma = 1.0 / (1.0 + jnp.exp(-gate_pre))
    activated = gate_pre * sigma
    inner = activated * up_pre
    grad_inner = gate_col * plain
    scaled = (gate_col * inner).astype(BF)
    grad_g = (grad_inner * up_pre * (sigma + activated * (1.0 - sigma))).astype(BF)
    grad_u = (grad_inner * activated).astype(BF)
    return inner, plain, scaled, grad_g, grad_u


def own_kernel(members, slots, experts, table_ref, normed_in, cot_own, cot_near, cot_two, cut_in, *refs):
    cot_in = [cot_own] + [cot_near.at[j] for j in range(1, members)]
    gate_hbm, up_hbm, down_hbm = refs[:3]
    (
        far_ref,
        last_ref,
        cut_near,
        two_out,
        moe_ref,
        mine_ref,
        router_ref,
        grad_gate_ref,
        grad_up_ref,
        grad_down_ref,
        gate_w,
        up_w,
        down_w,
        normed,
        cot,
        all_inner,
        all_g,
        all_u,
        parts,
        swapped,
        joined,
        arrived,
        stage_gate,
        stage_up,
        stage_down,
        gates,
        shares,
        sems,
        weight_sems,
        local_sems,
        stage_sems,
        moe_stage,
        moe_sems,
    ) = refs[3:]
    f = lax.axis_index("fsdp")
    c = lax.axis_index("context")
    t = lax.axis_index("tensor")
    here = gate_w.shape[0]
    hidden = gate_w.shape[2]
    tokens = normed_in.shape[0]
    side = tokens // 2
    width = cot.shape[2]
    evens = range(2, members, 2)
    beside = {"fsdp": partner(f)}
    opposite = {"tensor": 1 - t}
    ahead = {"context": lax.rem(c + 1, slots)}
    behind = {"context": lax.rem(c + slots - 1, slots)}
    apart = {j: {"fsdp": lax.rem(f + j, members)} for j in evens}
    owner = {j: {"fsdp": lax.rem(f + members - j, members)} for j in evens}

    net = Sender(sems)
    near_core = net.add(normed_in, normed.at[1], beside)
    near_far = {j: net.add(normed_in, normed.at[j], apart[j]) for j in evens}
    near_relay = {j: net.add(normed.at[j], normed.at[j + 1], beside) for j in evens}
    hop, whole, half, cross, relay_half, relay_cross = {}, {}, {}, {}, {}, {}
    lower_half, upper_half = pl.ds(0, side), pl.ds(side, side)
    piece = pl.ds(pl.multiple_of(t * side, side), side)
    whole_slots = range(1, slots - 1)
    for s in range(1, slots):
        origin = normed_in if s == 1 else far_ref.at[s - 2, 0]
        hop[s] = net.add(origin, far_ref.at[s - 1, 0] if s < slots - 1 else last_ref, ahead)
    for s in whole_slots:
        now = far_ref.at[s - 1]
        whole[s] = net.add(now.at[0], now.at[1], beside)
        for j in evens:
            half[s, j] = net.add(now.at[0, piece], now.at[j, lower_half], apart[j])
            cross[s, j] = net.add(now.at[j, lower_half], now.at[j, upper_half], opposite)
            relay_half[s, j] = net.add(now.at[j, lower_half], now.at[j + 1, lower_half], beside)
            relay_cross[s, j] = net.add(now.at[j, upper_half], now.at[j + 1, upper_half], beside)
    cuts = [
        net.add(cut_in.at[j], cut_near.at[j], {"fsdp": target(f, j, members)})
        for j in range(1, members)
    ]
    two_whole = net.add(cot_two, two_out.at[0], beside)
    two_half, two_cross, two_relay, two_relay_cross = {}, {}, {}, {}
    for j in evens:
        low, high = two_out.at[j - 1, lower_half], two_out.at[j - 1, upper_half]
        two_half[j] = net.add(cot_two.at[piece], low, apart[j])
        two_cross[j] = net.add(low, high, opposite)
        two_relay[j] = net.add(low, two_out.at[j, lower_half], beside)
        two_relay_cross[j] = net.add(high, two_out.at[j, upper_half], beside)
    swap = {
        j: net.add(parts.at[j + 1], swapped.at[j // 2], beside) for j in range(0, members, 2)
    }
    home = {j: net.add(joined.at[j // 2], arrived.at[j // 2], owner[j]) for j in evens}

    weight_copies = [
        (
            pltpu.make_async_copy(gate_hbm.at[e], gate_w.at[e], weight_sems.at[0, e]),
            pltpu.make_async_copy(up_hbm.at[e], up_w.at[e], weight_sems.at[1, e]),
            pltpu.make_async_copy(down_hbm.at[e], down_w.at[e], weight_sems.at[2, e]),
        )
        for e in range(here)
    ]
    local = [pltpu.make_async_copy(normed_in, normed.at[0], local_sems.at[0])]
    for j in range(members):
        local.append(pltpu.make_async_copy(cot_in[j], cot.at[j], local_sems.at[1 + j]))
    for copy in local + list(weight_copies[0]):
        copy.start()
    greet(
        [{"fsdp": target(f, j, members)} for j in range(1, members)] + [opposite, ahead, behind]
    )
    near_core.start()
    for j in evens:
        near_far[j].start()
    hop[1].start()
    for e in range(1, here):
        for copy in weight_copies[e]:
            copy.start()
    for copy in local:
        copy.wait()
    near_core.wait_recv()

    chunk = width // 3
    thin = width // 3
    step = 2 * tokens

    def prepare(pair):
        at = pl.ds(pl.multiple_of(pair * step, step), step)
        tail = normed[pl.ds(2 * pair, 2), :, width:].reshape(step, LANES)
        gates[at, :] = gates_of(tail, experts)
        shares[at, :] = jnp.zeros((step, LANES), F32)

    def hidden_pass(pair):
        def one_expert(e, carry):
            @pl.when(pair == 0)
            def _():
                pltpu.make_async_copy(gate_hbm.at[e], gate_w.at[e], weight_sems.at[0, e]).wait()
                pltpu.make_async_copy(up_hbm.at[e], up_w.at[e], weight_sems.at[1, e]).wait()
                pltpu.make_async_copy(down_hbm.at[e], down_w.at[e], weight_sems.at[2, e]).wait()

            at = pl.ds(pl.multiple_of(pair * step, step), step)
            both = pl.ds(2 * pair, 2)
            columns = pl.ds(pl.multiple_of(e * hidden, LANES), hidden)
            inner, plain, scaled, grad_g, grad_u = hidden_terms(
                normed[both, :, :width].reshape(step, width),
                cot[both].reshape(step, width),
                gate_column(gates[at, :], f * here + e),
                gate_w[e],
                up_w[e],
                down_w[e],
            )
            all_inner[at, columns] = scaled
            all_g[at, columns] = grad_g
            all_u[at, columns] = grad_u
            share = jnp.sum(inner * plain, axis=-1, keepdims=True)
            lane = lax.broadcasted_iota(jnp.int32, (step, LANES), 1)
            shares[at, :] = jnp.where(lane == f * here + e, share, shares[at, :])
            return carry

        lax.fori_loop(0, here, one_expert, 0)

    def grad_pass(pair):
        def one_block(b, carry):
            at = pl.ds(pl.multiple_of(b * tokens, tokens), tokens)
            mean = jnp.sum(gates[at, :] * shares[at, :], axis=-1, keepdims=True)
            logits = (gates[at, :] * (shares[at, :] - mean)).astype(BF)
            router_ref[...] += tn(logits, normed[b, :, :width])[:PAD]

            def one_chunk(k, inner_carry):
                part = pl.ds(pl.multiple_of(k * thin, LANES), thin)
                total = nn(logits[:, :PAD], table_ref[:, part])
                for e in range(here):
                    columns = slice(e * hidden, (e + 1) * hidden)
                    total = total + nt(all_g[at, columns], gate_w[e, part, :])
                    total = total + nt(all_u[at, columns], up_w[e, part, :])
                parts[b, :, part] = total.astype(BF)
                return inner_carry

            return lax.fori_loop(0, width // thin, one_chunk, carry)

        lax.fori_loop(2 * pair, 2 * pair + 2, one_block, 0)

    def slot_arrived(s):
        hop[s].wait_recv()
        if s + 1 < slots:
            hop[s + 1].start()
        if s in whole_slots:
            whole[s].start()
            for j in evens:
                half[s, j].start()

    def half_arrived(s):
        if s in whole_slots:
            for j in evens:
                half[s, j].wait_recv()
                cross[s, j].start()
                relay_half[s, j].start()

    def cross_arrived(s):
        if s in whole_slots:
            for j in evens:
                cross[s, j].wait_recv()
                relay_cross[s, j].start()

    def moe_pass(pair):
        def one_moe(b, carry):
            at = pl.ds(pl.multiple_of(b * tokens, tokens), tokens)
            slot = lax.rem(b, 2)
            copy = pltpu.make_async_copy(moe_stage.at[slot], moe_ref.at[b], moe_sems.at[slot])
            pl.when(b >= 2)(copy.wait)

            def one_chunk(k, inner_carry):
                part = pl.ds(pl.multiple_of(k * thin, LANES), thin)
                down = down_w[:, :, part].reshape(here * hidden, thin)
                moe_stage[slot, :, part] = nn(all_inner[at, :], down).astype(BF)
                return inner_carry

            lax.fori_loop(0, width // thin, one_chunk, 0)
            copy.start()
            return carry

        lax.fori_loop(2 * pair, 2 * pair + 2, one_moe, 0)

    def far_ready():
        for j in evens:
            near_relay[j].wait_recv()

    def near_done():
        swap[0].start()
        for j in evens:
            near_far[j].wait_recv()
            near_relay[j].start()
        slot_arrived(1)
        for copy in [two_whole] + [two_half[j] for j in evens]:
            copy.start()

    def all_done():
        for j in evens:
            swap[j].start()
        if slots > 2:
            slot_arrived(2)
        for j in evens:
            swap[j].wait_recv()
            joined[j // 2] = (parts[j].astype(F32) + swapped[j // 2].astype(F32)).astype(BF)
            home[j].start()
        for copy in cuts:
            copy.start()
        cross_arrived(1)
        for j in evens:
            two_half[j].wait_recv()
            two_cross[j].start()
            two_relay[j].start()

    router_ref[...] = jnp.zeros_like(router_ref)

    def one_pair(pair, carry):
        pl.when(pair == 1)(far_ready)
        prepare(pair)
        hidden_pass(pair)
        pl.when(pair == 1)(functools.partial(half_arrived, 1))
        grad_pass(pair)
        pl.when(pair == 0)(near_done)
        pl.when(pair == members // 2 - 1)(all_done)
        moe_pass(pair)
        return carry

    lax.fori_loop(0, members // 2, one_pair, 0)
    for slot in range(2):
        pltpu.make_async_copy(moe_stage.at[slot], moe_ref.at[slot], moe_sems.at[slot]).wait()
    buffers = stage_gate.shape[0]

    def stage_copies(e, b):
        return (
            pltpu.make_async_copy(stage_gate.at[b], grad_gate_ref.at[e], stage_sems.at[0, b]),
            pltpu.make_async_copy(stage_up.at[b], grad_up_ref.at[e], stage_sems.at[1, b]),
            pltpu.make_async_copy(stage_down.at[b], grad_down_ref.at[e], stage_sems.at[2, b]),
        )

    def sum_home():
        swap[0].wait_recv()
        total = parts[0].astype(F32) + swapped[0].astype(F32)
        for j in evens:
            home[j].wait_recv()
            total = total + arrived[j // 2].astype(F32)
        mine_ref[...] = total.astype(BF)

    def middle_slots():
        half_arrived(2)
        for j in evens:
            two_cross[j].wait_recv()
            two_relay_cross[j].start()

    def later_slots():
        cross_arrived(2)
        for s in range(3, slots - 1):
            slot_arrived(s)
            half_arrived(s)
            cross_arrived(s)

    def weights_of(e, carry):
        b = lax.rem(e, buffers)

        @pl.when(e >= buffers)
        def _():
            for copy in stage_copies(e, b):
                copy.wait()

        columns = pl.ds(pl.multiple_of(e * hidden, LANES), hidden)
        rows = members * tokens

        def one_chunk(k, inner_carry):
            part = pl.ds(pl.multiple_of(k * chunk, LANES), chunk)
            left = normed[:, :, part].reshape(rows, chunk)
            right = cot[:, :, part].reshape(rows, chunk)
            stage_gate[b, part, :] = tn(left, all_g[:, columns])
            stage_up[b, part, :] = tn(left, all_u[:, columns])
            stage_down[b, :, part] = tn(all_inner[:, columns], right)
            return inner_carry

        lax.fori_loop(0, 3, one_chunk, 0)
        for copy in stage_copies(e, b):
            copy.start()
        pl.when(e == min(1, here - 1))(middle_slots)
        pl.when(e == here - 1)(sum_home)
        pl.when(e == here - 1)(later_slots)
        return carry

    lax.fori_loop(0, here, weights_of, 0)
    for e in range(max(here - buffers, 0), here):
        for copy in stage_copies(e, e % buffers):
            copy.wait()
    for s in whole_slots:
        whole[s].wait_recv()
        for j in evens:
            relay_half[s, j].wait_recv()
            relay_cross[s, j].wait_recv()
    for copy in cuts:
        copy.wait_recv()
    hop[slots - 1].wait_recv()
    two_whole.wait_recv()
    for j in evens:
        two_relay[j].wait_recv()
        two_relay_cross[j].wait_recv()
    for copy in net.made:
        copy.wait_send()


def own(table, normed, cotangent, cot_near, cot_two, normed_cut, gate_w, up_w, down_w, experts, slots):
    members = cot_near.shape[0]
    tokens, width = cotangent.shape
    here, _, hidden = gate_w.shape
    rows = members * tokens
    halves = members // 2
    buffers = 2 if members <= 4 else 1
    far = halves - 1
    copies = 1 + 2 * far + (slots - 1) * (2 + 4 * far) + halves + far + 1 + 4 * far + members - 1
    token_block = (tokens, width)
    return pl.pallas_call(
        functools.partial(own_kernel, members, slots, experts),
        out_shape=(
            shape((slots - 2, members, tokens, width + LANES), BF),
            shape((tokens, width + LANES), BF),
            shape(normed_cut.shape, BF),
            shape((members - 1, tokens, width), BF),
            shape((members, tokens, width), BF),
            shape(token_block, BF),
            shape((PAD, width), F32),
            shape(gate_w.shape, F32),
            shape(up_w.shape, F32),
            shape(down_w.shape, F32),
        ),
        in_specs=[VMEM] + [ANY] * 8,
        out_specs=(ANY, ANY, ANY, ANY, ANY, VMEM, VMEM, ANY, ANY, ANY),
        scratch_shapes=[
            pltpu.VMEM(gate_w.shape, BF),
            pltpu.VMEM(up_w.shape, BF),
            pltpu.VMEM(down_w.shape, BF),
            pltpu.VMEM((members, tokens, width + LANES), BF),
            pltpu.VMEM((members, tokens, width), BF),
            pltpu.VMEM((rows, here * hidden), BF),
            pltpu.VMEM((rows, here * hidden), BF),
            pltpu.VMEM((rows, here * hidden), BF),
            pltpu.VMEM((members,) + token_block, BF),
            pltpu.VMEM((halves,) + token_block, BF),
            pltpu.VMEM((halves,) + token_block, BF),
            pltpu.VMEM((halves,) + token_block, BF),
            pltpu.VMEM((buffers, width, hidden), F32),
            pltpu.VMEM((buffers, width, hidden), F32),
            pltpu.VMEM((buffers, hidden, width), F32),
            pltpu.VMEM((rows, LANES), F32),
            pltpu.VMEM((rows, LANES), F32),
            pltpu.SemaphoreType.DMA((2, copies)),
            pltpu.SemaphoreType.DMA((3, here)),
            pltpu.SemaphoreType.DMA((1 + members,)),
            pltpu.SemaphoreType.DMA((3, buffers)),
            pltpu.VMEM((2,) + token_block, BF),
            pltpu.SemaphoreType.DMA((2,)),
        ],
        compiler_params=pltpu.CompilerParams(
            vmem_limit_bytes=63 << 20, collective_id=1, has_side_effects=True
        ),
        name="own",
        cost_estimate=pl.CostEstimate(
            flops=18 * rows * width * hidden * here,
            bytes_accessed=18 * here * width * hidden,
            transcendentals=0,
        ),
    )(table, normed, cotangent, cot_near, cot_two, normed_cut, gate_w, up_w, down_w)


class Plan:
    def __init__(self, number, ins, outs, scratch, copies, build):
        self.number = number
        self.ins = ins
        self.outs = outs
        self.scratch = scratch
        self.copies = copies
        self.build = build


def more_weights_kernel(sources, counts, plan, experts, begin, index, *refs):
    in_normed, in_cot = counts
    refs = list(refs)

    def take(number):
        front = refs[:number]
        del refs[:number]
        return front

    normed_in = take(in_normed)
    cot_in = take(in_cot)
    gate_w, up_w, down_w, old_gate, old_up, old_down = take(6)
    plan_in = take(len(plan.ins))
    new_gate, new_up, new_down = take(3)
    plan_out = take(len(plan.outs))
    normed, cot, gates, all_inner, all_g, all_u, sems, remote_sems = take(8)
    plan_scratch = refs
    members, tokens, width = cot.shape
    rows = members * tokens
    here = index[1]
    step_at = pl.program_id(0)
    net = Sender(remote_sems)
    devices, begin_plan, ready, after, finish = plan.build(net, plan_in, plan_out, plan_scratch)
    last = pl.num_programs(0) - 1

    @pl.when(step_at == 0)
    def _():
        copies = []
        for group, refs_in, whole in ((0, normed_in, normed), (1, cot_in, cot)):
            for number, lead, first, count in sources[group]:
                ref = refs_in[number]
                ref = ref if lead is None else ref.at[lead]
                place = whole.at[first] if count == 1 else whole.at[pl.ds(first, count)]
                copies.append(pltpu.make_async_copy(ref, place, sems.at[len(copies)]))
        for copy in copies:
            copy.start()
        if devices:
            greet(devices)
        begin_plan()
        for copy in copies:
            copy.wait()
        gates[...] = gates_of(normed[:, :, width:].reshape(rows, LANES), experts)
        ready()

    expert = index[0] * here + begin + step_at
    many = 1 if plan.number in TILE_ONE else 2
    step = many * tokens

    def one_tile(b, carry):
        at = pl.ds(pl.multiple_of(b * step, step), step)
        pair = pl.ds(many * b, many)
        _, _, scaled, grad_g, grad_u = hidden_terms(
            normed[pair, :, :width].reshape(step, width),
            cot[pair].reshape(step, width),
            gate_column(gates[at, :], expert),
            gate_w[0],
            up_w[0],
            down_w[0],
        )
        all_inner[at, :] = scaled
        all_g[at, :] = grad_g
        all_u[at, :] = grad_u
        return carry

    straight = plan.number is None and rows <= 1024
    if straight:
        for b in range(rows // step):
            one_tile(b, 0)
    else:
        lax.fori_loop(0, rows // step, one_tile, 0)
    pieces = 1 if straight else 6 if plan.number in CHUNK_SIX else 3
    chunk = width // pieces

    def one_chunk(k, carry):
        at = pl.ds(pl.multiple_of(k * chunk, LANES), chunk)
        left = normed[:, :, at].reshape(rows, chunk)
        right = cot[:, :, at].reshape(rows, chunk)
        new_gate[0, at, :] = old_gate[0, at, :] + tn(left, all_g[...])
        new_up[0, at, :] = old_up[0, at, :] + tn(left, all_u[...])
        new_down[0, :, at] = old_down[0, :, at] + tn(all_inner[...], right)
        return carry

    if straight:
        one_chunk(0, 0)
    else:
        lax.fori_loop(0, pieces, one_chunk, 0)
    for number, hook in enumerate(after):
        pl.when(step_at == jnp.minimum(number, last))(hook)
    pl.when(step_at == last)(finish)


def more_weights(begin, count, index, normed, cotangent, sources, weights, earlier, experts, plan):
    here, width, hidden = weights[0].shape
    tokens = cotangent[0].shape[-2]
    members = max(first + many for _, _, first, many in sources[1])
    rows = members * tokens
    pick = lambda e: (e + begin, 0, 0)
    wide = pl.BlockSpec((1, width, hidden), pick)
    tall = pl.BlockSpec((1, hidden, width), pick)
    base = 1 + len(normed) + len(cotangent) + 3
    results = pl.pallas_call(
        functools.partial(
            more_weights_kernel,
            sources,
            (len(normed), len(cotangent)),
            plan,
            experts,
            begin,
        ),
        out_shape=tuple(shape(item.shape, F32) for item in earlier)
        + tuple(item for item, _ in plan.outs),
        grid=(count,),
        in_specs=[SMEM]
        + [ANY] * (len(normed) + len(cotangent))
        + [wide, wide, tall] * 2
        + [spec for _, spec in plan.ins],
        out_specs=(wide, wide, tall) + tuple(spec for _, spec in plan.outs),
        scratch_shapes=[
            pltpu.VMEM((members, tokens, width + LANES), BF),
            pltpu.VMEM((members, tokens, width), BF),
            pltpu.VMEM((rows, LANES), F32),
            pltpu.VMEM((rows, hidden), BF),
            pltpu.VMEM((rows, hidden), BF),
            pltpu.VMEM((rows, hidden), BF),
            pltpu.SemaphoreType.DMA((4,)),
            pltpu.SemaphoreType.DMA((2, plan.copies)),
        ]
        + list(plan.scratch),
        input_output_aliases={base + i: i for i in range(3)} if count < here else {},
        compiler_params=pltpu.CompilerParams(
            vmem_limit_bytes=63 << 20,
            collective_id=plan.number,
            has_side_effects=plan.number is not None,
        ),
        name="weights_" + str(plan.number),
        cost_estimate=pl.CostEstimate(
            flops=12 * rows * width * hidden * count,
            bytes_accessed=count * 30 * width * hidden + 4 * rows * width,
            transcendentals=0,
        ),
    )(index, *normed, *cotangent, *weights, *earlier, *[item for item, _ in plan.ins])
    return results[:3], results[3:]


def places(members, slots):
    f = lax.axis_index("fsdp")
    c = lax.axis_index("context")
    t = lax.axis_index("tensor")
    fsdp = {j: {"fsdp": target(f, j, members)} for j in range(1, members)}
    return f, c, t, fsdp, {"tensor": 1 - t}


def nothing():
    pass


def home_plan(number, members, slots, grad_part, moe_parts, cot_two):
    tokens, width = grad_part.shape
    halves = members // 2
    evens = range(2, members, 2)

    def build(net, ins, outs, scratch):
        part, moe_in, two_in = ins
        other, moe_mine, hops = outs
        own_part, swapped, joined, arrived, local = scratch
        f, c, t, fsdp, opposite = places(members, slots)
        cross_part = net.add(part, other, opposite)
        ahead = {"context": lax.rem(c + 1, slots)}
        behind = {"context": lax.rem(c + slots - 1, slots)}
        late = [
            net.add(two_in if i == 0 else hops.at[i - 1], hops.at[i], ahead)
            for i in range(slots - 3)
        ]
        swap = [net.add(moe_in.at[2 * i + 1], swapped.at[i], fsdp[1]) for i in range(halves)]
        home = {
            j: net.add(
                joined.at[j // 2], arrived.at[j // 2], {"fsdp": lax.rem(f + members - j, members)}
            )
            for j in evens
        }
        loads = [
            pltpu.make_async_copy(moe_in.at[2 * i], own_part.at[i], local.at[i])
            for i in range(halves)
        ]

        def start():
            for copy in [cross_part] + swap[1:] + swap[:1] + loads + late[:1]:
                copy.start()

        def ready():
            for copy in loads:
                copy.wait()
            for j in evens:
                swap[j // 2].wait_recv()
                joined[j // 2] = (
                    own_part[j // 2].astype(F32) + swapped[j // 2].astype(F32)
                ).astype(BF)
                home[j].start()

        def finish():
            swap[0].wait_recv()
            total = own_part[0].astype(F32) + swapped[0].astype(F32)
            for j in evens:
                home[j].wait_recv()
                total = total + arrived[j // 2].astype(F32)
            moe_mine[...] = total.astype(BF)
            cross_part.wait_recv()
            for i, copy in enumerate(late):
                copy.wait_recv()
                for following in late[i + 1 : i + 2]:
                    following.start()
            for copy in net.made:
                copy.wait_send()

        devices = [fsdp[1], opposite, ahead, behind] + [fsdp[j] for j in evens]
        return devices, start, ready, [], finish

    block = (halves, tokens, width)
    return Plan(
        number,
        [(grad_part, ANY), (moe_parts, ANY), (cot_two, ANY)],
        [
            (shape((tokens, width), BF), ANY),
            (shape((tokens, width), BF), VMEM),
            (shape((max(slots - 3, 1), tokens, width), BF), ANY),
        ],
        [pltpu.VMEM(block, BF)] * 4 + [pltpu.SemaphoreType.DMA((halves,))],
        1 + halves + halves - 1 + slots - 3,
        build,
    )


def keys_plan(number, members, slots, attention, grad_b, normed_last, cot_hops, late):
    heads, grad_heads, att, lse, turns, kv = attention
    _, tokens, cut = grad_b.shape
    wide = normed_last.shape[1]
    width = cot_hops.shape[2]
    side = tokens // 2
    evens = range(2, members, 2)
    groups = lse.shape[0]
    many = lse.shape[2]
    far = members // 2 - 1

    def build(net, ins, outs, scratch):
        heads_ref, grad_ref, att_ref, lse_ref, turns_ref, kv_ref = ins[:6]
        grad_in, last_in, hops_in, att_in = ins[6:]
        grad_q, own_kv, received, grad_near, spread_out, cot_out, att_near = outs
        grad_kv, wide_ref, acc, turned = scratch
        f, c, t, fsdp, opposite = places(members, slots)
        piece = pl.ds(pl.multiple_of(t * side, side), side)
        lower_half, upper_half = pl.ds(0, side), pl.ds(side, side)
        first_back = net.used
        net.used += slots - 1

        def back(s):
            at = first_back + s - 1
            return pltpu.make_async_remote_copy(
                src_ref=grad_kv.at[s - 1],
                dst_ref=received.at[s - 1],
                send_sem=net.sems.at[0, at],
                recv_sem=net.sems.at[1, at],
                device_id={"context": lax.rem(c + slots - s, slots)},
                device_id_type=pl.DeviceIdType.MESH,
            )

        cuts = []
        for j in range(1, members):
            cuts.append(net.add(grad_in.at[j], grad_near.at[j], fsdp[j]))
        sources = [(last_in, spread_out)]
        sources += [(hops_in.at[i], cot_out.at[i]) for i in range(late)]
        att_core = net.add(att_in, att_near.at[1], fsdp[1])
        att_far = [net.add(att_in, att_near.at[j], fsdp[j]) for j in evens]
        att_relay = [net.add(att_near.at[j], att_near.at[j + 1], fsdp[1]) for j in evens]
        whole, half, cross, relay, relay_cross = [], [], [], [], []
        for source, place in sources:
            whole.append(net.add(source, place.at[0], fsdp[1]))
            for j in evens:
                low, high = place.at[j - 1, lower_half], place.at[j - 1, upper_half]
                half.append(net.add(source.at[piece], low, fsdp[j]))
                cross.append(net.add(low, high, opposite))
                relay.append(net.add(low, place.at[j, lower_half], fsdp[1]))
                relay_cross.append(net.add(high, place.at[j, upper_half], fsdp[1]))

        def through(i, carry):
            s = slots - 1 - i

            @pl.when(c >= s)
            def _():
                attend_back_slot(s, heads_ref, grad_ref, lse_ref, kv_ref, wide_ref, acc, own_kv)

                @pl.when(s > 0)
                def _():
                    grad_kv[s - 1] = own_kv[...].astype(BF)
                    back(s).start()

            return carry

        def start():
            for copy in half + att_far + cuts + whole + [att_core]:
                copy.start()
            attend_back_start(heads_ref, grad_ref, att_ref, wide_ref, acc)
            lax.fori_loop(0, slots, through, 0)
            pass_on(0, far)
            attend_back_end(turns_ref, acc, turned, grad_q)

        def pass_on(low, high):
            for copy, following, other in list(zip(half, cross, relay))[low:high]:
                copy.wait_recv()
                following.start()
                other.start()

        def first():
            pass_on(far, len(half))

        def second():
            for copy, following in zip(att_far, att_relay):
                copy.wait_recv()
                following.start()

        def finish():
            for copy, following in zip(cross, relay_cross):
                copy.wait_recv()
                following.start()
            for s in range(1, slots):
                pl.when(c + s < slots)(back(s).wait_recv)
                pl.when(c >= s)(back(s).wait_send)
            for copy in cuts + whole + relay + relay_cross + att_relay + [att_core]:
                copy.wait_recv()
            for copy in net.made:
                copy.wait_send()

        devices = list(fsdp.values()) + [opposite]
        devices += [{"context": lax.rem(c + s, slots)} for s in range(1, slots)]
        return devices, start, nothing, [first, second], finish

    far = members // 2 - 1
    return Plan(
        number,
        [(item, VMEM) for item in attention]
        + [(grad_b, ANY), (normed_last, ANY), (cot_hops, ANY), (att, ANY)],
        [
            (shape(att.shape, BF), VMEM),
            (shape(kv.shape[1:], F32), VMEM),
            (shape((slots - 1,) + kv.shape[1:], BF), ANY),
            (shape((members, tokens, cut), BF), ANY),
            (shape((members - 1, tokens, wide), BF), ANY),
            (shape((max(late, 1), members - 1, tokens, width), BF), ANY),
            (shape((members,) + att.shape, BF), ANY),
        ],
        [
            pltpu.VMEM((slots - 1,) + kv.shape[1:], BF),
            pltpu.VMEM((groups, many, 2 * HEAD), BF),
            pltpu.VMEM((groups, many, HEAD), F32),
            pltpu.VMEM(att.shape, F32),
        ],
        (slots - 1) + (members - 1) + (1 + late) * (1 + 4 * far) + 1 + 2 * far,
        build,
    )


def rows_plan(
    number, members, slots, part_one, joined, router, gain_one, gain_two, payload
):
    tokens, width = part_one.shape
    cut = width // members
    evens = range(2, members, 2)
    rows = payload.shape[0] // slots

    def build(net, ins, outs, scratch):
        part_in, joined_in, router_ref, one_ref, two_ref, payload_in = ins
        other, joined_near, small_near, chunks = outs
        small_mine, small_other, small_sum, small_got, small_cut = scratch
        f, c, t, fsdp, opposite = places(members, slots)
        part_sent = net.add(part_in, other, opposite)
        small_sent = net.add(small_mine, small_other, opposite)
        core = net.add(joined_in, joined_near.at[1], fsdp[1])
        far_copy = {j: net.add(joined_in, joined_near.at[j], fsdp[j]) for j in evens}
        relay = {j: net.add(joined_near.at[j], joined_near.at[j + 1], fsdp[1]) for j in evens}
        small_cuts = []
        for j in range(1, members):
            small_cuts.append(net.add(small_cut.at[j], small_got.at[j], fsdp[j]))
        shares = []
        for s in range(1, slots):
            owner = lax.rem(c + s, slots)
            at = pl.ds(pl.multiple_of(owner * rows, 16), rows)
            shares.append(net.add(payload_in.at[at], chunks.at[s], {"context": owner}))

        def start():
            small = router_ref[...]
            row = lax.broadcasted_iota(jnp.int32, small.shape, 0)
            small = jnp.where(row == PAD - 8, one_ref[...], small)
            small = jnp.where(row == PAD - 7, 0.5 * two_ref[...], small)
            small_mine[...] = small.astype(BF)
            small_sent.start()
            for copy in [part_sent, core] + [far_copy[j] for j in evens] + shares:
                copy.start()

        def ready():
            small_sent.wait_recv()
            small_sum[...] = (small_mine[...].astype(F32) + small_other[...].astype(F32)).astype(BF)
            small_got[0] = columns_of(small_sum, f, cut)
            for j in range(1, members):
                small_cut[j] = columns_of(small_sum, target(f, j, members), cut)
            for copy in small_cuts:
                copy.start()

        def second():
            for j in evens:
                far_copy[j].wait_recv()
                relay[j].start()

        def finish():
            for copy in [part_sent, core] + [relay[j] for j in evens] + small_cuts + shares:
                copy.wait_recv()
            small_near[...] = small_got[...]
            for copy in net.made:
                copy.wait_send()

        devices = list(fsdp.values()) + [opposite]
        devices += [{"context": lax.rem(c + s, slots)} for s in range(1, slots)]
        return devices, start, ready, [nothing, second], finish

    far = members // 2 - 1
    small = (PAD, width)
    return Plan(
        number,
        [(part_one, ANY), (joined, ANY)]
        + [(router, VMEM), (gain_one, VMEM), (gain_two, VMEM), (payload, ANY)],
        [
            (shape((tokens, width), BF), ANY),
            (shape((members,) + joined.shape, BF), ANY),
            (shape((members, PAD, cut), BF), VMEM),
            (shape((slots, rows, payload.shape[1]), BF), ANY),
        ],
        [pltpu.VMEM(small, BF)] * 3 + [pltpu.VMEM((members, PAD, cut), BF)] * 2,
        2 + 1 + 2 * far + (members - 1) + (slots - 1),
        build,
    )


def chunk_plan(number, members, slots, payload, moe_mine):
    rows = payload.shape[0] // slots

    def build(net, ins, outs, scratch):
        f, c, t, fsdp, opposite = places(members, slots)
        copies = [net.add(ins[1], outs[1], opposite)]
        for s in range(1, slots):
            owner = lax.rem(c + s, slots)
            at = pl.ds(pl.multiple_of(owner * rows, 16), rows)
            copies.append(net.add(ins[0].at[at], outs[0].at[s], {"context": owner}))

        def start():
            for copy in copies:
                copy.start()

        def finish():
            for copy in copies:
                copy.wait_recv()
                copy.wait_send()

        devices = [{"context": lax.rem(c + s, slots)} for s in range(1, slots)]
        return devices + [opposite], start, nothing, [], finish

    return Plan(
        number,
        [(payload, ANY), (moe_mine, ANY)],
        [
            (shape((slots, rows, payload.shape[1]), BF), ANY),
            (shape(moe_mine.shape, BF), ANY),
        ],
        [],
        slots,
        build,
    )


def middle_kernel(members, index, hidden_ref, cot_ref, mine_ref, theirs_ref, table_ref, weights_ref, *refs):
    grad_ref, grad_b_ref, heads_ref, gain_ref, rounded, columns, summed = refs
    f = index[0]
    cut = weights_ref.shape[2]
    gain = table_ref[...].astype(F32)[PAD - 7 : PAD - 6, :]
    gain_ref[...] = jnp.zeros(gain_ref.shape, F32)
    tile = 64

    def one_tile(i, carry):
        at = pl.ds(pl.multiple_of(i * tile, tile), tile)
        hidden = hidden_ref[at, :]
        normed_grad = mine_ref[at, :].astype(F32) + theirs_ref[at, :].astype(F32)
        scale = lax.rsqrt(jnp.mean(hidden * hidden, axis=-1, keepdims=True) + norm_eps)
        weighted = normed_grad * gain
        cubed = scale * scale * scale
        grad = (
            cot_ref[at, :].astype(F32)
            + scale * weighted
            - hidden * cubed * jnp.mean(weighted * hidden, axis=-1, keepdims=True)
        )
        gain_ref[...] += jnp.sum(normed_grad * hidden * scale, axis=0, keepdims=True)
        grad_ref[at, :] = grad
        rounded[at, :] = grad.astype(BF)
        return carry

    lax.fori_loop(0, hidden_ref.shape[0] // tile, one_tile, 0)
    for j in range(members):
        grad_b_ref[j] = columns_of(rounded, target(f, j, members), cut)
        columns[j] = columns_of(rounded, member(f, j, members), cut)
    summed[...] = nt(columns[0], weights_ref[0])

    def one_member(j, carry):
        summed[...] += nt(columns[j], weights_ref[j])
        return carry

    lax.fori_loop(1, members, one_member, 0)
    total = summed[...].astype(BF)
    for h in range(heads_ref.shape[0]):
        heads_ref[h] = total[:, h * HEAD : (h + 1) * HEAD]


def middle(index, hidden, cotangent, mine, theirs, table, weights, after=()):
    members = weights.shape[0]
    tokens, width = hidden.shape
    heads = weights[0].shape[0] // HEAD
    return call(
        functools.partial(middle_kernel, members),
        (
            shape((tokens, width), F32),
            shape((members, tokens, width // members), BF),
            shape((heads, tokens, HEAD), BF),
            shape((1, width), F32),
        ),
        [SMEM] + [VMEM] * 6,
        (VMEM,) * 4,
        [
            pltpu.VMEM((tokens, width), BF),
            pltpu.VMEM((members, tokens, width // members), BF),
            pltpu.VMEM((tokens, heads * HEAD), F32),
        ],
        2 * tokens * width * heads * HEAD,
        16 * tokens * width,
        "middle",
        after,
    )(index, hidden, cotangent, mine, theirs, table, weights)


def lower_kernel(members, slots, index, grad_q_ref, own_ref, rows_ref, turns_ref, *refs):
    others = refs[0]
    weights = refs[1]
    joined_ref, part_ref, gain_ref = refs[2:]
    f = index[0]
    cut = weights.shape[1]
    total = own_ref[...]
    for s in range(1, slots):
        total = total + jnp.where(index[1] + s < slots, others[s - 1].astype(F32), 0.0)
    half = total.shape[1] // 2
    q_wide = grad_q_ref.shape[1]
    joined_ref[:, :q_wide] = grad_q_ref[...]
    keys = rotate(total[:, :half], turns_ref[:, :LANES], -turns_ref[:, LANES:])
    joined_ref[:, q_wide : q_wide + half] = keys.astype(BF)
    joined_ref[:, q_wide + half :] = total[:, half:].astype(BF)
    rows = rows_ref[...].astype(F32)
    scale = lax.rsqrt(jnp.mean(rows * rows, axis=-1, keepdims=True) + norm_eps)

    def one_pair(p, carry):
        owner = lax.rem(f + members - 2 * p, members)
        first = nt(joined_ref[...], weights[2 * p]).astype(BF)
        second = nt(joined_ref[...], weights[2 * p + 1]).astype(BF)
        put_columns(part_ref, owner, first, second)
        return carry

    lax.fori_loop(0, members // 2, one_pair, 0)
    gain_ref[...] = jnp.sum(part_ref[...].astype(F32) * rows * scale, axis=0, keepdims=True)


def lower(index, grad_q, own_kv, others, rows, turns, weights, after=()):
    members = len(weights)
    tokens, width = rows.shape
    wide = weights[0].shape[1]
    return call(
        functools.partial(lower_kernel, members, others.shape[0] + 1),
        (shape((tokens, wide), BF), shape((tokens, width), BF), shape((1, width), F32)),
        [SMEM] + [VMEM] * 6,
        (VMEM,) * 3,
        [],
        2 * tokens * width * wide,
        2 * width * wide,
        "lower",
        after,
    )(index, grad_q, own_kv, rows, turns, others, weights)


def last_kernel(
    rows_ref, grad_ref, mine_ref, theirs_ref, table_ref, hidden_ref, moe_ref, other_ref, out_ref, result_ref
):
    gain = table_ref[...].astype(F32)[PAD - 8 : PAD - 7, :]
    tile = 64

    def one_tile(i, carry):
        at = pl.ds(pl.multiple_of(i * tile, tile), tile)
        moe = moe_ref[at, :].astype(F32) + other_ref[at, :].astype(F32)
        result_ref[at, :] = (hidden_ref[at, :] + moe).astype(BF)
        rows = rows_ref[at, :].astype(F32)
        normed_grad = mine_ref[at, :].astype(F32) + theirs_ref[at, :].astype(F32)
        scale = lax.rsqrt(jnp.mean(rows * rows, axis=-1, keepdims=True) + norm_eps)
        weighted = normed_grad * gain
        cubed = scale * scale * scale
        out_ref[at, :] = (
            grad_ref[at, :]
            + scale * weighted
            - rows * cubed * jnp.mean(weighted * rows, axis=-1, keepdims=True)
        ).astype(BF)
        return carry

    lax.fori_loop(0, rows_ref.shape[0] // tile, one_tile, 0)


def last(rows, grad, mine, theirs, table, hidden, moe, other):
    tokens, width = rows.shape
    return call(
        last_kernel,
        (shape((tokens, width), BF), shape((tokens, width), BF)),
        [VMEM] * 8,
        (VMEM, VMEM),
        [],
        16 * tokens * width,
        20 * tokens * width,
        "last",
    )(rows, grad, mine, theirs, table, hidden, moe, other)


def product_kernel(extra, left_own, left, right_own, right, *refs):
    members = left.shape[0]
    out_ref = refs[-2]
    mine = [ref[0] if len(ref.shape) == 3 else ref[...] for ref in (left_own, right_own)]
    summed = refs[-1]
    summed[...] = tn(*mine)

    def one_member(j, carry):
        summed[...] += tn(left[j], right[j])
        return carry

    lax.fori_loop(1, members, one_member, 0)
    total = summed[...]
    rows, columns = total.shape
    out_ref[:rows, :] = total.astype(BF)
    if extra:
        small = refs[0]
        summed = small[0].astype(F32)
        for j in range(1, members):
            summed = summed + small[j].astype(F32)
        out_ref[rows:, :] = jnp.zeros((out_ref.shape[0] - rows, columns), BF)
        out_ref[rows : rows + PAD, : summed.shape[1]] = summed.astype(BF)


def product(left_own, left, right_own, right, small, extra_rows, name):
    members, tokens, rows = left.shape
    columns = right.shape[2]
    return call(
        functools.partial(product_kernel, len(small)),
        shape((rows + extra_rows, columns), BF),
        [VMEM] * (4 + len(small)),
        VMEM,
        [pltpu.VMEM((rows, columns), F32)],
        2 * members * tokens * rows * columns,
        4 * rows * columns,
        name,
    )(left_own, left, right_own, right, *small)


def chunk_sum(place, whole_ref, parts_ref):
    slots, rows, _ = parts_ref.shape
    total = whole_ref[pl.ds(pl.multiple_of(place * rows, 16), rows), :].astype(F32)
    for s in range(1, slots):
        total = total + parts_ref[s].astype(F32)
    return total.astype(BF)


def joint_sum_kernel(index, whole_ref, parts_ref, more_whole, more_parts, out_ref):
    rows, wide = parts_ref.shape[1:]
    many, columns = more_parts.shape[1:]
    out_ref[:rows, :] = chunk_sum(index[1], whole_ref, parts_ref)
    more = chunk_sum(index[1], more_whole, more_parts)
    fold = wide // columns
    each = many // fold
    if fold * columns < wide:
        out_ref[rows:, :] = jnp.zeros((each, wide), BF)
    for k in range(fold):
        out_ref[rows:, k * columns : (k + 1) * columns] = more[k * each : (k + 1) * each, :]


def joint_sum(index, whole, parts, more_whole, more_parts):
    slots, rows, columns = parts.shape
    many, narrow = more_parts.shape[1:]
    extra = many // (columns // narrow)
    return call(
        joint_sum_kernel,
        shape((rows + extra, columns), BF),
        [SMEM] + [VMEM] * 4,
        VMEM,
        [],
        slots * rows * columns,
        2 * (slots + 1) * rows * columns,
        "joint_sum",
    )(index, whole, parts, more_whole, more_parts)


def spread_kernel(slots, experts, index, *refs):
    parts = refs[:slots]
    query_ref, key_ref, value_ref, out_ref, one_ref, two_ref, router_ref, whole = refs[slots:]
    place = index[1]
    cut, q_wide = query_ref.shape
    kv_wide = key_ref.shape[1]
    rows = whole.shape[0] // slots
    many, columns = out_ref.shape
    each = parts[0].shape[0] - rows
    fold = parts[0].shape[1] // columns
    for s in range(slots):
        owner = lax.rem(place + slots - s, slots)
        whole[pl.ds(pl.multiple_of(owner * rows, 16), rows), :] = parts[s][:rows, :].astype(F32)
        for k in range(fold):
            base = owner * (many // slots) + k * each
            out_ref[pl.ds(pl.multiple_of(base, 16), each), :] = parts[s][
                rows:, k * columns : (k + 1) * columns
            ].astype(F32)
    query_ref[...] = whole[:cut, :q_wide]
    key_ref[...] = whole[:cut, q_wide : q_wide + kv_wide]
    value_ref[...] = whole[:cut, q_wide + kv_wide :]
    small = whole[cut : cut + PAD, :cut]
    one_ref[...] = small[PAD - 8]
    two_ref[...] = small[PAD - 7]
    router_ref[...] = small[:experts]


def spread(index, parts, rows, dims, experts):
    slots = len(parts)
    columns = parts[0].shape[1]
    return call(
        functools.partial(spread_kernel, slots, experts),
        tuple(shape(item, F32) for item in dims),
        [SMEM] + [VMEM] * slots,
        (VMEM,) * len(dims),
        [pltpu.VMEM((slots * rows, columns), F32)],
        slots * rows * columns,
        6 * slots * rows * columns,
        "spread",
    )(index, *parts)


def build(members, slots):
    def ring(item, step):
        return lax.ppermute(item, "context", [(i, (i + step) % slots) for i in range(slots)])

    def per_device(
        tokens,
        positions,
        expert_ids,
        norm1_gain,
        w_query,
        w_key,
        w_value,
        w_out,
        norm2_gain,
        w_router,
        w_gate,
        w_up,
        w_down,
        grad_output,
    ):
        rows = tokens[0]
        cotangent = grad_output[0]
        block = rows.shape[0]
        width = rows.shape[1]
        experts = w_router.shape[1]
        here = w_gate.shape[0]
        kv_wide = w_key.shape[1]
        q_wide = w_query.shape[1]
        f = lax.axis_index("fsdp")
        c = lax.axis_index("context")
        c_index = c.reshape(1)
        index = jnp.stack([f, c])
        f_here = jnp.stack([f, jnp.int32(here)])

        half = HEAD // 2
        lane = np.arange(2 * LANES)
        freq = np.exp(-math.log(10000.0) * 2.0 * np.arange(half, dtype=np.float32) / HEAD)
        sign = np.where(lane % HEAD < half, -1.0, 1.0).astype(np.float32)
        angle = positions[0].astype(F32)[:, None] * freq.astype(np.float32)[lane % half][None, :]
        turns = jnp.where((lane < LANES)[None, :], jnp.cos(angle), jnp.sin(angle) * sign[None, :])

        (
            table,
            normed_one,
            heads,
            kv_slots,
            att,
            lse,
            hidden,
            normed,
            qkv_w,
            out_mine,
            cot_near,
            cot_done,
            cot_two,
            normed_cut,
        ) = forward(
            (w_query, w_key, w_value),
            w_out,
            cotangent,
            (w_router.T, norm1_gain, norm2_gain),
            rows,
            turns,
            expert_ids[0].T,
            members,
            slots,
        )

        results = own(
            table,
            normed,
            cotangent,
            cot_near,
            cot_two,
            normed_cut,
            w_gate,
            w_up,
            w_down,
            experts,
            slots,
        )
        normed_slots, normed_last, normed_near, two_far, moe_parts = results[:5]
        grad_part, router_grad, *expert_grads = results[5:]


        parts = 2 if here % 2 == 0 else here
        queue = []
        for s in range(1, slots - 1):
            queue += [(s, p * (here // parts), here // parts) for p in range(parts)]

        def fill(plan, item, grads, normed_far=None, cot_far=None):
            s, begin, many = item
            if s < slots - 1:
                normed_refs, normed_from = [normed_slots], ((0, s - 1, 0, members),)
            else:
                normed_refs = [normed_last, normed_far]
                normed_from = ((0, None, 0, 1), (1, None, 1, members - 1))
            if s == 1:
                cot_refs, cot_from = [cot_done], ((0, 0, 0, members),)
            else:
                cot_refs = [cot_two, two_far] if s == 2 else [cot_hops, cot_far]
                lead = None if s == 2 else s - 3
                cot_from = ((0, lead, 0, 1), (1, lead, 1, members - 1))
            return more_weights(
                begin,
                many,
                f_here,
                normed_refs,
                cot_refs,
                (normed_from, cot_from),
                (w_gate, w_up, w_down),
                grads,
                experts,
                plan,
            )

        plan = home_plan(2, members, slots, grad_part, moe_parts, cot_two)
        expert_grads, (grad_other, moe_mine, cot_hops) = fill(plan, queue[0], expert_grads)

        grad_hidden, grad_hidden_b, grad_heads, gain_two = middle(
            index, hidden, cotangent, grad_part, grad_other, table, out_mine
        )
        attention = (heads, grad_heads, att, lse, turns, kv_slots)
        plan = keys_plan(
            3, members, slots, attention, grad_hidden_b, normed_last, cot_hops, max(slots - 3, 0)
        )
        expert_grads, results = fill(plan, queue[1], expert_grads)
        grad_q, own_kv, received, grad_near, normed_far, cot_far, att_near = results
        out_payload = product(att, att_near, grad_hidden_b, grad_near, (), 0, "out_grad")
        joined, part_one, gain_one = lower(
            index, grad_q, own_kv, received, rows, turns, qkv_w
        )
        plan = rows_plan(
            4,
            members,
            slots,
            part_one,
            joined,
            router_grad,
            gain_one,
            gain_two,
            out_payload,
        )
        expert_grads, results = fill(plan, queue[2], expert_grads, normed_far, cot_far)
        other_one, joined_near, small_near, out_chunks = results
        payload = product(
            normed_cut, normed_near, joined, joined_near, (small_near,), 2 * PAD, "qkv_grad"
        )
        plan = chunk_plan(5, members, slots, payload, moe_mine)
        expert_grads, (qkv_chunks, moe_other) = fill(
            plan, queue[3], expert_grads, normed_far, cot_far
        )
        total = joint_sum(index, payload, qkv_chunks, out_payload, out_chunks)
        shared = [total] + [ring(total, s) for s in range(1, slots)]
        grad_tokens, output = last(
            rows, grad_hidden, part_one, other_one, table, hidden, moe_mine, moe_other
        )
        none = Plan(None, [], [], [], 1, lambda *_: ([], nothing, nothing, [], nothing))
        for item in queue[4:] + [(slots - 1, 0, here)]:
            expert_grads, _ = fill(none, item, expert_grads, normed_far, cot_far)
        cut = w_query.shape[0]
        grad_query, grad_key, grad_value, grad_out, grad_one, grad_two, grad_router = spread(
            index,
            shared,
            payload.shape[0] // slots,
            (
                w_query.shape,
                w_key.shape,
                w_value.shape,
                w_out.shape,
                (cut,),
                (cut,),
                (experts, cut),
            ),
            experts,
        )
        return (
            output[None],
            grad_tokens[None],
            grad_one,
            grad_query,
            grad_key,
            grad_value,
            grad_out,
            grad_two,
            grad_router.T,
            expert_grads[0],
            expert_grads[1],
            expert_grads[2],
        )

    return per_device


def solution(mesh):
    return jax.shard_map(
        build(mesh.shape["fsdp"], mesh.shape["context"]),
        mesh=mesh,
        in_specs=(
            P("fsdp", "context", None),
            P("fsdp", "context"),
            P("fsdp", "context", None),
            P("fsdp"),
            P("fsdp", "tensor"),
            P("fsdp", "tensor"),
            P("fsdp", "tensor"),
            P("tensor", "fsdp"),
            P("fsdp"),
            P("fsdp", None),
            P("fsdp", None, "tensor"),
            P("fsdp", None, "tensor"),
            P("fsdp", "tensor", None),
            P("fsdp", "context", None),
        ),
        out_specs=(
            P("fsdp", "context", None),
            P("fsdp", "context", None),
            P("fsdp"),
            P("fsdp", "tensor"),
            P("fsdp", "tensor"),
            P("fsdp", "tensor"),
            P("tensor", "fsdp"),
            P("fsdp"),
            P("fsdp", None),
            P("fsdp", None, "tensor"),
            P("fsdp", None, "tensor"),
            P("fsdp", "tensor", None),
        ),
        check_vma=False,
    )
```

```python
import functools
import math

import jax
import jax.numpy as jnp
import numpy as np
from jax import lax
from jax.experimental import pallas as pl
from jax.experimental.pallas import tpu as pltpu
from jax.sharding import PartitionSpec as P

HEAD = 64
LANES = 128
PAD = 32
norm_eps = 1e-06
masked_score = -1e30
BF = jnp.bfloat16
F32 = jnp.float32
TILE_ONE = (5,)
CHUNK_SIX = (5,)
VMEM = pl.BlockSpec(memory_space=pltpu.VMEM)
SMEM = pl.BlockSpec(memory_space=pltpu.SMEM)
ANY = pl.BlockSpec(memory_space=pl.ANY)


def nn(left, right):
    return jnp.dot(left, right, preferred_element_type=F32)


def nt(left, right):
    return lax.dot_general(left, right, (((1,), (1,)), ((), ())), preferred_element_type=F32)


def tn(left, right):
    return lax.dot_general(left, right, (((0,), (0,)), ((), ())), preferred_element_type=F32)


def partner(f):
    return f + 1 - 2 * lax.rem(f, 2)


def member(f, j, members):
    base = lax.rem(f + members - (j - j % 2), members)
    return base if j % 2 == 0 else partner(base)


def columns_of(ref, owner, cut):
    if cut % LANES == 0:
        return ref[:, pl.ds(pl.multiple_of(owner * cut, LANES), cut)]
    pair = ref[:, pl.ds(pl.multiple_of(lax.div(owner, 2) * (2 * cut), LANES), 2 * cut)]
    return jnp.where(lax.rem(owner, 2) == 0, pair[:, :cut], pair[:, cut:])


def put_columns(ref, owner, first, second):
    cut = first.shape[1]
    if cut % LANES == 0:
        ref[:, pl.ds(pl.multiple_of(owner * cut, LANES), cut)] = first
        ref[:, pl.ds(pl.multiple_of(partner(owner) * cut, LANES), cut)] = second
    else:
        even = lax.rem(owner, 2) == 0
        both = [jnp.where(even, first, second), jnp.where(even, second, first)]
        at = pl.ds(pl.multiple_of(lax.div(owner, 2) * (2 * cut), LANES), 2 * cut)
        ref[:, at] = jnp.concatenate(both, axis=1)


def shape(dims, kind):
    return jax.ShapeDtypeStruct(dims, kind)


def call(kernel, outs, specs, out_specs, scratch, flops, moved, name, after=(), **more):
    skip = len(after)

    def body(*refs):
        kernel(*refs[skip:])

    run = pl.pallas_call(
        body,
        out_shape=outs,
        in_specs=[ANY] * skip + list(specs),
        out_specs=out_specs,
        scratch_shapes=scratch,
        compiler_params=pltpu.CompilerParams(vmem_limit_bytes=60 << 20),
        name=name,
        cost_estimate=pl.CostEstimate(flops=flops, bytes_accessed=moved, transcendentals=0),
        **more,
    )
    return lambda *operands: run(*after, *operands)


def rotate(rows, cos, sin):
    wide = rows.shape[1]
    count = wide // LANES
    after = pltpu.roll(rows, wide - HEAD // 2, 1)
    before = pltpu.roll(rows, HEAD // 2, 1)
    lane = lax.broadcasted_iota(jnp.int32, rows.shape, 1) % HEAD
    partner = jnp.where(lane < HEAD // 2, after, before)
    cos_all = jnp.concatenate([cos] * count, axis=1)
    sin_all = jnp.concatenate([sin] * count, axis=1)
    return rows * cos_all + partner * sin_all


class Sender:
    def __init__(self, sems):
        self.sems = sems
        self.used = 0
        self.made = []

    def add(self, source, target, device):
        copy = pltpu.make_async_remote_copy(
            src_ref=source,
            dst_ref=target,
            send_sem=self.sems.at[0, self.used],
            recv_sem=self.sems.at[1, self.used],
            device_id=device,
            device_id_type=pl.DeviceIdType.MESH,
        )
        self.used += 1
        self.made.append(copy)
        return copy


def greet(devices):
    barrier = pltpu.get_barrier_semaphore()
    for device in devices:
        pl.semaphore_signal(
            barrier, inc=1, device_id=device, device_id_type=pl.DeviceIdType.MESH
        )
    pl.semaphore_wait(barrier, len(devices))


def target(f, j, members):
    start = f if j % 2 == 0 else partner(f)
    return lax.rem(start + j - j % 2, members)


def attend_slot(s, heads_ref, kv, top, sums, acc):
    groups = top.shape[0]
    tokens = heads_ref.shape[1]
    repeat = heads_ref.shape[0] // groups
    half = kv.shape[2] // 2
    many = repeat * tokens
    keys = lax.broadcasted_iota(jnp.int32, (tokens, many), 0)
    queries = lax.broadcasted_iota(jnp.int32, (tokens, many), 1) % tokens
    allowed = keys <= queries + jnp.where(s == 0, 0, tokens)
    for g in range(groups):
        q = heads_ref[g * repeat : (g + 1) * repeat].reshape(many, HEAD)
        score = jnp.where(allowed, nt(kv[s, :, g * HEAD : (g + 1) * HEAD], q), masked_score)
        value = kv[s, :, half + g * HEAD : half + (g + 1) * HEAD]
        old = top[g]
        high = jnp.maximum(old, jnp.max(score, axis=0, keepdims=True))
        shrink = jnp.exp(old - high)
        weight = jnp.where(allowed, jnp.exp(score - high), 0.0)
        sums[g] = sums[g] * shrink + jnp.sum(weight, axis=0, keepdims=True)
        acc[g] = acc[g] * shrink + tn(value, weight.astype(BF))
        top[g] = high


def attend_end(att_ref, lse_ref, top, sums, acc):
    groups, _, many = top.shape
    tokens = att_ref.shape[0]
    repeat = many // tokens
    for g in range(groups):
        lse_ref[g] = top[g] + jnp.log(sums[g])
        done = jnp.transpose(acc[g] / sums[g]).astype(BF)
        for r in range(repeat):
            h = g * repeat + r
            att_ref[:, h * HEAD : (h + 1) * HEAD] = done[r * tokens : (r + 1) * tokens]


def forward_kernel(
    members,
    slots,
    query_in,
    key_in,
    value_in,
    wout_in,
    cot_in,
    router_ref,
    one_ref,
    two_ref,
    rows_ref,
    turns_ref,
    ids_ref,
    *refs,
):
    (
        table_ref,
        normed_one_ref,
        heads_ref,
        kv_out,
        att_ref,
        lse_ref,
        hidden_ref,
        normed_ref,
        qkv_out,
        wout_out,
        cot_near,
        cot_done,
        cot_two,
        cut_ref,
        small,
        qkv,
        mine,
        theirs,
        kv,
        total,
        first,
        second,
        other,
        top,
        sums,
        acc,
        sems,
        local_sems,
    ) = refs
    f = lax.axis_index("fsdp")
    c = lax.axis_index("context")
    t = lax.axis_index("tensor")
    tokens, width = rows_ref.shape
    side = tokens // 2
    experts, cut = router_ref.shape
    evens = range(2, members, 2)
    beside = {"fsdp": partner(f)}
    opposite = {"tensor": 1 - t}
    ahead = {"context": lax.rem(c + 1, slots)}
    apart = {j: {"fsdp": lax.rem(f + j, members)} for j in evens}
    lower_half, upper_half = pl.ds(0, side), pl.ds(side, side)
    piece = pl.ds(pl.multiple_of(t * side, side), side)

    net = Sender(sems)
    small_sent = [
        net.add(small.at[0], small.at[j], {"fsdp": target(f, j, members)}) for j in range(1, members)
    ]

    def family(source, place):
        return (
            net.add(source, place.at[1], beside),
            {j: net.add(source, place.at[j], apart[j]) for j in evens},
            {j: net.add(place.at[j], place.at[j + 1], beside) for j in evens},
        )

    q_wide, kv_wide = query_in.shape[1], key_in.shape[1]
    bounds = (0, q_wide, q_wide + kv_wide, q_wide + 2 * kv_wide)
    projections = [
        (source, pl.ds(low, high - low))
        for source, low, high in zip((query_in, key_in, value_in), bounds, bounds[1:])
    ]
    groups_of = {"query": projections[:1], "keys": projections[1:]}
    spans = {"query": pl.ds(0, q_wide), "keys": pl.ds(q_wide, 2 * kv_wide)}
    qkv_core, qkv_far, qkv_relay = {}, {}, {}
    for name in ("keys", "query"):
        qkv_core[name] = [net.add(source, qkv.at[1, :, at], beside) for source, at in groups_of[name]]
        qkv_far[name] = {
            j: [net.add(source, qkv.at[j, :, at], apart[j]) for source, at in groups_of[name]]
            for j in evens
        }
        span = spans[name]
        qkv_relay[name] = {
            j: net.add(qkv.at[j, :, span], qkv.at[j + 1, :, span], beside) for j in evens
        }
    out_core, out_far, out_relay = family(wout_in, mine)
    out_cross = {j: net.add(wout_in if j == 0 else mine.at[j], theirs.at[j], opposite) for j in range(0, members, 2)}
    out_cross_relay = {j: net.add(theirs.at[j], theirs.at[j + 1], beside) for j in range(0, members, 2)}
    cot_core, cot_far, cot_relay = family(cot_in, cot_near)
    done = cot_done.shape[0]
    hop, whole, half, cross, relay_half, relay_cross = {}, {}, {}, {}, {}, {}
    hop[1] = net.add(cot_in, cot_done.at[0, 0], ahead)
    if slots > 2:
        hop[2] = net.add(cot_done.at[0, 0], cot_two, ahead)
    for s in range(1, done + 1):
        now = cot_done.at[s - 1]
        whole[s] = net.add(now.at[0], now.at[1], beside)
        for j in evens:
            half[s, j] = net.add(now.at[0, piece], now.at[j, lower_half], apart[j])
            cross[s, j] = net.add(now.at[j, lower_half], now.at[j, upper_half], opposite)
            relay_half[s, j] = net.add(now.at[j, lower_half], now.at[j + 1, lower_half], beside)
            relay_cross[s, j] = net.add(now.at[j, upper_half], now.at[j + 1, upper_half], beside)
    plain = len(net.made)
    first_later = net.used
    net.used += slots - 1

    def later(s):
        at = first_later + s - 1
        return pltpu.make_async_remote_copy(
            src_ref=kv.at[s - 1],
            dst_ref=kv.at[s],
            send_sem=sems.at[0, at],
            recv_sem=sems.at[1, at],
            device_id=ahead,
            device_id_type=pl.DeviceIdType.MESH,
        )

    plain_made = net.made[:plain]
    att_sent = net.add(att_ref, other, opposite)

    locals_in = [
        pltpu.make_async_copy(source, qkv.at[0, :, at], sem)
        for (source, at), sem in zip(projections, [local_sems.at[i] for i in (0, 1, 2)])
    ]
    locals_in.append(pltpu.make_async_copy(wout_in, mine.at[0], local_sems.at[5 + slots]))
    qkv_saved = pltpu.make_async_copy(qkv, qkv_out, local_sems.at[3])
    out_saved = pltpu.make_async_copy(mine, wout_out, local_sems.at[4])
    kv_saved = [
        pltpu.make_async_copy(kv.at[s], kv_out.at[s], local_sems.at[5 + s]) for s in range(slots)
    ]
    for copy in locals_in:
        copy.start()
    small[0] = jnp.zeros((PAD, cut), BF)
    small[0, :experts, :] = router_ref[...]
    small[0, PAD - 8, :] = one_ref[...]
    small[0, PAD - 7, :] = two_ref[...]
    greet(
        [{"fsdp": target(f, j, members)} for j in range(1, members)]
        + [opposite]
        + [ahead, {"context": lax.rem(c + slots - 1, slots)}]
    )
    for copy in small_sent:
        copy.start()
    for name in ("keys", "query"):
        for copies in [qkv_core[name]] + [qkv_far[name][j] for j in evens]:
            for copy in copies:
                copy.start()
    for copy in [out_core, out_cross[0]] + [out_far[j] for j in evens]:
        copy.start()
    hop[1].start()
    cot_core.start()

    rows = rows_ref[...].astype(F32)
    scale = lax.rsqrt(jnp.mean(rows * rows, axis=-1, keepdims=True) + norm_eps)
    hidden_ref[...] = rows * scale
    for copy in locals_in:
        copy.wait()
    for copy in small_sent:
        copy.wait_recv()

    for j in range(0, members, 2):
        put_columns(table_ref, member(f, j, members), small[j], small[j + 1])
    gain = table_ref[...].astype(F32)[PAD - 8 : PAD - 7, :]
    normed_one_ref[...] = (hidden_ref[...] * gain).astype(BF)
    for j in range(members):
        cut_ref[j] = columns_of(normed_one_ref, target(f, j, members), cut)

    total[...] = jnp.zeros(total.shape, F32)

    def product_of(name):
        span = spans[name]

        def far_arrived(j):
            for copy in qkv_far[name][j]:
                copy.wait_recv()
            qkv_relay[name][j].start()

        def core_arrived():
            for copy in qkv_core[name]:
                copy.wait_recv()

        def one_pair(p, carry):
            owner = lax.rem(f + members - 2 * p, members)
            for j in evens:
                pl.when(2 * p == j)(functools.partial(far_arrived, j))
            left = columns_of(normed_one_ref, owner, cut)
            total[:, span] += nn(left, qkv[2 * p, :, span])
            pl.when(p == 0)(core_arrived)
            for j in evens:
                pl.when(2 * p == j)(qkv_relay[name][j].wait_recv)
            left = columns_of(normed_one_ref, partner(owner), cut)
            total[:, span] += nn(left, qkv[2 * p + 1, :, span])
            return carry

        lax.fori_loop(0, members // 2, one_pair, 0)

    cos = turns_ref[:, :LANES]
    sin = turns_ref[:, LANES:]
    product_of("keys")
    kv[0, :, :kv_wide] = rotate(total[:, q_wide : q_wide + kv_wide], cos, sin).astype(BF)
    kv[0, :, kv_wide:] = total[:, q_wide + kv_wide :].astype(BF)
    pl.when(c + 1 < slots)(later(1).start)
    hop[1].wait_recv()
    if slots > 2:
        pl.when(c == slots - 1)(hop[2].start)
    whole[1].start()
    for j in evens:
        half[1, j].start()
    for j in evens:
        cot_far[j].start()
    product_of("query")
    qkv_saved.start()
    turned = (rotate(total[:, :q_wide], cos, sin) * (1.0 / math.sqrt(HEAD))).astype(BF)
    for h in range(q_wide // HEAD):
        heads_ref[h] = turned[:, h * HEAD : (h + 1) * HEAD]
    top[...] = jnp.full(top.shape, masked_score, F32)
    sums[...] = jnp.zeros(sums.shape, F32)
    acc[...] = jnp.zeros(acc.shape, F32)
    def weights_arrived():
        for j in evens:
            out_far[j].wait_recv()
            out_relay[j].start()
            out_cross[j].start()
        out_cross[0].wait_recv()
        out_cross_relay[0].start()


    def half_arrived(s):
        for j in evens:
            half[s, j].wait_recv()
            relay_half[s, j].start()
            cross[s, j].start()

    def keys_arrived(s, carry):
        @pl.when(c >= s)
        def _():
            @pl.when(s > 0)
            def _():
                later(s).wait_recv()

                @pl.when((c + 1 < slots) & (s + 1 < slots))
                def _():
                    later(s + 1).start()

            if slots > 2:
                pl.when((s == c) & (c + 1 < slots))(hop[2].start)
            attend_slot(s, heads_ref, kv, top, sums, acc)

        pl.when(s == 0)(weights_arrived)
        pl.when(s == 1)(functools.partial(half_arrived, 1))
        return carry

    lax.fori_loop(0, slots, keys_arrived, 0)
    kv_saved[0].start()
    for s in range(1, slots):
        pl.when(c >= s)(kv_saved[s].start)
    attend_end(att_ref, lse_ref, top, sums, acc)
    att_sent.start()

    out_core.wait_recv()
    for j in evens:
        out_relay[j].wait_recv()
    out_saved.start()
    def mixed(left, weights, place):
        def one_pair(p, carry):
            owner = lax.rem(f + members - 2 * p, members)
            pair = nn(left[...], weights[2 * p]), nn(left[...], weights[2 * p + 1])
            put_columns(place, owner, *pair)
            return carry

        lax.fori_loop(0, members // 2, one_pair, 0)

    mixed(att_ref, mine, first)
    for j in evens:
        out_cross[j].wait_recv()
        out_cross_relay[j].start()
    for j in evens:
        cross[1, j].wait_recv()
        relay_cross[1, j].start()
    for j in range(0, members, 2):
        out_cross_relay[j].wait_recv()
    att_sent.wait_recv()
    mixed(other, theirs, second)

    gain_two = table_ref[...].astype(F32)[PAD - 7 : PAD - 6, :]
    tile = 64

    def one_tile(i, carry):
        at = pl.ds(pl.multiple_of(i * tile, tile), tile)
        hidden = rows_ref[at, :].astype(F32) + (first[at, :] + second[at, :])
        hidden_ref[at, :] = hidden
        scale = lax.rsqrt(jnp.mean(hidden * hidden, axis=-1, keepdims=True) + norm_eps)
        normed_ref[at, :width] = (hidden * scale * gain_two).astype(BF)
        return carry

    lax.fori_loop(0, tokens // tile, one_tile, 0)
    logits = nt(normed_ref[:, :width], table_ref[...])
    lanes = lax.broadcasted_iota(jnp.int32, logits.shape, 1)
    ids = jnp.transpose(ids_ref[...].astype(F32)).astype(jnp.int32)
    mask = ids[:, 0:1] == lanes
    for k in range(1, ids.shape[1]):
        mask = mask | (ids[:, k : k + 1] == lanes)
    logits = jnp.where(mask, logits, masked_score)
    weight = jnp.where(mask, jnp.exp(logits - jnp.max(logits, axis=-1, keepdims=True)), 0.0)
    gates = weight / jnp.sum(weight, axis=-1, keepdims=True)
    upper = gates.astype(BF).astype(F32)
    lower = gates - upper
    blank = jnp.zeros((gates.shape[0], LANES - 2 * PAD), F32)
    normed_ref[:, width:] = jnp.concatenate([upper, lower, blank], axis=1).astype(BF)

    for j in evens:
        cot_far[j].wait_recv()
        cot_relay[j].start()
    if slots > 2:
        hop[2].wait_recv()
    cot_core.wait_recv()
    for j in evens:
        cot_relay[j].wait_recv()
    for s in range(1, done + 1):
        whole[s].wait_recv()
        for j in evens:
            relay_half[s, j].wait_recv()
            relay_cross[s, j].wait_recv()
    qkv_saved.wait()
    out_saved.wait()
    kv_saved[0].wait()
    for s in range(1, slots):
        pl.when(c >= s)(kv_saved[s].wait)
    for copy in plain_made:
        copy.wait_send()
    for s in range(1, slots):
        pl.when((c >= s - 1) & (c + 1 < slots))(later(s).wait_send)
    att_sent.wait_send()


def forward(projections, wout, cotangent, small, rows, turns, ids, members, slots):
    tokens, width = rows.shape
    cut, q_wide = projections[0].shape
    kv_wide = projections[1].shape[1]
    wide = q_wide + 2 * kv_wide
    heads = q_wide // HEAD
    groups = kv_wide // HEAD
    many = heads // groups * tokens
    halves = members // 2
    far = halves - 1
    done = 1
    copies = (members - 1) + 2 * (1 + 2 * far) + 3 * (1 + far) + 2 * far + 2 * halves
    copies += (slots - 1) + 1 + done * (1 + 4 * far) + 2
    return pl.pallas_call(
        functools.partial(forward_kernel, members, slots),
        out_shape=(
            shape((PAD, width), BF),
            shape((tokens, width), BF),
            shape((heads, tokens, HEAD), BF),
            shape((slots, tokens, 2 * kv_wide), BF),
            shape((tokens, q_wide), BF),
            shape((groups, 1, many), F32),
            shape((tokens, width), F32),
            shape((tokens, width + LANES), BF),
            shape((members, cut, wide), BF),
            shape((members,) + wout.shape, BF),
            shape((members, tokens, width), BF),
            shape((done, members, tokens, width), BF),
            shape((tokens, width), BF),
            shape((members, tokens, width // members), BF),
        ),
        in_specs=[ANY] * 5 + [VMEM] * 6,
        out_specs=(VMEM, VMEM, VMEM, ANY, VMEM, VMEM, VMEM, VMEM) + (ANY,) * 5 + (VMEM,),
        scratch_shapes=[
            pltpu.VMEM((members, PAD, cut), BF),
            pltpu.VMEM((members, cut, wide), BF),
            pltpu.VMEM((members,) + wout.shape, BF),
            pltpu.VMEM((members,) + wout.shape, BF),
            pltpu.VMEM((slots, tokens, 2 * kv_wide), BF),
            pltpu.VMEM((tokens, wide), F32),
            pltpu.VMEM((tokens, width), F32),
            pltpu.VMEM((tokens, width), F32),
            pltpu.VMEM((tokens, q_wide), BF),
            pltpu.VMEM((groups, 1, many), F32),
            pltpu.VMEM((groups, 1, many), F32),
            pltpu.VMEM((groups, HEAD, many), F32),
            pltpu.SemaphoreType.DMA((2, copies)),
            pltpu.SemaphoreType.DMA((7 + slots,)),
        ],
        compiler_params=pltpu.CompilerParams(
            vmem_limit_bytes=60 << 20, collective_id=0, has_side_effects=True
        ),
        name="forward",
        cost_estimate=pl.CostEstimate(
            flops=8 * tokens * width * wide, bytes_accessed=8 * width * wide, transcendentals=0
        ),
    )(*projections, wout, cotangent, *small, rows, turns, ids)


def attend_back_start(heads_ref, grad_ref, att_ref, wide, acc):
    groups, many, _ = wide.shape
    repeat = heads_ref.shape[0] // groups
    lane = lax.broadcasted_iota(jnp.int32, (many, 2 * HEAD), 1)
    for g in range(groups):
        grad = grad_ref[g * repeat : (g + 1) * repeat].reshape(many, HEAD).astype(F32)
        out = jnp.concatenate(
            [
                att_ref[:, (g * repeat + r) * HEAD : (g * repeat + r + 1) * HEAD]
                for r in range(repeat)
            ],
            axis=0,
        )
        delta = jnp.sum(grad * out.astype(F32), axis=-1, keepdims=True)
        upper = delta.astype(BF).astype(F32)
        both = jnp.concatenate([grad, jnp.zeros((many, HEAD), F32)], axis=1)
        both = jnp.where(lane == HEAD, -upper, jnp.where(lane == HEAD + 1, upper - delta, both))
        wide[g] = both.astype(BF)
        acc[g] = jnp.zeros((many, HEAD), F32)


def attend_back_slot(s, heads_ref, grad_ref, lse_ref, kv, wide, acc, grad_kv):
    groups, many, _ = wide.shape
    tokens = heads_ref.shape[1]
    repeat = heads_ref.shape[0] // groups
    half = kv.shape[2] // 2
    keys = lax.broadcasted_iota(jnp.int32, (tokens, many), 0)
    queries = lax.broadcasted_iota(jnp.int32, (tokens, many), 1) % tokens
    allowed = keys <= queries + jnp.where(s == 0, 0, tokens)
    for g in range(groups):
        at = slice(g * HEAD, (g + 1) * HEAD)
        behind = slice(half + g * HEAD, half + (g + 1) * HEAD)
        q = heads_ref[g * repeat : (g + 1) * repeat].reshape(many, HEAD)
        grad = grad_ref[g * repeat : (g + 1) * repeat].reshape(many, HEAD)
        key = kv[s, :, at]
        value = kv[s, :, behind]
        value = jnp.concatenate([value, jnp.ones_like(value)], axis=1)
        prob = jnp.where(allowed, jnp.exp(nt(key, q) - lse_ref[g]), 0.0)
        grad_score = (prob * nt(value, wide[g])).astype(BF)
        grad_kv[:, at] = nn(grad_score, q)
        grad_kv[:, behind] = nn(prob.astype(BF), grad)
        acc[g] += tn(grad_score, key)


def attend_back_end(turns_ref, acc, turned, grad_q_ref):
    groups, many, _ = acc.shape
    tokens = turned.shape[0]
    repeat = many // tokens
    for g in range(groups):
        done = acc[g] * (1.0 / math.sqrt(HEAD))
        for r in range(repeat):
            h = g * repeat + r
            turned[:, h * HEAD : (h + 1) * HEAD] = done[r * tokens : (r + 1) * tokens]
    grad_q_ref[...] = rotate(turned[...], turns_ref[:, :LANES], -turns_ref[:, LANES:]).astype(BF)


def gates_of(tail, experts):
    rows = tail.astype(F32)
    both = rows + pltpu.roll(rows, LANES - PAD, 1)
    lane = lax.broadcasted_iota(jnp.int32, both.shape, 1)
    return jnp.where(lane < experts, both, 0.0)


def gate_column(gates, expert):
    lane = lax.broadcasted_iota(jnp.int32, gates.shape, 1)
    return jnp.sum(jnp.where(lane == expert, gates, 0.0), axis=-1, keepdims=True)


def hidden_terms(normed, cotangent, gate_col, gate_w, up_w, down_w):
    gate_pre = nn(normed, gate_w)
    up_pre = nn(normed, up_w)
    plain = nt(cotangent, down_w)
    sigma = 1.0 / (1.0 + jnp.exp(-gate_pre))
    activated = gate_pre * sigma
    inner = activated * up_pre
    grad_inner = gate_col * plain
    scaled = (gate_col * inner).astype(BF)
    grad_g = (grad_inner * up_pre * (sigma + activated * (1.0 - sigma))).astype(BF)
    grad_u = (grad_inner * activated).astype(BF)
    return inner, plain, scaled, grad_g, grad_u


def own_kernel(members, slots, experts, table_ref, normed_in, cot_own, cot_near, cot_two, cut_in, *refs):
    cot_in = [cot_own] + [cot_near.at[j] for j in range(1, members)]
    gate_hbm, up_hbm, down_hbm = refs[:3]
    (
        far_ref,
        last_ref,
        cut_near,
        two_out,
        moe_ref,
        mine_ref,
        router_ref,
        grad_gate_ref,
        grad_up_ref,
        grad_down_ref,
        gate_w,
        up_w,
        down_w,
        normed,
        cot,
        all_inner,
        all_g,
        all_u,
        parts,
        swapped,
        joined,
        arrived,
        stage_gate,
        stage_up,
        stage_down,
        gates,
        shares,
        sems,
        weight_sems,
        local_sems,
        stage_sems,
        moe_stage,
        moe_sems,
    ) = refs[3:]
    f = lax.axis_index("fsdp")
    c = lax.axis_index("context")
    t = lax.axis_index("tensor")
    here = gate_w.shape[0]
    hidden = gate_w.shape[2]
    tokens = normed_in.shape[0]
    side = tokens // 2
    width = cot.shape[2]
    evens = range(2, members, 2)
    beside = {"fsdp": partner(f)}
    opposite = {"tensor": 1 - t}
    ahead = {"context": lax.rem(c + 1, slots)}
    behind = {"context": lax.rem(c + slots - 1, slots)}
    apart = {j: {"fsdp": lax.rem(f + j, members)} for j in evens}
    owner = {j: {"fsdp": lax.rem(f + members - j, members)} for j in evens}

    net = Sender(sems)
    near_core = net.add(normed_in, normed.at[1], beside)
    near_far = {j: net.add(normed_in, normed.at[j], apart[j]) for j in evens}
    near_relay = {j: net.add(normed.at[j], normed.at[j + 1], beside) for j in evens}
    hop, whole, half, cross, relay_half, relay_cross = {}, {}, {}, {}, {}, {}
    lower_half, upper_half = pl.ds(0, side), pl.ds(side, side)
    piece = pl.ds(pl.multiple_of(t * side, side), side)
    whole_slots = range(1, slots - 1)
    for s in range(1, slots):
        origin = normed_in if s == 1 else far_ref.at[s - 2, 0]
        hop[s] = net.add(origin, far_ref.at[s - 1, 0] if s < slots - 1 else last_ref, ahead)
    for s in whole_slots:
        now = far_ref.at[s - 1]
        whole[s] = net.add(now.at[0], now.at[1], beside)
        for j in evens:
            half[s, j] = net.add(now.at[0, piece], now.at[j, lower_half], apart[j])
            cross[s, j] = net.add(now.at[j, lower_half], now.at[j, upper_half], opposite)
            relay_half[s, j] = net.add(now.at[j, lower_half], now.at[j + 1, lower_half], beside)
            relay_cross[s, j] = net.add(now.at[j, upper_half], now.at[j + 1, upper_half], beside)
    cuts = [
        net.add(cut_in.at[j], cut_near.at[j], {"fsdp": target(f, j, members)})
        for j in range(1, members)
    ]
    two_whole = net.add(cot_two, two_out.at[0], beside)
    two_half, two_cross, two_relay, two_relay_cross = {}, {}, {}, {}
    for j in evens:
        low, high = two_out.at[j - 1, lower_half], two_out.at[j - 1, upper_half]
        two_half[j] = net.add(cot_two.at[piece], low, apart[j])
        two_cross[j] = net.add(low, high, opposite)
        two_relay[j] = net.add(low, two_out.at[j, lower_half], beside)
        two_relay_cross[j] = net.add(high, two_out.at[j, upper_half], beside)
    swap = {
        j: net.add(parts.at[j + 1], swapped.at[j // 2], beside) for j in range(0, members, 2)
    }
    home = {j: net.add(joined.at[j // 2], arrived.at[j // 2], owner[j]) for j in evens}

    weight_copies = [
        (
            pltpu.make_async_copy(gate_hbm.at[e], gate_w.at[e], weight_sems.at[0, e]),
            pltpu.make_async_copy(up_hbm.at[e], up_w.at[e], weight_sems.at[1, e]),
            pltpu.make_async_copy(down_hbm.at[e], down_w.at[e], weight_sems.at[2, e]),
        )
        for e in range(here)
    ]
    local = [pltpu.make_async_copy(normed_in, normed.at[0], local_sems.at[0])]
    for j in range(members):
        local.append(pltpu.make_async_copy(cot_in[j], cot.at[j], local_sems.at[1 + j]))
    for copy in local + list(weight_copies[0]):
        copy.start()
    greet(
        [{"fsdp": target(f, j, members)} for j in range(1, members)] + [opposite, ahead, behind]
    )
    near_core.start()
    for j in evens:
        near_far[j].start()
    hop[1].start()
    for e in range(1, here):
        for copy in weight_copies[e]:
            copy.start()
    for copy in local:
        copy.wait()
    near_core.wait_recv()

    chunk = width // 3
    thin = width // 3
    step = 2 * tokens

    def prepare(pair):
        at = pl.ds(pl.multiple_of(pair * step, step), step)
        tail = normed[pl.ds(2 * pair, 2), :, width:].reshape(step, LANES)
        gates[at, :] = gates_of(tail, experts)
        shares[at, :] = jnp.zeros((step, LANES), F32)

    def hidden_pass(pair):
        def one_expert(e, carry):
            @pl.when(pair == 0)
            def _():
                pltpu.make_async_copy(gate_hbm.at[e], gate_w.at[e], weight_sems.at[0, e]).wait()
                pltpu.make_async_copy(up_hbm.at[e], up_w.at[e], weight_sems.at[1, e]).wait()
                pltpu.make_async_copy(down_hbm.at[e], down_w.at[e], weight_sems.at[2, e]).wait()

            at = pl.ds(pl.multiple_of(pair * step, step), step)
            both = pl.ds(2 * pair, 2)
            columns = pl.ds(pl.multiple_of(e * hidden, LANES), hidden)
            inner, plain, scaled, grad_g, grad_u = hidden_terms(
                normed[both, :, :width].reshape(step, width),
                cot[both].reshape(step, width),
                gate_column(gates[at, :], f * here + e),
                gate_w[e],
                up_w[e],
                down_w[e],
            )
            all_inner[at, columns] = scaled
            all_g[at, columns] = grad_g
            all_u[at, columns] = grad_u
            share = jnp.sum(inner * plain, axis=-1, keepdims=True)
            lane = lax.broadcasted_iota(jnp.int32, (step, LANES), 1)
            shares[at, :] = jnp.where(lane == f * here + e, share, shares[at, :])
            return carry

        lax.fori_loop(0, here, one_expert, 0)

    def grad_pass(pair):
        def one_block(b, carry):
            at = pl.ds(pl.multiple_of(b * tokens, tokens), tokens)
            mean = jnp.sum(gates[at, :] * shares[at, :], axis=-1, keepdims=True)
            logits = (gates[at, :] * (shares[at, :] - mean)).astype(BF)
            router_ref[...] += tn(logits, normed[b, :, :width])[:PAD]

            def one_chunk(k, inner_carry):
                part = pl.ds(pl.multiple_of(k * thin, LANES), thin)
                total = nn(logits[:, :PAD], table_ref[:, part])
                for e in range(here):
                    columns = slice(e * hidden, (e + 1) * hidden)
                    total = total + nt(all_g[at, columns], gate_w[e, part, :])
                    total = total + nt(all_u[at, columns], up_w[e, part, :])
                parts[b, :, part] = total.astype(BF)
                return inner_carry

            return lax.fori_loop(0, width // thin, one_chunk, carry)

        lax.fori_loop(2 * pair, 2 * pair + 2, one_block, 0)

    def slot_arrived(s):
        hop[s].wait_recv()
        if s + 1 < slots:
            hop[s + 1].start()
        if s in whole_slots:
            whole[s].start()
            for j in evens:
                half[s, j].start()

    def half_arrived(s):
        if s in whole_slots:
            for j in evens:
                half[s, j].wait_recv()
                cross[s, j].start()
                relay_half[s, j].start()

    def cross_arrived(s):
        if s in whole_slots:
            for j in evens:
                cross[s, j].wait_recv()
                relay_cross[s, j].start()

    def moe_pass(pair):
        def one_moe(b, carry):
            at = pl.ds(pl.multiple_of(b * tokens, tokens), tokens)
            slot = lax.rem(b, 2)
            copy = pltpu.make_async_copy(moe_stage.at[slot], moe_ref.at[b], moe_sems.at[slot])
            pl.when(b >= 2)(copy.wait)

            def one_chunk(k, inner_carry):
                part = pl.ds(pl.multiple_of(k * thin, LANES), thin)
                down = down_w[:, :, part].reshape(here * hidden, thin)
                moe_stage[slot, :, part] = nn(all_inner[at, :], down).astype(BF)
                return inner_carry

            lax.fori_loop(0, width // thin, one_chunk, 0)
            copy.start()
            return carry

        lax.fori_loop(2 * pair, 2 * pair + 2, one_moe, 0)

    def far_ready():
        for j in evens:
            near_relay[j].wait_recv()

    def near_done():
        swap[0].start()
        for j in evens:
            near_far[j].wait_recv()
            near_relay[j].start()
        slot_arrived(1)
        for copy in [two_whole] + [two_half[j] for j in evens]:
            copy.start()

    def all_done():
        for j in evens:
            swap[j].start()
        if slots > 2:
            slot_arrived(2)
        for j in evens:
            swap[j].wait_recv()
            joined[j // 2] = (parts[j].astype(F32) + swapped[j // 2].astype(F32)).astype(BF)
            home[j].start()
        for copy in cuts:
            copy.start()
        cross_arrived(1)
        for j in evens:
            two_half[j].wait_recv()
            two_cross[j].start()
            two_relay[j].start()

    router_ref[...] = jnp.zeros_like(router_ref)

    def one_pair(pair, carry):
        pl.when(pair == 1)(far_ready)
        prepare(pair)
        hidden_pass(pair)
        pl.when(pair == 1)(functools.partial(half_arrived, 1))
        grad_pass(pair)
        pl.when(pair == 0)(near_done)
        pl.when(pair == members // 2 - 1)(all_done)
        moe_pass(pair)
        return carry

    lax.fori_loop(0, members // 2, one_pair, 0)
    for slot in range(2):
        pltpu.make_async_copy(moe_stage.at[slot], moe_ref.at[slot], moe_sems.at[slot]).wait()
    buffers = stage_gate.shape[0]

    def stage_copies(e, b):
        return (
            pltpu.make_async_copy(stage_gate.at[b], grad_gate_ref.at[e], stage_sems.at[0, b]),
            pltpu.make_async_copy(stage_up.at[b], grad_up_ref.at[e], stage_sems.at[1, b]),
            pltpu.make_async_copy(stage_down.at[b], grad_down_ref.at[e], stage_sems.at[2, b]),
        )

    def sum_home():
        swap[0].wait_recv()
        total = parts[0].astype(F32) + swapped[0].astype(F32)
        for j in evens:
            home[j].wait_recv()
            total = total + arrived[j // 2].astype(F32)
        mine_ref[...] = total.astype(BF)

    def middle_slots():
        half_arrived(2)
        for j in evens:
            two_cross[j].wait_recv()
            two_relay_cross[j].start()

    def later_slots():
        cross_arrived(2)
        for s in range(3, slots - 1):
            slot_arrived(s)
            half_arrived(s)
            cross_arrived(s)

    def weights_of(e, carry):
        b = lax.rem(e, buffers)

        @pl.when(e >= buffers)
        def _():
            for copy in stage_copies(e, b):
                copy.wait()

        columns = pl.ds(pl.multiple_of(e * hidden, LANES), hidden)
        rows = members * tokens

        def one_chunk(k, inner_carry):
            part = pl.ds(pl.multiple_of(k * chunk, LANES), chunk)
            left = normed[:, :, part].reshape(rows, chunk)
            right = cot[:, :, part].reshape(rows, chunk)
            stage_gate[b, part, :] = tn(left, all_g[:, columns])
            stage_up[b, part, :] = tn(left, all_u[:, columns])
            stage_down[b, :, part] = tn(all_inner[:, columns], right)
            return inner_carry

        lax.fori_loop(0, 3, one_chunk, 0)
        for copy in stage_copies(e, b):
            copy.start()
        pl.when(e == min(1, here - 1))(middle_slots)
        pl.when(e == here - 1)(sum_home)
        pl.when(e == here - 1)(later_slots)
        return carry

    lax.fori_loop(0, here, weights_of, 0)
    for e in range(max(here - buffers, 0), here):
        for copy in stage_copies(e, e % buffers):
            copy.wait()
    for s in whole_slots:
        whole[s].wait_recv()
        for j in evens:
            relay_half[s, j].wait_recv()
            relay_cross[s, j].wait_recv()
    for copy in cuts:
        copy.wait_recv()
    hop[slots - 1].wait_recv()
    two_whole.wait_recv()
    for j in evens:
        two_relay[j].wait_recv()
        two_relay_cross[j].wait_recv()
    for copy in net.made:
        copy.wait_send()


def own(table, normed, cotangent, cot_near, cot_two, normed_cut, gate_w, up_w, down_w, experts, slots):
    members = cot_near.shape[0]
    tokens, width = cotangent.shape
    here, _, hidden = gate_w.shape
    rows = members * tokens
    halves = members // 2
    buffers = 2 if members <= 4 else 1
    far = halves - 1
    copies = 1 + 2 * far + (slots - 1) * (2 + 4 * far) + halves + far + 1 + 4 * far + members - 1
    token_block = (tokens, width)
    return pl.pallas_call(
        functools.partial(own_kernel, members, slots, experts),
        out_shape=(
            shape((slots - 2, members, tokens, width + LANES), BF),
            shape((tokens, width + LANES), BF),
            shape(normed_cut.shape, BF),
            shape((members - 1, tokens, width), BF),
            shape((members, tokens, width), BF),
            shape(token_block, BF),
            shape((PAD, width), F32),
            shape(gate_w.shape, F32),
            shape(up_w.shape, F32),
            shape(down_w.shape, F32),
        ),
        in_specs=[VMEM] + [ANY] * 8,
        out_specs=(ANY, ANY, ANY, ANY, ANY, VMEM, VMEM, ANY, ANY, ANY),
        scratch_shapes=[
            pltpu.VMEM(gate_w.shape, BF),
            pltpu.VMEM(up_w.shape, BF),
            pltpu.VMEM(down_w.shape, BF),
            pltpu.VMEM((members, tokens, width + LANES), BF),
            pltpu.VMEM((members, tokens, width), BF),
            pltpu.VMEM((rows, here * hidden), BF),
            pltpu.VMEM((rows, here * hidden), BF),
            pltpu.VMEM((rows, here * hidden), BF),
            pltpu.VMEM((members,) + token_block, BF),
            pltpu.VMEM((halves,) + token_block, BF),
            pltpu.VMEM((halves,) + token_block, BF),
            pltpu.VMEM((halves,) + token_block, BF),
            pltpu.VMEM((buffers, width, hidden), F32),
            pltpu.VMEM((buffers, width, hidden), F32),
            pltpu.VMEM((buffers, hidden, width), F32),
            pltpu.VMEM((rows, LANES), F32),
            pltpu.VMEM((rows, LANES), F32),
            pltpu.SemaphoreType.DMA((2, copies)),
            pltpu.SemaphoreType.DMA((3, here)),
            pltpu.SemaphoreType.DMA((1 + members,)),
            pltpu.SemaphoreType.DMA((3, buffers)),
            pltpu.VMEM((2,) + token_block, BF),
            pltpu.SemaphoreType.DMA((2,)),
        ],
        compiler_params=pltpu.CompilerParams(
            vmem_limit_bytes=63 << 20, collective_id=1, has_side_effects=True
        ),
        name="own",
        cost_estimate=pl.CostEstimate(
            flops=18 * rows * width * hidden * here,
            bytes_accessed=18 * here * width * hidden,
            transcendentals=0,
        ),
    )(table, normed, cotangent, cot_near, cot_two, normed_cut, gate_w, up_w, down_w)


class Plan:
    def __init__(self, number, ins, outs, scratch, copies, build):
        self.number = number
        self.ins = ins
        self.outs = outs
        self.scratch = scratch
        self.copies = copies
        self.build = build


def more_weights_kernel(sources, counts, plan, experts, begin, index, *refs):
    in_normed, in_cot = counts
    refs = list(refs)

    def take(number):
        front = refs[:number]
        del refs[:number]
        return front

    normed_in = take(in_normed)
    cot_in = take(in_cot)
    gate_w, up_w, down_w, old_gate, old_up, old_down = take(6)
    plan_in = take(len(plan.ins))
    new_gate, new_up, new_down = take(3)
    plan_out = take(len(plan.outs))
    normed, cot, gates, all_inner, all_g, all_u, sems, remote_sems = take(8)
    plan_scratch = refs
    members, tokens, width = cot.shape
    rows = members * tokens
    here = index[1]
    step_at = pl.program_id(0)
    net = Sender(remote_sems)
    devices, begin_plan, ready, after, finish = plan.build(net, plan_in, plan_out, plan_scratch)
    last = pl.num_programs(0) - 1

    @pl.when(step_at == 0)
    def _():
        copies = []
        for group, refs_in, whole in ((0, normed_in, normed), (1, cot_in, cot)):
            for number, lead, first, count in sources[group]:
                ref = refs_in[number]
                ref = ref if lead is None else ref.at[lead]
                place = whole.at[first] if count == 1 else whole.at[pl.ds(first, count)]
                copies.append(pltpu.make_async_copy(ref, place, sems.at[len(copies)]))
        for copy in copies:
            copy.start()
        if devices:
            greet(devices)
        begin_plan()
        for copy in copies:
            copy.wait()
        gates[...] = gates_of(normed[:, :, width:].reshape(rows, LANES), experts)
        ready()

    expert = index[0] * here + begin + step_at
    many = 1 if plan.number in TILE_ONE else 2
    step = many * tokens

    def one_tile(b, carry):
        at = pl.ds(pl.multiple_of(b * step, step), step)
        pair = pl.ds(many * b, many)
        _, _, scaled, grad_g, grad_u = hidden_terms(
            normed[pair, :, :width].reshape(step, width),
            cot[pair].reshape(step, width),
            gate_column(gates[at, :], expert),
            gate_w[0],
            up_w[0],
            down_w[0],
        )
        all_inner[at, :] = scaled
        all_g[at, :] = grad_g
        all_u[at, :] = grad_u
        return carry

    straight = plan.number is None and rows <= 1024
    if straight:
        for b in range(rows // step):
            one_tile(b, 0)
    else:
        lax.fori_loop(0, rows // step, one_tile, 0)
    pieces = 1 if straight else 6 if plan.number in CHUNK_SIX else 3
    chunk = width // pieces

    def one_chunk(k, carry):
        at = pl.ds(pl.multiple_of(k * chunk, LANES), chunk)
        left = normed[:, :, at].reshape(rows, chunk)
        right = cot[:, :, at].reshape(rows, chunk)
        new_gate[0, at, :] = old_gate[0, at, :] + tn(left, all_g[...])
        new_up[0, at, :] = old_up[0, at, :] + tn(left, all_u[...])
        new_down[0, :, at] = old_down[0, :, at] + tn(all_inner[...], right)
        return carry

    if straight:
        one_chunk(0, 0)
    else:
        lax.fori_loop(0, pieces, one_chunk, 0)
    for number, hook in enumerate(after):
        pl.when(step_at == jnp.minimum(number, last))(hook)
    pl.when(step_at == last)(finish)


def more_weights(begin, count, index, normed, cotangent, sources, weights, earlier, experts, plan):
    here, width, hidden = weights[0].shape
    tokens = cotangent[0].shape[-2]
    members = max(first + many for _, _, first, many in sources[1])
    rows = members * tokens
    pick = lambda e: (e + begin, 0, 0)
    wide = pl.BlockSpec((1, width, hidden), pick)
    tall = pl.BlockSpec((1, hidden, width), pick)
    base = 1 + len(normed) + len(cotangent) + 3
    results = pl.pallas_call(
        functools.partial(
            more_weights_kernel,
            sources,
            (len(normed), len(cotangent)),
            plan,
            experts,
            begin,
        ),
        out_shape=tuple(shape(item.shape, F32) for item in earlier)
        + tuple(item for item, _ in plan.outs),
        grid=(count,),
        in_specs=[SMEM]
        + [ANY] * (len(normed) + len(cotangent))
        + [wide, wide, tall] * 2
        + [spec for _, spec in plan.ins],
        out_specs=(wide, wide, tall) + tuple(spec for _, spec in plan.outs),
        scratch_shapes=[
            pltpu.VMEM((members, tokens, width + LANES), BF),
            pltpu.VMEM((members, tokens, width), BF),
            pltpu.VMEM((rows, LANES), F32),
            pltpu.VMEM((rows, hidden), BF),
            pltpu.VMEM((rows, hidden), BF),
            pltpu.VMEM((rows, hidden), BF),
            pltpu.SemaphoreType.DMA((4,)),
            pltpu.SemaphoreType.DMA((2, plan.copies)),
        ]
        + list(plan.scratch),
        input_output_aliases={base + i: i for i in range(3)} if count < here else {},
        compiler_params=pltpu.CompilerParams(
            vmem_limit_bytes=63 << 20,
            collective_id=plan.number,
            has_side_effects=plan.number is not None,
        ),
        name="weights_" + str(plan.number),
        cost_estimate=pl.CostEstimate(
            flops=12 * rows * width * hidden * count,
            bytes_accessed=count * 30 * width * hidden + 4 * rows * width,
            transcendentals=0,
        ),
    )(index, *normed, *cotangent, *weights, *earlier, *[item for item, _ in plan.ins])
    return results[:3], results[3:]


def places(members, slots):
    f = lax.axis_index("fsdp")
    c = lax.axis_index("context")
    t = lax.axis_index("tensor")
    fsdp = {j: {"fsdp": target(f, j, members)} for j in range(1, members)}
    return f, c, t, fsdp, {"tensor": 1 - t}


def nothing():
    pass


def home_plan(number, members, slots, grad_part, moe_parts, cot_two):
    tokens, width = grad_part.shape
    halves = members // 2
    evens = range(2, members, 2)

    def build(net, ins, outs, scratch):
        part, moe_in, two_in = ins
        other, moe_mine, hops = outs
        own_part, swapped, joined, arrived, local = scratch
        f, c, t, fsdp, opposite = places(members, slots)
        cross_part = net.add(part, other, opposite)
        ahead = {"context": lax.rem(c + 1, slots)}
        behind = {"context": lax.rem(c + slots - 1, slots)}
        late = [
            net.add(two_in if i == 0 else hops.at[i - 1], hops.at[i], ahead)
            for i in range(slots - 3)
        ]
        swap = [net.add(moe_in.at[2 * i + 1], swapped.at[i], fsdp[1]) for i in range(halves)]
        home = {
            j: net.add(
                joined.at[j // 2], arrived.at[j // 2], {"fsdp": lax.rem(f + members - j, members)}
            )
            for j in evens
        }
        loads = [
            pltpu.make_async_copy(moe_in.at[2 * i], own_part.at[i], local.at[i])
            for i in range(halves)
        ]

        def start():
            for copy in [cross_part] + swap[1:] + swap[:1] + loads + late[:1]:
                copy.start()

        def ready():
            for copy in loads:
                copy.wait()
            for j in evens:
                swap[j // 2].wait_recv()
                joined[j // 2] = (
                    own_part[j // 2].astype(F32) + swapped[j // 2].astype(F32)
                ).astype(BF)
                home[j].start()

        def finish():
            swap[0].wait_recv()
            total = own_part[0].astype(F32) + swapped[0].astype(F32)
            for j in evens:
                home[j].wait_recv()
                total = total + arrived[j // 2].astype(F32)
            moe_mine[...] = total.astype(BF)
            cross_part.wait_recv()
            for i, copy in enumerate(late):
                copy.wait_recv()
                for following in late[i + 1 : i + 2]:
                    following.start()
            for copy in net.made:
                copy.wait_send()

        devices = [fsdp[1], opposite, ahead, behind] + [fsdp[j] for j in evens]
        return devices, start, ready, [], finish

    block = (halves, tokens, width)
    return Plan(
        number,
        [(grad_part, ANY), (moe_parts, ANY), (cot_two, ANY)],
        [
            (shape((tokens, width), BF), ANY),
            (shape((tokens, width), BF), VMEM),
            (shape((max(slots - 3, 1), tokens, width), BF), ANY),
        ],
        [pltpu.VMEM(block, BF)] * 4 + [pltpu.SemaphoreType.DMA((halves,))],
        1 + halves + halves - 1 + slots - 3,
        build,
    )


def keys_plan(number, members, slots, attention, grad_b, normed_last, cot_hops, late):
    heads, grad_heads, att, lse, turns, kv = attention
    _, tokens, cut = grad_b.shape
    wide = normed_last.shape[1]
    width = cot_hops.shape[2]
    side = tokens // 2
    evens = range(2, members, 2)
    groups = lse.shape[0]
    many = lse.shape[2]
    far = members // 2 - 1

    def build(net, ins, outs, scratch):
        heads_ref, grad_ref, att_ref, lse_ref, turns_ref, kv_ref = ins[:6]
        grad_in, last_in, hops_in, att_in = ins[6:]
        grad_q, own_kv, received, grad_near, spread_out, cot_out, att_near = outs
        grad_kv, wide_ref, acc, turned = scratch
        f, c, t, fsdp, opposite = places(members, slots)
        piece = pl.ds(pl.multiple_of(t * side, side), side)
        lower_half, upper_half = pl.ds(0, side), pl.ds(side, side)
        first_back = net.used
        net.used += slots - 1

        def back(s):
            at = first_back + s - 1
            return pltpu.make_async_remote_copy(
                src_ref=grad_kv.at[s - 1],
                dst_ref=received.at[s - 1],
                send_sem=net.sems.at[0, at],
                recv_sem=net.sems.at[1, at],
                device_id={"context": lax.rem(c + slots - s, slots)},
                device_id_type=pl.DeviceIdType.MESH,
            )

        cuts = []
        for j in range(1, members):
            cuts.append(net.add(grad_in.at[j], grad_near.at[j], fsdp[j]))
        sources = [(last_in, spread_out)]
        sources += [(hops_in.at[i], cot_out.at[i]) for i in range(late)]
        att_core = net.add(att_in, att_near.at[1], fsdp[1])
        att_far = [net.add(att_in, att_near.at[j], fsdp[j]) for j in evens]
        att_relay = [net.add(att_near.at[j], att_near.at[j + 1], fsdp[1]) for j in evens]
        whole, half, cross, relay, relay_cross = [], [], [], [], []
        for source, place in sources:
            whole.append(net.add(source, place.at[0], fsdp[1]))
            for j in evens:
                low, high = place.at[j - 1, lower_half], place.at[j - 1, upper_half]
                half.append(net.add(source.at[piece], low, fsdp[j]))
                cross.append(net.add(low, high, opposite))
                relay.append(net.add(low, place.at[j, lower_half], fsdp[1]))
                relay_cross.append(net.add(high, place.at[j, upper_half], fsdp[1]))

        def through(i, carry):
            s = slots - 1 - i

            @pl.when(c >= s)
            def _():
                attend_back_slot(s, heads_ref, grad_ref, lse_ref, kv_ref, wide_ref, acc, own_kv)

                @pl.when(s > 0)
                def _():
                    grad_kv[s - 1] = own_kv[...].astype(BF)
                    back(s).start()

            return carry

        def start():
            for copy in half + att_far + cuts + whole + [att_core]:
                copy.start()
            attend_back_start(heads_ref, grad_ref, att_ref, wide_ref, acc)
            lax.fori_loop(0, slots, through, 0)
            pass_on(0, far)
            attend_back_end(turns_ref, acc, turned, grad_q)

        def pass_on(low, high):
            for copy, following, other in list(zip(half, cross, relay))[low:high]:
                copy.wait_recv()
                following.start()
                other.start()

        def first():
            pass_on(far, len(half))

        def second():
            for copy, following in zip(att_far, att_relay):
                copy.wait_recv()
                following.start()

        def finish():
            for copy, following in zip(cross, relay_cross):
                copy.wait_recv()
                following.start()
            for s in range(1, slots):
                pl.when(c + s < slots)(back(s).wait_recv)
                pl.when(c >= s)(back(s).wait_send)
            for copy in cuts + whole + relay + relay_cross + att_relay + [att_core]:
                copy.wait_recv()
            for copy in net.made:
                copy.wait_send()

        devices = list(fsdp.values()) + [opposite]
        devices += [{"context": lax.rem(c + s, slots)} for s in range(1, slots)]
        return devices, start, nothing, [first, second], finish

    far = members // 2 - 1
    return Plan(
        number,
        [(item, VMEM) for item in attention]
        + [(grad_b, ANY), (normed_last, ANY), (cot_hops, ANY), (att, ANY)],
        [
            (shape(att.shape, BF), VMEM),
            (shape(kv.shape[1:], F32), VMEM),
            (shape((slots - 1,) + kv.shape[1:], BF), ANY),
            (shape((members, tokens, cut), BF), ANY),
            (shape((members - 1, tokens, wide), BF), ANY),
            (shape((max(late, 1), members - 1, tokens, width), BF), ANY),
            (shape((members,) + att.shape, BF), ANY),
        ],
        [
            pltpu.VMEM((slots - 1,) + kv.shape[1:], BF),
            pltpu.VMEM((groups, many, 2 * HEAD), BF),
            pltpu.VMEM((groups, many, HEAD), F32),
            pltpu.VMEM(att.shape, F32),
        ],
        (slots - 1) + (members - 1) + (1 + late) * (1 + 4 * far) + 1 + 2 * far,
        build,
    )


def rows_plan(
    number, members, slots, part_one, joined, router, gain_one, gain_two, payload
):
    tokens, width = part_one.shape
    cut = width // members
    evens = range(2, members, 2)
    rows = payload.shape[0] // slots

    def build(net, ins, outs, scratch):
        part_in, joined_in, router_ref, one_ref, two_ref, payload_in = ins
        other, joined_near, small_near, chunks = outs
        small_mine, small_other, small_sum, small_got, small_cut = scratch
        f, c, t, fsdp, opposite = places(members, slots)
        part_sent = net.add(part_in, other, opposite)
        small_sent = net.add(small_mine, small_other, opposite)
        core = net.add(joined_in, joined_near.at[1], fsdp[1])
        far_copy = {j: net.add(joined_in, joined_near.at[j], fsdp[j]) for j in evens}
        relay = {j: net.add(joined_near.at[j], joined_near.at[j + 1], fsdp[1]) for j in evens}
        small_cuts = []
        for j in range(1, members):
            small_cuts.append(net.add(small_cut.at[j], small_got.at[j], fsdp[j]))
        shares = []
        for s in range(1, slots):
            owner = lax.rem(c + s, slots)
            at = pl.ds(pl.multiple_of(owner * rows, 16), rows)
            shares.append(net.add(payload_in.at[at], chunks.at[s], {"context": owner}))

        def start():
            small = router_ref[...]
            row = lax.broadcasted_iota(jnp.int32, small.shape, 0)
            small = jnp.where(row == PAD - 8, one_ref[...], small)
            small = jnp.where(row == PAD - 7, 0.5 * two_ref[...], small)
            small_mine[...] = small.astype(BF)
            small_sent.start()
            for copy in [part_sent, core] + [far_copy[j] for j in evens] + shares:
                copy.start()

        def ready():
            small_sent.wait_recv()
            small_sum[...] = (small_mine[...].astype(F32) + small_other[...].astype(F32)).astype(BF)
            small_got[0] = columns_of(small_sum, f, cut)
            for j in range(1, members):
                small_cut[j] = columns_of(small_sum, target(f, j, members), cut)
            for copy in small_cuts:
                copy.start()

        def second():
            for j in evens:
                far_copy[j].wait_recv()
                relay[j].start()

        def finish():
            for copy in [part_sent, core] + [relay[j] for j in evens] + small_cuts + shares:
                copy.wait_recv()
            small_near[...] = small_got[...]
            for copy in net.made:
                copy.wait_send()

        devices = list(fsdp.values()) + [opposite]
        devices += [{"context": lax.rem(c + s, slots)} for s in range(1, slots)]
        return devices, start, ready, [nothing, second], finish

    far = members // 2 - 1
    small = (PAD, width)
    return Plan(
        number,
        [(part_one, ANY), (joined, ANY)]
        + [(router, VMEM), (gain_one, VMEM), (gain_two, VMEM), (payload, ANY)],
        [
            (shape((tokens, width), BF), ANY),
            (shape((members,) + joined.shape, BF), ANY),
            (shape((members, PAD, cut), BF), VMEM),
            (shape((slots, rows, payload.shape[1]), BF), ANY),
        ],
        [pltpu.VMEM(small, BF)] * 3 + [pltpu.VMEM((members, PAD, cut), BF)] * 2,
        2 + 1 + 2 * far + (members - 1) + (slots - 1),
        build,
    )


def chunk_plan(number, members, slots, payload, moe_mine):
    rows = payload.shape[0] // slots

    def build(net, ins, outs, scratch):
        f, c, t, fsdp, opposite = places(members, slots)
        copies = [net.add(ins[1], outs[1], opposite)]
        for s in range(1, slots):
            owner = lax.rem(c + s, slots)
            at = pl.ds(pl.multiple_of(owner * rows, 16), rows)
            copies.append(net.add(ins[0].at[at], outs[0].at[s], {"context": owner}))

        def start():
            for copy in copies:
                copy.start()

        def finish():
            for copy in copies:
                copy.wait_recv()
                copy.wait_send()

        devices = [{"context": lax.rem(c + s, slots)} for s in range(1, slots)]
        return devices + [opposite], start, nothing, [], finish

    return Plan(
        number,
        [(payload, ANY), (moe_mine, ANY)],
        [
            (shape((slots, rows, payload.shape[1]), BF), ANY),
            (shape(moe_mine.shape, BF), ANY),
        ],
        [],
        slots,
        build,
    )


def middle_kernel(members, index, hidden_ref, cot_ref, mine_ref, theirs_ref, table_ref, weights_ref, *refs):
    grad_ref, grad_b_ref, heads_ref, gain_ref, rounded, columns, summed = refs
    f = index[0]
    cut = weights_ref.shape[2]
    gain = table_ref[...].astype(F32)[PAD - 7 : PAD - 6, :]
    gain_ref[...] = jnp.zeros(gain_ref.shape, F32)
    tile = 64

    def one_tile(i, carry):
        at = pl.ds(pl.multiple_of(i * tile, tile), tile)
        hidden = hidden_ref[at, :]
        normed_grad = mine_ref[at, :].astype(F32) + theirs_ref[at, :].astype(F32)
        scale = lax.rsqrt(jnp.mean(hidden * hidden, axis=-1, keepdims=True) + norm_eps)
        weighted = normed_grad * gain
        cubed = scale * scale * scale
        grad = (
            cot_ref[at, :].astype(F32)
            + scale * weighted
            - hidden * cubed * jnp.mean(weighted * hidden, axis=-1, keepdims=True)
        )
        gain_ref[...] += jnp.sum(normed_grad * hidden * scale, axis=0, keepdims=True)
        grad_ref[at, :] = grad
        rounded[at, :] = grad.astype(BF)
        return carry

    lax.fori_loop(0, hidden_ref.shape[0] // tile, one_tile, 0)
    for j in range(members):
        grad_b_ref[j] = columns_of(rounded, target(f, j, members), cut)
        columns[j] = columns_of(rounded, member(f, j, members), cut)
    summed[...] = nt(columns[0], weights_ref[0])

    def one_member(j, carry):
        summed[...] += nt(columns[j], weights_ref[j])
        return carry

    lax.fori_loop(1, members, one_member, 0)
    total = summed[...].astype(BF)
    for h in range(heads_ref.shape[0]):
        heads_ref[h] = total[:, h * HEAD : (h + 1) * HEAD]


def middle(index, hidden, cotangent, mine, theirs, table, weights, after=()):
    members = weights.shape[0]
    tokens, width = hidden.shape
    heads = weights[0].shape[0] // HEAD
    return call(
        functools.partial(middle_kernel, members),
        (
            shape((tokens, width), F32),
            shape((members, tokens, width // members), BF),
            shape((heads, tokens, HEAD), BF),
            shape((1, width), F32),
        ),
        [SMEM] + [VMEM] * 6,
        (VMEM,) * 4,
        [
            pltpu.VMEM((tokens, width), BF),
            pltpu.VMEM((members, tokens, width // members), BF),
            pltpu.VMEM((tokens, heads * HEAD), F32),
        ],
        2 * tokens * width * heads * HEAD,
        16 * tokens * width,
        "middle",
        after,
    )(index, hidden, cotangent, mine, theirs, table, weights)


def lower_kernel(members, slots, index, grad_q_ref, own_ref, rows_ref, turns_ref, *refs):
    others = refs[0]
    weights = refs[1]
    joined_ref, part_ref, gain_ref = refs[2:]
    f = index[0]
    cut = weights.shape[1]
    total = own_ref[...]
    for s in range(1, slots):
        total = total + jnp.where(index[1] + s < slots, others[s - 1].astype(F32), 0.0)
    half = total.shape[1] // 2
    q_wide = grad_q_ref.shape[1]
    joined_ref[:, :q_wide] = grad_q_ref[...]
    keys = rotate(total[:, :half], turns_ref[:, :LANES], -turns_ref[:, LANES:])
    joined_ref[:, q_wide : q_wide + half] = keys.astype(BF)
    joined_ref[:, q_wide + half :] = total[:, half:].astype(BF)
    rows = rows_ref[...].astype(F32)
    scale = lax.rsqrt(jnp.mean(rows * rows, axis=-1, keepdims=True) + norm_eps)

    def one_pair(p, carry):
        owner = lax.rem(f + members - 2 * p, members)
        first = nt(joined_ref[...], weights[2 * p]).astype(BF)
        second = nt(joined_ref[...], weights[2 * p + 1]).astype(BF)
        put_columns(part_ref, owner, first, second)
        return carry

    lax.fori_loop(0, members // 2, one_pair, 0)
    gain_ref[...] = jnp.sum(part_ref[...].astype(F32) * rows * scale, axis=0, keepdims=True)


def lower(index, grad_q, own_kv, others, rows, turns, weights, after=()):
    members = len(weights)
    tokens, width = rows.shape
    wide = weights[0].shape[1]
    return call(
        functools.partial(lower_kernel, members, others.shape[0] + 1),
        (shape((tokens, wide), BF), shape((tokens, width), BF), shape((1, width), F32)),
        [SMEM] + [VMEM] * 6,
        (VMEM,) * 3,
        [],
        2 * tokens * width * wide,
        2 * width * wide,
        "lower",
        after,
    )(index, grad_q, own_kv, rows, turns, others, weights)


def last_kernel(
    rows_ref, grad_ref, mine_ref, theirs_ref, table_ref, hidden_ref, moe_ref, other_ref, out_ref, result_ref
):
    gain = table_ref[...].astype(F32)[PAD - 8 : PAD - 7, :]
    moe = moe_ref[...].astype(F32) + other_ref[...].astype(F32)
    result_ref[...] = (hidden_ref[...] + moe).astype(BF)
    rows = rows_ref[...].astype(F32)
    normed_grad = mine_ref[...].astype(F32) + theirs_ref[...].astype(F32)
    scale = lax.rsqrt(jnp.mean(rows * rows, axis=-1, keepdims=True) + norm_eps)
    weighted = normed_grad * gain
    cubed = scale * scale * scale
    out_ref[...] = (
        grad_ref[...]
        + scale * weighted
        - rows * cubed * jnp.mean(weighted * rows, axis=-1, keepdims=True)
    ).astype(BF)


def last(rows, grad, mine, theirs, table, hidden, moe, other):
    tokens, width = rows.shape
    tile = 64
    part = pl.BlockSpec((tile, width), lambda i: (i, 0))
    whole = pl.BlockSpec(table.shape, lambda i: (0, 0))
    return call(
        last_kernel,
        (shape((tokens, width), BF), shape((tokens, width), BF)),
        [part] * 4 + [whole] + [part] * 3,
        (part, part),
        [],
        16 * tokens * width,
        20 * tokens * width,
        "last",
        grid=(tokens // tile,),
    )(rows, grad, mine, theirs, table, hidden, moe, other)


def product_kernel(extra, left_own, left, right_own, right, *refs):
    members = left.shape[0]
    out_ref = refs[-2]
    mine = [ref[0] if len(ref.shape) == 3 else ref[...] for ref in (left_own, right_own)]
    summed = refs[-1]
    summed[...] = tn(*mine)

    def one_member(j, carry):
        summed[...] += tn(left[j], right[j])
        return carry

    lax.fori_loop(1, members, one_member, 0)
    total = summed[...]
    rows, columns = total.shape
    out_ref[:rows, :] = total.astype(BF)
    if extra:
        small = refs[0]
        summed = small[0].astype(F32)
        for j in range(1, members):
            summed = summed + small[j].astype(F32)
        out_ref[rows:, :] = jnp.zeros((out_ref.shape[0] - rows, columns), BF)
        out_ref[rows : rows + PAD, : summed.shape[1]] = summed.astype(BF)


def product(left_own, left, right_own, right, small, extra_rows, name):
    members, tokens, rows = left.shape
    columns = right.shape[2]
    return call(
        functools.partial(product_kernel, len(small)),
        shape((rows + extra_rows, columns), BF),
        [VMEM] * (4 + len(small)),
        VMEM,
        [pltpu.VMEM((rows, columns), F32)],
        2 * members * tokens * rows * columns,
        4 * rows * columns,
        name,
    )(left_own, left, right_own, right, *small)


def chunk_sum(place, whole_ref, parts_ref):
    slots, rows, _ = parts_ref.shape
    total = whole_ref[pl.ds(pl.multiple_of(place * rows, 16), rows), :].astype(F32)
    for s in range(1, slots):
        total = total + parts_ref[s].astype(F32)
    return total.astype(BF)


def joint_sum_kernel(index, whole_ref, parts_ref, more_whole, more_parts, out_ref):
    rows, wide = parts_ref.shape[1:]
    many, columns = more_parts.shape[1:]
    out_ref[:rows, :] = chunk_sum(index[1], whole_ref, parts_ref)
    more = chunk_sum(index[1], more_whole, more_parts)
    fold = wide // columns
    each = many // fold
    if fold * columns < wide:
        out_ref[rows:, :] = jnp.zeros((each, wide), BF)
    for k in range(fold):
        out_ref[rows:, k * columns : (k + 1) * columns] = more[k * each : (k + 1) * each, :]


def joint_sum(index, whole, parts, more_whole, more_parts):
    slots, rows, columns = parts.shape
    many, narrow = more_parts.shape[1:]
    extra = many // (columns // narrow)
    return call(
        joint_sum_kernel,
        shape((rows + extra, columns), BF),
        [SMEM] + [VMEM] * 4,
        VMEM,
        [],
        slots * rows * columns,
        2 * (slots + 1) * rows * columns,
        "joint_sum",
    )(index, whole, parts, more_whole, more_parts)


def spread_kernel(slots, experts, index, *refs):
    parts = refs[:slots]
    query_ref, key_ref, value_ref, out_ref, one_ref, two_ref, router_ref, whole = refs[slots:]
    place = index[1]
    cut, q_wide = query_ref.shape
    kv_wide = key_ref.shape[1]
    rows = whole.shape[0] // slots
    many, columns = out_ref.shape
    each = parts[0].shape[0] - rows
    fold = parts[0].shape[1] // columns
    for s in range(slots):
        owner = lax.rem(place + slots - s, slots)
        whole[pl.ds(pl.multiple_of(owner * rows, 16), rows), :] = parts[s][:rows, :].astype(F32)
        for k in range(fold):
            base = owner * (many // slots) + k * each
            out_ref[pl.ds(pl.multiple_of(base, 16), each), :] = parts[s][
                rows:, k * columns : (k + 1) * columns
            ].astype(F32)
    query_ref[...] = whole[:cut, :q_wide]
    key_ref[...] = whole[:cut, q_wide : q_wide + kv_wide]
    value_ref[...] = whole[:cut, q_wide + kv_wide :]
    small = whole[cut : cut + PAD, :cut]
    one_ref[...] = small[PAD - 8]
    two_ref[...] = small[PAD - 7]
    router_ref[...] = small[:experts]


def spread(index, parts, rows, dims, experts):
    slots = len(parts)
    columns = parts[0].shape[1]
    return call(
        functools.partial(spread_kernel, slots, experts),
        tuple(shape(item, F32) for item in dims),
        [SMEM] + [VMEM] * slots,
        (VMEM,) * len(dims),
        [pltpu.VMEM((slots * rows, columns), F32)],
        slots * rows * columns,
        6 * slots * rows * columns,
        "spread",
    )(index, *parts)


def build(members, slots):
    def ring(item, step):
        return lax.ppermute(item, "context", [(i, (i + step) % slots) for i in range(slots)])

    def per_device(
        tokens,
        positions,
        expert_ids,
        norm1_gain,
        w_query,
        w_key,
        w_value,
        w_out,
        norm2_gain,
        w_router,
        w_gate,
        w_up,
        w_down,
        grad_output,
    ):
        rows = tokens[0]
        cotangent = grad_output[0]
        block = rows.shape[0]
        width = rows.shape[1]
        experts = w_router.shape[1]
        here = w_gate.shape[0]
        kv_wide = w_key.shape[1]
        q_wide = w_query.shape[1]
        f = lax.axis_index("fsdp")
        c = lax.axis_index("context")
        c_index = c.reshape(1)
        index = jnp.stack([f, c])
        f_here = jnp.stack([f, jnp.int32(here)])

        half = HEAD // 2
        lane = np.arange(2 * LANES)
        freq = np.exp(-math.log(10000.0) * 2.0 * np.arange(half, dtype=np.float32) / HEAD)
        sign = np.where(lane % HEAD < half, -1.0, 1.0).astype(np.float32)
        angle = positions[0].astype(F32)[:, None] * freq.astype(np.float32)[lane % half][None, :]
        turns = jnp.where((lane < LANES)[None, :], jnp.cos(angle), jnp.sin(angle) * sign[None, :])

        (
            table,
            normed_one,
            heads,
            kv_slots,
            att,
            lse,
            hidden,
            normed,
            qkv_w,
            out_mine,
            cot_near,
            cot_done,
            cot_two,
            normed_cut,
        ) = forward(
            (w_query, w_key, w_value),
            w_out,
            cotangent,
            (w_router.T, norm1_gain, norm2_gain),
            rows,
            turns,
            expert_ids[0].T,
            members,
            slots,
        )

        results = own(
            table,
            normed,
            cotangent,
            cot_near,
            cot_two,
            normed_cut,
            w_gate,
            w_up,
            w_down,
            experts,
            slots,
        )
        normed_slots, normed_last, normed_near, two_far, moe_parts = results[:5]
        grad_part, router_grad, *expert_grads = results[5:]


        parts = 2 if here % 2 == 0 else here
        queue = []
        for s in range(1, slots - 1):
            queue += [(s, p * (here // parts), here // parts) for p in range(parts)]

        def fill(plan, item, grads, normed_far=None, cot_far=None):
            s, begin, many = item
            if s < slots - 1:
                normed_refs, normed_from = [normed_slots], ((0, s - 1, 0, members),)
            else:
                normed_refs = [normed_last, normed_far]
                normed_from = ((0, None, 0, 1), (1, None, 1, members - 1))
            if s == 1:
                cot_refs, cot_from = [cot_done], ((0, 0, 0, members),)
            else:
                cot_refs = [cot_two, two_far] if s == 2 else [cot_hops, cot_far]
                lead = None if s == 2 else s - 3
                cot_from = ((0, lead, 0, 1), (1, lead, 1, members - 1))
            return more_weights(
                begin,
                many,
                f_here,
                normed_refs,
                cot_refs,
                (normed_from, cot_from),
                (w_gate, w_up, w_down),
                grads,
                experts,
                plan,
            )

        plan = home_plan(2, members, slots, grad_part, moe_parts, cot_two)
        expert_grads, (grad_other, moe_mine, cot_hops) = fill(plan, queue[0], expert_grads)

        grad_hidden, grad_hidden_b, grad_heads, gain_two = middle(
            index, hidden, cotangent, grad_part, grad_other, table, out_mine
        )
        attention = (heads, grad_heads, att, lse, turns, kv_slots)
        plan = keys_plan(
            3, members, slots, attention, grad_hidden_b, normed_last, cot_hops, max(slots - 3, 0)
        )
        expert_grads, results = fill(plan, queue[1], expert_grads)
        grad_q, own_kv, received, grad_near, normed_far, cot_far, att_near = results
        out_payload = product(att, att_near, grad_hidden_b, grad_near, (), 0, "out_grad")
        joined, part_one, gain_one = lower(
            index, grad_q, own_kv, received, rows, turns, qkv_w
        )
        plan = rows_plan(
            4,
            members,
            slots,
            part_one,
            joined,
            router_grad,
            gain_one,
            gain_two,
            out_payload,
        )
        expert_grads, results = fill(plan, queue[2], expert_grads, normed_far, cot_far)
        other_one, joined_near, small_near, out_chunks = results
        payload = product(
            normed_cut, normed_near, joined, joined_near, (small_near,), 2 * PAD, "qkv_grad"
        )
        plan = chunk_plan(5, members, slots, payload, moe_mine)
        expert_grads, (qkv_chunks, moe_other) = fill(
            plan, queue[3], expert_grads, normed_far, cot_far
        )
        total = joint_sum(index, payload, qkv_chunks, out_payload, out_chunks)
        shared = [total] + [ring(total, s) for s in range(1, slots)]
        grad_tokens, output = last(
            rows, grad_hidden, part_one, other_one, table, hidden, moe_mine, moe_other
        )
        none = Plan(None, [], [], [], 1, lambda *_: ([], nothing, nothing, [], nothing))
        for item in queue[4:] + [(slots - 1, 0, here)]:
            expert_grads, _ = fill(none, item, expert_grads, normed_far, cot_far)
        cut = w_query.shape[0]
        grad_query, grad_key, grad_value, grad_out, grad_one, grad_two, grad_router = spread(
            index,
            shared,
            payload.shape[0] // slots,
            (
                w_query.shape,
                w_key.shape,
                w_value.shape,
                w_out.shape,
                (cut,),
                (cut,),
                (experts, cut),
            ),
            experts,
        )
        return (
            output[None],
            grad_tokens[None],
            grad_one,
            grad_query,
            grad_key,
            grad_value,
            grad_out,
            grad_two,
            grad_router.T,
            expert_grads[0],
            expert_grads[1],
            expert_grads[2],
        )

    return per_device


def solution(mesh):
    return jax.shard_map(
        build(mesh.shape["fsdp"], mesh.shape["context"]),
        mesh=mesh,
        in_specs=(
            P("fsdp", "context", None),
            P("fsdp", "context"),
            P("fsdp", "context", None),
            P("fsdp"),
            P("fsdp", "tensor"),
            P("fsdp", "tensor"),
            P("fsdp", "tensor"),
            P("tensor", "fsdp"),
            P("fsdp"),
            P("fsdp", None),
            P("fsdp", None, "tensor"),
            P("fsdp", None, "tensor"),
            P("fsdp", "tensor", None),
            P("fsdp", "context", None),
        ),
        out_specs=(
            P("fsdp", "context", None),
            P("fsdp", "context", None),
            P("fsdp"),
            P("fsdp", "tensor"),
            P("fsdp", "tensor"),
            P("fsdp", "tensor"),
            P("tensor", "fsdp"),
            P("fsdp"),
            P("fsdp", None),
            P("fsdp", None, "tensor"),
            P("fsdp", None, "tensor"),
            P("fsdp", "tensor", None),
        ),
        check_vma=False,
    )
```
